32 devices in a mesh: dp: 4 (over z), ep: 8 (over y, x, core).
Axes of the slice: x: 2, y: 2, z: 4, core: 2. Of those that a mesh axis runs over, the one named last changes fastest.
Arguments:
- x_tokens: bfloat16 [49152, 1024], P(('dp', 'ep'))
- w_router: float32 [1024, 32], replicated
- expert_ids: int32 [49152, 8], P(('dp', 'ep'))
- w_gate: bfloat16 [32, 1024, 512], P('ep')
- w_up: bfloat16 [32, 1024, 512], P('ep')
- w_down: bfloat16 [32, 512, 1024], P('ep')
- dy_tokens: bfloat16 [49152, 1024], P(('dp', 'ep'))
Outputs:
- output 1: bfloat16 [49152, 1024], P(('dp', 'ep'))
- output 2: float32 [], replicated
- output 3: bfloat16 [49152, 1024], P(('dp', 'ep'))
- output 4: float32 [1024, 32], replicated
- output 5: bfloat16 [32, 1024, 512], P('ep')
- output 6: bfloat16 [32, 1024, 512], P('ep')
- output 7: bfloat16 [32, 512, 1024], P('ep')
All inputs are finite; a program needn't handle non-finite values.
Results may differ from the reference program's by a relative error of at most 0.012767.
Values are sent between devices in bfloat16 or wider.
A program may use at most 1 GiB of HBM per device.

```python
import jax
import jax.numpy as jnp
from jax import lax

TOKENS = 1536
D_MODEL = 1024
D_FF = 512
EXPERTS = 32
TOP_K = 8
DEVICES = 32

AUX_COEF = 0.01
CAPACITY = (5 * TOP_K * TOKENS + 4 * EXPERTS - 1) // (4 * EXPERTS)
HOT_COUNT = max(1, EXPERTS // 8)


def draw_ids(base_key):
    key_rot, key_base, key_rest = jax.random.split(base_key, 3)
    rotation = jax.random.randint(key_rot, (DEVICES, 1), 0, EXPERTS)
    token_pos = jnp.arange(TOKENS)[None, :]
    base_draw = jax.random.randint(key_base, (DEVICES, TOKENS), 0, 2 * EXPERTS)
    hot_pick = rotation + (base_draw - EXPERTS) % HOT_COUNT
    first_pick = jnp.where(base_draw < EXPERTS, base_draw, hot_pick)
    first_pick = jnp.where(token_pos < EXPERTS, rotation + token_pos, first_pick) % EXPERTS
    scores = jax.random.randint(key_rest, (DEVICES * TOKENS, EXPERTS - 1), 0, 1 << 20)
    rank_order = jnp.argsort(scores * EXPERTS + jnp.arange(EXPERTS - 1)[None, :], axis=1)
    first_col = first_pick.reshape(DEVICES * TOKENS, 1)
    others = (first_col + rank_order[:, : TOP_K - 1] + 1) % EXPERTS
    return jnp.concatenate([first_col, others], axis=1).astype(jnp.int32)


def setup_inputs(seed: int = 0) -> dict:
    key_list = jax.random.split(jax.random.key(seed), 7)
    n_total = TOKENS * DEVICES
    x_tokens = jax.random.normal(key_list[0], (n_total, D_MODEL), jnp.float32).astype(jnp.bfloat16)
    w_router = jax.random.normal(key_list[1], (D_MODEL, EXPERTS), jnp.float32) * D_MODEL ** -0.5
    expert_ids = draw_ids(key_list[2])
    w_gate = (jax.random.normal(key_list[3], (EXPERTS, D_MODEL, D_FF), jnp.float32) * D_MODEL ** -0.5).astype(jnp.bfloat16)
    w_up = (jax.random.normal(key_list[4], (EXPERTS, D_MODEL, D_FF), jnp.float32) * D_MODEL ** -0.5).astype(jnp.bfloat16)
    w_down = (jax.random.normal(key_list[5], (EXPERTS, D_FF, D_MODEL), jnp.float32) * D_FF ** -0.5).astype(jnp.bfloat16)
    dy_tokens = jax.random.normal(key_list[6], (n_total, D_MODEL), jnp.float32).astype(jnp.bfloat16)
    return {'x_tokens': x_tokens, 'w_router': w_router, 'expert_ids': expert_ids, 'w_gate': w_gate, 'w_up': w_up, 'w_down': w_down, 'dy_tokens': dy_tokens}


def moe_forward(x_tokens, w_router, w_gate, w_up, w_down, expert_ids):
    n_total = TOKENS * DEVICES
    x_wide = x_tokens.astype(jnp.float32)
    router_prob = jax.nn.softmax(jnp.dot(x_wide, w_router, preferred_element_type=jnp.float32), axis=-1)
    chosen = expert_ids[:, :, None] == jnp.arange(EXPERTS)[None, None, :]
    picked = jnp.sum(jnp.where(chosen, router_prob[:, None, :], 0.0), axis=-1)
    gate_val = picked / jnp.sum(picked, axis=1, keepdims=True)
    load_frac = jnp.sum(chosen.astype(jnp.float32), axis=(0, 1)) / (n_total * TOP_K)
    aux_loss = AUX_COEF * EXPERTS * jnp.sum(load_frac * jnp.mean(router_prob, axis=0))

    hit_mask = chosen.reshape(DEVICES, TOKENS * TOP_K, EXPERTS).astype(jnp.int32)
    position = jnp.sum((jnp.cumsum(hit_mask, axis=1) - hit_mask) * hit_mask, axis=2)
    flat_ids = expert_ids.reshape(DEVICES, TOKENS * TOP_K)
    slot_idx = jnp.where(position < CAPACITY, flat_ids * CAPACITY + position, EXPERTS * CAPACITY)
    assign_all = jnp.arange(TOKENS * TOP_K, dtype=jnp.int32)
    source_idx = jax.vmap(lambda slot_row: jnp.full((EXPERTS * CAPACITY,), TOKENS * TOP_K, jnp.int32).at[slot_row].set(assign_all, mode='drop'))(slot_idx)
    gate_w = w_gate.astype(jnp.float32)
    up_w = w_up.astype(jnp.float32)
    down_w = w_down.astype(jnp.float32)

    def one_source(src_block):
        x_blk, slot_row, src_row, gate_blk = src_block
        x_disp = jnp.take(x_blk, src_row // TOP_K, axis=0, mode='fill', fill_value=0.0).reshape(EXPERTS, CAPACITY, D_MODEL)
        act_a = jnp.einsum('ecd,edf->ecf', x_disp, gate_w)
        act_b = jnp.einsum('ecd,edf->ecf', x_disp, up_w)
        hidden = (jax.nn.silu(act_a) * act_b).astype(jnp.bfloat16)
        out_rows = jnp.einsum('ecf,efd->ecd', hidden.astype(jnp.float32), down_w).astype(jnp.bfloat16)
        out_rows = out_rows.reshape(EXPERTS * CAPACITY, D_MODEL)
        rows_back = jnp.take(out_rows, slot_row, axis=0, mode='fill', fill_value=0).reshape(TOKENS, TOP_K, D_MODEL)
        return jnp.sum(gate_blk[:, :, None] * rows_back.astype(jnp.float32), axis=1)

    y_wide = lax.map(jax.checkpoint(one_source), (x_wide.reshape(DEVICES, TOKENS, D_MODEL), slot_idx, source_idx, gate_val.reshape(DEVICES, TOKENS, TOP_K)))
    y_tokens = y_wide.reshape(n_total, D_MODEL).astype(jnp.bfloat16)
    return y_tokens, aux_loss


def reference(x_tokens, w_router, expert_ids, w_gate, w_up, w_down, dy_tokens):
    def loss_parts(x_in, router_in, gate_in, up_in, down_in):
        return moe_forward(x_in, router_in, gate_in, up_in, down_in, expert_ids)

    (y_tokens, aux_loss), pullback = jax.vjp(loss_parts, x_tokens, w_router, w_gate, w_up, w_down)
    dx_tokens, dw_router, dw_gate, dw_up, dw_down = pullback((dy_tokens, jnp.ones_like(aux_loss)))
    return y_tokens, aux_loss, dx_tokens, dw_router, dw_gate, dw_up, dw_down
```

```python
import functools

import jax
import jax.numpy as jnp
import numpy as np
from jax import lax
from jax.experimental import pallas as pl
from jax.experimental.pallas import tpu as pltpu
from jax.sharding import PartitionSpec as P

AUX_COEF = 0.01
BLK = 256
TILE = 256
WIN = 128
LANES = 128
ALIGN = 16
NOT_KEPT = -65536.0
VMEM_LIMIT = 63 * 1024 * 1024
CORE, X, Y = 1, 2, 4
FAR = X | Y
HALVES = TENSORS = range(2)
CHUNKS = range(4)
SOURCES = range(8)
FIRST, LAST = 0, -1
SEND, RECV = 0, 1
STAGES = 3
SLOTS = 8
LAG = 3
MESH = pl.DeviceIdType.MESH


f32 = jnp.float32
bf16 = jnp.bfloat16
i32 = jnp.int32
ANY = pl.BlockSpec(memory_space=pl.ANY)
SMEM = pl.BlockSpec(memory_space=pltpu.SMEM)
VMEM = pl.BlockSpec(memory_space=pltpu.VMEM)
DMA = pltpu.SemaphoreType.DMA
Shape = jax.ShapeDtypeStruct


def capacity_of(tokens, top_k, experts):
    return (5 * top_k * tokens + 4 * experts - 1) // (4 * experts)


def dot(a, b, ca=1, cb=0):
    return lax.dot_general(a, b, (((ca,), (cb,)), ((), ())), preferred_element_type=f32)


def dot_nt(a, b):
    return dot(a, b, 1, 1)


def dot_tn(a, b):
    return dot(a, b, 0, 0)


def params(**more):
    return pltpu.CompilerParams(dimension_semantics=("arbitrary",), vmem_limit_bytes=VMEM_LIMIT, **more)


def cost(flops, moved):
    return pl.CostEstimate(flops=flops, bytes_accessed=moved, transcendentals=FIRST)


def iota(shape, dim):
    return lax.broadcasted_iota(i32, shape, dim)


def span(start, size, multiple=None):
    return pl.ds(pl.multiple_of(start, multiple or size), size)


def lane_sum(v):
    return jnp.sum(v, axis=1, keepdims=True)


def row_sum(v):
    return jnp.sum(v, axis=0, keepdims=True)


def where0(mask, v):
    return jnp.where(mask, v, jnp.zeros_like(v))


def one_hot(mask):
    return jnp.where(mask, 1.0, 0.0).astype(bf16)


def split3(v):
    hi = v.astype(bf16)
    rest = v - hi.astype(f32)
    mid = rest.astype(bf16)
    return hi, mid, (rest - mid.astype(f32)).astype(bf16)


def loop(start, stop, body):
    def step(i, carry):
        body(i)
        return carry

    lax.fori_loop(start, stop, step, FIRST)


def chosen_mask(ids, experts):
    rows = iota((experts, ids.shape[1]), FIRST)
    return functools.reduce(jnp.logical_or, [rows == ids[j : j + 1, :] for j in range(ids.shape[FIRST])])


def router_kernel(capacity, local, x_ref, w_ref, ids_ref, tab_ref, prob_ref, carry):
    step = pl.program_id(FIRST)
    steps = pl.num_programs(FIRST)
    experts = w_ref.shape[1]

    @pl.when(step == FIRST)
    def _():
        carry[...] = jnp.zeros_like(carry)
        tab_ref[...] = jnp.zeros_like(tab_ref)

    x = x_ref[...]
    hi, mid, low = [dot(x, part) for part in split3(w_ref[...])]
    logits = jnp.transpose(hi + (mid + low))
    expo = jnp.exp(logits - jnp.max(logits, axis=FIRST, keepdims=True))
    prob = expo / row_sum(expo)
    chosen = chosen_mask(ids_ref[...], experts)
    hits = jnp.where(chosen, 1.0, 0.0)
    gate = where0(chosen, prob / row_sum(where0(chosen, prob)))
    earlier = one_hot(iota((BLK, BLK), FIRST) < iota((BLK, BLK), 1))
    before = carry[:, :1]
    pos = dot(hits.astype(bf16), earlier) + before
    pos = jnp.where(chosen & (pos < capacity), pos, NOT_KEPT)
    prob_ref[...] = prob
    after = before + lane_sum(hits)
    lane = iota((experts, LANES), 1)
    first = where0(lane == step, jnp.minimum(before, capacity) + jnp.zeros((experts, LANES), f32))
    first = first + where0((lane == step + 1) & (step == steps - 1), jnp.minimum(after, capacity) + jnp.zeros((experts, LANES), f32))
    stat = where0(lane == FIRST, lane_sum(hits) + jnp.zeros((experts, LANES), f32))
    stat = stat + where0(lane == 1, lane_sum(prob) + jnp.zeros((experts, LANES), f32))
    tail = slice(tab_ref.shape[LAST] - LANES, None)
    for d in range(experts // local):
        rows = slice(d * local, (d + 1) * local)
        tab_ref[d, :local, span(step * BLK, BLK)] = gate[rows]
        tab_ref[d, local:, span(step * BLK, BLK)] = pos[rows]
        tab_ref[d, :local, tail] += stat[rows]
        tab_ref[d, local:, tail] += first[rows]
    carry[:, :1] = after


def run_router(x_loc, w_router, ids_t, capacity, local, devices):
    tokens, d_model = x_loc.shape
    experts = w_router.shape[1]
    top_k = ids_t.shape[FIRST]
    table = (devices, 2 * local, tokens + LANES)
    return pl.pallas_call(
        functools.partial(router_kernel, capacity, local),
        grid=(tokens // BLK,),
        in_specs=[pl.BlockSpec((BLK, d_model), lambda i: (i, FIRST)), VMEM, pl.BlockSpec((top_k, BLK), lambda i: (FIRST, i))],
        out_specs=[VMEM, pl.BlockSpec((experts, BLK), lambda i: (FIRST, i))],
        out_shape=[Shape(table, f32), Shape((experts, tokens), f32)],
        scratch_shapes=[pltpu.VMEM((experts, LANES), f32)],
        compiler_params=params(),
        cost_estimate=cost(2 * tokens * d_model * BLK, 2 * tokens * d_model),
        name="router",
    )(x_loc, w_router, ids_t)


class Blocks:
    def __init__(self, starts_ref, bmap_ref, nb, half):
        self.starts, self.bmap, self.nb, self.half = starts_ref, bmap_ref, nb, half
        self.per_chunk = half // BLK
        self.count = self.per_chunk * len(CHUNKS)

    def info(self, i, e):
        flat = self.bmap[i]
        at = (flat // self.nb) * 64 + e * ALIGN + flat % self.nb
        first = self.starts[at]
        return flat, first, self.starts[at + 1] - first

    def total(self, e):
        return sum(self.info(i, e)[LAST] for i in range(self.count))

    def at_chunk_end(self, i, fn):
        for c in CHUNKS:
            pl.when(i == (c + 1) * self.per_chunk - 1)(functools.partial(fn, c))

    def at_chunk_start(self, i, fn):
        for c in CHUNKS:
            pl.when(i == c * self.per_chunk)(functools.partial(fn, c))

    def rows(self, c):
        return pl.ds(c * self.half, self.half)


def aligned(row):
    base = (row // ALIGN) * ALIGN
    return base, row - base


def window_count(shift, count):
    return (shift + count + WIN - 1) // WIN


def tiles_of(total):
    return (total + TILE - 1) // TILE


def row_tiles(total, body):
    tiles = tiles_of(total)
    pairs = tiles // 2
    loop(FIRST, pairs, lambda i: body(i * (2 * TILE), 2 * TILE))
    pl.when(tiles > 2 * pairs)(lambda: body(pairs * (2 * TILE), TILE))


def grad_kernel(has_in, last, nb, local, half, *refs):
    refs = list(refs)

    def take(n):
        got = refs[:n]
        del refs[:n]
        return got

    starts_ref, bmap_ref, tab_ref = take(3)
    tok_refs = take(len(CHUNKS)), take(len(CHUNKS))
    w1_ref, w3_ref, w2_ref = take(3)
    acc_in = take(2 * has_in)
    row_outs = take(3)
    outs = take(3 if last else 2)
    xv, dv, xr, dr, acc13, acc2, stage, tok_sem, in_sem, out_sem, row_sem = refs
    accs = acc13, acc2
    e = pl.program_id(FIRST)
    slot = e % 2
    d_model = xv.shape[1]
    d_ff = w1_ref.shape[LAST]
    blocks = Blocks(starts_ref, bmap_ref, nb, half)

    def token_copies(c):
        return [pltpu.make_async_copy(src[c], dst.at[blocks.rows(c)], tok_sem.at[w, c]) for w, (src, dst) in enumerate(zip(tok_refs, (xv, dv)))]

    def in_copies():
        return [pltpu.make_async_copy(src.at[e], dst.at[slot], in_sem.at[k]) for k, (src, dst) in enumerate(zip(acc_in, accs))]

    def out_copies(ee, ss):
        return [pltpu.make_async_copy(src.at[ss], dst.at[ee], out_sem.at[ss, k]) for k, (src, dst) in enumerate(zip(accs, outs))]

    def start(copies):
        for cp in copies:
            cp.start()

    def wait(copies):
        for cp in copies:
            cp.wait()

    @pl.when(e == FIRST)
    def _():
        for c in CHUNKS:
            start(token_copies(c))

    if not last:
        pl.when(e >= 2)(lambda: wait(out_copies(e - 2, slot)))
    start(in_copies())
    if not has_in:
        for acc in accs:
            acc[slot] = jnp.zeros(acc.shape[1:], f32)

    row_iota = iota((WIN, BLK), FIRST).astype(f32)
    head_row = iota((ALIGN, d_model), FIRST)

    def dispatch(i, row):
        pl.when(e == FIRST)(lambda: blocks.at_chunk_start(i, lambda c: wait(token_copies(c))))
        flat, first, count = blocks.info(i, e)
        base, shift = aligned(row)
        gate = tab_ref[flat, pl.ds(e, 1), :]
        pos = tab_ref[flat, pl.ds(local + e, 1), :]
        tok = span(i * BLK, BLK)

        def window(k):
            pick = (pos + (shift - first - k * WIN).astype(f32)) == row_iota
            one = one_hot(pick)
            gate_row = lane_sum(where0(pick, gate + jnp.zeros_like(row_iota)))
            return dot(one, xv[tok, :]).astype(bf16), (dot(one, dv[tok, :]) * gate_row).astype(bf16)

        for new, rows in zip(window(i32(FIRST)), (xr, dr)):
            head = span(base, ALIGN)
            rows[head, :] = jnp.where(head_row < shift, rows[head, :], new[:ALIGN])
            rows[span(base + ALIGN, WIN - ALIGN, ALIGN), :] = new[ALIGN:]

        def more(k):
            for new, rows in zip(window(k), (xr, dr)):
                rows[span(base + k * WIN, WIN, ALIGN), :] = new

        loop(1, window_count(shift, count), more)
        return row + count

    total = lax.fori_loop(FIRST, blocks.count, dispatch, i32(FIRST))

    def clear(i):
        for rows in (xr, dr):
            rows[span(i * ALIGN, ALIGN), :] = jnp.zeros((ALIGN, d_model), bf16)

    loop((total + ALIGN - 1) // ALIGN, tiles_of(total) * (TILE // ALIGN), clear)
    wait(in_copies())

    def tile(at, size):
        rows = span(at, size)
        xt = xr[rows, :]
        dt = dr[rows, :]
        act_a = dot(xt, w1_ref[FIRST])
        act_b = dot(xt, w3_ref[FIRST])
        d_hidden = dot_nt(dt, w2_ref[FIRST]).astype(bf16).astype(f32)
        sig = 1.0 / (1.0 + jnp.exp(-act_a))
        silu = act_a * sig
        hidden = (silu * act_b).astype(bf16)
        d_a = (d_hidden * act_b * sig * (1.0 + act_a * (1.0 - sig))).astype(bf16)
        d_b = (d_hidden * silu).astype(bf16)
        copies = []
        for k, (value, out) in enumerate(zip((hidden, d_a, d_b), row_outs)):
            stage[k, :size] = value
            copies.append(pltpu.make_async_copy(stage.at[k, :size], out.at[e, rows], row_sem.at[k]))
        start(copies)
        acc13[slot, :, :d_ff] += dot_tn(xt, d_a)
        acc13[slot, :, d_ff:] += dot_tn(xt, d_b)
        acc2[slot] += dot_tn(hidden, dt)
        wait(copies)

    row_tiles(total, tile)

    if last:
        for out, value in zip(outs, (acc13[slot, :, :d_ff], acc13[slot, :, d_ff:], acc2[slot])):
            out[FIRST] = value.astype(bf16)
    else:
        start(out_copies(e, slot))

        @pl.when(e == pl.num_programs(FIRST) - 1)
        def _():
            wait(out_copies(e - 1, 1 - slot))
            wait(out_copies(e, slot))


def per_expert(*shape):
    return pl.BlockSpec((1, *shape), lambda e: (e,) + (FIRST,) * len(shape))


def block_map(group, nb):
    hb = nb // 2
    return np.asarray([src * nb + part * hb + b for src, part in group for b in range(hb)], np.int32)


def run_grad(starts, tab, group, xs, ds, weights, acc, last, nb, row_cap):
    local, d_model, d_ff = weights[FIRST].shape
    half = xs[FIRST].shape[FIRST]
    w_specs = [per_expert(*w.shape[1:]) for w in weights]
    sums = [(local, d_model, 2 * d_ff), (local, d_ff, d_model)]
    rows = [Shape((local, row_cap, d_ff), bf16)] * 3
    out_shape = rows + ([Shape(w.shape, bf16) for w in weights] if last else [Shape(s, f32) for s in sums])
    out_specs = [ANY] * 3 + (w_specs if last else [ANY] * 2)
    tokens = pltpu.VMEM((len(CHUNKS) * half, d_model), bf16)
    packed = pltpu.VMEM((row_cap + WIN, d_model), bf16)
    out = pl.pallas_call(
        functools.partial(grad_kernel, bool(acc), last, nb, local, half),
        grid=(local,),
        in_specs=[SMEM, SMEM, VMEM] + [ANY] * (2 * len(CHUNKS)) + w_specs + [ANY] * len(acc),
        out_specs=out_specs,
        out_shape=out_shape,
        scratch_shapes=[tokens, tokens, packed, packed]
        + [pltpu.VMEM((2, *s[1:]), f32) for s in sums]
        + [pltpu.VMEM((3, 2 * TILE, d_ff), bf16), DMA((2, len(CHUNKS))), DMA((2,)), DMA((2, 2)), DMA((3,))],
        compiler_params=params(),
        cost_estimate=cost(12 * len(CHUNKS) * half * d_model * d_ff, 40 << 20),
        name="expert_grad",
    )(starts, block_map(group, nb), tab, *xs, *ds, *weights, *acc)
    return out[:3], out[3:]


def out_writer(blocks, values, outs, sems):
    def copy(c):
        return pltpu.make_async_copy(values.at[blocks.rows(c)], outs[c], sems.at[c])

    return copy


def y_kernel(nb, local, half, starts_ref, bmap_ref, tab_ref, h_ref, w2_ref, *refs):
    n = len(CHUNKS)
    d_refs, y_refs = refs[:n], refs[n : 2 * n]
    dg_ref, o_rows, dv, yv, zacc, yacc, dgacc, tok_sem, out_sem = refs[2 * n :]
    e = pl.program_id(FIRST)
    blocks = Blocks(starts_ref, bmap_ref, nb, half)
    d_model = dv.shape[1]
    token_copy = lambda c: pltpu.make_async_copy(d_refs[c], dv.at[blocks.rows(c)], tok_sem.at[c])
    out_copy = out_writer(blocks, yv, y_refs, out_sem)

    @pl.when(e == FIRST)
    def _():
        for c in CHUNKS:
            token_copy(c).start()

    total = blocks.total(e)

    def tile(at, size):
        o_rows[e, span(at, size), :] = dot(h_ref[FIRST, span(at, size), :], w2_ref[FIRST]).astype(bf16)

    row_tiles(total, tile)
    o_rows[e, span(tiles_of(total) * TILE, WIN), :] = jnp.zeros((WIN, d_model), bf16)

    @pl.when(e == local - 1)
    def _():
        for c in CHUNKS:
            token_copy(c).wait()
        lane = iota((BLK, WIN), 1).astype(f32)
        dg_lane = iota((BLK, LANES), 1)
        width = 2 * LANES
        columns = [slice(k * width, (k + 1) * width) for k in range(d_model // width)]

        def combine(i, rows_at):
            infos = [blocks.info(i, ee) for ee in range(local)]
            places = [aligned(r) for r in rows_at]
            windows = [window_count(place[1], info[LAST]) for place, info in zip(places, infos)]
            tab_t = jnp.transpose(tab_ref[infos[FIRST][FIRST]])
            tok = span(i * BLK, BLK)
            gates = [tab_t[:, ee : ee + 1] for ee in range(local)]

            def pick(ee, k):
                shifted = tab_t[:, local + ee : local + ee + 1] + (places[ee][1] - infos[ee][1] - k * WIN).astype(f32)
                return one_hot(shifted == lane)

            def held(ee, k, cols):
                return o_rows[ee, span(places[ee][FIRST] + k * WIN, WIN, ALIGN), cols]

            def put_dg(sums):
                dg = sum(where0(dg_lane == ee, lane_sum(s) + jnp.zeros((BLK, LANES), f32)) for ee, s in enumerate(sums))
                dg_ref[i] = jnp.transpose(dg)[: 2 * local, :]

            simple = functools.reduce(jnp.logical_and, [w <= 1 for w in windows])

            @pl.when(simple)
            def _():
                picks = [pick(ee, i32(FIRST)) for ee in range(local)]
                sums = [None] * local
                for cols in columns:
                    dy = dv[tok, cols].astype(f32)
                    y = None
                    for ee in range(local):
                        z = dot(picks[ee], held(ee, i32(FIRST), cols))
                        prod = dy * z
                        part = prod[:, :LANES] + prod[:, LANES:]
                        sums[ee] = part if sums[ee] is None else sums[ee] + part
                        y = gates[ee] * z if y is None else y + gates[ee] * z
                    yv[tok, cols] = y.astype(bf16)
                put_dg(sums)

            @pl.when(jnp.logical_not(simple))
            def _():
                yacc[...] = jnp.zeros_like(yacc)
                for ee in range(local):
                    zacc[...] = jnp.zeros_like(zacc)

                    def more(k, ee=ee):
                        zacc[...] += dot(pick(ee, k), held(ee, k, slice(None)))

                    loop(FIRST, windows[ee], more)
                    yacc[...] += gates[ee] * zacc[...]
                    dgacc[ee] = lane_sum(dv[tok, :].astype(f32) * zacc[...]) * jnp.where(dg_lane == FIRST, 1.0, 0.0)
                yv[tok, :] = yacc[...].astype(bf16)
                put_dg([dgacc[ee] for ee in range(local)])

            blocks.at_chunk_end(i, lambda c: out_copy(c).start())
            return tuple(r + info[LAST] for r, info in zip(rows_at, infos))

        lax.fori_loop(FIRST, blocks.count, combine, (i32(FIRST),) * local)
        for c in CHUNKS:
            out_copy(c).wait()


def run_y(starts, tab, group, h_rows, w2, ds, nb):
    local, d_ff, d_model = w2.shape
    row_cap = h_rows.shape[1]
    half = ds[FIRST].shape[FIRST]
    n = len(CHUNKS)
    dg_shape = (n * half // BLK, 2 * local, BLK)
    block = pltpu.VMEM((BLK, d_model), f32)
    tokens = pltpu.VMEM((n * half, d_model), bf16)
    out = pl.pallas_call(
        functools.partial(y_kernel, nb, local, half),
        grid=(local,),
        in_specs=[SMEM, SMEM, VMEM, per_expert(row_cap, d_ff), per_expert(d_ff, d_model)] + [ANY] * n,
        out_specs=[ANY] * n + [VMEM],
        out_shape=[Shape((half, d_model), bf16)] * n + [Shape(dg_shape, f32)],
        scratch_shapes=[pltpu.VMEM((local, row_cap + WIN, d_model), bf16), tokens, tokens, block, block, pltpu.VMEM((local, BLK, LANES), f32), DMA((n,)), DMA((n,))],
        compiler_params=params(),
        cost_estimate=cost(4 * n * half * d_model * d_ff, 20 << 20),
        name="expert_y",
    )(starts, block_map(group, nb), tab, h_rows, w2, *ds)
    return out[:n], out[n]


def dx_kernel(nb, local, half, starts_ref, bmap_ref, tab_ref, da_ref, db_ref, w1_ref, w3_ref, *refs):
    n = len(CHUNKS)
    y_refs = refs[:n]
    o_rows, yv, zacc, out_sem = refs[n:]
    e = pl.program_id(FIRST)
    blocks = Blocks(starts_ref, bmap_ref, nb, half)
    d_model = yv.shape[1]
    out_copy = out_writer(blocks, yv, y_refs, out_sem)
    total = blocks.total(e)

    def tile(at, size):
        rows = span(at, size)
        grad = dot_nt(da_ref[FIRST, rows, :], w1_ref[FIRST]) + dot_nt(db_ref[FIRST, rows, :], w3_ref[FIRST])
        o_rows[e, rows, :] = grad.astype(bf16)

    row_tiles(total, tile)
    o_rows[e, span(tiles_of(total) * TILE, WIN), :] = jnp.zeros((WIN, d_model), bf16)

    @pl.when(e == local - 1)
    def _():
        lane = iota((BLK, WIN), 1).astype(f32)

        def combine(i, rows_at):
            infos = [blocks.info(i, ee) for ee in range(local)]
            places = [aligned(r) for r in rows_at]
            windows = [window_count(place[1], info[LAST]) for place, info in zip(places, infos)]
            tab_t = jnp.transpose(tab_ref[infos[FIRST][FIRST]])
            tok = span(i * BLK, BLK)

            def pick(ee, k):
                shifted = tab_t[:, local + ee : local + ee + 1] + (places[ee][1] - infos[ee][1] - k * WIN).astype(f32)
                return one_hot(shifted == lane), o_rows[ee, span(places[ee][FIRST] + k * WIN, WIN, ALIGN), :]

            simple = functools.reduce(jnp.logical_and, [w <= 1 for w in windows])

            @pl.when(simple)
            def _():
                pairs = [[pick(ee + k, i32(FIRST)) for k in HALVES] for ee in range(FIRST, local, 2)]
                sums = [dot(jnp.concatenate([p[FIRST] for p in pair], axis=1), jnp.concatenate([p[1] for p in pair], axis=FIRST)) for pair in pairs]
                yv[tok, :] = sum(sums[1:], sums[FIRST]).astype(bf16)

            @pl.when(jnp.logical_not(simple))
            def _():
                zacc[...] = jnp.zeros_like(zacc)
                for ee in range(local):

                    def more(k, ee=ee):
                        zacc[...] += dot(*pick(ee, k))

                    loop(FIRST, windows[ee], more)
                yv[tok, :] = zacc[...].astype(bf16)

            blocks.at_chunk_end(i, lambda c: out_copy(c).start())
            return tuple(r + info[LAST] for r, info in zip(rows_at, infos))

        lax.fori_loop(FIRST, blocks.count, combine, (i32(FIRST),) * local)
        for c in CHUNKS:
            out_copy(c).wait()


def run_dx(starts, tab, group, da_rows, db_rows, w1, w3, nb, half):
    local, d_model, d_ff = w1.shape
    row_cap = da_rows.shape[1]
    n = len(CHUNKS)
    return pl.pallas_call(
        functools.partial(dx_kernel, nb, local, half),
        grid=(local,),
        in_specs=[SMEM, SMEM, VMEM] + [per_expert(row_cap, d_ff)] * 2 + [per_expert(d_model, d_ff)] * 2,
        out_specs=[ANY] * n,
        out_shape=[Shape((half, d_model), bf16)] * n,
        scratch_shapes=[pltpu.VMEM((local, row_cap + WIN, d_model), bf16), pltpu.VMEM((n * half, d_model), bf16), pltpu.VMEM((BLK, d_model), f32), DMA((n,))],
        compiler_params=params(),
        cost_estimate=cost(6 * n * half * d_model * d_ff, 20 << 20),
        name="expert_dx",
    )(starts, block_map(group, nb), tab, da_rows, db_rows, w1, w3)


def router_grad_kernel(scale, x_ref, prob_ref, dg_ref, ids_ref, load_ref, dlog_ref, dw_ref):
    step = pl.program_id(FIRST)
    prob = prob_ref[...]
    dg = dg_ref[...]
    chosen = chosen_mask(ids_ref[...], prob.shape[FIRST])
    gate_sum = row_sum(where0(chosen, prob))
    gate = where0(chosen, prob / gate_sum)
    d_pick = (dg - row_sum(gate * dg)) / gate_sum
    d_prob = where0(chosen, d_pick) + scale * load_ref[:, :1]
    d_logit = prob * (d_prob - row_sum(prob * d_prob))
    dlog_ref[...] = d_logit
    hi, mid, low = [dot(part, x_ref[...]) for part in split3(d_logit)]

    @pl.when(step == FIRST)
    def _():
        dw_ref[...] = jnp.zeros_like(dw_ref)

    dw_ref[...] += hi + (mid + low)


def run_router_grad(x_loc, prob_t, dg_t, ids_t, load, scale):
    tokens, d_model = x_loc.shape
    experts = prob_t.shape[FIRST]
    lanes = lambda n: pl.BlockSpec((n, BLK), lambda i: (FIRST, i))
    return pl.pallas_call(
        functools.partial(router_grad_kernel, scale),
        grid=(tokens // BLK,),
        in_specs=[pl.BlockSpec((BLK, d_model), lambda i: (i, FIRST)), lanes(experts), lanes(experts), lanes(ids_t.shape[FIRST]), VMEM],
        out_specs=[lanes(experts), VMEM],
        out_shape=[Shape((experts, tokens), f32), Shape((experts, d_model), f32)],
        compiler_params=params(),
        cost_estimate=cost(2 * tokens * d_model * BLK, 2 * tokens * d_model),
        name="router_grad",
    )(x_loc, prob_t, dg_t, ids_t, load)


def final_kernel(dlog_ref, wt_ref, a_ref, b_ref, c_ref, out_ref):
    lhs = split3(dlog_ref[...])
    rhs = split3(wt_ref[...])
    terms = [(i, j) for i in range(3) for j in range(3 - i)]
    left = jnp.concatenate([lhs[i] for i, _ in terms], axis=FIRST)
    right = jnp.concatenate([rhs[j] for _, j in terms], axis=FIRST)
    rows = [ref[...].astype(f32) for ref in (a_ref, b_ref, c_ref)]
    out_ref[...] = (dot_tn(left, right) + sum(rows[1:], rows[FIRST])).astype(bf16)


def run_final(dlog_t, w_t, parts):
    experts, tokens = dlog_t.shape
    d_model = w_t.shape[1]
    rows = pl.BlockSpec((BLK, d_model), lambda i: (i, FIRST))
    return pl.pallas_call(
        final_kernel,
        grid=(tokens // BLK,),
        in_specs=[pl.BlockSpec((experts, BLK), lambda i: (FIRST, i)), VMEM, rows, rows, rows],
        out_specs=rows,
        out_shape=Shape((tokens, d_model), bf16),
        compiler_params=params(),
        cost_estimate=cost(2 * tokens * d_model * BLK, 8 * tokens * d_model),
        name="final_dx",
    )(dlog_t, w_t, *parts)


NEAR = (X, Y)
RELAYED = {(Y, 0): 0, (X, 1): 1}
OPS = [
    (t, src, h)
    for step in ([(FAR, 0), (FAR, 1)], [(X, 0), (Y, 1)], [(X, 1), (Y, 0)], [(FIRST, 0), (FIRST, 1)])
    for t in TENSORS
    for src, h in step
]


def add_rows(dst, src):
    def body(i):
        rows = span(i * LANES, LANES)
        dst[rows, :] = (dst[rows, :].astype(f32) + src[rows, :].astype(f32)).astype(bf16)

    loop(FIRST, dst.shape[FIRST] // LANES, body)


def exchange_kernel(half, mats, *refs):
    refs = list(refs)

    def take(n):
        got = refs[:n]
        del refs[:n]
        return got

    parts = [[take(len(HALVES)) for _ in SOURCES] for _ in TENSORS]
    dws = take(mats)
    outs = [take(len(NEAR) + 1) for _ in TENSORS]
    dw_outs = take(mats)
    land, far_land, stage, z_one, z_two, z_stage = take(6)
    core_sem, stage_sem, far_sem, near_sem, own_sem, z_sem, keep_sem, load_sem, credit_one, credit_two = refs

    me = lax.axis_index("ep")
    z = lax.axis_index("dp")
    peer = {bit: me + bit - 2 * bit * ((me // bit) % 2) for bit in (CORE, X, Y)}
    z_peer = z + 1 - 2 * (z % 2)
    z_cross = 3 - z
    is_end = (z % 3) == FIRST
    is_mid = (z % 3) != FIRST

    barrier = pltpu.get_barrier_semaphore()
    ids = [{"ep": p} for p in peer.values()] + [{"dp": z_peer}, {"dp": z_cross}]
    for device in ids:
        pl.semaphore_signal(barrier, device_id=device, device_id_type=MESH)
    pl.semaphore_wait(barrier, len(ids))

    def remote(src, dst, sems, at, device):
        send, recv = sems.at[(SEND, *at)], sems.at[(RECV, *at)]
        return pltpu.make_async_remote_copy(src_ref=src, dst_ref=dst, send_sem=send, recv_sem=recv, device_id=device, device_id_type=MESH)

    def rows_at(h):
        return pl.ds(h * half, half)

    def core_copy(i):
        t, src, h = OPS[i]
        return remote(parts[t][src | CORE][h], land.at[i], core_sem, (i,), {"ep": peer[CORE]})

    def stage_copy(i):
        t, src, h = OPS[i]
        return pltpu.make_async_copy(parts[t][src][h], stage.at[i % STAGES], stage_sem.at[i % STAGES])

    def far_copy(i):
        t, _, h = OPS[i]
        return remote(land.at[i], far_land.at[t, h], far_sem, (t, h), {"ep": peer[NEAR[h]]})

    def near_copy(i):
        t, src, h = OPS[i]
        k = NEAR.index(src)
        return remote(land.at[i], outs[t][k].at[rows_at(h)], near_sem, (t, k, h), {"ep": peer[src]})

    def own_copy(i):
        t, _, h = OPS[i]
        return pltpu.make_async_copy(land.at[i], outs[t][LAST].at[rows_at(h)], own_sem.at[t, h])

    def out_copy(i):
        src = OPS[i][1]
        return (far_copy if src == FAR else near_copy if src else own_copy)(i)

    def reduce_op(i):
        t, src, h = OPS[i]
        stage_copy(i).wait()
        core_copy(i).wait_recv()
        add_rows(land.at[i], stage.at[i % STAGES])
        if i + STAGES < len(OPS):
            stage_copy(i + STAGES).start()
        if (src, h) in RELAYED:
            far_copy(OPS.index((t, FAR, RELAYED[src, h]))).wait_recv()
            add_rows(land.at[i], far_land.at[t, RELAYED[src, h]])

    rows_per = z_one.shape[1]
    chunks = [(m, e, k) for e in range(dws[FIRST].shape[FIRST]) for m in range(mats) for k in HALVES]
    n = len(chunks)

    def piece(arrays, c):
        m, e, k = chunks[c]
        return arrays[m].at[e, pl.ds(k * rows_per, rows_per)]

    def one_copy(c):
        return remote(piece(dws, c), z_one.at[c % SLOTS], z_sem, (FIRST, c), {"dp": z_peer})

    def two_copy(c):
        return remote(z_one.at[c % SLOTS], z_two.at[c % SLOTS], z_sem, (1, c), {"dp": z_cross})

    def three_copy(c):
        return remote(z_two.at[c % SLOTS], piece(dw_outs, c), z_sem, (2, c), {"dp": z_peer})

    def keep_copy(c):
        return pltpu.make_async_copy(z_two.at[c % SLOTS], piece(dw_outs, c), keep_sem.at[c])

    def load_copy(c):
        return pltpu.make_async_copy(piece(dws, c), z_stage.at[c % STAGES], load_sem.at[c % STAGES])

    def first_add(c):
        load_copy(c).wait()
        one_copy(c).wait_recv()
        add_rows(z_one.at[c % SLOTS], z_stage.at[c % STAGES])
        if c + STAGES < n:
            load_copy(c + STAGES).start()

    def second_add(c):
        two_copy(c).wait()
        add_rows(z_two.at[c % SLOTS], z_one.at[c % SLOTS])
        if c + SLOTS < n:
            pl.semaphore_signal(credit_one, device_id={"dp": z_peer}, device_id_type=MESH)

    def retire(c):
        three_copy(c).wait_send()
        keep_copy(c).wait()
        if c + SLOTS < n:
            pl.semaphore_signal(credit_two, device_id={"dp": z_cross}, device_id_type=MESH)

    @pl.when(is_end)
    def _():
        for c in range(SLOTS):
            one_copy(c).start()

    @pl.when(is_mid)
    def _():
        for c in range(STAGES):
            load_copy(c).start()

    for i in range(len(OPS)):
        core_copy(i).start()
        if i < STAGES:
            stage_copy(i).start()

    todo = list(range(len(OPS)))
    for tick in range(n + LAG):
        mine = todo[: 2 if tick < 2 else 1]
        todo = todo[len(mine) :]
        for i in mine:
            reduce_op(i)

        @pl.when(is_mid)
        def _():
            back = tick - 1
            if tick < n:
                first_add(tick)
            if back in range(n):
                second_add(back)
            if tick < n:
                if tick >= SLOTS:
                    pl.semaphore_wait(credit_two, 1)
                two_copy(tick).start()
            if back in range(n):
                three_copy(back).start()
                keep_copy(back).start()
            if tick >= LAG:
                retire(tick - LAG)

        for i in mine:
            out_copy(i).start()

        @pl.when(is_end)
        def _():
            if tick + SLOTS < n:
                pl.semaphore_wait(credit_one, 1)
                one_copy(tick + SLOTS).start()

    for i in todo:
        reduce_op(i)
        out_copy(i).start()

    @pl.when(is_end)
    def _():
        for c in range(n):
            one_copy(c).wait_send()
            three_copy(c).wait_recv()

    for i in range(len(OPS)):
        core_copy(i).wait_send()
        (out_copy(i).wait_send if OPS[i][1] == FAR else out_copy(i).wait)()


def run_exchange(parts, dws):
    half, d_model = parts[FIRST][FIRST][FIRST].shape
    local, rows, cols = dws[FIRST].shape
    chunk = (rows // 2, cols)
    n = local * len(dws) * len(HALVES)
    whole = Shape((2 * half, d_model), bf16)
    flat = [v for tensor in parts for source in tensor for v in source] + list(dws)
    terms = len(NEAR) + 1
    out = pl.pallas_call(
        functools.partial(exchange_kernel, half, len(dws)),
        in_specs=[ANY] * len(flat),
        out_specs=[ANY] * (terms * len(TENSORS) + len(dws)),
        out_shape=[whole] * (terms * len(TENSORS)) + [Shape(v.shape, bf16) for v in dws],
        scratch_shapes=[
            pltpu.VMEM((len(OPS), half, d_model), bf16),
            pltpu.VMEM((len(TENSORS), len(HALVES), half, d_model), bf16),
            pltpu.VMEM((STAGES, half, d_model), bf16),
            pltpu.VMEM((SLOTS, *chunk), bf16),
            pltpu.VMEM((SLOTS, *chunk), bf16),
            pltpu.VMEM((STAGES, *chunk), bf16),
            DMA((2, len(OPS))),
            DMA((STAGES,)),
            DMA((2, 2, 2)),
            DMA((2, 2, 2, 2)),
            DMA((2, 2)),
            DMA((2, 3, n)),
            DMA((n,)),
            DMA((STAGES,)),
            pltpu.SemaphoreType.REGULAR,
            pltpu.SemaphoreType.REGULAR,
        ],
        compiler_params=pltpu.CompilerParams(vmem_limit_bytes=VMEM_LIMIT, collective_id=FIRST, has_side_effects=True),
        cost_estimate=cost(1 << 37, 200 << 20),
        name="exchange",
    )(*flat)
    return [out[:terms], out[terms : 2 * terms]], out[2 * terms :]


def hop(v, bit):
    return lax.ppermute(v, "ep", [(i, i ^ bit) for i in SOURCES])


def gather_halves(v):
    half = v.shape[FIRST] // 2
    got = {(FIRST, h): v[h * half : (h + 1) * half] for h in HALVES}
    for h in HALVES:
        for bit in (CORE, X, Y):
            got[bit, h] = hop(got[FIRST, h], bit)
    for h in HALVES:
        got[FAR, h] = hop(got[(Y, X)[h], h], NEAR[h])
        for far in (X, Y, FAR):
            got[far | CORE, h] = hop(got[far, h], CORE)
    return got


def relative(v, me):
    shape = v.shape
    v = v.reshape((2, 2, 2) + shape[1:])
    for axis, bit in enumerate((Y, X, CORE)):
        v = jnp.where((me & bit) != FIRST, jnp.flip(v, axis), v)
    return v.reshape(shape)


GROUPS = (
    [(src, h) for src in (FIRST, CORE) for h in HALVES],
    [(src, FIRST) for src in (X, X | CORE, Y, Y | CORE)],
    [(src, 1) for src in (X, X | CORE, Y, Y | CORE)],
    [(src, h) for h in HALVES for src in (FAR, FAR | CORE)],
)


def solution(mesh):
    dp_size = mesh.shape["dp"]
    ep_size = mesh.shape["ep"]
    row_spec = P(("dp", "ep"), None)
    expert_spec = P("ep", None, None)
    whole_spec = P(None, None)

    def per_device(x_loc, w_router, ids_loc, w1, w3, w2, dy_loc):
        tokens, d_model = x_loc.shape
        top_k = ids_loc.shape[1]
        experts = w_router.shape[1]
        local = w1.shape[FIRST]
        capacity = capacity_of(tokens, top_k, experts)
        n_total = tokens * dp_size * ep_size
        half = tokens // 2
        nb = tokens // BLK
        row_cap = tiles_of(len(CHUNKS) * min(capacity, half)) * TILE
        me = lax.axis_index("ep")

        xs = gather_halves(x_loc)
        ds = gather_halves(dy_loc)

        ids_t = ids_loc.T
        send_tab, prob_t = run_router(x_loc, w_router, ids_t, capacity, local, ep_size)
        tab_rel = relative(lax.all_to_all(send_tab, "ep", FIRST, FIRST, tiled=True), me)
        tab = tab_rel[:, :, :tokens].reshape(ep_size, 2 * local, nb, BLK).transpose(0, 2, 1, 3).reshape(ep_size * nb, 2 * local, BLK)
        starts = tab_rel[:, local:, tokens : tokens + ALIGN].astype(i32).reshape(LAST)
        stats = jnp.sum(tab_rel[:, :local, tokens:], axis=FIRST)
        for step in (1, 2):
            stats = stats + lax.ppermute(stats, "dp", [(i, i ^ step) for i in range(dp_size)])

        acc = ()
        rows = []
        for g, group in enumerate(GROUPS):
            last = g == len(GROUPS) - 1
            got, acc = run_grad(starts, tab, group, [xs[k] for k in group], [ds[k] for k in group], (w1, w3, w2), acc, last, nb, row_cap)
            rows.append(got)
        dw1, dw3, dw2 = acc
        starts, dw2 = lax.optimization_barrier((starts, dw2))
        dw2 = lax.psum(dw2, "dp")

        parts = {}, {}
        dg_part = {}
        for group, got in zip(GROUPS, rows):
            outs, dg = run_y(starts, tab, group, got[FIRST], w2, [ds[k] for k in group], nb)
            parts[FIRST].update(zip(group, outs))
            dg = dg.reshape(len(CHUNKS), half // BLK, 2 * local, BLK)[:, :, :local]
            dg_part.update({k: dg[i] for i, k in enumerate(group)})
        for group, got in zip(GROUPS, rows):
            parts[1].update(zip(group, run_dx(starts, tab, group, got[1], got[2], w1, w3, nb, half)))

        dg_all = jnp.stack([jnp.concatenate([dg_part[s, h] for h in HALVES], axis=FIRST) for s in SOURCES])
        dg_all = relative(dg_all.transpose(0, 2, 1, 3).reshape(ep_size, local, tokens), me)
        dg_all = jnp.concatenate([dg_all, jnp.broadcast_to(stats, (ep_size, *stats.shape))], axis=2)
        dg_all = lax.all_to_all(dg_all, "ep", FIRST, FIRST, tiled=True).reshape(experts, tokens + LANES)
        load = dg_all[:, tokens:]
        share = AUX_COEF * experts / (n_total * top_k * n_total)
        aux_loss = share * jnp.sum(load[:, FIRST] * load[:, 1])
        dlog_t, dwr_t = run_router_grad(x_loc, prob_t, dg_all[:, :tokens], ids_t, load, share)
        dw_router = lax.psum(dwr_t, ("dp", "ep")).T

        sums, grads = run_exchange([[[part[s, h] for h in HALVES] for s in SOURCES] for part in parts], [dw1, dw3])
        y_loc = sum(v.astype(f32) for v in sums[FIRST]).astype(bf16)
        dx_loc = run_final(dlog_t, w_router.T, sums[1])
        return y_loc, aux_loss, dx_loc, dw_router, *grads, dw2

    return jax.shard_map(
        per_device,
        mesh=mesh,
        in_specs=(row_spec, whole_spec, row_spec, expert_spec, expert_spec, expert_spec, row_spec),
        out_specs=(row_spec, P(), row_spec, whole_spec, expert_spec, expert_spec, expert_spec),
        check_vma=False,
    )
```

```python
import functools

import jax
import jax.numpy as jnp
import numpy as np
from jax import lax
from jax.experimental import pallas as pl
from jax.experimental.pallas import tpu as pltpu
from jax.sharding import PartitionSpec as P

AUX_COEF = 0.01
BLK = 256
TILE = 256
WIN = 128
LANES = 128
ALIGN = 16
NOT_KEPT = -65536.0
VMEM_LIMIT = 63 * 1024 * 1024
CORE, X, Y = 1, 2, 4
FAR = X | Y
HALVES = TENSORS = range(2)
CHUNKS = range(4)
SOURCES = range(8)
FIRST, LAST = 0, -1
SEND, RECV = 0, 1
STAGES = 3
SLOTS = 8
LAG = 3
MESH = pl.DeviceIdType.MESH


f32 = jnp.float32
bf16 = jnp.bfloat16
i32 = jnp.int32
ANY = pl.BlockSpec(memory_space=pl.ANY)
SMEM = pl.BlockSpec(memory_space=pltpu.SMEM)
VMEM = pl.BlockSpec(memory_space=pltpu.VMEM)
DMA = pltpu.SemaphoreType.DMA
Shape = jax.ShapeDtypeStruct


def capacity_of(tokens, top_k, experts):
    return (5 * top_k * tokens + 4 * experts - 1) // (4 * experts)


def dot(a, b, ca=1, cb=0):
    return lax.dot_general(a, b, (((ca,), (cb,)), ((), ())), preferred_element_type=f32)


def dot_nt(a, b):
    return dot(a, b, 1, 1)


def dot_tn(a, b):
    return dot(a, b, 0, 0)


def params(**more):
    return pltpu.CompilerParams(dimension_semantics=("arbitrary",), vmem_limit_bytes=VMEM_LIMIT, **more)


def cost(flops, moved):
    return pl.CostEstimate(flops=flops, bytes_accessed=moved, transcendentals=FIRST)


def iota(shape, dim):
    return lax.broadcasted_iota(i32, shape, dim)


def span(start, size, multiple=None):
    return pl.ds(pl.multiple_of(start, multiple or size), size)


def lane_sum(v):
    return jnp.sum(v, axis=1, keepdims=True)


def row_sum(v):
    return jnp.sum(v, axis=0, keepdims=True)


def where0(mask, v):
    return jnp.where(mask, v, jnp.zeros_like(v))


def one_hot(mask):
    return jnp.where(mask, 1.0, 0.0).astype(bf16)


def split3(v):
    hi = v.astype(bf16)
    rest = v - hi.astype(f32)
    mid = rest.astype(bf16)
    return hi, mid, (rest - mid.astype(f32)).astype(bf16)


def loop(start, stop, body):
    def step(i, carry):
        body(i)
        return carry

    lax.fori_loop(start, stop, step, FIRST)


def chosen_mask(ids, experts):
    rows = iota((experts, ids.shape[1]), FIRST)
    return functools.reduce(jnp.logical_or, [rows == ids[j : j + 1, :] for j in range(ids.shape[FIRST])])


def router_kernel(capacity, local, x_ref, w_ref, ids_ref, tab_ref, prob_ref, carry):
    step = pl.program_id(FIRST)
    steps = pl.num_programs(FIRST)
    experts = w_ref.shape[1]

    @pl.when(step == FIRST)
    def _():
        carry[...] = jnp.zeros_like(carry)
        tab_ref[...] = jnp.zeros_like(tab_ref)

    x = x_ref[...]
    hi, mid, low = [dot(x, part) for part in split3(w_ref[...])]
    logits = jnp.transpose(hi + (mid + low))
    expo = jnp.exp(logits - jnp.max(logits, axis=FIRST, keepdims=True))
    prob = expo / row_sum(expo)
    chosen = chosen_mask(ids_ref[...], experts)
    hits = jnp.where(chosen, 1.0, 0.0)
    gate = where0(chosen, prob / row_sum(where0(chosen, prob)))
    earlier = one_hot(iota((BLK, BLK), FIRST) < iota((BLK, BLK), 1))
    before = carry[:, :1]
    pos = dot(hits.astype(bf16), earlier) + before
    pos = jnp.where(chosen & (pos < capacity), pos, NOT_KEPT)
    prob_ref[...] = prob
    after = before + lane_sum(hits)
    lane = iota((experts, LANES), 1)
    first = where0(lane == step, jnp.minimum(before, capacity) + jnp.zeros((experts, LANES), f32))
    first = first + where0((lane == step + 1) & (step == steps - 1), jnp.minimum(after, capacity) + jnp.zeros((experts, LANES), f32))
    stat = where0(lane == FIRST, lane_sum(hits) + jnp.zeros((experts, LANES), f32))
    stat = stat + where0(lane == 1, lane_sum(prob) + jnp.zeros((experts, LANES), f32))
    tail = slice(tab_ref.shape[LAST] - LANES, None)
    for d in range(experts // local):
        rows = slice(d * local, (d + 1) * local)
        tab_ref[d, :local, span(step * BLK, BLK)] = gate[rows]
        tab_ref[d, local:, span(step * BLK, BLK)] = pos[rows]
        tab_ref[d, :local, tail] += stat[rows]
        tab_ref[d, local:, tail] += first[rows]
    carry[:, :1] = after


def run_router(x_loc, w_router, ids_t, capacity, local, devices):
    tokens, d_model = x_loc.shape
    experts = w_router.shape[1]
    top_k = ids_t.shape[FIRST]
    table = (devices, 2 * local, tokens + LANES)
    return pl.pallas_call(
        functools.partial(router_kernel, capacity, local),
        grid=(tokens // BLK,),
        in_specs=[pl.BlockSpec((BLK, d_model), lambda i: (i, FIRST)), VMEM, pl.BlockSpec((top_k, BLK), lambda i: (FIRST, i))],
        out_specs=[VMEM, pl.BlockSpec((experts, BLK), lambda i: (FIRST, i))],
        out_shape=[Shape(table, f32), Shape((experts, tokens), f32)],
        scratch_shapes=[pltpu.VMEM((experts, LANES), f32)],
        compiler_params=params(),
        cost_estimate=cost(2 * tokens * d_model * BLK, 2 * tokens * d_model),
        name="router",
    )(x_loc, w_router, ids_t)


class Blocks:
    def __init__(self, starts_ref, bmap_ref, nb, half):
        self.starts, self.bmap, self.nb, self.half = starts_ref, bmap_ref, nb, half
        self.per_chunk = half // BLK
        self.count = self.per_chunk * len(CHUNKS)

    def info(self, i, e):
        flat = self.bmap[i]
        at = (flat // self.nb) * 64 + e * ALIGN + flat % self.nb
        first = self.starts[at]
        return flat, first, self.starts[at + 1] - first

    def total(self, e):
        return sum(self.info(i, e)[LAST] for i in range(self.count))

    def at_chunk_end(self, i, fn):
        for c in CHUNKS:
            pl.when(i == (c + 1) * self.per_chunk - 1)(functools.partial(fn, c))

    def at_chunk_start(self, i, fn):
        for c in CHUNKS:
            pl.when(i == c * self.per_chunk)(functools.partial(fn, c))

    def rows(self, c):
        return pl.ds(c * self.half, self.half)


def aligned(row):
    base = (row // ALIGN) * ALIGN
    return base, row - base


def window_count(shift, count):
    return (shift + count + WIN - 1) // WIN


def tiles_of(total):
    return (total + TILE - 1) // TILE


def row_tiles(total, body):
    tiles = tiles_of(total)
    pairs = tiles // 2
    loop(FIRST, pairs, lambda i: body(i * (2 * TILE), 2 * TILE))
    pl.when(tiles > 2 * pairs)(lambda: body(pairs * (2 * TILE), TILE))


def grad_kernel(has_in, last, nb, local, half, *refs):
    refs = list(refs)

    def take(n):
        got = refs[:n]
        del refs[:n]
        return got

    starts_ref, bmap_ref, tab_ref = take(3)
    tok_refs = take(len(CHUNKS)), take(len(CHUNKS))
    w1_ref, w3_ref, w2_ref = take(3)
    acc_in = take(2 * has_in)
    row_outs = take(3)
    outs = take(3 if last else 2)
    xv, dv, xr, dr, acc13, acc2, stage, tok_sem, in_sem, out_sem, row_sem = refs
    accs = acc13, acc2
    e = pl.program_id(FIRST)
    slot = e % 2
    d_model = xv.shape[1]
    d_ff = w1_ref.shape[LAST]
    blocks = Blocks(starts_ref, bmap_ref, nb, half)

    def token_copies(c):
        return [pltpu.make_async_copy(src[c], dst.at[blocks.rows(c)], tok_sem.at[w, c]) for w, (src, dst) in enumerate(zip(tok_refs, (xv, dv)))]

    def in_copies():
        return [pltpu.make_async_copy(src.at[e], dst.at[slot], in_sem.at[k]) for k, (src, dst) in enumerate(zip(acc_in, accs))]

    def out_copies(ee, ss):
        return [pltpu.make_async_copy(src.at[ss], dst.at[ee], out_sem.at[ss, k]) for k, (src, dst) in enumerate(zip(accs, outs))]

    def start(copies):
        for cp in copies:
            cp.start()

    def wait(copies):
        for cp in copies:
            cp.wait()

    @pl.when(e == FIRST)
    def _():
        for c in CHUNKS:
            start(token_copies(c))

    if not last:
        pl.when(e >= 2)(lambda: wait(out_copies(e - 2, slot)))
    start(in_copies())
    if not has_in:
        for acc in accs:
            acc[slot] = jnp.zeros(acc.shape[1:], f32)

    row_iota = iota((WIN, BLK), FIRST).astype(f32)
    head_row = iota((ALIGN, d_model), FIRST)

    def dispatch(i, row):
        pl.when(e == FIRST)(lambda: blocks.at_chunk_start(i, lambda c: wait(token_copies(c))))
        flat, first, count = blocks.info(i, e)
        base, shift = aligned(row)
        gate = tab_ref[flat, pl.ds(e, 1), :]
        pos = tab_ref[flat, pl.ds(local + e, 1), :]
        tok = span(i * BLK, BLK)

        def window(k):
            pick = (pos + (shift - first - k * WIN).astype(f32)) == row_iota
            one = one_hot(pick)
            gate_row = lane_sum(where0(pick, gate + jnp.zeros_like(row_iota)))
            return dot(one, xv[tok, :]).astype(bf16), (dot(one, dv[tok, :]) * gate_row).astype(bf16)

        for new, rows in zip(window(i32(FIRST)), (xr, dr)):
            head = span(base, ALIGN)
            rows[head, :] = jnp.where(head_row < shift, rows[head, :], new[:ALIGN])
            rows[span(base + ALIGN, WIN - ALIGN, ALIGN), :] = new[ALIGN:]

        def more(k):
            for new, rows in zip(window(k), (xr, dr)):
                rows[span(base + k * WIN, WIN, ALIGN), :] = new

        loop(1, window_count(shift, count), more)
        return row + count

    total = lax.fori_loop(FIRST, blocks.count, dispatch, i32(FIRST))

    def clear(i):
        for rows in (xr, dr):
            rows[span(i * ALIGN, ALIGN), :] = jnp.zeros((ALIGN, d_model), bf16)

    loop((total + ALIGN - 1) // ALIGN, tiles_of(total) * (TILE // ALIGN), clear)
    wait(in_copies())

    def tile(at, size):
        rows = span(at, size)
        xt = xr[rows, :]
        dt = dr[rows, :]
        act_a = dot(xt, w1_ref[FIRST])
        act_b = dot(xt, w3_ref[FIRST])
        d_hidden = dot_nt(dt, w2_ref[FIRST]).astype(bf16).astype(f32)
        sig = 1.0 / (1.0 + jnp.exp(-act_a))
        silu = act_a * sig
        hidden = (silu * act_b).astype(bf16)
        d_a = (d_hidden * act_b * sig * (1.0 + act_a * (1.0 - sig))).astype(bf16)
        d_b = (d_hidden * silu).astype(bf16)
        copies = []
        for k, (value, out) in enumerate(zip((hidden, d_a, d_b), row_outs)):
            stage[k, :size] = value
            copies.append(pltpu.make_async_copy(stage.at[k, :size], out.at[e, rows], row_sem.at[k]))
        start(copies)
        acc13[slot, :, :d_ff] += dot_tn(xt, d_a)
        acc13[slot, :, d_ff:] += dot_tn(xt, d_b)
        acc2[slot] += dot_tn(hidden, dt)
        wait(copies)

    row_tiles(total, tile)

    if last:
        for out, value in zip(outs, (acc13[slot, :, :d_ff], acc13[slot, :, d_ff:], acc2[slot])):
            out[FIRST] = value.astype(bf16)
    else:
        start(out_copies(e, slot))

        @pl.when(e == pl.num_programs(FIRST) - 1)
        def _():
            wait(out_copies(e - 1, 1 - slot))
            wait(out_copies(e, slot))


def per_expert(*shape):
    return pl.BlockSpec((1, *shape), lambda e: (e,) + (FIRST,) * len(shape))


def block_map(group, nb):
    hb = nb // 2
    return np.asarray([src * nb + part * hb + b for src, part in group for b in range(hb)], np.int32)


def run_grad(starts, tab, group, xs, ds, weights, acc, last, nb, row_cap):
    local, d_model, d_ff = weights[FIRST].shape
    half = xs[FIRST].shape[FIRST]
    w_specs = [per_expert(*w.shape[1:]) for w in weights]
    sums = [(local, d_model, 2 * d_ff), (local, d_ff, d_model)]
    rows = [Shape((local, row_cap, d_ff), bf16)] * 3
    out_shape = rows + ([Shape(w.shape, bf16) for w in weights] if last else [Shape(s, f32) for s in sums])
    out_specs = [ANY] * 3 + (w_specs if last else [ANY] * 2)
    tokens = pltpu.VMEM((len(CHUNKS) * half, d_model), bf16)
    packed = pltpu.VMEM((row_cap + WIN, d_model), bf16)
    out = pl.pallas_call(
        functools.partial(grad_kernel, bool(acc), last, nb, local, half),
        grid=(local,),
        in_specs=[SMEM, SMEM, VMEM] + [ANY] * (2 * len(CHUNKS)) + w_specs + [ANY] * len(acc),
        out_specs=out_specs,
        out_shape=out_shape,
        scratch_shapes=[tokens, tokens, packed, packed]
        + [pltpu.VMEM((2, *s[1:]), f32) for s in sums]
        + [pltpu.VMEM((3, 2 * TILE, d_ff), bf16), DMA((2, len(CHUNKS))), DMA((2,)), DMA((2, 2)), DMA((3,))],
        compiler_params=params(),
        cost_estimate=cost(12 * len(CHUNKS) * half * d_model * d_ff, 40 << 20),
        name="expert_grad",
    )(starts, block_map(group, nb), tab, *xs, *ds, *weights, *acc)
    return out[:3], out[3:]


def out_writer(blocks, values, outs, sems):
    def copy(c):
        return pltpu.make_async_copy(values.at[blocks.rows(c)], outs[c], sems.at[c])

    return copy


def y_kernel(nb, local, half, starts_ref, bmap_ref, tab_ref, h_ref, w2_ref, *refs):
    n = len(CHUNKS)
    d_refs, y_refs = refs[:n], refs[n : 2 * n]
    dg_ref, o_rows, dv, yv, zacc, yacc, dgacc, tok_sem, out_sem = refs[2 * n :]
    e = pl.program_id(FIRST)
    blocks = Blocks(starts_ref, bmap_ref, nb, half)
    d_model = dv.shape[1]
    token_copy = lambda c: pltpu.make_async_copy(d_refs[c], dv.at[blocks.rows(c)], tok_sem.at[c])
    out_copy = out_writer(blocks, yv, y_refs, out_sem)

    @pl.when(e == FIRST)
    def _():
        for c in CHUNKS:
            token_copy(c).start()

    total = blocks.total(e)

    def tile(at, size):
        o_rows[e, span(at, size), :] = dot(h_ref[FIRST, span(at, size), :], w2_ref[FIRST]).astype(bf16)

    row_tiles(total, tile)
    o_rows[e, span(tiles_of(total) * TILE, WIN), :] = jnp.zeros((WIN, d_model), bf16)

    @pl.when(e == local - 1)
    def _():
        for c in CHUNKS:
            token_copy(c).wait()
        lane = iota((BLK, WIN), 1).astype(f32)
        dg_lane = iota((BLK, LANES), 1)
        width = 2 * LANES
        columns = [slice(k * width, (k + 1) * width) for k in range(d_model // width)]

        def combine(i, rows_at):
            infos = [blocks.info(i, ee) for ee in range(local)]
            places = [aligned(r) for r in rows_at]
            windows = [window_count(place[1], info[LAST]) for place, info in zip(places, infos)]
            tab_t = jnp.transpose(tab_ref[infos[FIRST][FIRST]])
            tok = span(i * BLK, BLK)
            gates = [tab_t[:, ee : ee + 1] for ee in range(local)]

            def pick(ee, k):
                shifted = tab_t[:, local + ee : local + ee + 1] + (places[ee][1] - infos[ee][1] - k * WIN).astype(f32)
                return one_hot(shifted == lane)

            def held(ee, k, cols):
                return o_rows[ee, span(places[ee][FIRST] + k * WIN, WIN, ALIGN), cols]

            def put_dg(sums):
                dg = sum(where0(dg_lane == ee, lane_sum(s) + jnp.zeros((BLK, LANES), f32)) for ee, s in enumerate(sums))
                dg_ref[i] = jnp.transpose(dg)[: 2 * local, :]

            simple = functools.reduce(jnp.logical_and, [w <= 1 for w in windows])

            @pl.when(simple)
            def _():
                picks = [pick(ee, i32(FIRST)) for ee in range(local)]
                sums = [None] * local
                for cols in columns:
                    dy = dv[tok, cols].astype(f32)
                    y = None
                    for ee in range(local):
                        z = dot(picks[ee], held(ee, i32(FIRST), cols))
                        prod = dy * z
                        part = prod[:, :LANES] + prod[:, LANES:]
                        sums[ee] = part if sums[ee] is None else sums[ee] + part
                        y = gates[ee] * z if y is None else y + gates[ee] * z
                    yv[tok, cols] = y.astype(bf16)
                put_dg(sums)

            @pl.when(jnp.logical_not(simple))
            def _():
                yacc[...] = jnp.zeros_like(yacc)
                for ee in range(local):
                    zacc[...] = jnp.zeros_like(zacc)

                    def more(k, ee=ee):
                        zacc[...] += dot(pick(ee, k), held(ee, k, slice(None)))

                    loop(FIRST, windows[ee], more)
                    yacc[...] += gates[ee] * zacc[...]
                    dgacc[ee] = lane_sum(dv[tok, :].astype(f32) * zacc[...]) * jnp.where(dg_lane == FIRST, 1.0, 0.0)
                yv[tok, :] = yacc[...].astype(bf16)
                put_dg([dgacc[ee] for ee in range(local)])

            blocks.at_chunk_end(i, lambda c: out_copy(c).start())
            return tuple(r + info[LAST] for r, info in zip(rows_at, infos))

        lax.fori_loop(FIRST, blocks.count, combine, (i32(FIRST),) * local)
        for c in CHUNKS:
            out_copy(c).wait()


def run_y(starts, tab, group, h_rows, w2, ds, nb):
    local, d_ff, d_model = w2.shape
    row_cap = h_rows.shape[1]
    half = ds[FIRST].shape[FIRST]
    n = len(CHUNKS)
    dg_shape = (n * half // BLK, 2 * local, BLK)
    block = pltpu.VMEM((BLK, d_model), f32)
    tokens = pltpu.VMEM((n * half, d_model), bf16)
    out = pl.pallas_call(
        functools.partial(y_kernel, nb, local, half),
        grid=(local,),
        in_specs=[SMEM, SMEM, VMEM, per_expert(row_cap, d_ff), per_expert(d_ff, d_model)] + [ANY] * n,
        out_specs=[ANY] * n + [VMEM],
        out_shape=[Shape((half, d_model), bf16)] * n + [Shape(dg_shape, f32)],
        scratch_shapes=[pltpu.VMEM((local, row_cap + WIN, d_model), bf16), tokens, tokens, block, block, pltpu.VMEM((local, BLK, LANES), f32), DMA((n,)), DMA((n,))],
        compiler_params=params(),
        cost_estimate=cost(4 * n * half * d_model * d_ff, 20 << 20),
        name="expert_y",
    )(starts, block_map(group, nb), tab, h_rows, w2, *ds)
    return out[:n], out[n]


def dx_kernel(nb, local, half, starts_ref, bmap_ref, tab_ref, da_ref, db_ref, w1_ref, w3_ref, *refs):
    n = len(CHUNKS)
    y_refs = refs[:n]
    o_rows, yv, zacc, out_sem = refs[n:]
    e = pl.program_id(FIRST)
    blocks = Blocks(starts_ref, bmap_ref, nb, half)
    d_model = yv.shape[1]
    out_copy = out_writer(blocks, yv, y_refs, out_sem)
    total = blocks.total(e)

    def tile(at, size):
        rows = span(at, size)
        grad = dot_nt(da_ref[FIRST, rows, :], w1_ref[FIRST]) + dot_nt(db_ref[FIRST, rows, :], w3_ref[FIRST])
        o_rows[e, rows, :] = grad.astype(bf16)

    row_tiles(total, tile)
    o_rows[e, span(tiles_of(total) * TILE, WIN), :] = jnp.zeros((WIN, d_model), bf16)

    @pl.when(e == local - 1)
    def _():
        lane = iota((BLK, WIN), 1).astype(f32)

        def combine(i, rows_at):
            infos = [blocks.info(i, ee) for ee in range(local)]
            places = [aligned(r) for r in rows_at]
            windows = [window_count(place[1], info[LAST]) for place, info in zip(places, infos)]
            tab_t = jnp.transpose(tab_ref[infos[FIRST][FIRST]])
            tok = span(i * BLK, BLK)

            def pick(ee, k):
                shifted = tab_t[:, local + ee : local + ee + 1] + (places[ee][1] - infos[ee][1] - k * WIN).astype(f32)
                return one_hot(shifted == lane), o_rows[ee, span(places[ee][FIRST] + k * WIN, WIN, ALIGN), :]

            simple = functools.reduce(jnp.logical_and, [w <= 1 for w in windows])

            @pl.when(simple)
            def _():
                pairs = [[pick(ee + k, i32(FIRST)) for k in HALVES] for ee in range(FIRST, local, 2)]
                sums = [dot(jnp.concatenate([p[FIRST] for p in pair], axis=1), jnp.concatenate([p[1] for p in pair], axis=FIRST)) for pair in pairs]
                yv[tok, :] = sum(sums[1:], sums[FIRST]).astype(bf16)

            @pl.when(jnp.logical_not(simple))
            def _():
                zacc[...] = jnp.zeros_like(zacc)
                for ee in range(local):

                    def more(k, ee=ee):
                        zacc[...] += dot(*pick(ee, k))

                    loop(FIRST, windows[ee], more)
                yv[tok, :] = zacc[...].astype(bf16)

            blocks.at_chunk_end(i, lambda c: out_copy(c).start())
            return tuple(r + info[LAST] for r, info in zip(rows_at, infos))

        lax.fori_loop(FIRST, blocks.count, combine, (i32(FIRST),) * local)
        for c in CHUNKS:
            out_copy(c).wait()


def run_dx(starts, tab, group, da_rows, db_rows, w1, w3, nb, half):
    local, d_model, d_ff = w1.shape
    row_cap = da_rows.shape[1]
    n = len(CHUNKS)
    return pl.pallas_call(
        functools.partial(dx_kernel, nb, local, half),
        grid=(local,),
        in_specs=[SMEM, SMEM, VMEM] + [per_expert(row_cap, d_ff)] * 2 + [per_expert(d_model, d_ff)] * 2,
        out_specs=[ANY] * n,
        out_shape=[Shape((half, d_model), bf16)] * n,
        scratch_shapes=[pltpu.VMEM((local, row_cap + WIN, d_model), bf16), pltpu.VMEM((n * half, d_model), bf16), pltpu.VMEM((BLK, d_model), f32), DMA((n,))],
        compiler_params=params(),
        cost_estimate=cost(6 * n * half * d_model * d_ff, 20 << 20),
        name="expert_dx",
    )(starts, block_map(group, nb), tab, da_rows, db_rows, w1, w3)


def router_grad_kernel(scale, x_ref, prob_ref, dg_ref, ids_ref, load_ref, dlog_ref, dw_ref):
    step = pl.program_id(FIRST)
    prob = prob_ref[...]
    dg = dg_ref[...]
    chosen = chosen_mask(ids_ref[...], prob.shape[FIRST])
    gate_sum = row_sum(where0(chosen, prob))
    gate = where0(chosen, prob / gate_sum)
    d_pick = (dg - row_sum(gate * dg)) / gate_sum
    d_prob = where0(chosen, d_pick) + scale * load_ref[:, :1]
    d_logit = prob * (d_prob - row_sum(prob * d_prob))
    dlog_ref[...] = d_logit
    hi, mid, low = [dot(part, x_ref[...]) for part in split3(d_logit)]

    @pl.when(step == FIRST)
    def _():
        dw_ref[...] = jnp.zeros_like(dw_ref)

    dw_ref[...] += hi + (mid + low)


def run_router_grad(x_loc, prob_t, dg_t, ids_t, load, scale):
    tokens, d_model = x_loc.shape
    experts = prob_t.shape[FIRST]
    lanes = lambda n: pl.BlockSpec((n, BLK), lambda i: (FIRST, i))
    return pl.pallas_call(
        functools.partial(router_grad_kernel, scale),
        grid=(tokens // BLK,),
        in_specs=[pl.BlockSpec((BLK, d_model), lambda i: (i, FIRST)), lanes(experts), lanes(experts), lanes(ids_t.shape[FIRST]), VMEM],
        out_specs=[lanes(experts), VMEM],
        out_shape=[Shape((experts, tokens), f32), Shape((experts, d_model), f32)],
        compiler_params=params(),
        cost_estimate=cost(2 * tokens * d_model * BLK, 2 * tokens * d_model),
        name="router_grad",
    )(x_loc, prob_t, dg_t, ids_t, load)


def final_kernel(dlog_ref, wt_ref, a_ref, b_ref, c_ref, out_ref):
    lhs = split3(dlog_ref[...])
    rhs = split3(wt_ref[...])
    terms = [(i, j) for i in range(3) for j in range(3 - i)]
    left = jnp.concatenate([lhs[i] for i, _ in terms], axis=FIRST)
    right = jnp.concatenate([rhs[j] for _, j in terms], axis=FIRST)
    rows = [ref[...].astype(f32) for ref in (a_ref, b_ref, c_ref)]
    out_ref[...] = (dot_tn(left, right) + sum(rows[1:], rows[FIRST])).astype(bf16)


def run_final(dlog_t, w_t, parts):
    experts, tokens = dlog_t.shape
    d_model = w_t.shape[1]
    rows = pl.BlockSpec((BLK, d_model), lambda i: (i, FIRST))
    return pl.pallas_call(
        final_kernel,
        grid=(tokens // BLK,),
        in_specs=[pl.BlockSpec((experts, BLK), lambda i: (FIRST, i)), VMEM, rows, rows, rows],
        out_specs=rows,
        out_shape=Shape((tokens, d_model), bf16),
        compiler_params=params(),
        cost_estimate=cost(2 * tokens * d_model * BLK, 8 * tokens * d_model),
        name="final_dx",
    )(dlog_t, w_t, *parts)


NEAR = (X, Y)
RELAYED = {(Y, 0): 0, (X, 1): 1}
OPS = [
    (t, src, h)
    for step in ([(FAR, 0), (FAR, 1)], [(X, 0), (Y, 1)], [(X, 1), (Y, 0)], [(FIRST, 0), (FIRST, 1)])
    for t in TENSORS
    for src, h in step
]


def add_rows(dst, src):
    def body(i):
        rows = span(i * LANES, LANES)
        dst[rows, :] = (dst[rows, :].astype(f32) + src[rows, :].astype(f32)).astype(bf16)

    loop(FIRST, dst.shape[FIRST] // LANES, body)


def exchange_kernel(half, mats, *refs):
    refs = list(refs)

    def take(n):
        got = refs[:n]
        del refs[:n]
        return got

    parts = [[take(len(HALVES)) for _ in SOURCES] for _ in TENSORS]
    dws = take(mats)
    outs = [take(len(NEAR) + 1) for _ in TENSORS]
    dw_outs = take(mats)
    land, far_land, stage, z_one, z_two, z_stage = take(6)
    core_sem, stage_sem, far_sem, near_sem, own_sem, z_sem, keep_sem, load_sem, credit_one, credit_two = refs

    me = lax.axis_index("ep")
    z = lax.axis_index("dp")
    peer = {bit: me + bit - 2 * bit * ((me // bit) % 2) for bit in (CORE, X, Y)}
    z_peer = z + 1 - 2 * (z % 2)
    z_cross = 3 - z
    is_end = (z % 3) == FIRST
    is_mid = (z % 3) != FIRST

    barrier = pltpu.get_barrier_semaphore()
    ids = [{"ep": p} for p in peer.values()] + [{"dp": z_peer}, {"dp": z_cross}]
    for device in ids:
        pl.semaphore_signal(barrier, device_id=device, device_id_type=MESH)
    pl.semaphore_wait(barrier, len(ids))

    def remote(src, dst, sems, at, device):
        send, recv = sems.at[(SEND, *at)], sems.at[(RECV, *at)]
        return pltpu.make_async_remote_copy(src_ref=src, dst_ref=dst, send_sem=send, recv_sem=recv, device_id=device, device_id_type=MESH)

    def rows_at(h):
        return pl.ds(h * half, half)

    def core_copy(i):
        t, src, h = OPS[i]
        return remote(parts[t][src | CORE][h], land.at[i], core_sem, (i,), {"ep": peer[CORE]})

    def stage_copy(i):
        t, src, h = OPS[i]
        return pltpu.make_async_copy(parts[t][src][h], stage.at[i % STAGES], stage_sem.at[i % STAGES])

    def far_copy(i):
        t, _, h = OPS[i]
        return remote(land.at[i], far_land.at[t, h], far_sem, (t, h), {"ep": peer[NEAR[h]]})

    def near_copy(i):
        t, src, h = OPS[i]
        k = NEAR.index(src)
        return remote(land.at[i], outs[t][k].at[rows_at(h)], near_sem, (t, k, h), {"ep": peer[src]})

    def own_copy(i):
        t, _, h = OPS[i]
        return pltpu.make_async_copy(land.at[i], outs[t][LAST].at[rows_at(h)], own_sem.at[t, h])

    def out_copy(i):
        src = OPS[i][1]
        return (far_copy if src == FAR else near_copy if src else own_copy)(i)

    def reduce_op(i):
        t, src, h = OPS[i]
        stage_copy(i).wait()
        core_copy(i).wait_recv()
        add_rows(land.at[i], stage.at[i % STAGES])
        if i + STAGES < len(OPS):
            stage_copy(i + STAGES).start()
        if (src, h) in RELAYED:
            far_copy(OPS.index((t, FAR, RELAYED[src, h]))).wait_recv()
            add_rows(land.at[i], far_land.at[t, RELAYED[src, h]])

    rows_per = z_one.shape[1]
    chunks = [(m, e, k) for e in range(dws[FIRST].shape[FIRST]) for m in range(mats) for k in HALVES]
    n = len(chunks)

    def piece(arrays, c):
        m, e, k = chunks[c]
        return arrays[m].at[e, pl.ds(k * rows_per, rows_per)]

    def one_copy(c):
        return remote(piece(dws, c), z_one.at[c % SLOTS], z_sem, (FIRST, c), {"dp": z_peer})

    def two_copy(c):
        return remote(z_one.at[c % SLOTS], z_two.at[c % SLOTS], z_sem, (1, c), {"dp": z_cross})

    def three_copy(c):
        return remote(z_two.at[c % SLOTS], piece(dw_outs, c), z_sem, (2, c), {"dp": z_peer})

    def keep_copy(c):
        return pltpu.make_async_copy(z_two.at[c % SLOTS], piece(dw_outs, c), keep_sem.at[c])

    def load_copy(c):
        return pltpu.make_async_copy(piece(dws, c), z_stage.at[c % STAGES], load_sem.at[c % STAGES])

    def first_add(c):
        load_copy(c).wait()
        one_copy(c).wait_recv()
        add_rows(z_one.at[c % SLOTS], z_stage.at[c % STAGES])
        if c + STAGES < n:
            load_copy(c + STAGES).start()

    def second_add(c):
        two_copy(c).wait()
        add_rows(z_two.at[c % SLOTS], z_one.at[c % SLOTS])
        if c + SLOTS < n:
            pl.semaphore_signal(credit_one, device_id={"dp": z_peer}, device_id_type=MESH)

    def retire(c):
        three_copy(c).wait_send()
        keep_copy(c).wait()
        if c + SLOTS < n:
            pl.semaphore_signal(credit_two, device_id={"dp": z_cross}, device_id_type=MESH)

    @pl.when(is_end)
    def _():
        for c in range(SLOTS):
            one_copy(c).start()

    @pl.when(is_mid)
    def _():
        for c in range(STAGES):
            load_copy(c).start()

    for i in range(len(OPS)):
        core_copy(i).start()
        if i < STAGES:
            stage_copy(i).start()

    todo = list(range(len(OPS)))
    for tick in range(n + LAG):
        mine = todo[: 2 if tick < 2 else 1]
        todo = todo[len(mine) :]
        for i in mine:
            reduce_op(i)

        @pl.when(is_mid)
        def _():
            back = tick - 1
            if tick < n:
                first_add(tick)
            if back in range(n):
                second_add(back)
            if tick < n:
                if tick >= SLOTS:
                    pl.semaphore_wait(credit_two, 1)
                two_copy(tick).start()
            if back in range(n):
                three_copy(back).start()
                keep_copy(back).start()
            if tick >= LAG:
                retire(tick - LAG)

        for i in mine:
            out_copy(i).start()

        @pl.when(is_end)
        def _():
            if tick + SLOTS < n:
                pl.semaphore_wait(credit_one, 1)
                one_copy(tick + SLOTS).start()

    for i in todo:
        reduce_op(i)
        out_copy(i).start()

    @pl.when(is_end)
    def _():
        for c in range(n):
            one_copy(c).wait_send()
            three_copy(c).wait_recv()

    for i in range(len(OPS)):
        core_copy(i).wait_send()
        (out_copy(i).wait_send if OPS[i][1] == FAR else out_copy(i).wait)()


def run_exchange(parts, dws):
    half, d_model = parts[FIRST][FIRST][FIRST].shape
    local, rows, cols = dws[FIRST].shape
    chunk = (rows // 2, cols)
    n = local * len(dws) * len(HALVES)
    whole = Shape((2 * half, d_model), bf16)
    flat = [v for tensor in parts for source in tensor for v in source] + list(dws)
    terms = len(NEAR) + 1
    out = pl.pallas_call(
        functools.partial(exchange_kernel, half, len(dws)),
        in_specs=[ANY] * len(flat),
        out_specs=[ANY] * (terms * len(TENSORS) + len(dws)),
        out_shape=[whole] * (terms * len(TENSORS)) + [Shape(v.shape, bf16) for v in dws],
        scratch_shapes=[
            pltpu.VMEM((len(OPS), half, d_model), bf16),
            pltpu.VMEM((len(TENSORS), len(HALVES), half, d_model), bf16),
            pltpu.VMEM((STAGES, half, d_model), bf16),
            pltpu.VMEM((SLOTS, *chunk), bf16),
            pltpu.VMEM((SLOTS, *chunk), bf16),
            pltpu.VMEM((STAGES, *chunk), bf16),
            DMA((2, len(OPS))),
            DMA((STAGES,)),
            DMA((2, 2, 2)),
            DMA((2, 2, 2, 2)),
            DMA((2, 2)),
            DMA((2, 3, n)),
            DMA((n,)),
            DMA((STAGES,)),
            pltpu.SemaphoreType.REGULAR,
            pltpu.SemaphoreType.REGULAR,
        ],
        compiler_params=pltpu.CompilerParams(vmem_limit_bytes=VMEM_LIMIT, collective_id=FIRST, has_side_effects=True),
        cost_estimate=cost(1 << 37, 200 << 20),
        name="exchange",
    )(*flat)
    return [out[:terms], out[terms : 2 * terms]], out[2 * terms :]


def hop(v, bit):
    return lax.ppermute(v, "ep", [(i, i ^ bit) for i in SOURCES])


def after(values, token):
    return lax.optimization_barrier((values, token))[FIRST]


def send_own(v):
    half = v.shape[FIRST] // 2
    got = {(FIRST, h): v[h * half : (h + 1) * half] for h in HALVES}
    for h in HALVES:
        for bit in (CORE, X, Y):
            got[bit, h] = hop(got[FIRST, h], bit)
    return got


def pass_on(got, h):
    got[FAR, h] = hop(got[(Y, X)[h], h], NEAR[h])
    for bit in NEAR:
        got[bit | CORE, h] = hop(got[bit, h], CORE)


def relative(v, me):
    shape = v.shape
    v = v.reshape((2, 2, 2) + shape[1:])
    for axis, bit in enumerate((Y, X, CORE)):
        v = jnp.where((me & bit) != FIRST, jnp.flip(v, axis), v)
    return v.reshape(shape)


GROUPS = (
    [(src, h) for src in (FIRST, CORE) for h in HALVES],
    [(src, FIRST) for src in (X, X | CORE, Y, Y | CORE)],
    [(src, 1) for src in (X, X | CORE, Y, Y | CORE)],
    [(src, h) for h in HALVES for src in (FAR, FAR | CORE)],
)


def solution(mesh):
    dp_size = mesh.shape["dp"]
    ep_size = mesh.shape["ep"]
    row_spec = P(("dp", "ep"), None)
    expert_spec = P("ep", None, None)
    whole_spec = P(None, None)

    def per_device(x_loc, w_router, ids_loc, w1, w3, w2, dy_loc):
        tokens, d_model = x_loc.shape
        top_k = ids_loc.shape[1]
        experts = w_router.shape[1]
        local = w1.shape[FIRST]
        capacity = capacity_of(tokens, top_k, experts)
        n_total = tokens * dp_size * ep_size
        half = tokens // 2
        nb = tokens // BLK
        row_cap = tiles_of(len(CHUNKS) * min(capacity, half)) * TILE
        me = lax.axis_index("ep")

        tokens_of = [send_own(v) for v in (x_loc, dy_loc)]

        ids_t = ids_loc.T
        send_tab, prob_t = run_router(x_loc, w_router, ids_t, capacity, local, ep_size)
        tab_rel = relative(lax.all_to_all(send_tab, "ep", FIRST, FIRST, tiled=True), me)
        tab = tab_rel[:, :, :tokens].reshape(ep_size, 2 * local, nb, BLK).transpose(0, 2, 1, 3).reshape(ep_size * nb, 2 * local, BLK)
        starts = tab_rel[:, local:, tokens : tokens + ALIGN].astype(i32).reshape(LAST)

        acc = ()
        rows = []
        for g, group in enumerate(GROUPS):
            if g:
                ready = [key for key in tokens_of[FIRST] if key[1] == g - 1 and key[FIRST] in NEAR] if g < len(GROUPS) - 1 else [(FAR, h) for h in HALVES]
                for got in tokens_of:
                    got.update(after({key: got[key] for key in ready}, acc[LAST]))
                for got in tokens_of:
                    if g < len(GROUPS) - 1:
                        pass_on(got, g - 1)
                    else:
                        for key in ready:
                            got[FAR | CORE, key[1]] = hop(got[key], CORE)
            last = g == len(GROUPS) - 1
            got, acc = run_grad(starts, tab, group, *[[got[k] for k in group] for got in tokens_of], (w1, w3, w2), acc, last, nb, row_cap)
            rows.append(got)
            if not g:
                stats = jnp.sum(after(tab_rel[:, :local, tokens:], acc[LAST]), axis=FIRST)
                for step in (1, 2):
                    stats = stats + lax.ppermute(stats, "dp", [(i, i ^ step) for i in range(dp_size)])
        dw1, dw3, dw2 = acc
        ds = tokens_of[1]
        starts, dw2 = lax.optimization_barrier((starts, dw2))
        dw2_sum = lax.psum(dw2, "dp")

        parts = {}, {}
        dg_part = {}
        for group, got in zip(GROUPS, rows):
            outs, dg = run_y(starts, tab, group, got[FIRST], w2, [ds[k] for k in group], nb)
            parts[FIRST].update(zip(group, outs))
            dg = dg.reshape(len(CHUNKS), half // BLK, 2 * local, BLK)[:, :, :local]
            dg_part.update({k: dg[i] for i, k in enumerate(group)})
        for g, (group, got) in enumerate(zip(GROUPS, rows)):
            if g == len(GROUPS) - 1:
                starts = after(starts, dw2_sum)
            parts[1].update(zip(group, run_dx(starts, tab, group, got[1], got[2], w1, w3, nb, half)))

        dg_all = jnp.stack([jnp.concatenate([dg_part[s, h] for h in HALVES], axis=FIRST) for s in SOURCES])
        dg_all = relative(dg_all.transpose(0, 2, 1, 3).reshape(ep_size, local, tokens), me)
        dg_all = jnp.concatenate([dg_all, jnp.broadcast_to(stats, (ep_size, *stats.shape))], axis=2)
        dg_all = lax.all_to_all(dg_all, "ep", FIRST, FIRST, tiled=True).reshape(experts, tokens + LANES)
        load = dg_all[:, tokens:]
        share = AUX_COEF * experts / (n_total * top_k * n_total)
        aux_loss = share * jnp.sum(load[:, FIRST] * load[:, 1])
        dlog_t, dwr_t = run_router_grad(x_loc, prob_t, dg_all[:, :tokens], ids_t, load, share)
        dw_router = lax.psum(after(dwr_t, dw2_sum), ("dp", "ep")).T

        sums, grads = run_exchange([[[part[s, h] for h in HALVES] for s in SOURCES] for part in parts], [dw1, dw3])
        y_loc = sum(v.astype(f32) for v in sums[FIRST]).astype(bf16)
        dx_loc = run_final(dlog_t, w_router.T, sums[1])
        return y_loc, aux_loss, dx_loc, dw_router, *grads, dw2_sum

    return jax.shard_map(
        per_device,
        mesh=mesh,
        in_specs=(row_spec, whole_spec, row_spec, expert_spec, expert_spec, expert_spec, row_spec),
        out_specs=(row_spec, P(), row_spec, whole_spec, expert_spec, expert_spec, expert_spec),
        check_vma=False,
    )
```

```python
import functools

import jax
import jax.numpy as jnp
import numpy as np
from jax import lax
from jax.experimental import pallas as pl
from jax.experimental.pallas import tpu as pltpu
from jax.sharding import PartitionSpec as P

AUX_COEF = 0.01
BLK = 256
TILE = 256
WIN = 128
LANES = 128
ALIGN = 16
NOT_KEPT = -65536.0
VMEM_LIMIT = 63 * 1024 * 1024
CORE, X, Y = 1, 2, 4
FAR = X | Y
HALVES = TENSORS = range(2)
RING = 4
SOURCES = range(8)
FIRST, LAST = 0, -1
SEND, RECV = 0, 1
STAGES = 3
SLOTS = 8
LAG = 3
MESH = pl.DeviceIdType.MESH

WHOLE, PARTS = (0, 6), ((0, 3), (3, 3))
GROUPS = (
    [(src, *WHOLE) for src in (FIRST, CORE)],
    [(bit | core, *PARTS[FIRST]) for bit in (X, Y) for core in (FIRST, CORE)],
    [(bit | core, *PARTS[1]) for bit in (X, Y) for core in (FIRST, CORE)],
    [(FAR | core, *part) for part in PARTS for core in (FIRST, CORE)],
)


f32 = jnp.float32
bf16 = jnp.bfloat16
i32 = jnp.int32
ANY = pl.BlockSpec(memory_space=pl.ANY)
SMEM = pl.BlockSpec(memory_space=pltpu.SMEM)
VMEM = pl.BlockSpec(memory_space=pltpu.VMEM)
DMA = pltpu.SemaphoreType.DMA
Shape = jax.ShapeDtypeStruct


def capacity_of(tokens, top_k, experts):
    return (5 * top_k * tokens + 4 * experts - 1) // (4 * experts)


def dot(a, b, ca=1, cb=0):
    return lax.dot_general(a, b, (((ca,), (cb,)), ((), ())), preferred_element_type=f32)


def dot_nt(a, b):
    return dot(a, b, 1, 1)


def dot_tn(a, b):
    return dot(a, b, 0, 0)


def grid_params(dims):
    return pltpu.CompilerParams(dimension_semantics=("arbitrary",) * dims, vmem_limit_bytes=VMEM_LIMIT)


def params():
    return grid_params(1)


def cost(flops, moved):
    return pl.CostEstimate(flops=flops, bytes_accessed=moved, transcendentals=FIRST)


def iota(shape, dim):
    return lax.broadcasted_iota(i32, shape, dim)


def span(start, size, multiple=None):
    return pl.ds(pl.multiple_of(start, multiple or size), size)


def lane_sum(v):
    return jnp.sum(v, axis=1, keepdims=True)


def row_sum(v):
    return jnp.sum(v, axis=0, keepdims=True)


def where0(mask, v):
    return jnp.where(mask, v, jnp.zeros_like(v))


def one_hot(mask):
    return jnp.where(mask, 1.0, 0.0).astype(bf16)


def split3(v):
    hi = v.astype(bf16)
    rest = v - hi.astype(f32)
    mid = rest.astype(bf16)
    return hi, mid, (rest - mid.astype(f32)).astype(bf16)


def loop(start, stop, body):
    def step(i, carry):
        body(i)
        return carry

    lax.fori_loop(start, stop, step, FIRST)


def chosen_mask(ids, experts):
    rows = iota((experts, ids.shape[1]), FIRST)
    return functools.reduce(jnp.logical_or, [rows == ids[j : j + 1, :] for j in range(ids.shape[FIRST])])


def router_kernel(capacity, local, x_ref, w_ref, ids_ref, tab_ref, prob_ref, carry):
    step = pl.program_id(FIRST)
    steps = pl.num_programs(FIRST)
    experts = w_ref.shape[1]

    @pl.when(step == FIRST)
    def _():
        carry[...] = jnp.zeros_like(carry)
        tab_ref[...] = jnp.zeros_like(tab_ref)

    x = x_ref[...]
    hi, mid, low = [dot(x, part) for part in split3(w_ref[...])]
    logits = jnp.transpose(hi + (mid + low))
    expo = jnp.exp(logits - jnp.max(logits, axis=FIRST, keepdims=True))
    prob = expo / row_sum(expo)
    chosen = chosen_mask(ids_ref[...], experts)
    hits = jnp.where(chosen, 1.0, 0.0)
    gate = where0(chosen, prob / row_sum(where0(chosen, prob)))
    earlier = one_hot(iota((BLK, BLK), FIRST) < iota((BLK, BLK), 1))
    before = carry[:, :1]
    pos = dot(hits.astype(bf16), earlier) + before
    pos = jnp.where(chosen & (pos < capacity), pos, NOT_KEPT)
    prob_ref[...] = prob
    after = before + lane_sum(hits)
    lane = iota((experts, LANES), 1)
    first = where0(lane == step, jnp.minimum(before, capacity) + jnp.zeros((experts, LANES), f32))
    first = first + where0((lane == step + 1) & (step == steps - 1), jnp.minimum(after, capacity) + jnp.zeros((experts, LANES), f32))
    stat = where0(lane == FIRST, lane_sum(hits) + jnp.zeros((experts, LANES), f32))
    stat = stat + where0(lane == 1, lane_sum(prob) + jnp.zeros((experts, LANES), f32))
    tail = slice(tab_ref.shape[LAST] - LANES, None)
    for d in range(experts // local):
        rows = slice(d * local, (d + 1) * local)
        tab_ref[d, :local, span(step * BLK, BLK)] = gate[rows]
        tab_ref[d, local:, span(step * BLK, BLK)] = pos[rows]
        tab_ref[d, :local, tail] += stat[rows]
        tab_ref[d, local:, tail] += first[rows]
    carry[:, :1] = after


def run_router(x_loc, w_router, ids_t, capacity, local, devices):
    tokens, d_model = x_loc.shape
    experts = w_router.shape[1]
    top_k = ids_t.shape[FIRST]
    table = (devices, 2 * local, tokens + LANES)
    return pl.pallas_call(
        functools.partial(router_kernel, capacity, local),
        grid=(tokens // BLK,),
        in_specs=[pl.BlockSpec((BLK, d_model), lambda i: (i, FIRST)), VMEM, pl.BlockSpec((top_k, BLK), lambda i: (FIRST, i))],
        out_specs=[VMEM, pl.BlockSpec((experts, BLK), lambda i: (FIRST, i))],
        out_shape=[Shape(table, f32), Shape((experts, tokens), f32)],
        scratch_shapes=[pltpu.VMEM((experts, LANES), f32)],
        compiler_params=params(),
        cost_estimate=cost(2 * tokens * d_model * BLK, 2 * tokens * d_model),
        name="router",
    )(x_loc, w_router, ids_t)


class Blocks:
    def __init__(self, starts_ref, bmap_ref, nb):
        self.starts, self.bmap, self.nb = starts_ref, bmap_ref, nb

    def info(self, i, e):
        flat = self.bmap[i]
        at = (flat // self.nb) * 64 + e * ALIGN + flat % self.nb
        first = self.starts[at]
        return flat, first, self.starts[at + 1] - first

    def total(self, start, count, e):
        return lax.fori_loop(start, start + count, lambda i, n: n + self.info(i, e)[LAST], i32(FIRST))


def aligned(row):
    base = (row // ALIGN) * ALIGN
    return base, row - base


def window_count(shift, count):
    return (shift + count + WIN - 1) // WIN


def padded(total):
    return (total + TILE - 1) // TILE * TILE


def row_tiles(total, body, size):
    tiles = (total + size - 1 - size // 2) // size
    loop(FIRST, tiles, lambda i: body(i * size, size))
    pl.when(padded(total) > tiles * size)(lambda: body(tiles * size, size // 2))


def start(copies):
    for cp in copies:
        cp.start()


def wait(copies):
    for cp in copies:
        cp.wait()


def taker(refs):
    refs = list(refs)

    def take(n=None):
        got = refs[:n]
        del refs[:n]
        return got

    return take


def offsets(pieces):
    counts = [count for _, _, count in pieces]
    return [(sum(counts[:k]), count) for k, count in enumerate(counts)]


def block_rows(first, count):
    return pl.ds(first * BLK, count * BLK)


def grad_kernel(g, last, nb, local, pieces, *refs):
    take = taker(refs)
    n = len(pieces)
    starts_ref, bmap_ref, tab_ref = take(3)
    tok_refs = take(n), take(n)
    w1_ref, w3_ref, w2_ref = take(3)
    acc_in = take(2 * bool(g))
    take(3 * bool(g))
    row_outs = take(3)
    outs = take(3 if last else 2)
    xv, dv, xr, dr, acc13, acc2, stage, tok_sem, in_sem, out_sem, row_sem = take()
    accs = acc13, acc2
    e = pl.program_id(FIRST)
    slot = e % 2
    d_model = xv.shape[1]
    d_ff = w1_ref.shape[LAST]
    blocks = Blocks(starts_ref, bmap_ref, nb)
    count = xv.shape[FIRST] // BLK

    def token_copies(c):
        rows = block_rows(*offsets(pieces)[c])
        return [pltpu.make_async_copy(src[c], dst.at[rows], tok_sem.at[w, c]) for w, (src, dst) in enumerate(zip(tok_refs, (xv, dv)))]

    def in_copies():
        return [pltpu.make_async_copy(src.at[e], dst.at[slot], in_sem.at[k]) for k, (src, dst) in enumerate(zip(acc_in, accs))]

    def out_copies(ee, ss):
        return [pltpu.make_async_copy(src.at[ss], dst.at[ee], out_sem.at[ss, k]) for k, (src, dst) in enumerate(zip(accs, outs))]

    @pl.when(e == FIRST)
    def _():
        for c in range(n):
            start(token_copies(c))

    if not last:
        pl.when(e >= 2)(lambda: wait(out_copies(e - 2, slot)))
    start(in_copies())
    if not g:
        for acc in accs:
            acc[slot] = jnp.zeros(acc.shape[1:], f32)

    row_iota = iota((WIN, BLK), FIRST).astype(f32)
    head_row = iota((ALIGN, d_model), FIRST)
    both = tuple(HALVES)

    def dispatch(i, rows_at):
        for c, (first, _) in enumerate(offsets(pieces)):
            pl.when((e == FIRST) & (i == first))(lambda: wait(token_copies(c)))
        tok = span(i * BLK, BLK)
        infos = [blocks.info(i, e + q) for q in both]
        places = [aligned(r) for r in rows_at]
        flat = infos[FIRST][FIRST]

        def picks(q, k):
            pos = tab_ref[flat, pl.ds(local + e + q, 1), :]
            gate = tab_ref[flat, pl.ds(e + q, 1), :]
            pick = (pos + (places[q][1] - infos[q][1] - k * WIN).astype(f32)) == row_iota
            return one_hot(pick), lane_sum(where0(pick, gate + jnp.zeros_like(row_iota)))

        def rows_for(one, gate_row):
            return dot(one, xv[tok, :]).astype(bf16), (dot(one, dv[tok, :]) * gate_row).astype(bf16)

        pair = [picks(q, i32(FIRST)) for q in both]
        new = rows_for(*[jnp.concatenate(v, axis=FIRST) for v in zip(*pair)])
        for q in both:
            base, shift = places[q]
            head = span(base, ALIGN)
            for value, rows in zip(new, (xr, dr)):
                value = value[q * WIN : (q + 1) * WIN]
                rows[q, head, :] = jnp.where(head_row < shift, rows[q, head, :], value[:ALIGN])
                rows[q, span(base + ALIGN, WIN - ALIGN, ALIGN), :] = value[ALIGN:]

            def more(k):
                for value, rows in zip(rows_for(*picks(q, k)), (xr, dr)):
                    rows[q, span(base + k * WIN, WIN, ALIGN), :] = value

            loop(1, window_count(shift, infos[q][LAST]), more)
        return tuple(r + info[LAST] for r, info in zip(rows_at, infos))

    @pl.when(slot == FIRST)
    def _():
        totals = lax.fori_loop(FIRST, count, dispatch, (i32(FIRST),) * len(both))
        for q in both:

            def clear(i):
                for rows in (xr, dr):
                    rows[q, span(i * ALIGN, ALIGN), :] = jnp.zeros((ALIGN, d_model), bf16)

            loop((totals[q] + ALIGN - 1) // ALIGN, padded(totals[q]) // ALIGN, clear)

    wait(in_copies())

    def tile(at, size):
        rows = span(at, size)
        xt = xr[slot, rows, :]
        dt = dr[slot, rows, :]
        act_a = dot(xt, w1_ref[FIRST])
        act_b = dot(xt, w3_ref[FIRST])
        d_hidden = dot_nt(dt, w2_ref[FIRST]).astype(bf16).astype(f32)
        sig = 1.0 / (1.0 + jnp.exp(-act_a))
        silu = act_a * sig
        hidden = (silu * act_b).astype(bf16)
        d_a = (d_hidden * act_b * sig * (1.0 + act_a * (1.0 - sig))).astype(bf16)
        d_b = (d_hidden * silu).astype(bf16)
        copies = []
        for k, (value, out) in enumerate(zip((hidden, d_a, d_b), row_outs)):
            stage[k, :size] = value
            copies.append(pltpu.make_async_copy(stage.at[k, :size], out.at[g, e, rows], row_sem.at[k]))
        start(copies)
        acc13[slot, :, :d_ff] += dot_tn(xt, d_a)
        acc13[slot, :, d_ff:] += dot_tn(xt, d_b)
        acc2[slot] += dot_tn(hidden, dt)
        wait(copies)

    row_tiles(blocks.total(FIRST, count, e), tile, 2 * TILE)

    if last:
        for out, value in zip(outs, (acc13[slot, :, :d_ff], acc13[slot, :, d_ff:], acc2[slot])):
            out[FIRST] = value.astype(bf16)
    else:
        start(out_copies(e, slot))

        @pl.when(e == pl.num_programs(FIRST) - 1)
        def _():
            wait(out_copies(e - 1, 1 - slot))
            wait(out_copies(e, slot))


def per_expert(*shape):
    return pl.BlockSpec((1, *shape), lambda e: (e,) + (FIRST,) * len(shape))


def block_map(pieces, nb):
    return np.asarray([src * nb + first + b for src, first, count in pieces for b in range(count)], np.int32)


def run_grad(starts, tab, g, xs, ds, weights, acc, rows, nb, row_cap):
    pieces = GROUPS[g]
    last = g == len(GROUPS) - 1
    local, d_model, d_ff = weights[FIRST].shape
    count = len(block_map(pieces, nb)) * BLK
    w_specs = [per_expert(*w.shape[1:]) for w in weights]
    sums = [(local, d_model, 2 * d_ff), (local, d_ff, d_model)]
    row_shape = [Shape((len(GROUPS), local, row_cap, d_ff), bf16)] * 3
    out_shape = row_shape + ([Shape(w.shape, bf16) for w in weights] if last else [Shape(s, f32) for s in sums])
    out_specs = [ANY] * 3 + (w_specs if last else [ANY] * 2)
    tokens = pltpu.VMEM((count, d_model), bf16)
    packed = pltpu.VMEM((2, row_cap + WIN, d_model), bf16)
    ins = [starts, block_map(pieces, nb), tab, *xs, *ds, *weights, *acc, *rows]
    out = pl.pallas_call(
        functools.partial(grad_kernel, g, last, nb, local, pieces),
        grid=(local,),
        in_specs=[SMEM, SMEM, VMEM] + [ANY] * (2 * len(pieces)) + w_specs + [ANY] * (len(acc) + len(rows)),
        out_specs=out_specs,
        out_shape=out_shape,
        scratch_shapes=[tokens, tokens, packed, packed]
        + [pltpu.VMEM((2, *s[1:]), f32) for s in sums]
        + [pltpu.VMEM((3, 2 * TILE, d_ff), bf16), DMA((2, len(pieces))), DMA((2,)), DMA((2, 2)), DMA((3,))],
        input_output_aliases={len(ins) - len(rows) + k: k for k in range(len(rows))},
        compiler_params=params(),
        cost_estimate=cost(12 * count * d_model * d_ff, 40 << 20),
        name="expert_grad",
    )(*ins)
    return out[:3], out[3:]


def group_spans(nb):
    counts = [len(block_map(pieces, nb)) for pieces in GROUPS]
    return np.asarray([v for k, c in enumerate(counts) for v in (sum(counts[:k]), c)], np.int32)


def per_group(*shape):
    return pl.BlockSpec((1, 1, *shape), lambda g, e: (g, e) + (FIRST,) * len(shape))


def per_local(*shape):
    return pl.BlockSpec((1, *shape), lambda g, e: (e,) + (FIRST,) * len(shape))


class Combine:
    def __init__(self, nb, local, starts_ref, bmap_ref, spans_ref, tab_ref, rows_ref, out_ref, ring, sems):
        step = pl.program_id(FIRST)
        self.e = pl.program_id(1)
        self.blocks = Blocks(starts_ref, bmap_ref, nb)
        self.first, self.count = spans_ref[2 * step], spans_ref[2 * step + 1]
        self.total = self.blocks.total(self.first, self.count, self.e)
        self.nb, self.local, self.tab_ref, self.rows_ref = nb, local, tab_ref, rows_ref
        self.out_ref, self.ring, self.sems = out_ref, ring, sems
        self.lane = iota((BLK, WIN), 1).astype(f32)

    def zero_tail(self):
        rows = span(padded(self.total), WIN)
        self.rows_ref[self.e, rows, :] = jnp.zeros((WIN, self.rows_ref.shape[LAST]), bf16)

    def pick(self, ee, k):
        place, info = self.places[ee], self.infos[ee]
        pos = self.tab_t[:, self.local + ee : self.local + ee + 1]
        return one_hot((pos + (place[1] - info[1] - k * WIN).astype(f32)) == self.lane)

    def held(self, ee, k, cols=slice(None)):
        return self.rows_ref[ee, span(self.places[ee][FIRST] + k * WIN, WIN, ALIGN), cols]

    def out_copy(self, i):
        flat = self.blocks.bmap[i]
        slot = i % RING
        return pltpu.make_async_copy(self.ring.at[slot], self.out_ref.at[flat // self.nb, span((flat % self.nb) * BLK, BLK)], self.sems.at[slot])

    def run(self, simple_body, full_body):
        def block(i, rows_at):
            ee = range(self.local)
            self.infos = [self.blocks.info(i, k) for k in ee]
            self.places = [aligned(r) for r in rows_at]
            self.windows = [window_count(self.places[k][1], self.infos[k][LAST]) for k in ee]
            self.flat = self.infos[FIRST][FIRST]
            self.tab_t = jnp.transpose(self.tab_ref[self.flat])
            self.tok = span((i - self.first) * BLK, BLK)
            pl.when(i - self.first >= RING)(lambda: self.out_copy(i - RING).wait())
            simple = functools.reduce(jnp.logical_and, [w <= 1 for w in self.windows])
            out = self.ring.at[i % RING]
            pl.when(simple)(lambda: simple_body(out))
            pl.when(jnp.logical_not(simple))(lambda: full_body(out))
            self.out_copy(i).start()
            return tuple(r + info[LAST] for r, info in zip(rows_at, self.infos))

        stop = self.first + self.count
        lax.fori_loop(self.first, stop, block, (i32(FIRST),) * self.local)
        loop(stop - RING, stop, lambda i: self.out_copy(i).wait())


def y_kernel(nb, local, starts_ref, bmap_ref, spans_ref, tab_ref, h_ref, w2_ref, *refs):
    take = taker(refs)
    d_refs = [take(len(pieces)) for pieces in GROUPS]
    y_ref, dg_ref, o_rows, dv, ring, zacc, yacc, dgacc, tok_sem, out_sem = take()
    all_rows = Combine(nb, local, starts_ref, bmap_ref, spans_ref, tab_ref, o_rows, y_ref, ring, out_sem)
    e = all_rows.e
    d_model = dv.shape[1]

    def token_copies(step):
        spots = offsets(GROUPS[step])
        return [pltpu.make_async_copy(src, dv.at[block_rows(*spot)], tok_sem.at[c]) for c, (src, spot) in enumerate(zip(d_refs[step], spots))]

    for step in range(len(GROUPS)):
        pl.when((pl.program_id(FIRST) == step) & (e == FIRST))(lambda: start(token_copies(step)))

    def tile(at, size):
        rows = span(at, size)
        o_rows[e, rows, :] = dot(h_ref[FIRST, FIRST, rows, :], w2_ref[FIRST]).astype(bf16)

    row_tiles(all_rows.total, tile, 2 * TILE)
    all_rows.zero_tail()

    @pl.when(e == local - 1)
    def _():
        for step in range(len(GROUPS)):
            pl.when(pl.program_id(FIRST) == step)(lambda: wait(token_copies(step)))
        dg_lane = iota((BLK, LANES), 1)
        width = 2 * LANES
        columns = [slice(k * width, (k + 1) * width) for k in range(d_model // width)]

        def gate(ee):
            return all_rows.tab_t[:, ee : ee + 1]

        def put_dg(sums):
            dg = sum(where0(dg_lane == ee, lane_sum(s) + jnp.zeros((BLK, LANES), f32)) for ee, s in enumerate(sums))
            dg_ref[all_rows.flat] = jnp.transpose(dg)[: 2 * local, :]

        def simple(out):
            picks = [all_rows.pick(ee, i32(FIRST)) for ee in range(local)]
            sums = [None] * local
            for cols in columns:
                dy = dv[all_rows.tok, cols].astype(f32)
                y = None
                for ee in range(local):
                    z = dot(picks[ee], all_rows.held(ee, i32(FIRST), cols))
                    prod = dy * z
                    part = prod[:, :LANES] + prod[:, LANES:]
                    sums[ee] = part if sums[ee] is None else sums[ee] + part
                    y = gate(ee) * z if y is None else y + gate(ee) * z
                out[:, cols] = y.astype(bf16)
            put_dg(sums)

        def full(out):
            yacc[...] = jnp.zeros_like(yacc)
            for ee in range(local):
                zacc[...] = jnp.zeros_like(zacc)

                def more(k):
                    zacc[...] += dot(all_rows.pick(ee, k), all_rows.held(ee, k))

                loop(FIRST, all_rows.windows[ee], more)
                yacc[...] += gate(ee) * zacc[...]
                dgacc[ee] = lane_sum(dv[all_rows.tok, :].astype(f32) * zacc[...]) * jnp.where(dg_lane == FIRST, 1.0, 0.0)
            out[...] = yacc[...].astype(bf16)
            put_dg([dgacc[ee] for ee in range(local)])

        all_rows.run(simple, full)


def combine_scratch(local, row_cap, d_model):
    return [pltpu.VMEM((local, row_cap + WIN, d_model), bf16)], [pltpu.VMEM((RING, BLK, d_model), bf16), pltpu.VMEM((BLK, d_model), f32)]


def all_pieces():
    return [p for pieces in GROUPS for p in pieces]


def run_y(starts, tab, h_rows, w2, ds, nb):
    local, d_ff, d_model = w2.shape
    row_cap = h_rows.shape[2]
    pieces = all_pieces()
    most = max(group_spans(nb)[1::2]) * BLK
    rows, work = combine_scratch(local, row_cap, d_model)
    return pl.pallas_call(
        functools.partial(y_kernel, nb, local),
        grid=(len(GROUPS), local),
        in_specs=[SMEM, SMEM, SMEM, VMEM, per_group(row_cap, d_ff), per_local(d_ff, d_model)] + [ANY] * len(pieces),
        out_specs=[ANY, VMEM],
        out_shape=[Shape((len(SOURCES), nb * BLK, d_model), bf16), Shape((tab.shape[FIRST], 2 * local, BLK), f32)],
        scratch_shapes=rows + [pltpu.VMEM((most, d_model), bf16)] + work + [work[LAST], pltpu.VMEM((local, BLK, LANES), f32), DMA((4,)), DMA((RING,))],
        compiler_params=grid_params(2),
        cost_estimate=cost(16 * nb * BLK * d_model * d_ff, 80 << 20),
        name="expert_y",
    )(starts, block_map(pieces, nb), group_spans(nb), tab, h_rows, w2, *[ds[p] for p in pieces])


def dx_kernel(nb, local, starts_ref, bmap_ref, spans_ref, tab_ref, da_ref, db_ref, w1_ref, w3_ref, dx_ref, o_rows, ring, zacc, out_sem):
    all_rows = Combine(nb, local, starts_ref, bmap_ref, spans_ref, tab_ref, o_rows, dx_ref, ring, out_sem)
    e = all_rows.e

    def tile(at, size):
        rows = span(at, size)
        grad = dot_nt(da_ref[FIRST, FIRST, rows, :], w1_ref[FIRST]) + dot_nt(db_ref[FIRST, FIRST, rows, :], w3_ref[FIRST])
        o_rows[e, rows, :] = grad.astype(bf16)

    row_tiles(all_rows.total, tile, 2 * TILE)
    all_rows.zero_tail()

    @pl.when(e == local - 1)
    def _():
        def simple(out):
            pairs = [(ee, ee + 1) for ee in range(FIRST, local, 2)]
            zero = i32(FIRST)
            sums = [
                dot(jnp.concatenate([all_rows.pick(ee, zero) for ee in pair], axis=1), jnp.concatenate([all_rows.held(ee, zero) for ee in pair], axis=FIRST))
                for pair in pairs
            ]
            out[...] = sum(sums[1:], sums[FIRST]).astype(bf16)

        def full(out):
            zacc[...] = jnp.zeros_like(zacc)
            for ee in range(local):

                def more(k):
                    zacc[...] += dot(all_rows.pick(ee, k), all_rows.held(ee, k))

                loop(FIRST, all_rows.windows[ee], more)
            out[...] = zacc[...].astype(bf16)

        all_rows.run(simple, full)


def run_dx(starts, tab, da_rows, db_rows, w1, w3, nb):
    local, d_model, d_ff = w1.shape
    row_cap = da_rows.shape[2]
    rows, work = combine_scratch(local, row_cap, d_model)
    return pl.pallas_call(
        functools.partial(dx_kernel, nb, local),
        grid=(len(GROUPS), local),
        in_specs=[SMEM, SMEM, SMEM, VMEM] + [per_group(row_cap, d_ff)] * 2 + [per_local(d_model, d_ff)] * 2,
        out_specs=ANY,
        out_shape=Shape((len(SOURCES), nb * BLK, d_model), bf16),
        scratch_shapes=rows + work + [DMA((RING,))],
        compiler_params=grid_params(2),
        cost_estimate=cost(32 * nb * BLK * d_model * d_ff, 80 << 20),
        name="expert_dx",
    )(starts, block_map(all_pieces(), nb), group_spans(nb), tab, da_rows, db_rows, w1, w3)


def router_grad_kernel(scale, x_ref, prob_ref, dg_ref, ids_ref, load_ref, dlog_ref, dw_ref):
    step = pl.program_id(FIRST)
    prob = prob_ref[...]
    dg = dg_ref[...]
    chosen = chosen_mask(ids_ref[...], prob.shape[FIRST])
    gate_sum = row_sum(where0(chosen, prob))
    gate = where0(chosen, prob / gate_sum)
    d_pick = (dg - row_sum(gate * dg)) / gate_sum
    d_prob = where0(chosen, d_pick) + scale * load_ref[:, :1]
    d_logit = prob * (d_prob - row_sum(prob * d_prob))
    dlog_ref[...] = d_logit
    hi, mid, low = [dot(part, x_ref[...]) for part in split3(d_logit)]

    @pl.when(step == FIRST)
    def _():
        dw_ref[...] = jnp.zeros_like(dw_ref)

    dw_ref[...] += hi + (mid + low)


def run_router_grad(x_loc, prob_t, dg_t, ids_t, load, scale):
    tokens, d_model = x_loc.shape
    experts = prob_t.shape[FIRST]
    lanes = lambda n: pl.BlockSpec((n, BLK), lambda i: (FIRST, i))
    return pl.pallas_call(
        functools.partial(router_grad_kernel, scale),
        grid=(tokens // BLK,),
        in_specs=[pl.BlockSpec((BLK, d_model), lambda i: (i, FIRST)), lanes(experts), lanes(experts), lanes(ids_t.shape[FIRST]), VMEM],
        out_specs=[lanes(experts), VMEM],
        out_shape=[Shape((experts, tokens), f32), Shape((experts, d_model), f32)],
        compiler_params=params(),
        cost_estimate=cost(2 * tokens * d_model * BLK, 2 * tokens * d_model),
        name="router_grad",
    )(x_loc, prob_t, dg_t, ids_t, load)


def final_kernel(dlog_ref, wt_ref, *refs):
    take = taker(refs)
    y_terms, dx_terms = [[ref[...].astype(f32) for ref in take(3)] for _ in TENSORS]
    y_ref, dx_ref = take()
    lhs = split3(dlog_ref[...])
    rhs = split3(wt_ref[...])
    terms = [(i, j) for i in range(3) for j in range(3 - i)]
    left = jnp.concatenate([lhs[i] for i, _ in terms], axis=FIRST)
    right = jnp.concatenate([rhs[j] for _, j in terms], axis=FIRST)
    dx_ref[...] = (dot_tn(left, right) + sum(dx_terms[1:], dx_terms[FIRST])).astype(bf16)
    y_ref[...] = sum(y_terms[1:], y_terms[FIRST]).astype(bf16)


def run_final(dlog_t, w_t, y_terms, dx_terms):
    experts, tokens = dlog_t.shape
    d_model = w_t.shape[1]
    size = tokens // 4
    rows = pl.BlockSpec((size, d_model), lambda i: (i, FIRST))
    return pl.pallas_call(
        final_kernel,
        grid=(tokens // size,),
        in_specs=[pl.BlockSpec((experts, size), lambda i: (FIRST, i)), VMEM] + [rows] * len([*y_terms, *dx_terms]),
        out_specs=[rows] * 2,
        out_shape=[Shape((tokens, d_model), bf16)] * 2,
        compiler_params=params(),
        cost_estimate=cost(2 * tokens * d_model * BLK, 16 * tokens * d_model),
        name="final",
    )(dlog_t, w_t, *y_terms, *dx_terms)


NEAR = (X, Y)
RELAYED = {(Y, 0): 0, (X, 1): 1}
OPS = [
    (t, src, h)
    for step in ([(FAR, 0), (FAR, 1)], [(X, 0), (Y, 1)], [(X, 1), (Y, 0)], [(FIRST, 0), (FIRST, 1)])
    for t in TENSORS
    for src, h in step
]


def add_rows(dst, src):
    def body(i):
        rows = span(i * LANES, LANES)
        dst[rows, :] = (dst[rows, :].astype(f32) + src[rows, :].astype(f32)).astype(bf16)

    loop(FIRST, dst.shape[FIRST] // LANES, body)


def exchange_kernel(half, mats, *refs):
    take = taker(refs)
    parts = take(len(TENSORS))
    dws = take(mats)
    outs = [take(len(NEAR) + 1) for _ in TENSORS]
    dw_outs = take(mats)
    land, far_land, stage, z_one, z_two, z_stage = take(6)
    core_sem, stage_sem, far_sem, near_sem, own_sem, z_sem, keep_sem, load_sem, credit_one, credit_two = take()

    me = lax.axis_index("ep")
    z = lax.axis_index("dp")
    peer = {bit: me + bit - 2 * bit * ((me // bit) % 2) for bit in (CORE, X, Y)}
    z_peer = z + 1 - 2 * (z % 2)
    z_cross = 3 - z
    is_end = (z % 3) == FIRST
    is_mid = (z % 3) != FIRST

    barrier = pltpu.get_barrier_semaphore()
    ids = [{"ep": p} for p in peer.values()] + [{"dp": z_peer}, {"dp": z_cross}]
    for device in ids:
        pl.semaphore_signal(barrier, device_id=device, device_id_type=MESH)
    pl.semaphore_wait(barrier, len(ids))

    def remote(src, dst, sems, at, device):
        send, recv = sems.at[(SEND, *at)], sems.at[(RECV, *at)]
        return pltpu.make_async_remote_copy(src_ref=src, dst_ref=dst, send_sem=send, recv_sem=recv, device_id=device, device_id_type=MESH)

    def rows_at(h):
        return pl.ds(h * half, half)

    def core_copy(i):
        t, src, h = OPS[i]
        return remote(parts[t].at[src | CORE, rows_at(h)], land.at[i], core_sem, (i,), {"ep": peer[CORE]})

    def stage_copy(i):
        t, src, h = OPS[i]
        return pltpu.make_async_copy(parts[t].at[src, rows_at(h)], stage.at[i % STAGES], stage_sem.at[i % STAGES])

    def far_copy(i):
        t, _, h = OPS[i]
        return remote(land.at[i], far_land.at[t, h], far_sem, (t, h), {"ep": peer[NEAR[h]]})

    def near_copy(i):
        t, src, h = OPS[i]
        k = NEAR.index(src)
        return remote(land.at[i], outs[t][k].at[rows_at(h)], near_sem, (t, k, h), {"ep": peer[src]})

    def own_copy(i):
        t, _, h = OPS[i]
        return pltpu.make_async_copy(land.at[i], outs[t][LAST].at[rows_at(h)], own_sem.at[t, h])

    def out_copy(i):
        src = OPS[i][1]
        return (far_copy if src == FAR else near_copy if src else own_copy)(i)

    def reduce_op(i):
        t, src, h = OPS[i]
        stage_copy(i).wait()
        core_copy(i).wait_recv()
        add_rows(land.at[i], stage.at[i % STAGES])
        if i + STAGES < len(OPS):
            stage_copy(i + STAGES).start()
        if (src, h) in RELAYED:
            far_copy(OPS.index((t, FAR, RELAYED[src, h]))).wait_recv()
            add_rows(land.at[i], far_land.at[t, RELAYED[src, h]])

    rows_per = z_one.shape[1]
    chunks = [(m, e, k) for e in range(dws[FIRST].shape[FIRST]) for m in range(mats) for k in HALVES]
    n = len(chunks)

    def piece(arrays, c):
        m, e, k = chunks[c]
        return arrays[m].at[e, pl.ds(k * rows_per, rows_per)]

    def one_copy(c):
        return remote(piece(dws, c), z_one.at[c % SLOTS], z_sem, (FIRST, c), {"dp": z_peer})

    def two_copy(c):
        return remote(z_one.at[c % SLOTS], z_two.at[c % SLOTS], z_sem, (1, c), {"dp": z_cross})

    def three_copy(c):
        return remote(z_two.at[c % SLOTS], piece(dw_outs, c), z_sem, (2, c), {"dp": z_peer})

    def keep_copy(c):
        return pltpu.make_async_copy(z_two.at[c % SLOTS], piece(dw_outs, c), keep_sem.at[c])

    def load_copy(c):
        return pltpu.make_async_copy(piece(dws, c), z_stage.at[c % STAGES], load_sem.at[c % STAGES])

    def first_add(c):
        load_copy(c).wait()
        one_copy(c).wait_recv()
        add_rows(z_one.at[c % SLOTS], z_stage.at[c % STAGES])
        if c + STAGES < n:
            load_copy(c + STAGES).start()

    def second_add(c):
        two_copy(c).wait()
        add_rows(z_two.at[c % SLOTS], z_one.at[c % SLOTS])
        if c + SLOTS < n:
            pl.semaphore_signal(credit_one, device_id={"dp": z_peer}, device_id_type=MESH)

    def retire(c):
        three_copy(c).wait_send()
        keep_copy(c).wait()
        if c + SLOTS < n:
            pl.semaphore_signal(credit_two, device_id={"dp": z_cross}, device_id_type=MESH)

    @pl.when(is_end)
    def _():
        for c in range(SLOTS):
            one_copy(c).start()

    @pl.when(is_mid)
    def _():
        for c in range(STAGES):
            load_copy(c).start()

    for i in range(len(OPS)):
        core_copy(i).start()
        if i < STAGES:
            stage_copy(i).start()

    todo = list(range(len(OPS)))
    for tick in range(n + LAG):
        mine = todo[: 2 if tick < 2 else 1]
        todo = todo[len(mine) :]
        for i in mine:
            reduce_op(i)

        @pl.when(is_mid)
        def _():
            back = tick - 1
            if tick < n:
                first_add(tick)
            if back in range(n):
                second_add(back)
            if tick < n:
                if tick >= SLOTS:
                    pl.semaphore_wait(credit_two, 1)
                two_copy(tick).start()
            if back in range(n):
                three_copy(back).start()
                keep_copy(back).start()
            if tick >= LAG:
                retire(tick - LAG)

        for i in mine:
            out_copy(i).start()

        @pl.when(is_end)
        def _():
            if tick + SLOTS < n:
                pl.semaphore_wait(credit_one, 1)
                one_copy(tick + SLOTS).start()

    for i in todo:
        reduce_op(i)
        out_copy(i).start()

    @pl.when(is_end)
    def _():
        for c in range(n):
            one_copy(c).wait_send()
            three_copy(c).wait_recv()

    for i in range(len(OPS)):
        core_copy(i).wait_send()
        (out_copy(i).wait_send if OPS[i][1] == FAR else out_copy(i).wait)()


def run_exchange(parts, dws):
    tokens, d_model = parts[FIRST].shape[1:]
    half = tokens // 2
    local, rows, cols = dws[FIRST].shape
    chunk = (rows // 2, cols)
    n = local * len(dws) * len(HALVES)
    whole = Shape((tokens, d_model), bf16)
    flat = list(parts) + list(dws)
    terms = len(NEAR) + 1
    out = pl.pallas_call(
        functools.partial(exchange_kernel, half, len(dws)),
        in_specs=[ANY] * len(flat),
        out_specs=[ANY] * (terms * len(TENSORS) + len(dws)),
        out_shape=[whole] * (terms * len(TENSORS)) + [Shape(v.shape, bf16) for v in dws],
        scratch_shapes=[
            pltpu.VMEM((len(OPS), half, d_model), bf16),
            pltpu.VMEM((len(TENSORS), len(HALVES), half, d_model), bf16),
            pltpu.VMEM((STAGES, half, d_model), bf16),
            pltpu.VMEM((SLOTS, *chunk), bf16),
            pltpu.VMEM((SLOTS, *chunk), bf16),
            pltpu.VMEM((STAGES, *chunk), bf16),
            DMA((2, len(OPS))),
            DMA((STAGES,)),
            DMA((2, 2, 2)),
            DMA((2, 2, 2, 2)),
            DMA((2, 2)),
            DMA((2, 3, n)),
            DMA((n,)),
            DMA((STAGES,)),
            pltpu.SemaphoreType.REGULAR,
            pltpu.SemaphoreType.REGULAR,
        ],
        compiler_params=pltpu.CompilerParams(vmem_limit_bytes=VMEM_LIMIT, collective_id=FIRST, has_side_effects=True),
        cost_estimate=cost(1 << 37, 200 << 20),
        name="exchange",
    )(*flat)
    return [out[:terms], out[terms : 2 * terms]], out[2 * terms :]


def hop(v, bit):
    return lax.ppermute(v, "ep", [(i, i ^ bit) for i in SOURCES])


def after(values, token):
    return lax.optimization_barrier((values, token))[FIRST]


def send_own(v):
    got = {(FIRST, *WHOLE): v, (CORE, *WHOLE): hop(v, CORE)}
    for part in PARTS:
        piece = v[part[FIRST] * BLK : sum(part) * BLK]
        for bit in NEAR:
            got[bit, *part] = hop(piece, bit)
    return got


def pass_on(got, h):
    part = PARTS[h]
    got[FAR, *part] = hop(got[(Y, X)[h], *part], NEAR[h])
    for bit in NEAR:
        got[bit | CORE, *part] = hop(got[bit, *part], CORE)


def relative(v, me):
    shape = v.shape
    v = v.reshape((2, 2, 2) + shape[1:])
    for axis, bit in enumerate((Y, X, CORE)):
        v = jnp.where((me & bit) != FIRST, jnp.flip(v, axis), v)
    return v.reshape(shape)


def solution(mesh):
    dp_size = mesh.shape["dp"]
    ep_size = mesh.shape["ep"]
    row_spec = P(("dp", "ep"), None)
    expert_spec = P("ep", None, None)
    whole_spec = P(None, None)

    def per_device(x_loc, w_router, ids_loc, w1, w3, w2, dy_loc):
        tokens, d_model = x_loc.shape
        top_k = ids_loc.shape[1]
        experts = w_router.shape[1]
        local = w1.shape[FIRST]
        capacity = capacity_of(tokens, top_k, experts)
        n_total = tokens * dp_size * ep_size
        nb = tokens // BLK
        row_cap = padded(4 * capacity)
        me = lax.axis_index("ep")

        gathered = [send_own(v) for v in (x_loc, dy_loc)]

        ids_t = ids_loc.T
        send_tab, prob_t = run_router(x_loc, w_router, ids_t, capacity, local, ep_size)
        tab_rel = relative(lax.all_to_all(send_tab, "ep", FIRST, FIRST, tiled=True), me)
        tab = tab_rel[:, :, :tokens].reshape(ep_size, 2 * local, nb, BLK).transpose(0, 2, 1, 3).reshape(ep_size * nb, 2 * local, BLK)
        starts = tab_rel[:, local:, tokens : tokens + ALIGN].astype(i32).reshape(LAST)

        acc = rows = ()
        for g, group in enumerate(GROUPS):
            if g:
                ready = [p for p in group if not p[FIRST] & CORE]
                for got in gathered:
                    got.update(after({p: got[p] for p in ready}, acc[LAST]))
                for got in gathered:
                    if g < len(GROUPS) - 1:
                        pass_on(got, g - 1)
                    else:
                        for src, *part in ready:
                            got[src | CORE, *part] = hop(got[src, *part], CORE)
            rows, acc = run_grad(starts, tab, g, *[[got[p] for p in group] for got in gathered], (w1, w3, w2), acc, rows, nb, row_cap)
            if not g:
                stats = jnp.sum(after(tab_rel[:, :local, tokens:], acc[LAST]), axis=FIRST)
                for step in (1, 2):
                    stats = stats + lax.ppermute(stats, "dp", [(i, i ^ step) for i in range(dp_size)])
                starts = after(starts, stats)
        dw1, dw3, dw2 = acc
        starts, dw2 = lax.optimization_barrier((starts, dw2))
        dw2_sum = lax.psum(dw2, "dp")

        y_part, dg = run_y(starts, tab, rows[FIRST], w2, gathered[1], nb)
        dg = dg[:, :local].reshape(ep_size, nb, local, BLK).transpose(0, 2, 1, 3).reshape(ep_size, local, tokens)
        dg = jnp.concatenate([relative(dg, me), jnp.broadcast_to(stats, (ep_size, *stats.shape))], axis=2)
        starts, dg = lax.optimization_barrier((starts, dg))
        dx_part = run_dx(starts, tab, rows[1], rows[2], w1, w3, nb)
        dg_all = lax.all_to_all(dg, "ep", FIRST, FIRST, tiled=True).reshape(experts, tokens + LANES)
        load = dg_all[:, tokens:]
        share = AUX_COEF * experts / (n_total * top_k * n_total)
        aux_loss = share * jnp.sum(load[:, FIRST] * load[:, 1])
        dlog_t, dwr_t = run_router_grad(x_loc, prob_t, dg_all[:, :tokens], ids_t, load, share)
        dw_router = lax.psum(after(dwr_t, dw2_sum), ("dp", "ep")).T

        sums, grads = run_exchange([y_part, dx_part], [dw1, dw3])
        y_loc, dx_loc = run_final(dlog_t, w_router.T, *sums)
        return y_loc, aux_loss, dx_loc, dw_router, *grads, dw2_sum

    return jax.shard_map(
        per_device,
        mesh=mesh,
        in_specs=(row_spec, whole_spec, row_spec, expert_spec, expert_spec, expert_spec, row_spec),
        out_specs=(row_spec, P(), row_spec, whole_spec, expert_spec, expert_spec, expert_spec),
        check_vma=False,
    )
```

```python
import functools

import jax
import jax.numpy as jnp
import numpy as np
from jax import lax
from jax.experimental import pallas as pl
from jax.experimental.pallas import tpu as pltpu
from jax.sharding import PartitionSpec as P

AUX_COEF = 0.01
BLK = 256
TILE = 256
WIN = 128
LANES = 128
ALIGN = 16
NOT_KEPT = -65536.0
VMEM_LIMIT = 63 * 1024 * 1024
CORE, X, Y = 1, 2, 4
FAR = X | Y
HALVES = TENSORS = range(2)
RING = 4
SOURCES = range(8)
FIRST, LAST = 0, -1
SEND, RECV = 0, 1
STAGES = 3
SLOTS = 8
LAG = 3
MESH = pl.DeviceIdType.MESH

WHOLE, PARTS = (0, 6), ((0, 3), (3, 3))
GROUPS = (
    [(src, *WHOLE) for src in (FIRST, CORE)],
    [(bit | core, *PARTS[FIRST]) for bit in (X, Y) for core in (FIRST, CORE)],
    [(bit | core, *PARTS[1]) for bit in (X, Y) for core in (FIRST, CORE)],
    [(FAR | core, *part) for part in PARTS for core in (FIRST, CORE)],
)


f32 = jnp.float32
bf16 = jnp.bfloat16
i32 = jnp.int32
ANY = pl.BlockSpec(memory_space=pl.ANY)
SMEM = pl.BlockSpec(memory_space=pltpu.SMEM)
VMEM = pl.BlockSpec(memory_space=pltpu.VMEM)
DMA = pltpu.SemaphoreType.DMA
Shape = jax.ShapeDtypeStruct


def capacity_of(tokens, top_k, experts):
    return (5 * top_k * tokens + 4 * experts - 1) // (4 * experts)


def dot(a, b, ca=1, cb=0):
    return lax.dot_general(a, b, (((ca,), (cb,)), ((), ())), preferred_element_type=f32)


def dot_nt(a, b):
    return dot(a, b, 1, 1)


def dot_tn(a, b):
    return dot(a, b, 0, 0)


def grid_params(dims):
    return pltpu.CompilerParams(dimension_semantics=("arbitrary",) * dims, vmem_limit_bytes=VMEM_LIMIT)


def params():
    return grid_params(1)


def cost(flops, moved):
    return pl.CostEstimate(flops=flops, bytes_accessed=moved, transcendentals=FIRST)


def iota(shape, dim):
    return lax.broadcasted_iota(i32, shape, dim)


def span(start, size, multiple=None):
    return pl.ds(pl.multiple_of(start, multiple or size), size)


def lane_sum(v):
    return jnp.sum(v, axis=1, keepdims=True)


def row_sum(v):
    return jnp.sum(v, axis=0, keepdims=True)


def where0(mask, v):
    return jnp.where(mask, v, jnp.zeros_like(v))


def one_hot(mask):
    return jnp.where(mask, 1.0, 0.0).astype(bf16)


def split3(v):
    hi = v.astype(bf16)
    rest = v - hi.astype(f32)
    mid = rest.astype(bf16)
    return hi, mid, (rest - mid.astype(f32)).astype(bf16)


def loop(start, stop, body):
    def step(i, carry):
        body(i)
        return carry

    lax.fori_loop(start, stop, step, FIRST)


def chosen_mask(ids, experts):
    rows = iota((experts, ids.shape[1]), FIRST)
    return functools.reduce(jnp.logical_or, [rows == ids[j : j + 1, :] for j in range(ids.shape[FIRST])])


def router_kernel(capacity, local, x_ref, w_ref, ids_ref, tab_ref, prob_ref, carry):
    step = pl.program_id(FIRST)
    steps = pl.num_programs(FIRST)
    experts = w_ref.shape[1]

    @pl.when(step == FIRST)
    def _():
        carry[...] = jnp.zeros_like(carry)
        tab_ref[...] = jnp.zeros_like(tab_ref)

    x = x_ref[...]
    hi, mid, low = [dot(x, part) for part in split3(w_ref[...])]
    logits = jnp.transpose(hi + (mid + low))
    expo = jnp.exp(logits - jnp.max(logits, axis=FIRST, keepdims=True))
    prob = expo / row_sum(expo)
    chosen = chosen_mask(ids_ref[...], experts)
    hits = jnp.where(chosen, 1.0, 0.0)
    gate = where0(chosen, prob / row_sum(where0(chosen, prob)))
    earlier = one_hot(iota((BLK, BLK), FIRST) < iota((BLK, BLK), 1))
    before = carry[:, :1]
    pos = dot(hits.astype(bf16), earlier) + before
    pos = jnp.where(chosen & (pos < capacity), pos, NOT_KEPT)
    prob_ref[...] = prob
    after = before + lane_sum(hits)
    lane = iota((experts, LANES), 1)
    first = where0(lane == step, jnp.minimum(before, capacity) + jnp.zeros((experts, LANES), f32))
    first = first + where0((lane == step + 1) & (step == steps - 1), jnp.minimum(after, capacity) + jnp.zeros((experts, LANES), f32))
    stat = where0(lane == FIRST, lane_sum(hits) + jnp.zeros((experts, LANES), f32))
    stat = stat + where0(lane == 1, lane_sum(prob) + jnp.zeros((experts, LANES), f32))
    tail = slice(tab_ref.shape[LAST] - LANES, None)
    for d in range(experts // local):
        rows = slice(d * local, (d + 1) * local)
        tab_ref[d, :local, span(step * BLK, BLK)] = gate[rows]
        tab_ref[d, local:, span(step * BLK, BLK)] = pos[rows]
        tab_ref[d, :local, tail] += stat[rows]
        tab_ref[d, local:, tail] += first[rows]
    carry[:, :1] = after


def run_router(x_loc, w_router, ids_t, capacity, local, devices):
    tokens, d_model = x_loc.shape
    experts = w_router.shape[1]
    top_k = ids_t.shape[FIRST]
    table = (devices, 2 * local, tokens + LANES)
    return pl.pallas_call(
        functools.partial(router_kernel, capacity, local),
        grid=(tokens // BLK,),
        in_specs=[pl.BlockSpec((BLK, d_model), lambda i: (i, FIRST)), VMEM, pl.BlockSpec((top_k, BLK), lambda i: (FIRST, i))],
        out_specs=[VMEM, pl.BlockSpec((experts, BLK), lambda i: (FIRST, i))],
        out_shape=[Shape(table, f32), Shape((experts, tokens), f32)],
        scratch_shapes=[pltpu.VMEM((experts, LANES), f32)],
        compiler_params=params(),
        cost_estimate=cost(2 * tokens * d_model * BLK, 2 * tokens * d_model),
        name="router",
    )(x_loc, w_router, ids_t)


class Blocks:
    def __init__(self, starts_ref, bmap_ref):
        self.starts, self.bmap = starts_ref, bmap_ref

    def info(self, i, e):
        at = self.bmap[2 * i + 1] + e * ALIGN
        first = self.starts[at]
        return self.bmap[2 * i], first, self.starts[at + 1] - first

    def total(self, start, count, e):
        return lax.fori_loop(start, start + count, lambda i, n: n + self.info(i, e)[LAST], i32(FIRST))


def aligned(row):
    base = (row // ALIGN) * ALIGN
    return base, row - base


def window_count(shift, count):
    return (shift + count + WIN - 1) // WIN


def padded(total):
    return (total + TILE - 1) // TILE * TILE


def row_tiles(total, body, size):
    tiles = (total + size - 1 - size // 2) // size
    loop(FIRST, tiles, lambda i: body(i * size, size))
    pl.when(padded(total) > tiles * size)(lambda: body(tiles * size, size // 2))


def start(copies):
    for cp in copies:
        cp.start()


def wait(copies):
    for cp in copies:
        cp.wait()


def taker(refs):
    refs = list(refs)

    def take(n=None):
        got = refs[:n]
        del refs[:n]
        return got

    return take


def block_count(pieces):
    return sum(count for _, _, count in pieces)


def offsets(pieces):
    counts = [count for _, _, count in pieces]
    return [(sum(counts[:k]), count) for k, count in enumerate(counts)]


def block_rows(first, count):
    return pl.ds(first * BLK, count * BLK)


def grad_kernel(g, last, local, pieces, *refs):
    take = taker(refs)
    n = len(pieces)
    starts_ref, bmap_ref, tab_ref = take(3)
    tok_refs = take(n), take(n)
    w1_ref, w3_ref, w2_ref = take(3)
    acc_in = take(2 * bool(g))
    take(3 * bool(g))
    row_outs = take(3)
    outs = take(3 if last else 2)
    xv, dv, xr, dr, acc13, acc2, stage, tok_sem, in_sem, out_sem, row_sem = take()
    accs = acc13, acc2
    e = pl.program_id(FIRST)
    slot = e % 2
    d_model = xv.shape[1]
    d_ff = w1_ref.shape[LAST]
    blocks = Blocks(starts_ref, bmap_ref)
    count = xv.shape[FIRST] // BLK

    parts = [(c, at, first + at) for c, (first, size) in enumerate(offsets(pieces)) for at in range(FIRST, size, 3)]

    def token_copies(k):
        c, at, to = parts[k]
        src_rows, dst_rows = block_rows(at, 3), block_rows(to, 3)
        return [pltpu.make_async_copy(src[c].at[src_rows], dst.at[dst_rows], tok_sem.at[w, k]) for w, (src, dst) in enumerate(zip(tok_refs, (xv, dv)))]

    def in_copies(ee, ss):
        return [pltpu.make_async_copy(src.at[ee], dst.at[ss], in_sem.at[ss, k]) for k, (src, dst) in enumerate(zip(acc_in, accs))]

    def out_copies(ee, ss):
        return [pltpu.make_async_copy(src.at[ss], dst.at[ee], out_sem.at[ss, k]) for k, (src, dst) in enumerate(zip(accs, outs))]

    @pl.when(e == FIRST)
    def _():
        for k in range(len(parts)):
            start(token_copies(k))

    if g:
        pl.when(e == FIRST)(lambda: start(in_copies(e, slot)))
    else:
        pl.when(e >= 2)(lambda: wait(out_copies(e - 2, slot)))
        for acc in accs:
            acc[slot] = jnp.zeros(acc.shape[1:], f32)

    def prefetch():
        if not last:
            pl.when(e > FIRST)(lambda: wait(out_copies(e - 1, 1 - slot)))
        start(in_copies(e + 1, 1 - slot))

    def maybe_prefetch(now):
        if g:
            pl.when(now & (e + 1 < local))(prefetch)

    row_iota = iota((WIN, BLK), FIRST).astype(f32)
    head_row = iota((ALIGN, d_model), FIRST)
    both = tuple(HALVES)

    def dispatch(i, rows_at):
        for k, (_, _, first) in enumerate(parts):
            pl.when((e == FIRST) & (i == first))(lambda: wait(token_copies(k)))
        tok = span(i * BLK, BLK)
        infos = [blocks.info(i, e + q) for q in both]
        places = [aligned(r) for r in rows_at]
        flat = infos[FIRST][FIRST]

        def picks(q, k):
            pos = tab_ref[flat, pl.ds(local + e + q, 1), :]
            gate = tab_ref[flat, pl.ds(e + q, 1), :]
            pick = (pos + (places[q][1] - infos[q][1] - k * WIN).astype(f32)) == row_iota
            return one_hot(pick), lane_sum(where0(pick, gate + jnp.zeros_like(row_iota)))

        def rows_for(one, gate_row):
            return dot(one, xv[tok, :]).astype(bf16), (dot(one, dv[tok, :]) * gate_row).astype(bf16)

        pair = [picks(q, i32(FIRST)) for q in both]
        new = rows_for(*[jnp.concatenate(v, axis=FIRST) for v in zip(*pair)])
        for q in both:
            base, shift = places[q]
            head = span(base, ALIGN)
            for value, rows in zip(new, (xr, dr)):
                value = value[q * WIN : (q + 1) * WIN]
                rows[q, head, :] = jnp.where(head_row < shift, rows[q, head, :], value[:ALIGN])
                rows[q, span(base + ALIGN, WIN - ALIGN, ALIGN), :] = value[ALIGN:]

            def more(k):
                for value, rows in zip(rows_for(*picks(q, k)), (xr, dr)):
                    rows[q, span(base + k * WIN, WIN, ALIGN), :] = value

            loop(1, window_count(shift, infos[q][LAST]), more)
        return tuple(r + info[LAST] for r, info in zip(rows_at, infos))

    @pl.when(slot == FIRST)
    def _():
        totals = lax.fori_loop(FIRST, count, dispatch, (i32(FIRST),) * len(both))
        for q in both:

            def clear(i):
                for rows in (xr, dr):
                    rows[q, span(i * ALIGN, ALIGN), :] = jnp.zeros((ALIGN, d_model), bf16)

            loop((totals[q] + ALIGN - 1) // ALIGN, padded(totals[q]) // ALIGN, clear)

    wait(in_copies(e, slot))

    def tile(at, size):
        maybe_prefetch(at == FIRST)
        rows = span(at, size)
        xt = xr[slot, rows, :]
        dt = dr[slot, rows, :]
        act_a = dot(xt, w1_ref[FIRST])
        act_b = dot(xt, w3_ref[FIRST])
        d_hidden = dot_nt(dt, w2_ref[FIRST]).astype(bf16).astype(f32)
        sig = 1.0 / (1.0 + jnp.exp(-act_a))
        silu = act_a * sig
        hidden = (silu * act_b).astype(bf16)
        d_a = (d_hidden * act_b * sig * (1.0 + act_a * (1.0 - sig))).astype(bf16)
        d_b = (d_hidden * silu).astype(bf16)
        copies = []
        for k, (value, out) in enumerate(zip((hidden, d_a, d_b), row_outs)):
            stage[k, :size] = value
            copies.append(pltpu.make_async_copy(stage.at[k, :size], out.at[g, e, rows], row_sem.at[k]))
        start(copies)
        acc13[slot, :, :d_ff] += dot_tn(xt, d_a)
        acc13[slot, :, d_ff:] += dot_tn(xt, d_b)
        acc2[slot] += dot_tn(hidden, dt)
        wait(copies)

    total = blocks.total(FIRST, count, e)
    maybe_prefetch(total == FIRST)
    row_tiles(total, tile, 2 * TILE)

    if last:
        for out, value in zip(outs, (acc13[slot, :, :d_ff], acc13[slot, :, d_ff:], acc2[slot])):
            out[FIRST] = value.astype(bf16)
    else:
        start(out_copies(e, slot))

        @pl.when(e == pl.num_programs(FIRST) - 1)
        def _():
            wait(out_copies(e - 1, 1 - slot))
            wait(out_copies(e, slot))


def per_expert(*shape):
    return pl.BlockSpec((1, *shape), lambda e: (e,) + (FIRST,) * len(shape))


def block_map(pieces, nb):
    spots = [(src, first + b) for src, first, count in pieces for b in range(count)]
    return np.asarray([v for src, b in spots for v in (src * nb + b, src * 4 * ALIGN + b)], np.int32)


def run_grad(starts, tab, g, xs, ds, weights, acc, rows, nb, row_cap):
    pieces = GROUPS[g]
    last = g == len(GROUPS) - 1
    local, d_model, d_ff = weights[FIRST].shape
    count = block_count(pieces) * BLK
    w_specs = [per_expert(*w.shape[1:]) for w in weights]
    sums = [(local, d_model, 2 * d_ff), (local, d_ff, d_model)]
    row_shape = [Shape((len(GROUPS), local, row_cap, d_ff), bf16)] * 3
    out_shape = row_shape + ([Shape(w.shape, bf16) for w in weights] if last else [Shape(s, f32) for s in sums])
    out_specs = [ANY] * 3 + (w_specs if last else [ANY] * 2)
    tokens = pltpu.VMEM((count, d_model), bf16)
    packed = pltpu.VMEM((2, row_cap + WIN, d_model), bf16)
    ins = [starts, block_map(pieces, nb), tab, *xs, *ds, *weights, *acc, *rows]
    out = pl.pallas_call(
        functools.partial(grad_kernel, g, last, local, pieces),
        grid=(local,),
        in_specs=[SMEM, SMEM, VMEM] + [ANY] * (2 * len(pieces)) + w_specs + [ANY] * (len(acc) + len(rows)),
        out_specs=out_specs,
        out_shape=out_shape,
        scratch_shapes=[tokens, tokens, packed, packed]
        + [pltpu.VMEM((2, *s[1:]), f32) for s in sums]
        + [pltpu.VMEM((3, 2 * TILE, d_ff), bf16), DMA((2, count // (3 * BLK))), DMA((2, 2)), DMA((2, 2)), DMA((3,))],
        input_output_aliases={len(ins) - len(rows) + k: k for k in range(len(rows))},
        compiler_params=params(),
        cost_estimate=cost(12 * count * d_model * d_ff, 40 << 20),
        name="expert_grad",
    )(*ins)
    return out[:3], out[3:]


def group_spans(groups):
    counts = [block_count(GROUPS[g]) for g in groups]
    return np.asarray([v for k, c in enumerate(counts) for v in (sum(counts[:k]), c)], np.int32)


def per_group(groups, *shape):
    return pl.BlockSpec((1, 1, *shape), lambda step, e: (step + groups[FIRST], e) + (FIRST,) * len(shape))


def per_local(*shape):
    return pl.BlockSpec((1, *shape), lambda g, e: (e,) + (FIRST,) * len(shape))


class Combine:
    def __init__(self, local, starts_ref, bmap_ref, spans_ref, tab_ref, rows_ref, out_ref, ring, sems):
        step = pl.program_id(FIRST)
        self.e = pl.program_id(1)
        self.blocks = Blocks(starts_ref, bmap_ref)
        self.first, self.count = spans_ref[2 * step], spans_ref[2 * step + 1]
        self.total = self.blocks.total(self.first, self.count, self.e)
        self.local, self.tab_ref, self.rows_ref = local, tab_ref, rows_ref
        self.out_ref, self.ring, self.sems = out_ref, ring, sems
        self.lane = iota((BLK, WIN), 1).astype(f32)

    def zero_tail(self):
        rows = span(padded(self.total), WIN)
        self.rows_ref[self.e, rows, :] = jnp.zeros((WIN, self.rows_ref.shape[LAST]), bf16)

    def pick(self, ee, k):
        place, info = self.places[ee], self.infos[ee]
        pos = self.tab_t[:, self.local + ee : self.local + ee + 1]
        return one_hot((pos + (place[1] - info[1] - k * WIN).astype(f32)) == self.lane)

    def held(self, ee, k, cols=slice(None)):
        return self.rows_ref[ee, span(self.places[ee][FIRST] + k * WIN, WIN, ALIGN), cols]

    def out_copy(self, i):
        slot = i % RING
        place = self.blocks.bmap[2 * i] - self.blocks.bmap[FIRST]
        return pltpu.make_async_copy(self.ring.at[slot], self.out_ref.at[place], self.sems.at[slot])

    def run(self, simple_body, full_body):
        def block(i, rows_at):
            ee = range(self.local)
            self.infos = [self.blocks.info(i, k) for k in ee]
            self.places = [aligned(r) for r in rows_at]
            self.windows = [window_count(self.places[k][1], self.infos[k][LAST]) for k in ee]
            self.flat = self.infos[FIRST][FIRST]
            self.tab_t = jnp.transpose(self.tab_ref[self.flat])
            self.tok = span((i - self.first) * BLK, BLK)
            pl.when(i - self.first >= RING)(lambda: self.out_copy(i - RING).wait())
            simple = functools.reduce(jnp.logical_and, [w <= 1 for w in self.windows])
            out = self.ring.at[i % RING]
            pl.when(simple)(lambda: simple_body(out))
            pl.when(jnp.logical_not(simple))(lambda: full_body(out))
            self.out_copy(i).start()
            return tuple(r + info[LAST] for r, info in zip(rows_at, self.infos))

        stop = self.first + self.count
        lax.fori_loop(self.first, stop, block, (i32(FIRST),) * self.local)
        loop(stop - RING, stop, lambda i: self.out_copy(i).wait())


def y_kernel(groups, local, starts_ref, bmap_ref, spans_ref, tab_ref, h_ref, w2_ref, *refs):
    take = taker(refs)
    d_refs = [take(len(GROUPS[g])) for g in groups]
    y_ref, dg_ref, o_rows, dv, ring, zacc, yacc, dgacc, tok_sem, out_sem = take()
    all_rows = Combine(local, starts_ref, bmap_ref, spans_ref, tab_ref, o_rows, y_ref, ring, out_sem)
    e = all_rows.e
    d_model = dv.shape[1]

    def token_copies(step):
        spots = offsets(GROUPS[groups[step]])
        return [pltpu.make_async_copy(src, dv.at[block_rows(*spot)], tok_sem.at[c]) for c, (src, spot) in enumerate(zip(d_refs[step], spots))]

    for step in range(len(groups)):
        pl.when((pl.program_id(FIRST) == step) & (e == FIRST))(lambda: start(token_copies(step)))

    def tile(at, size):
        rows = span(at, size)
        o_rows[e, rows, :] = dot(h_ref[FIRST, FIRST, rows, :], w2_ref[FIRST]).astype(bf16)

    row_tiles(all_rows.total, tile, 2 * TILE)
    all_rows.zero_tail()

    @pl.when(e == local - 1)
    def _():
        for step in range(len(groups)):
            pl.when(pl.program_id(FIRST) == step)(lambda: wait(token_copies(step)))
        dg_lane = iota((BLK, LANES), 1)
        width = 2 * LANES
        columns = [slice(k * width, (k + 1) * width) for k in range(d_model // width)]

        def gate(ee):
            return all_rows.tab_t[:, ee : ee + 1]

        def put_dg(sums):
            dg = sum(where0(dg_lane == ee, lane_sum(s) + jnp.zeros((BLK, LANES), f32)) for ee, s in enumerate(sums))
            dg_ref[all_rows.flat - all_rows.blocks.bmap[FIRST]] = jnp.transpose(dg)[: 2 * local, :]

        def simple(out):
            picks = [all_rows.pick(ee, i32(FIRST)) for ee in range(local)]
            sums = [None] * local
            for cols in columns:
                dy = dv[all_rows.tok, cols].astype(f32)
                y = None
                for ee in range(local):
                    z = dot(picks[ee], all_rows.held(ee, i32(FIRST), cols))
                    prod = dy * z
                    part = prod[:, :LANES] + prod[:, LANES:]
                    sums[ee] = part if sums[ee] is None else sums[ee] + part
                    y = gate(ee) * z if y is None else y + gate(ee) * z
                out[:, cols] = y.astype(bf16)
            put_dg(sums)

        def full(out):
            yacc[...] = jnp.zeros_like(yacc)
            for ee in range(local):
                zacc[...] = jnp.zeros_like(zacc)

                def more(k):
                    zacc[...] += dot(all_rows.pick(ee, k), all_rows.held(ee, k))

                loop(FIRST, all_rows.windows[ee], more)
                yacc[...] += gate(ee) * zacc[...]
                dgacc[ee] = lane_sum(dv[all_rows.tok, :].astype(f32) * zacc[...]) * jnp.where(dg_lane == FIRST, 1.0, 0.0)
            out[...] = yacc[...].astype(bf16)
            put_dg([dgacc[ee] for ee in range(local)])

        all_rows.run(simple, full)


def combine_scratch(local, row_cap, d_model):
    return [pltpu.VMEM((local, row_cap + WIN, d_model), bf16)], [pltpu.VMEM((RING, BLK, d_model), bf16), pltpu.VMEM((BLK, d_model), f32)]


def run_y(groups, starts, tab, h_rows, w2, ds, nb):
    local, d_ff, d_model = w2.shape
    row_cap = h_rows.shape[2]
    pieces = [p for g in groups for p in GROUPS[g]]
    spans = group_spans(groups)
    blocks = block_count(pieces)
    rows, work = combine_scratch(local, row_cap, d_model)
    return pl.pallas_call(
        functools.partial(y_kernel, groups, local),
        grid=(len(groups), local),
        in_specs=[SMEM, SMEM, SMEM, VMEM, per_group(groups, row_cap, d_ff), per_local(d_ff, d_model)] + [ANY] * len(pieces),
        out_specs=[ANY, VMEM],
        out_shape=[Shape((blocks, BLK, d_model), bf16), Shape((blocks, 2 * local, BLK), f32)],
        scratch_shapes=rows + [pltpu.VMEM((max(spans[1::2]) * BLK, d_model), bf16)] + work + [work[LAST], pltpu.VMEM((local, BLK, LANES), f32), DMA((4,)), DMA((RING,))],
        compiler_params=grid_params(2),
        cost_estimate=cost(4 * blocks * BLK * d_model * d_ff, 20 << 20),
        name="expert_y",
    )(starts, block_map(pieces, nb), spans, tab, h_rows, w2, *[ds[p] for p in pieces])


def dx_kernel(local, starts_ref, bmap_ref, spans_ref, tab_ref, da_ref, db_ref, w1_ref, w3_ref, dx_ref, o_rows, ring, zacc, out_sem):
    all_rows = Combine(local, starts_ref, bmap_ref, spans_ref, tab_ref, o_rows, dx_ref, ring, out_sem)
    e = all_rows.e

    def tile(at, size):
        rows = span(at, size)
        grad = dot_nt(da_ref[FIRST, FIRST, rows, :], w1_ref[FIRST]) + dot_nt(db_ref[FIRST, FIRST, rows, :], w3_ref[FIRST])
        o_rows[e, rows, :] = grad.astype(bf16)

    row_tiles(all_rows.total, tile, 2 * TILE)
    all_rows.zero_tail()

    @pl.when(e == local - 1)
    def _():
        def simple(out):
            pairs = [(ee, ee + 1) for ee in range(FIRST, local, 2)]
            zero = i32(FIRST)
            sums = [
                dot(jnp.concatenate([all_rows.pick(ee, zero) for ee in pair], axis=1), jnp.concatenate([all_rows.held(ee, zero) for ee in pair], axis=FIRST))
                for pair in pairs
            ]
            out[...] = sum(sums[1:], sums[FIRST]).astype(bf16)

        def full(out):
            zacc[...] = jnp.zeros_like(zacc)
            for ee in range(local):

                def more(k):
                    zacc[...] += dot(all_rows.pick(ee, k), all_rows.held(ee, k))

                loop(FIRST, all_rows.windows[ee], more)
            out[...] = zacc[...].astype(bf16)

        all_rows.run(simple, full)


def run_dx(groups, starts, tab, da_rows, db_rows, w1, w3, nb):
    local, d_model, d_ff = w1.shape
    row_cap = da_rows.shape[2]
    pieces = [p for g in groups for p in GROUPS[g]]
    blocks = block_count(pieces)
    rows, work = combine_scratch(local, row_cap, d_model)
    return pl.pallas_call(
        functools.partial(dx_kernel, local),
        grid=(len(groups), local),
        in_specs=[SMEM, SMEM, SMEM, VMEM] + [per_group(groups, row_cap, d_ff)] * 2 + [per_local(d_model, d_ff)] * 2,
        out_specs=ANY,
        out_shape=Shape((blocks, BLK, d_model), bf16),
        scratch_shapes=rows + work + [DMA((RING,))],
        compiler_params=grid_params(2),
        cost_estimate=cost(6 * blocks * BLK * d_model * d_ff, 20 << 20),
        name="expert_dx",
    )(starts, block_map(pieces, nb), group_spans(groups), tab, da_rows, db_rows, w1, w3)


def router_grad_kernel(scale, x_ref, prob_ref, dg_ref, ids_ref, load_ref, dlog_ref, dw_ref):
    step = pl.program_id(FIRST)
    prob = prob_ref[...]
    dg = dg_ref[...]
    chosen = chosen_mask(ids_ref[...], prob.shape[FIRST])
    gate_sum = row_sum(where0(chosen, prob))
    gate = where0(chosen, prob / gate_sum)
    d_pick = (dg - row_sum(gate * dg)) / gate_sum
    d_prob = where0(chosen, d_pick) + scale * load_ref[:, :1]
    d_logit = prob * (d_prob - row_sum(prob * d_prob))
    dlog_ref[...] = d_logit
    hi, mid, low = [dot(part, x_ref[...]) for part in split3(d_logit)]

    @pl.when(step == FIRST)
    def _():
        dw_ref[...] = jnp.zeros_like(dw_ref)

    dw_ref[...] += hi + (mid + low)


def run_router_grad(x_loc, prob_t, dg_t, ids_t, load, scale):
    tokens, d_model = x_loc.shape
    experts = prob_t.shape[FIRST]
    lanes = lambda n: pl.BlockSpec((n, BLK), lambda i: (FIRST, i))
    return pl.pallas_call(
        functools.partial(router_grad_kernel, scale),
        grid=(tokens // BLK,),
        in_specs=[pl.BlockSpec((BLK, d_model), lambda i: (i, FIRST)), lanes(experts), lanes(experts), lanes(ids_t.shape[FIRST]), VMEM],
        out_specs=[lanes(experts), VMEM],
        out_shape=[Shape((experts, tokens), f32), Shape((experts, d_model), f32)],
        compiler_params=params(),
        cost_estimate=cost(2 * tokens * d_model * BLK, 2 * tokens * d_model),
        name="router_grad",
    )(x_loc, prob_t, dg_t, ids_t, load)


def final_kernel(dlog_ref, wt_ref, *refs):
    take = taker(refs)
    y_terms, dx_terms = [[ref[...].astype(f32) for ref in take(3)] for _ in TENSORS]
    y_ref, dx_ref = take()
    lhs = split3(dlog_ref[...])
    rhs = split3(wt_ref[...])
    terms = [(i, j) for i in range(3) for j in range(3 - i)]
    left = jnp.concatenate([lhs[i] for i, _ in terms], axis=FIRST)
    right = jnp.concatenate([rhs[j] for _, j in terms], axis=FIRST)
    dx_ref[...] = (dot_tn(left, right) + sum(dx_terms[1:], dx_terms[FIRST])).astype(bf16)
    y_ref[...] = sum(y_terms[1:], y_terms[FIRST]).astype(bf16)


def run_final(dlog_t, w_t, y_terms, dx_terms):
    experts, tokens = dlog_t.shape
    d_model = w_t.shape[1]
    size = tokens // 4
    rows = pl.BlockSpec((size, d_model), lambda i: (i, FIRST))
    return pl.pallas_call(
        final_kernel,
        grid=(tokens // size,),
        in_specs=[pl.BlockSpec((experts, size), lambda i: (FIRST, i)), VMEM] + [rows] * len([*y_terms, *dx_terms]),
        out_specs=[rows] * 2,
        out_shape=[Shape((tokens, d_model), bf16)] * 2,
        compiler_params=params(),
        cost_estimate=cost(2 * tokens * d_model * BLK, 16 * tokens * d_model),
        name="final",
    )(dlog_t, w_t, *y_terms, *dx_terms)


NEAR = (X, Y)
RELAYED = {(Y, 0): 0, (X, 1): 1}
OPS = [
    (t, src, h)
    for step in ([(FAR, 0), (FAR, 1)], [(X, 0), (Y, 1)], [(X, 1), (Y, 0)], [(FIRST, 0), (FIRST, 1)])
    for t in TENSORS
    for src, h in step
]


def add_rows(dst, src):
    def body(i):
        rows = span(i * LANES, LANES)
        dst[rows, :] = (dst[rows, :].astype(f32) + src[rows, :].astype(f32)).astype(bf16)

    loop(FIRST, dst.shape[FIRST] // LANES, body)


def exchange_kernel(half, mats, *refs):
    take = taker(refs)
    parts = [take(2) for _ in TENSORS]
    dws = take(mats)
    outs = [take(len(NEAR) + 1) for _ in TENSORS]
    dw_outs = take(mats)
    land, far_land, stage, z_one, z_two, z_stage = take(6)
    core_sem, stage_sem, far_sem, near_sem, own_sem, z_sem, keep_sem, load_sem, credit_one, credit_two = take()

    me = lax.axis_index("ep")
    z = lax.axis_index("dp")
    peer = {bit: me + bit - 2 * bit * ((me // bit) % 2) for bit in (CORE, X, Y)}
    z_peer = z + 1 - 2 * (z % 2)
    z_cross = 3 - z
    is_end = (z % 3) == FIRST
    is_mid = (z % 3) != FIRST

    barrier = pltpu.get_barrier_semaphore()
    ids = [{"ep": p} for p in peer.values()] + [{"dp": z_peer}, {"dp": z_cross}]
    for device in ids:
        pl.semaphore_signal(barrier, device_id=device, device_id_type=MESH)
    pl.semaphore_wait(barrier, len(ids))

    def remote(src, dst, sems, at, device):
        send, recv = sems.at[(SEND, *at)], sems.at[(RECV, *at)]
        return pltpu.make_async_remote_copy(src_ref=src, dst_ref=dst, send_sem=send, recv_sem=recv, device_id=device, device_id_type=MESH)

    def rows_at(h):
        return pl.ds(h * half, half)

    def part(t, src, h):
        own, rest = parts[t]
        return own.at[src, rows_at(h)] if src <= CORE else rest.at[src - 2, rows_at(h)]

    def core_copy(i):
        t, src, h = OPS[i]
        return remote(part(t, src | CORE, h), land.at[i], core_sem, (i,), {"ep": peer[CORE]})

    def stage_copy(i):
        t, src, h = OPS[i]
        return pltpu.make_async_copy(part(t, src, h), stage.at[i % STAGES], stage_sem.at[i % STAGES])

    def far_copy(i):
        t, _, h = OPS[i]
        return remote(land.at[i], far_land.at[t, h], far_sem, (t, h), {"ep": peer[NEAR[h]]})

    def near_copy(i):
        t, src, h = OPS[i]
        k = NEAR.index(src)
        return remote(land.at[i], outs[t][k].at[rows_at(h)], near_sem, (t, k, h), {"ep": peer[src]})

    def own_copy(i):
        t, _, h = OPS[i]
        return pltpu.make_async_copy(land.at[i], outs[t][LAST].at[rows_at(h)], own_sem.at[t, h])

    def out_copy(i):
        src = OPS[i][1]
        return (far_copy if src == FAR else near_copy if src else own_copy)(i)

    def reduce_op(i):
        t, src, h = OPS[i]
        stage_copy(i).wait()
        core_copy(i).wait_recv()
        add_rows(land.at[i], stage.at[i % STAGES])
        if i + STAGES < len(OPS):
            stage_copy(i + STAGES).start()
        if (src, h) in RELAYED:
            far_copy(OPS.index((t, FAR, RELAYED[src, h]))).wait_recv()
            add_rows(land.at[i], far_land.at[t, RELAYED[src, h]])

    rows_per = z_one.shape[1]
    chunks = [(m, e, k) for e in range(dws[FIRST].shape[FIRST]) for m in range(mats) for k in HALVES]
    n = len(chunks)

    def piece(arrays, c):
        m, e, k = chunks[c]
        return arrays[m].at[e, pl.ds(k * rows_per, rows_per)]

    def one_copy(c):
        return remote(piece(dws, c), z_one.at[c % SLOTS], z_sem, (FIRST, c), {"dp": z_peer})

    def two_copy(c):
        return remote(z_one.at[c % SLOTS], z_two.at[c % SLOTS], z_sem, (1, c), {"dp": z_cross})

    def three_copy(c):
        return remote(z_two.at[c % SLOTS], piece(dw_outs, c), z_sem, (2, c), {"dp": z_peer})

    def keep_copy(c):
        return pltpu.make_async_copy(z_two.at[c % SLOTS], piece(dw_outs, c), keep_sem.at[c])

    def load_copy(c):
        return pltpu.make_async_copy(piece(dws, c), z_stage.at[c % STAGES], load_sem.at[c % STAGES])

    def first_add(c):
        load_copy(c).wait()
        one_copy(c).wait_recv()
        add_rows(z_one.at[c % SLOTS], z_stage.at[c % STAGES])
        if c + STAGES < n:
            load_copy(c + STAGES).start()

    def second_add(c):
        two_copy(c).wait()
        add_rows(z_two.at[c % SLOTS], z_one.at[c % SLOTS])
        if c + SLOTS < n:
            pl.semaphore_signal(credit_one, device_id={"dp": z_peer}, device_id_type=MESH)

    def retire(c):
        three_copy(c).wait_send()
        keep_copy(c).wait()
        if c + SLOTS < n:
            pl.semaphore_signal(credit_two, device_id={"dp": z_cross}, device_id_type=MESH)

    @pl.when(is_end)
    def _():
        for c in range(SLOTS):
            one_copy(c).start()

    @pl.when(is_mid)
    def _():
        for c in range(STAGES):
            load_copy(c).start()

    for i in range(len(OPS)):
        core_copy(i).start()
        if i < STAGES:
            stage_copy(i).start()

    todo = list(range(len(OPS)))
    for tick in range(n + LAG):
        mine = todo[: 2 if tick < 2 else 1]
        todo = todo[len(mine) :]
        for i in mine:
            reduce_op(i)

        @pl.when(is_mid)
        def _():
            back = tick - 1
            if tick < n:
                first_add(tick)
            if back in range(n):
                second_add(back)
            if tick < n:
                if tick >= SLOTS:
                    pl.semaphore_wait(credit_two, 1)
                two_copy(tick).start()
            if back in range(n):
                three_copy(back).start()
                keep_copy(back).start()
            if tick >= LAG:
                retire(tick - LAG)

        for i in mine:
            out_copy(i).start()

        @pl.when(is_end)
        def _():
            if tick + SLOTS < n:
                pl.semaphore_wait(credit_one, 1)
                one_copy(tick + SLOTS).start()

    for i in todo:
        reduce_op(i)
        out_copy(i).start()

    @pl.when(is_end)
    def _():
        for c in range(n):
            one_copy(c).wait_send()
            three_copy(c).wait_recv()

    for i in range(len(OPS)):
        core_copy(i).wait_send()
        (out_copy(i).wait_send if OPS[i][1] == FAR else out_copy(i).wait)()


def run_exchange(parts, dws):
    tokens, d_model = parts[FIRST][FIRST].shape[1:]
    half = tokens // 2
    local, rows, cols = dws[FIRST].shape
    chunk = (rows // 2, cols)
    n = local * len(dws) * len(HALVES)
    whole = Shape((tokens, d_model), bf16)
    flat = [v for tensor in parts for v in tensor] + list(dws)
    terms = len(NEAR) + 1
    out = pl.pallas_call(
        functools.partial(exchange_kernel, half, len(dws)),
        in_specs=[ANY] * len(flat),
        out_specs=[ANY] * (terms * len(TENSORS) + len(dws)),
        out_shape=[whole] * (terms * len(TENSORS)) + [Shape(v.shape, bf16) for v in dws],
        scratch_shapes=[
            pltpu.VMEM((len(OPS), half, d_model), bf16),
            pltpu.VMEM((len(TENSORS), len(HALVES), half, d_model), bf16),
            pltpu.VMEM((STAGES, half, d_model), bf16),
            pltpu.VMEM((SLOTS, *chunk), bf16),
            pltpu.VMEM((SLOTS, *chunk), bf16),
            pltpu.VMEM((STAGES, *chunk), bf16),
            DMA((2, len(OPS))),
            DMA((STAGES,)),
            DMA((2, 2, 2)),
            DMA((2, 2, 2, 2)),
            DMA((2, 2)),
            DMA((2, 3, n)),
            DMA((n,)),
            DMA((STAGES,)),
            pltpu.SemaphoreType.REGULAR,
            pltpu.SemaphoreType.REGULAR,
        ],
        compiler_params=pltpu.CompilerParams(vmem_limit_bytes=VMEM_LIMIT, collective_id=FIRST, has_side_effects=True),
        cost_estimate=cost(1 << 37, 200 << 20),
        name="exchange",
    )(*flat)
    return [out[:terms], out[terms : 2 * terms]], out[2 * terms :]


def hop(v, bit):
    return lax.ppermute(v, "ep", [(i, i ^ bit) for i in SOURCES])


def after(values, token):
    return lax.optimization_barrier((values, token))[FIRST]


def send_own(v):
    pieces = [v[first * BLK : (first + count) * BLK] for first, count in PARTS]
    got = {(bit, *part): hop(piece, bit) for part, piece in zip(PARTS, pieces) for bit in NEAR}
    got.update({(FIRST, *WHOLE): v, (CORE, *WHOLE): hop(v, CORE)})
    return got, pieces


def pass_on(got, h):
    part = PARTS[h]
    got[FAR, *part] = hop(got[(Y, X)[h], *part], NEAR[h])
    for bit in NEAR:
        got[bit | CORE, *part] = hop(got[bit, *part], CORE)


def relative(v, me):
    shape = v.shape
    v = v.reshape((2, 2, 2) + shape[1:])
    for axis, bit in enumerate((Y, X, CORE)):
        v = jnp.where((me & bit) != FIRST, jnp.flip(v, axis), v)
    return v.reshape(shape)


def solution(mesh):
    dp_size = mesh.shape["dp"]
    ep_size = mesh.shape["ep"]
    row_spec = P(("dp", "ep"), None)
    expert_spec = P("ep", None, None)
    whole_spec = P(None, None)

    def per_device(x_loc, w_router, ids_loc, w1, w3, w2, dy_loc):
        tokens, d_model = x_loc.shape
        top_k = ids_loc.shape[1]
        experts = w_router.shape[1]
        local = w1.shape[FIRST]
        capacity = capacity_of(tokens, top_k, experts)
        n_total = tokens * dp_size * ep_size
        nb = tokens // BLK
        row_cap = padded(4 * capacity)
        me = lax.axis_index("ep")

        gathered, pieces = zip(*[send_own(v) for v in (x_loc, dy_loc)])

        ids_t, x_router = after((ids_loc.T, x_loc), pieces)
        send_tab, prob_t = run_router(x_router, w_router, ids_t, capacity, local, ep_size)
        tab_rel = relative(lax.all_to_all(send_tab, "ep", FIRST, FIRST, tiled=True), me)
        tab = tab_rel[:, :, :tokens].reshape(ep_size, 2 * local, nb, BLK).transpose(0, 2, 1, 3).reshape(ep_size * nb, 2 * local, BLK)
        starts = tab_rel[:, local:, tokens : tokens + ALIGN].astype(i32).reshape(LAST)

        def y_of(groups, starts):
            return run_y(groups, starts, tab, rows[FIRST], w2, gathered[1], nb)

        def dx_of(groups, starts):
            return run_dx(groups, starts, tab, rows[1], rows[2], w1, w3, nb)

        acc = rows = ()
        own, rest = (FIRST,), (1, 2, 3)
        for g, group in enumerate(GROUPS):
            if g:
                ready = [p for p in group if not p[FIRST] & CORE]
                for got in gathered:
                    got.update(after({p: got[p] for p in ready}, acc[LAST]))
                for got in gathered:
                    if g < len(GROUPS) - 1:
                        pass_on(got, g - 1)
                    else:
                        for src, *part in ready:
                            got[src | CORE, *part] = hop(got[src, *part], CORE)
                here = after(starts, [[got[p] for p in ready] for got in gathered])
                if g == 2:
                    y_own, dg_own = y_of(own, here)
                    starts = after(starts, dg_own)
                if g > 2:
                    dx_own = dx_of(own, here)
                    starts = after(starts, dx_own)
            rows, acc = run_grad(starts, tab, g, *[[got[p] for p in group] for got in gathered], (w1, w3, w2), acc, rows, nb, row_cap)
            if not g:
                stats = jnp.sum(after(tab_rel[:, :local, tokens:], acc[LAST]), axis=FIRST)
                for step in (1, 2):
                    stats = stats + lax.ppermute(stats, "dp", [(i, i ^ step) for i in range(dp_size)])
                starts = after(starts, stats)
        dw1, dw3, dw2 = acc
        starts, dw2 = lax.optimization_barrier((starts, dw2))
        dw2_sum = lax.psum(dw2, "dp")

        y_rest, dg_rest = y_of(rest, starts)
        dg = jnp.concatenate([dg_own, dg_rest], axis=FIRST)
        dg = dg[:, :local].reshape(ep_size, nb, local, BLK).transpose(0, 2, 1, 3).reshape(ep_size, local, tokens)
        dg = jnp.concatenate([relative(dg, me), jnp.broadcast_to(stats, (ep_size, *stats.shape))], axis=2)
        starts, dg = lax.optimization_barrier((starts, dg))
        dx_rest = dx_of(rest, starts)
        dg_all = lax.all_to_all(dg, "ep", FIRST, FIRST, tiled=True).reshape(experts, tokens + LANES)
        load = dg_all[:, tokens:]
        share = AUX_COEF * experts / (n_total * top_k * n_total)
        aux_loss = share * jnp.sum(load[:, FIRST] * load[:, 1])
        dlog_t, dwr_t = run_router_grad(x_loc, prob_t, dg_all[:, :tokens], ids_t, load, share)
        dw_router = lax.psum(after(dwr_t, dw2_sum), ("dp", "ep")).T

        parts = [[v.reshape(LAST, tokens, d_model) for v in pair] for pair in ((y_own, y_rest), (dx_own, dx_rest))]
        sums, grads = run_exchange(parts, [dw1, dw3])
        y_loc, dx_loc = run_final(dlog_t, w_router.T, *sums)
        return y_loc, aux_loss, dx_loc, dw_router, *grads, dw2_sum

    return jax.shard_map(
        per_device,
        mesh=mesh,
        in_specs=(row_spec, whole_spec, row_spec, expert_spec, expert_spec, expert_spec, row_spec),
        out_specs=(row_spec, P(), row_spec, whole_spec, expert_spec, expert_spec, expert_spec),
        check_vma=False,
    )
```

```python
import functools

import jax
import jax.numpy as jnp
import numpy as np
from jax import lax
from jax.experimental import pallas as pl
from jax.experimental.pallas import tpu as pltpu
from jax.sharding import PartitionSpec as P


AUX_COEF = 0.01
BLK = 256
TILE = 256
WIN = 128
LANES = 128
ALIGN = 16
NOT_KEPT = -65536.0
VMEM_LIMIT = 63 * 1024 * 1024
CORE, X, Y = 1, 2, 4
FAR = X | Y
HALVES = TENSORS = range(2)
RING = 4
SOURCES = range(8)
FIRST, LAST = 0, -1
SEND, RECV = 0, 1
STAGES = 3
SLOTS = 16
SPLIT = range(4)
LAG = 3
MESH = pl.DeviceIdType.MESH

WHOLE, PARTS = (0, 6), ((0, 3), (3, 3))
GROUPS = (
    [(src, *WHOLE) for src in (FIRST, CORE)],
    [(bit | core, *PARTS[FIRST]) for bit in (X, Y) for core in (FIRST, CORE)],
    [(bit | core, *PARTS[1]) for bit in (X, Y) for core in (FIRST, CORE)],
    [(FAR | core, *part) for part in PARTS for core in (FIRST, CORE)],
)


f32 = jnp.float32
bf16 = jnp.bfloat16
i32 = jnp.int32
ANY = pl.BlockSpec(memory_space=pl.ANY)
SMEM = pl.BlockSpec(memory_space=pltpu.SMEM)
VMEM = pl.BlockSpec(memory_space=pltpu.VMEM)
DMA = pltpu.SemaphoreType.DMA
Shape = jax.ShapeDtypeStruct


def capacity_of(tokens, top_k, experts):
    return (5 * top_k * tokens + 4 * experts - 1) // (4 * experts)


def dot(a, b, ca=1, cb=0):
    return lax.dot_general(a, b, (((ca,), (cb,)), ((), ())), preferred_element_type=f32)


def dot_nt(a, b):
    return dot(a, b, 1, 1)


def dot_tn(a, b):
    return dot(a, b, 0, 0)


def grid_params(dims):
    return pltpu.CompilerParams(dimension_semantics=("arbitrary",) * dims, vmem_limit_bytes=VMEM_LIMIT)


def params():
    return grid_params(1)


def cost(flops, moved):
    return pl.CostEstimate(flops=flops, bytes_accessed=moved, transcendentals=FIRST)


def iota(shape, dim):
    return lax.broadcasted_iota(i32, shape, dim)


def span(start, size, multiple=None):
    return pl.ds(pl.multiple_of(start, multiple or size), size)


def lane_sum(v):
    return jnp.sum(v, axis=1, keepdims=True)


def row_sum(v):
    return jnp.sum(v, axis=0, keepdims=True)


def where0(mask, v):
    return jnp.where(mask, v, jnp.zeros_like(v))


def one_hot(mask):
    return jnp.where(mask, 1.0, 0.0).astype(bf16)


def split3(v):
    hi = v.astype(bf16)
    rest = v - hi.astype(f32)
    mid = rest.astype(bf16)
    return hi, mid, (rest - mid.astype(f32)).astype(bf16)


def loop(start, stop, body):
    def step(i, carry):
        body(i)
        return carry

    lax.fori_loop(start, stop, step, FIRST)


def chosen_mask(ids, experts):
    rows = iota((experts, ids.shape[1]), FIRST)
    return functools.reduce(jnp.logical_or, [rows == ids[j : j + 1, :] for j in range(ids.shape[FIRST])])


def router_kernel(capacity, local, x_ref, w_ref, ids_ref, tab_ref, prob_ref, carry):
    step = pl.program_id(FIRST)
    steps = pl.num_programs(FIRST)
    experts = w_ref.shape[1]

    @pl.when(step == FIRST)
    def _():
        carry[...] = jnp.zeros_like(carry)
        tab_ref[...] = jnp.zeros_like(tab_ref)

    x = x_ref[...]
    hi, mid, low = [dot(x, part) for part in split3(w_ref[...])]
    logits = jnp.transpose(hi + (mid + low))
    expo = jnp.exp(logits - jnp.max(logits, axis=FIRST, keepdims=True))
    prob = expo / row_sum(expo)
    chosen = chosen_mask(ids_ref[...], experts)
    hits = jnp.where(chosen, 1.0, 0.0)
    gate = where0(chosen, prob / row_sum(where0(chosen, prob)))
    earlier = one_hot(iota((BLK, BLK), FIRST) < iota((BLK, BLK), 1))
    before = carry[:, :1]
    pos = dot(hits.astype(bf16), earlier) + before
    pos = jnp.where(chosen & (pos < capacity), pos, NOT_KEPT)
    prob_ref[...] = prob
    after = before + lane_sum(hits)
    lane = iota((experts, LANES), 1)
    first = where0(lane == step, jnp.minimum(before, capacity) + jnp.zeros((experts, LANES), f32))
    first = first + where0((lane == step + 1) & (step == steps - 1), jnp.minimum(after, capacity) + jnp.zeros((experts, LANES), f32))
    stat = where0(lane == FIRST, lane_sum(hits) + jnp.zeros((experts, LANES), f32))
    stat = stat + where0(lane == 1, lane_sum(prob) + jnp.zeros((experts, LANES), f32))
    tail = slice(tab_ref.shape[LAST] - LANES, None)
    for d in range(experts // local):
        rows = slice(d * local, (d + 1) * local)
        tab_ref[d, :local, span(step * BLK, BLK)] = gate[rows]
        tab_ref[d, local:, span(step * BLK, BLK)] = pos[rows]
        tab_ref[d, :local, tail] += stat[rows]
        tab_ref[d, local:, tail] += first[rows]
    carry[:, :1] = after


def run_router(x_loc, w_router, ids_t, capacity, local, devices):
    tokens, d_model = x_loc.shape
    experts = w_router.shape[1]
    top_k = ids_t.shape[FIRST]
    table = (devices, 2 * local, tokens + LANES)
    return pl.pallas_call(
        functools.partial(router_kernel, capacity, local),
        grid=(tokens // BLK,),
        in_specs=[pl.BlockSpec((BLK, d_model), lambda i: (i, FIRST)), VMEM, pl.BlockSpec((top_k, BLK), lambda i: (FIRST, i))],
        out_specs=[VMEM, pl.BlockSpec((experts, BLK), lambda i: (FIRST, i))],
        out_shape=[Shape(table, f32), Shape((experts, tokens), f32)],
        scratch_shapes=[pltpu.VMEM((experts, LANES), f32)],
        compiler_params=params(),
        cost_estimate=cost(2 * tokens * d_model * BLK, 2 * tokens * d_model),
        name="router",
    )(x_loc, w_router, ids_t)


class Blocks:
    def __init__(self, starts_ref, bmap_ref):
        self.starts, self.bmap = starts_ref, bmap_ref

    def info(self, i, e):
        at = self.bmap[2 * i + 1] + e * ALIGN
        first = self.starts[at]
        return self.bmap[2 * i], first, self.starts[at + 1] - first

    def total(self, start, count, e):
        return lax.fori_loop(start, start + count, lambda i, n: n + self.info(i, e)[LAST], i32(FIRST))


def aligned(row):
    base = (row // ALIGN) * ALIGN
    return base, row - base


def window_count(shift, count):
    return (shift + count + WIN - 1) // WIN


def padded(total):
    return (total + TILE - 1) // TILE * TILE


def row_tiles(total, body, size):
    tiles = (total + size - 1 - size // 2) // size
    loop(FIRST, tiles, lambda i: body(i * size, size))
    pl.when(padded(total) > tiles * size)(lambda: body(tiles * size, size // 2))


def start(copies):
    for cp in copies:
        cp.start()


def wait(copies):
    for cp in copies:
        cp.wait()


def taker(refs):
    refs = list(refs)

    def take(n=None):
        got = refs[:n]
        del refs[:n]
        return got

    return take


def block_count(pieces):
    return sum(count for _, _, count in pieces)


def offsets(pieces):
    counts = [count for _, _, count in pieces]
    return [(sum(counts[:k]), count) for k, count in enumerate(counts)]


def block_rows(first, count):
    return pl.ds(first * BLK, count * BLK)


def grad_kernel(g, last, local, pieces, *refs):
    take = taker(refs)
    n = len(pieces)
    starts_ref, bmap_ref, tab_ref = take(3)
    tok_refs = take(n), take(n)
    w1_ref, w3_ref, w2_ref = take(3)
    acc_in = take(2 * bool(g))
    take(3 * bool(g))
    row_outs = take(3)
    outs = take(3 if last else 2)
    xv, dv, xr, dr, acc13, acc2, stage, tok_sem, in_sem, out_sem, row_sem = take()
    accs = acc13, acc2
    e = pl.program_id(FIRST)
    slot = e % 2
    d_model = xv.shape[1]
    d_ff = w1_ref.shape[LAST]
    blocks = Blocks(starts_ref, bmap_ref)
    count = xv.shape[FIRST] // BLK

    parts = [(c, at, first + at) for c, (first, size) in enumerate(offsets(pieces)) for at in range(FIRST, size, 3)]

    def token_copies(k):
        c, at, to = parts[k]
        src_rows, dst_rows = block_rows(at, 3), block_rows(to, 3)
        return [pltpu.make_async_copy(src[c].at[src_rows], dst.at[dst_rows], tok_sem.at[w, k]) for w, (src, dst) in enumerate(zip(tok_refs, (xv, dv)))]

    def in_copies(ee, ss):
        return [pltpu.make_async_copy(src.at[ee], dst.at[ss], in_sem.at[ss, k]) for k, (src, dst) in enumerate(zip(acc_in, accs))]

    def out_copies(ee, ss):
        return [pltpu.make_async_copy(src.at[ss], dst.at[ee], out_sem.at[ss, k]) for k, (src, dst) in enumerate(zip(accs, outs))]

    @pl.when(e == FIRST)
    def _():
        for k in range(len(parts)):
            start(token_copies(k))

    if g:
        pl.when(e == FIRST)(lambda: start(in_copies(e, slot)))
    else:
        pl.when(e >= 2)(lambda: wait(out_copies(e - 2, slot)))
        for acc in accs:
            acc[slot] = jnp.zeros(acc.shape[1:], f32)

    def prefetch():
        if not last:
            pl.when(e > FIRST)(lambda: wait(out_copies(e - 1, 1 - slot)))
        start(in_copies(e + 1, 1 - slot))

    def maybe_prefetch(now):
        if g:
            pl.when(now & (e + 1 < local))(prefetch)

    row_iota = iota((WIN, BLK), FIRST).astype(f32)
    head_row = iota((ALIGN, d_model), FIRST)
    both = tuple(HALVES)

    def dispatch(i, rows_at):
        for k, (_, _, first) in enumerate(parts):
            pl.when((e == FIRST) & (i == first))(lambda: wait(token_copies(k)))
        tok = span(i * BLK, BLK)
        infos = [blocks.info(i, e + q) for q in both]
        places = [aligned(r) for r in rows_at]
        flat = infos[FIRST][FIRST]

        def picks(q, k):
            pos = tab_ref[flat, pl.ds(local + e + q, 1), :]
            gate = tab_ref[flat, pl.ds(e + q, 1), :]
            pick = (pos + (places[q][1] - infos[q][1] - k * WIN).astype(f32)) == row_iota
            return one_hot(pick), lane_sum(where0(pick, gate + jnp.zeros_like(row_iota)))

        def rows_for(one, gate_row):
            return dot(one, xv[tok, :]).astype(bf16), (dot(one, dv[tok, :]) * gate_row).astype(bf16)

        pair = [picks(q, i32(FIRST)) for q in both]
        new = rows_for(*[jnp.concatenate(v, axis=FIRST) for v in zip(*pair)])
        for q in both:
            base, shift = places[q]
            head = span(base, ALIGN)
            for value, rows in zip(new, (xr, dr)):
                value = value[q * WIN : (q + 1) * WIN]
                rows[q, head, :] = jnp.where(head_row < shift, rows[q, head, :], value[:ALIGN])
                rows[q, span(base + ALIGN, WIN - ALIGN, ALIGN), :] = value[ALIGN:]

            def more(k):
                for value, rows in zip(rows_for(*picks(q, k)), (xr, dr)):
                    rows[q, span(base + k * WIN, WIN, ALIGN), :] = value

            loop(1, window_count(shift, infos[q][LAST]), more)
        return tuple(r + info[LAST] for r, info in zip(rows_at, infos))

    @pl.when(slot == FIRST)
    def _():
        totals = lax.fori_loop(FIRST, count, dispatch, (i32(FIRST),) * len(both))
        for q in both:

            def clear(i):
                for rows in (xr, dr):
                    rows[q, span(i * ALIGN, ALIGN), :] = jnp.zeros((ALIGN, d_model), bf16)

            loop((totals[q] + ALIGN - 1) // ALIGN, padded(totals[q]) // ALIGN, clear)

    wait(in_copies(e, slot))

    def tile(at, size):
        maybe_prefetch(at == FIRST)
        rows = span(at, size)
        xt = xr[slot, rows, :]
        dt = dr[slot, rows, :]
        act_a = dot(xt, w1_ref[FIRST])
        act_b = dot(xt, w3_ref[FIRST])
        d_hidden = dot_nt(dt, w2_ref[FIRST]).astype(bf16).astype(f32)
        sig = 1.0 / (1.0 + jnp.exp(-act_a))
        silu = act_a * sig
        hidden = (silu * act_b).astype(bf16)
        d_a = (d_hidden * act_b * sig * (1.0 + act_a * (1.0 - sig))).astype(bf16)
        d_b = (d_hidden * silu).astype(bf16)
        copies = []
        for k, (value, out) in enumerate(zip((hidden, d_a, d_b), row_outs)):
            stage[k, :size] = value
            copies.append(pltpu.make_async_copy(stage.at[k, :size], out.at[g, e, rows], row_sem.at[k]))
        start(copies)
        acc13[slot, :, :d_ff] += dot_tn(xt, d_a)
        acc13[slot, :, d_ff:] += dot_tn(xt, d_b)
        acc2[slot] += dot_tn(hidden, dt)
        wait(copies)

    total = blocks.total(FIRST, count, e)
    maybe_prefetch(total == FIRST)
    row_tiles(total, tile, 2 * TILE)

    if last:
        for out, value in zip(outs, (acc13[slot, :, :d_ff], acc13[slot, :, d_ff:], acc2[slot])):
            out[FIRST] = value.astype(bf16)
    else:
        start(out_copies(e, slot))

        @pl.when(e == pl.num_programs(FIRST) - 1)
        def _():
            wait(out_copies(e - 1, 1 - slot))
            wait(out_copies(e, slot))


def per_expert(*shape):
    return pl.BlockSpec((1, *shape), lambda e: (e,) + (FIRST,) * len(shape))


def block_map(pieces, nb):
    spots = [(src, first + b) for src, first, count in pieces for b in range(count)]
    return np.asarray([v for src, b in spots for v in (src * nb + b, src * 4 * ALIGN + b)], np.int32)


def run_grad(starts, tab, g, xs, ds, weights, acc, rows, nb, row_cap):
    pieces = GROUPS[g]
    last = g == len(GROUPS) - 1
    local, d_model, d_ff = weights[FIRST].shape
    count = block_count(pieces) * BLK
    w_specs = [per_expert(*w.shape[1:]) for w in weights]
    sums = [(local, d_model, 2 * d_ff), (local, d_ff, d_model)]
    row_shape = [Shape((len(GROUPS), local, row_cap, d_ff), bf16)] * 3
    out_shape = row_shape + ([Shape(w.shape, bf16) for w in weights] if last else [Shape(s, f32) for s in sums])
    out_specs = [ANY] * 3 + (w_specs if last else [ANY] * 2)
    tokens = pltpu.VMEM((count, d_model), bf16)
    packed = pltpu.VMEM((2, row_cap + WIN, d_model), bf16)
    ins = [starts, block_map(pieces, nb), tab, *xs, *ds, *weights, *acc, *rows]
    out = pl.pallas_call(
        functools.partial(grad_kernel, g, last, local, pieces),
        grid=(local,),
        in_specs=[SMEM, SMEM, VMEM] + [ANY] * (2 * len(pieces)) + w_specs + [ANY] * (len(acc) + len(rows)),
        out_specs=out_specs,
        out_shape=out_shape,
        scratch_shapes=[tokens, tokens, packed, packed]
        + [pltpu.VMEM((2, *s[1:]), f32) for s in sums]
        + [pltpu.VMEM((3, 2 * TILE, d_ff), bf16), DMA((2, count // (3 * BLK))), DMA((2, 2)), DMA((2, 2)), DMA((3,))],
        input_output_aliases={len(ins) - len(rows) + k: k for k in range(len(rows))},
        compiler_params=params(),
        cost_estimate=cost(12 * count * d_model * d_ff, 40 << 20),
        name="expert_grad",
    )(*ins)
    return out[:3], out[3:]


def group_spans(groups):
    counts = [block_count(GROUPS[g]) for g in groups]
    return np.asarray([v for k, c in enumerate(counts) for v in (sum(counts[:k]), c)], np.int32)


def per_group(groups, *shape):
    return pl.BlockSpec((1, 1, *shape), lambda step, e: (step + groups[FIRST], e) + (FIRST,) * len(shape))


def per_local(*shape):
    return pl.BlockSpec((1, *shape), lambda g, e: (e,) + (FIRST,) * len(shape))


class Combine:
    def __init__(self, local, starts_ref, bmap_ref, spans_ref, tab_ref, rows_ref, out_ref, ring, sems):
        step = pl.program_id(FIRST)
        self.e = pl.program_id(1)
        self.blocks = Blocks(starts_ref, bmap_ref)
        self.first, self.count = spans_ref[2 * step], spans_ref[2 * step + 1]
        self.total = self.blocks.total(self.first, self.count, self.e)
        self.local, self.tab_ref, self.rows_ref = local, tab_ref, rows_ref
        self.out_ref, self.ring, self.sems = out_ref, ring, sems
        self.lane = iota((BLK, WIN), 1).astype(f32)

    def zero_tail(self):
        rows = span(padded(self.total), WIN)
        self.rows_ref[self.e, rows, :] = jnp.zeros((WIN, self.rows_ref.shape[LAST]), bf16)

    def pick(self, ee, k):
        place, info = self.places[ee], self.infos[ee]
        pos = self.tab_t[:, self.local + ee : self.local + ee + 1]
        return one_hot((pos + (place[1] - info[1] - k * WIN).astype(f32)) == self.lane)

    def held(self, ee, k, cols=slice(None)):
        return self.rows_ref[ee, span(self.places[ee][FIRST] + k * WIN, WIN, ALIGN), cols]

    def out_copy(self, i):
        slot = i % RING
        place = self.blocks.bmap[2 * i] - self.blocks.bmap[FIRST]
        return pltpu.make_async_copy(self.ring.at[slot], self.out_ref.at[place], self.sems.at[slot])

    def run(self, simple_body, full_body):
        def block(i, rows_at):
            ee = range(self.local)
            self.infos = [self.blocks.info(i, k) for k in ee]
            self.places = [aligned(r) for r in rows_at]
            self.windows = [window_count(self.places[k][1], self.infos[k][LAST]) for k in ee]
            self.flat = self.infos[FIRST][FIRST]
            self.tab_t = jnp.transpose(self.tab_ref[self.flat])
            self.tok = span((i - self.first) * BLK, BLK)
            pl.when(i - self.first >= RING)(lambda: self.out_copy(i - RING).wait())
            simple = functools.reduce(jnp.logical_and, [w <= 1 for w in self.windows])
            out = self.ring.at[i % RING]
            pl.when(simple)(lambda: simple_body(out))
            pl.when(jnp.logical_not(simple))(lambda: full_body(out))
            self.out_copy(i).start()
            return tuple(r + info[LAST] for r, info in zip(rows_at, self.infos))

        stop = self.first + self.count
        lax.fori_loop(self.first, stop, block, (i32(FIRST),) * self.local)
        loop(stop - RING, stop, lambda i: self.out_copy(i).wait())


def y_kernel(groups, local, starts_ref, bmap_ref, spans_ref, tab_ref, h_ref, w2_ref, *refs):
    take = taker(refs)
    d_refs = [take(len(GROUPS[g])) for g in groups]
    y_ref, dg_ref, o_rows, dv, ring, zacc, yacc, dgacc, tok_sem, out_sem = take()
    all_rows = Combine(local, starts_ref, bmap_ref, spans_ref, tab_ref, o_rows, y_ref, ring, out_sem)
    e = all_rows.e
    d_model = dv.shape[1]

    def token_copies(step):
        spots = offsets(GROUPS[groups[step]])
        return [pltpu.make_async_copy(src, dv.at[block_rows(*spot)], tok_sem.at[c]) for c, (src, spot) in enumerate(zip(d_refs[step], spots))]

    for step in range(len(groups)):
        pl.when((pl.program_id(FIRST) == step) & (e == FIRST))(lambda: start(token_copies(step)))

    def tile(at, size):
        rows = span(at, size)
        o_rows[e, rows, :] = dot(h_ref[FIRST, FIRST, rows, :], w2_ref[FIRST]).astype(bf16)

    row_tiles(all_rows.total, tile, 2 * TILE)
    all_rows.zero_tail()

    @pl.when(e == local - 1)
    def _():
        for step in range(len(groups)):
            pl.when(pl.program_id(FIRST) == step)(lambda: wait(token_copies(step)))
        dg_lane = iota((BLK, LANES), 1)
        width = 2 * LANES
        columns = [slice(k * width, (k + 1) * width) for k in range(d_model // width)]

        def gate(ee):
            return all_rows.tab_t[:, ee : ee + 1]

        def put_dg(sums):
            dg = sum(where0(dg_lane == ee, lane_sum(s) + jnp.zeros((BLK, LANES), f32)) for ee, s in enumerate(sums))
            dg_ref[all_rows.flat - all_rows.blocks.bmap[FIRST]] = jnp.transpose(dg)[: 2 * local, :]

        def simple(out):
            picks = [all_rows.pick(ee, i32(FIRST)) for ee in range(local)]
            sums = [None] * local
            for cols in columns:
                dy = dv[all_rows.tok, cols].astype(f32)
                y = None
                for ee in range(local):
                    z = dot(picks[ee], all_rows.held(ee, i32(FIRST), cols))
                    prod = dy * z
                    part = prod[:, :LANES] + prod[:, LANES:]
                    sums[ee] = part if sums[ee] is None else sums[ee] + part
                    y = gate(ee) * z if y is None else y + gate(ee) * z
                out[:, cols] = y.astype(bf16)
            put_dg(sums)

        def full(out):
            yacc[...] = jnp.zeros_like(yacc)
            for ee in range(local):
                zacc[...] = jnp.zeros_like(zacc)

                def more(k):
                    zacc[...] += dot(all_rows.pick(ee, k), all_rows.held(ee, k))

                loop(FIRST, all_rows.windows[ee], more)
                yacc[...] += gate(ee) * zacc[...]
                dgacc[ee] = lane_sum(dv[all_rows.tok, :].astype(f32) * zacc[...]) * jnp.where(dg_lane == FIRST, 1.0, 0.0)
            out[...] = yacc[...].astype(bf16)
            put_dg([dgacc[ee] for ee in range(local)])

        all_rows.run(simple, full)


def combine_scratch(local, row_cap, d_model):
    return [pltpu.VMEM((local, row_cap + WIN, d_model), bf16)], [pltpu.VMEM((RING, BLK, d_model), bf16), pltpu.VMEM((BLK, d_model), f32)]


def run_y(groups, starts, tab, h_rows, w2, ds, nb):
    local, d_ff, d_model = w2.shape
    row_cap = h_rows.shape[2]
    pieces = [p for g in groups for p in GROUPS[g]]
    spans = group_spans(groups)
    blocks = block_count(pieces)
    rows, work = combine_scratch(local, row_cap, d_model)
    return pl.pallas_call(
        functools.partial(y_kernel, groups, local),
        grid=(len(groups), local),
        in_specs=[SMEM, SMEM, SMEM, VMEM, per_group(groups, row_cap, d_ff), per_local(d_ff, d_model)] + [ANY] * len(pieces),
        out_specs=[ANY, VMEM],
        out_shape=[Shape((blocks, BLK, d_model), bf16), Shape((blocks, 2 * local, BLK), f32)],
        scratch_shapes=rows + [pltpu.VMEM((max(spans[1::2]) * BLK, d_model), bf16)] + work + [work[LAST], pltpu.VMEM((local, BLK, LANES), f32), DMA((4,)), DMA((RING,))],
        compiler_params=grid_params(2),
        cost_estimate=cost(4 * blocks * BLK * d_model * d_ff, 20 << 20),
        name="expert_y",
    )(starts, block_map(pieces, nb), spans, tab, h_rows, w2, *[ds[p] for p in pieces])


def dx_kernel(local, starts_ref, bmap_ref, spans_ref, tab_ref, da_ref, db_ref, w1_ref, w3_ref, dx_ref, o_rows, ring, zacc, out_sem):
    all_rows = Combine(local, starts_ref, bmap_ref, spans_ref, tab_ref, o_rows, dx_ref, ring, out_sem)
    e = all_rows.e

    def tile(at, size):
        rows = span(at, size)
        grad = dot_nt(da_ref[FIRST, FIRST, rows, :], w1_ref[FIRST]) + dot_nt(db_ref[FIRST, FIRST, rows, :], w3_ref[FIRST])
        o_rows[e, rows, :] = grad.astype(bf16)

    row_tiles(all_rows.total, tile, 2 * TILE)
    all_rows.zero_tail()

    @pl.when(e == local - 1)
    def _():
        def simple(out):
            pairs = [(ee, ee + 1) for ee in range(FIRST, local, 2)]
            zero = i32(FIRST)
            sums = [
                dot(jnp.concatenate([all_rows.pick(ee, zero) for ee in pair], axis=1), jnp.concatenate([all_rows.held(ee, zero) for ee in pair], axis=FIRST))
                for pair in pairs
            ]
            out[...] = sum(sums[1:], sums[FIRST]).astype(bf16)

        def full(out):
            zacc[...] = jnp.zeros_like(zacc)
            for ee in range(local):

                def more(k):
                    zacc[...] += dot(all_rows.pick(ee, k), all_rows.held(ee, k))

                loop(FIRST, all_rows.windows[ee], more)
            out[...] = zacc[...].astype(bf16)

        all_rows.run(simple, full)


def run_dx(groups, starts, tab, da_rows, db_rows, w1, w3, nb):
    local, d_model, d_ff = w1.shape
    row_cap = da_rows.shape[2]
    pieces = [p for g in groups for p in GROUPS[g]]
    blocks = block_count(pieces)
    rows, work = combine_scratch(local, row_cap, d_model)
    return pl.pallas_call(
        functools.partial(dx_kernel, local),
        grid=(len(groups), local),
        in_specs=[SMEM, SMEM, SMEM, VMEM] + [per_group(groups, row_cap, d_ff)] * 2 + [per_local(d_model, d_ff)] * 2,
        out_specs=ANY,
        out_shape=Shape((blocks, BLK, d_model), bf16),
        scratch_shapes=rows + work + [DMA((RING,))],
        compiler_params=grid_params(2),
        cost_estimate=cost(6 * blocks * BLK * d_model * d_ff, 20 << 20),
        name="expert_dx",
    )(starts, block_map(pieces, nb), group_spans(groups), tab, da_rows, db_rows, w1, w3)


def router_grad_kernel(scale, x_ref, prob_ref, dg_ref, ids_ref, load_ref, dlog_ref, dw_ref):
    step = pl.program_id(FIRST)
    prob = prob_ref[...]
    dg = dg_ref[...]
    chosen = chosen_mask(ids_ref[...], prob.shape[FIRST])
    gate_sum = row_sum(where0(chosen, prob))
    gate = where0(chosen, prob / gate_sum)
    d_pick = (dg - row_sum(gate * dg)) / gate_sum
    d_prob = where0(chosen, d_pick) + scale * load_ref[:, :1]
    d_logit = prob * (d_prob - row_sum(prob * d_prob))
    dlog_ref[...] = d_logit
    hi, mid, low = [dot(part, x_ref[...]) for part in split3(d_logit)]

    @pl.when(step == FIRST)
    def _():
        dw_ref[...] = jnp.zeros_like(dw_ref)

    dw_ref[...] += hi + (mid + low)


def run_router_grad(x_loc, prob_t, dg_t, ids_t, load, scale):
    tokens, d_model = x_loc.shape
    experts = prob_t.shape[FIRST]
    lanes = lambda n: pl.BlockSpec((n, BLK), lambda i: (FIRST, i))
    return pl.pallas_call(
        functools.partial(router_grad_kernel, scale),
        grid=(tokens // BLK,),
        in_specs=[pl.BlockSpec((BLK, d_model), lambda i: (i, FIRST)), lanes(experts), lanes(experts), lanes(ids_t.shape[FIRST]), VMEM],
        out_specs=[lanes(experts), VMEM],
        out_shape=[Shape((experts, tokens), f32), Shape((experts, d_model), f32)],
        compiler_params=params(),
        cost_estimate=cost(2 * tokens * d_model * BLK, 2 * tokens * d_model),
        name="router_grad",
    )(x_loc, prob_t, dg_t, ids_t, load)


def final_kernel(dlog_ref, wt_ref, *refs):
    take = taker(refs)
    y_terms, dx_terms = [[ref[...].astype(f32) for ref in take(3)] for _ in TENSORS]
    y_ref, dx_ref = take()
    lhs = split3(dlog_ref[...])
    rhs = split3(wt_ref[...])
    terms = [(i, j) for i in range(3) for j in range(3 - i)]
    left = jnp.concatenate([lhs[i] for i, _ in terms], axis=FIRST)
    right = jnp.concatenate([rhs[j] for _, j in terms], axis=FIRST)
    dx_ref[...] = (dot_tn(left, right) + sum(dx_terms[1:], dx_terms[FIRST])).astype(bf16)
    y_ref[...] = sum(y_terms[1:], y_terms[FIRST]).astype(bf16)


def run_final(dlog_t, w_t, y_terms, dx_terms):
    experts, tokens = dlog_t.shape
    d_model = w_t.shape[1]
    size = tokens // 4
    rows = pl.BlockSpec((size, d_model), lambda i: (i, FIRST))
    return pl.pallas_call(
        final_kernel,
        grid=(tokens // size,),
        in_specs=[pl.BlockSpec((experts, size), lambda i: (FIRST, i)), VMEM] + [rows] * len([*y_terms, *dx_terms]),
        out_specs=[rows] * 2,
        out_shape=[Shape((tokens, d_model), bf16)] * 2,
        compiler_params=params(),
        cost_estimate=cost(2 * tokens * d_model * BLK, 16 * tokens * d_model),
        name="final",
    )(dlog_t, w_t, *y_terms, *dx_terms)


NEAR = (X, Y)
RELAYED = {(Y, 0): 0, (X, 1): 1}
OPS = [
    (t, src, h)
    for step in ([(FAR, 0), (FAR, 1)], [(X, 0), (Y, 1)], [(X, 1), (Y, 0)], [(FIRST, 0), (FIRST, 1)])
    for t in TENSORS
    for src, h in step
]


def add_rows(dst, src):
    step = min(LANES, dst.shape[FIRST])

    def body(i):
        rows = span(i * step, step)
        dst[rows, :] = (dst[rows, :].astype(f32) + src[rows, :].astype(f32)).astype(bf16)

    loop(FIRST, dst.shape[FIRST] // step, body)


def exchange_kernel(half, mats, *refs):
    take = taker(refs)
    parts = [take(2) for _ in TENSORS]
    dws = take(mats)
    outs = [take(len(NEAR) + 1) for _ in TENSORS]
    dw_outs = take(mats)
    land, far_land, stage, z_one, z_two, z_stage = take(6)
    core_sem, stage_sem, far_sem, near_sem, own_sem, z_sem, keep_sem, load_sem, credit_one, credit_two = take()

    me = lax.axis_index("ep")
    z = lax.axis_index("dp")
    peer = {bit: me + bit - 2 * bit * ((me // bit) % 2) for bit in (CORE, X, Y)}
    z_peer = z + 1 - 2 * (z % 2)
    z_cross = 3 - z
    is_end = (z % 3) == FIRST
    is_mid = (z % 3) != FIRST

    barrier = pltpu.get_barrier_semaphore()
    ids = [{"ep": p} for p in peer.values()] + [{"dp": z_peer}, {"dp": z_cross}]
    for device in ids:
        pl.semaphore_signal(barrier, device_id=device, device_id_type=MESH)
    pl.semaphore_wait(barrier, len(ids))

    def remote(src, dst, sems, at, device):
        send, recv = sems.at[(SEND, *at)], sems.at[(RECV, *at)]
        return pltpu.make_async_remote_copy(src_ref=src, dst_ref=dst, send_sem=send, recv_sem=recv, device_id=device, device_id_type=MESH)

    def rows_at(h):
        return pl.ds(h * half, half)

    def part(t, src, h):
        own, rest = parts[t]
        return own.at[src, rows_at(h)] if src <= CORE else rest.at[src - 2, rows_at(h)]

    def core_copy(i):
        t, src, h = OPS[i]
        return remote(part(t, src | CORE, h), land.at[i], core_sem, (i,), {"ep": peer[CORE]})

    def stage_copy(i):
        t, src, h = OPS[i]
        return pltpu.make_async_copy(part(t, src, h), stage.at[i % STAGES], stage_sem.at[i % STAGES])

    def far_copy(i):
        t, _, h = OPS[i]
        return remote(land.at[i], far_land.at[t, h], far_sem, (t, h), {"ep": peer[NEAR[h]]})

    def near_copy(i):
        t, src, h = OPS[i]
        k = NEAR.index(src)
        return remote(land.at[i], outs[t][k].at[rows_at(h)], near_sem, (t, k, h), {"ep": peer[src]})

    def own_copy(i):
        t, _, h = OPS[i]
        return pltpu.make_async_copy(land.at[i], outs[t][LAST].at[rows_at(h)], own_sem.at[t, h])

    def out_copy(i):
        src = OPS[i][1]
        return (far_copy if src == FAR else near_copy if src else own_copy)(i)

    def reduce_op(i):
        t, src, h = OPS[i]
        stage_copy(i).wait()
        core_copy(i).wait_recv()
        add_rows(land.at[i], stage.at[i % STAGES])
        if i + STAGES < len(OPS):
            stage_copy(i + STAGES).start()
        if (src, h) in RELAYED:
            far_copy(OPS.index((t, FAR, RELAYED[src, h]))).wait_recv()
            add_rows(land.at[i], far_land.at[t, RELAYED[src, h]])

    rows_per = z_one.shape[1]
    chunks = [(m, e, k) for e in range(dws[FIRST].shape[FIRST]) for m in range(mats) for k in SPLIT]
    n = len(chunks)

    def piece(arrays, c):
        m, e, k = chunks[c]
        return arrays[m].at[e, pl.ds(k * rows_per, rows_per)]

    def one_copy(c):
        return remote(piece(dws, c), z_one.at[c % SLOTS], z_sem, (FIRST, c), {"dp": z_peer})

    def two_copy(c):
        return remote(z_one.at[c % SLOTS], z_two.at[c % SLOTS], z_sem, (1, c), {"dp": z_cross})

    def three_copy(c):
        return remote(z_two.at[c % SLOTS], piece(dw_outs, c), z_sem, (2, c), {"dp": z_peer})

    def keep_copy(c):
        return pltpu.make_async_copy(z_two.at[c % SLOTS], piece(dw_outs, c), keep_sem.at[c])

    def load_copy(c):
        return pltpu.make_async_copy(piece(dws, c), z_stage.at[c % STAGES], load_sem.at[c % STAGES])

    def first_add(c):
        load_copy(c).wait()
        one_copy(c).wait_recv()
        add_rows(z_one.at[c % SLOTS], z_stage.at[c % STAGES])
        if c + STAGES < n:
            load_copy(c + STAGES).start()

    def second_add(c):
        two_copy(c).wait()
        add_rows(z_two.at[c % SLOTS], z_one.at[c % SLOTS])
        if c + SLOTS < n:
            pl.semaphore_signal(credit_one, device_id={"dp": z_peer}, device_id_type=MESH)

    def retire(c):
        three_copy(c).wait_send()
        keep_copy(c).wait()
        if c + SLOTS < n:
            pl.semaphore_signal(credit_two, device_id={"dp": z_cross}, device_id_type=MESH)

    @pl.when(is_end)
    def _():
        for c in range(SLOTS):
            one_copy(c).start()

    @pl.when(is_mid)
    def _():
        for c in range(STAGES):
            load_copy(c).start()

    for i in range(len(OPS)):
        core_copy(i).start()
        if i < STAGES:
            stage_copy(i).start()

    todo = list(range(len(OPS)))
    for tick in range(n + LAG):
        mine = todo[: 2 if tick < 2 else tick % 2]
        todo = todo[len(mine) :]
        for i in mine:
            reduce_op(i)

        @pl.when(is_mid)
        def _():
            back = tick - 1
            if tick < n:
                first_add(tick)
            if back in range(n):
                second_add(back)
            if tick < n:
                if tick >= SLOTS:
                    pl.semaphore_wait(credit_two, 1)
                two_copy(tick).start()
            if back in range(n):
                three_copy(back).start()
                keep_copy(back).start()
            if tick >= LAG:
                retire(tick - LAG)

        for i in mine:
            out_copy(i).start()

        @pl.when(is_end)
        def _():
            if tick + SLOTS < n:
                pl.semaphore_wait(credit_one, 1)
                one_copy(tick + SLOTS).start()

    for i in todo:
        reduce_op(i)
        out_copy(i).start()

    @pl.when(is_end)
    def _():
        for c in range(n):
            one_copy(c).wait_send()
            three_copy(c).wait_recv()

    for i in range(len(OPS)):
        core_copy(i).wait_send()
        (out_copy(i).wait_send if OPS[i][1] == FAR else out_copy(i).wait)()


def run_exchange(parts, dws):
    tokens, d_model = parts[FIRST][FIRST].shape[1:]
    half = tokens // 2
    local, rows, cols = dws[FIRST].shape
    chunk = (rows // len(SPLIT), cols)
    n = local * len(dws) * len(SPLIT)
    whole = Shape((tokens, d_model), bf16)
    flat = [v for tensor in parts for v in tensor] + list(dws)
    terms = len(NEAR) + 1
    out = pl.pallas_call(
        functools.partial(exchange_kernel, half, len(dws)),
        in_specs=[ANY] * len(flat),
        out_specs=[ANY] * (terms * len(TENSORS) + len(dws)),
        out_shape=[whole] * (terms * len(TENSORS)) + [Shape(v.shape, bf16) for v in dws],
        scratch_shapes=[
            pltpu.VMEM((len(OPS), half, d_model), bf16),
            pltpu.VMEM((len(TENSORS), len(HALVES), half, d_model), bf16),
            pltpu.VMEM((STAGES, half, d_model), bf16),
            pltpu.VMEM((SLOTS, *chunk), bf16),
            pltpu.VMEM((SLOTS, *chunk), bf16),
            pltpu.VMEM((STAGES, *chunk), bf16),
            DMA((2, len(OPS))),
            DMA((STAGES,)),
            DMA((2, 2, 2)),
            DMA((2, 2, 2, 2)),
            DMA((2, 2)),
            DMA((2, 3, n)),
            DMA((n,)),
            DMA((STAGES,)),
            pltpu.SemaphoreType.REGULAR,
            pltpu.SemaphoreType.REGULAR,
        ],
        compiler_params=pltpu.CompilerParams(vmem_limit_bytes=VMEM_LIMIT, collective_id=FIRST, has_side_effects=True),
        cost_estimate=cost(1 << 37, 200 << 20),
        name="exchange",
    )(*flat)
    return [out[:terms], out[terms : 2 * terms]], out[2 * terms :]


def hop(v, bit):
    return lax.ppermute(v, "ep", [(i, i ^ bit) for i in SOURCES])


def after(values, token):
    return lax.optimization_barrier((values, token))[FIRST]


def send_own(v):
    pieces = [v[first * BLK : (first + count) * BLK] for first, count in PARTS]
    got = {(FIRST, *WHOLE): v, (CORE, *WHOLE): hop(v, CORE)}
    for part, piece in zip(PARTS, pieces):
        got.update({(bit, *part): hop(piece, bit) for bit in NEAR})
    return got, pieces


def pass_on(got, h):
    part = PARTS[h]
    got[FAR, *part] = hop(got[(Y, X)[h], *part], NEAR[h])
    for bit in NEAR:
        got[bit | CORE, *part] = hop(got[bit, *part], CORE)


def relative(v, me):
    shape = v.shape
    v = v.reshape((2, 2, 2) + shape[1:])
    for axis, bit in enumerate((Y, X, CORE)):
        v = jnp.where((me & bit) != FIRST, jnp.flip(v, axis), v)
    return v.reshape(shape)


def solution(mesh):
    dp_size = mesh.shape["dp"]
    ep_size = mesh.shape["ep"]
    row_spec = P(("dp", "ep"), None)
    expert_spec = P("ep", None, None)
    whole_spec = P(None, None)

    def per_device(x_loc, w_router, ids_loc, w1, w3, w2, dy_loc):
        tokens, d_model = x_loc.shape
        top_k = ids_loc.shape[1]
        experts = w_router.shape[1]
        local = w1.shape[FIRST]
        capacity = capacity_of(tokens, top_k, experts)
        n_total = tokens * dp_size * ep_size
        nb = tokens // BLK
        row_cap = padded(4 * capacity)
        me = lax.axis_index("ep")

        gathered, pieces = zip(*[send_own(v) for v in (x_loc, dy_loc)])

        ids_t, x_router = after((ids_loc.T, x_loc), pieces)
        send_tab, prob_t = run_router(x_router, w_router, ids_t, capacity, local, ep_size)
        tab_rel = relative(lax.all_to_all(send_tab, "ep", FIRST, FIRST, tiled=True), me)
        tab = tab_rel[:, :, :tokens].reshape(ep_size, 2 * local, nb, BLK).transpose(0, 2, 1, 3).reshape(ep_size * nb, 2 * local, BLK)
        starts = tab_rel[:, local:, tokens : tokens + ALIGN].astype(i32).reshape(LAST)

        def y_of(groups, starts):
            return run_y(groups, starts, tab, rows[FIRST], w2, gathered[1], nb)

        def dx_of(groups, starts):
            return run_dx(groups, starts, tab, rows[1], rows[2], w1, w3, nb)

        acc = rows = ()
        own, rest = (FIRST,), (1, 2, 3)
        for g, group in enumerate(GROUPS):
            if g:
                ready = [p for p in group if not p[FIRST] & CORE]
                for got in gathered:
                    got.update(after({p: got[p] for p in ready}, acc[LAST]))
                for got in gathered:
                    if g < len(GROUPS) - 1:
                        pass_on(got, g - 1)
                    else:
                        for src, *part in ready:
                            got[src | CORE, *part] = hop(got[src, *part], CORE)
                here = after(starts, [[got[p] for p in ready] for got in gathered])
                if g == 2:
                    y_own, dg_own = y_of(own, here)
                    starts = after(starts, dg_own)
                if g > 2:
                    dx_own = dx_of(own, here)
                    starts = after(starts, dx_own)
            rows, acc = run_grad(starts, tab, g, *[[got[p] for p in group] for got in gathered], (w1, w3, w2), acc, rows, nb, row_cap)
            if not g:
                stats = jnp.sum(after(tab_rel[:, :local, tokens:], acc[LAST]), axis=FIRST)
                for step in (1, 2):
                    stats = stats + lax.ppermute(stats, "dp", [(i, i ^ step) for i in range(dp_size)])
                starts = after(starts, stats)
        dw1, dw3, dw2 = acc
        starts, dw2 = lax.optimization_barrier((starts, dw2))
        dw2_sum = lax.psum(dw2, "dp")

        y_rest, dg_rest = y_of(rest, starts)
        dg = jnp.concatenate([dg_own, dg_rest], axis=FIRST)
        dg = dg[:, :local].reshape(ep_size, nb, local, BLK).transpose(0, 2, 1, 3).reshape(ep_size, local, tokens)
        dg = jnp.concatenate([relative(dg, me), jnp.broadcast_to(stats, (ep_size, *stats.shape))], axis=2)
        starts, dg = lax.optimization_barrier((starts, dg))
        dx_rest = dx_of(rest, starts)
        dg_all = lax.all_to_all(dg, "ep", FIRST, FIRST, tiled=True).reshape(experts, tokens + LANES)
        load = dg_all[:, tokens:]
        share = AUX_COEF * experts / (n_total * top_k * n_total)
        aux_loss = share * jnp.sum(load[:, FIRST] * load[:, 1])
        dlog_t, dwr_t = run_router_grad(x_loc, prob_t, dg_all[:, :tokens], ids_t, load, share)
        dw_router = lax.psum(dwr_t, ("dp", "ep")).T

        parts = [[v.reshape(LAST, tokens, d_model) for v in pair] for pair in ((y_own, y_rest), (dx_own, dx_rest))]
        sums, grads = run_exchange(parts, [dw1, dw3])
        y_loc, dx_loc = run_final(dlog_t, w_router.T, *sums)
        return y_loc, aux_loss, dx_loc, dw_router, *grads, dw2_sum

    return jax.shard_map(
        per_device,
        mesh=mesh,
        in_specs=(row_spec, whole_spec, row_spec, expert_spec, expert_spec, expert_spec, row_spec),
        out_specs=(row_spec, P(), row_spec, whole_spec, expert_spec, expert_spec, expert_spec),
        check_vma=False,
    )
```

```python
import functools

import jax
import jax.numpy as jnp
import numpy as np
from jax import lax
from jax.experimental import pallas as pl
from jax.experimental.pallas import tpu as pltpu
from jax.sharding import PartitionSpec as P


AUX_COEF = 0.01
BLK = 256
TILE = 256
WIN = 128
LANES = 128
ALIGN = 16
NOT_KEPT = -65536.0
VMEM_LIMIT = 63 * 1024 * 1024
CORE, X, Y = 1, 2, 4
FAR = X | Y
HALVES = TENSORS = range(2)
RING = 4
SOURCES = range(8)
FIRST, LAST = 0, -1
SEND, RECV = 0, 1
STAGES = 3
SLOTS = 16
SPLIT = range(4)
BACK, LAG = 2, 4
MESH = pl.DeviceIdType.MESH

WHOLE, PARTS = (0, 6), ((0, 3), (3, 3))
GROUPS = (
    [(src, *WHOLE) for src in (FIRST, CORE)],
    [(bit | core, *PARTS[FIRST]) for bit in (X, Y) for core in (FIRST, CORE)],
    [(bit | core, *PARTS[1]) for bit in (X, Y) for core in (FIRST, CORE)],
    [(FAR | core, *part) for part in PARTS for core in (FIRST, CORE)],
)


f32 = jnp.float32
bf16 = jnp.bfloat16
i32 = jnp.int32
ANY = pl.BlockSpec(memory_space=pl.ANY)
SMEM = pl.BlockSpec(memory_space=pltpu.SMEM)
VMEM = pl.BlockSpec(memory_space=pltpu.VMEM)
DMA = pltpu.SemaphoreType.DMA
Shape = jax.ShapeDtypeStruct


def capacity_of(tokens, top_k, experts):
    return (5 * top_k * tokens + 4 * experts - 1) // (4 * experts)


def dot(a, b, ca=1, cb=0):
    return lax.dot_general(a, b, (((ca,), (cb,)), ((), ())), preferred_element_type=f32)


def dot_nt(a, b):
    return dot(a, b, 1, 1)


def dot_tn(a, b):
    return dot(a, b, 0, 0)


def grid_params(dims):
    return pltpu.CompilerParams(dimension_semantics=("arbitrary",) * dims, vmem_limit_bytes=VMEM_LIMIT)


def params():
    return grid_params(1)


def cost(flops, moved):
    return pl.CostEstimate(flops=flops, bytes_accessed=moved, transcendentals=FIRST)


def iota(shape, dim):
    return lax.broadcasted_iota(i32, shape, dim)


def span(start, size, multiple=None):
    return pl.ds(pl.multiple_of(start, multiple or size), size)


def lane_sum(v):
    return jnp.sum(v, axis=1, keepdims=True)


def row_sum(v):
    return jnp.sum(v, axis=0, keepdims=True)


def where0(mask, v):
    return jnp.where(mask, v, jnp.zeros_like(v))


def one_hot(mask):
    return jnp.where(mask, 1.0, 0.0).astype(bf16)


def split3(v):
    hi = v.astype(bf16)
    rest = v - hi.astype(f32)
    mid = rest.astype(bf16)
    return hi, mid, (rest - mid.astype(f32)).astype(bf16)


def loop(start, stop, body):
    def step(i, carry):
        body(i)
        return carry

    lax.fori_loop(start, stop, step, FIRST)


def chosen_mask(ids, experts):
    rows = iota((experts, ids.shape[1]), FIRST)
    return functools.reduce(jnp.logical_or, [rows == ids[j : j + 1, :] for j in range(ids.shape[FIRST])])


def router_kernel(capacity, local, x_ref, w_ref, ids_ref, tab_ref, prob_ref, carry):
    step = pl.program_id(FIRST)
    steps = pl.num_programs(FIRST)
    experts = w_ref.shape[1]

    @pl.when(step == FIRST)
    def _():
        carry[...] = jnp.zeros_like(carry)
        tab_ref[...] = jnp.zeros_like(tab_ref)

    x = x_ref[...]
    hi, mid, low = [dot(x, part) for part in split3(w_ref[...])]
    logits = jnp.transpose(hi + (mid + low))
    expo = jnp.exp(logits - jnp.max(logits, axis=FIRST, keepdims=True))
    prob = expo / row_sum(expo)
    chosen = chosen_mask(ids_ref[...], experts)
    hits = jnp.where(chosen, 1.0, 0.0)
    gate = where0(chosen, prob / row_sum(where0(chosen, prob)))
    earlier = one_hot(iota((BLK, BLK), FIRST) < iota((BLK, BLK), 1))
    before = carry[:, :1]
    pos = dot(hits.astype(bf16), earlier) + before
    pos = jnp.where(chosen & (pos < capacity), pos, NOT_KEPT)
    prob_ref[...] = prob
    after = before + lane_sum(hits)
    lane = iota((experts, LANES), 1)
    first = where0(lane == step, jnp.minimum(before, capacity) + jnp.zeros((experts, LANES), f32))
    first = first + where0((lane == step + 1) & (step == steps - 1), jnp.minimum(after, capacity) + jnp.zeros((experts, LANES), f32))
    stat = where0(lane == FIRST, lane_sum(hits) + jnp.zeros((experts, LANES), f32))
    stat = stat + where0(lane == 1, lane_sum(prob) + jnp.zeros((experts, LANES), f32))
    tail = slice(tab_ref.shape[LAST] - LANES, None)
    for d in range(experts // local):
        rows = slice(d * local, (d + 1) * local)
        tab_ref[d, :local, span(step * BLK, BLK)] = gate[rows]
        tab_ref[d, local:, span(step * BLK, BLK)] = pos[rows]
        tab_ref[d, :local, tail] += stat[rows]
        tab_ref[d, local:, tail] += first[rows]
    carry[:, :1] = after


def run_router(x_loc, w_router, ids_t, capacity, local, devices):
    tokens, d_model = x_loc.shape
    experts = w_router.shape[1]
    top_k = ids_t.shape[FIRST]
    table = (devices, 2 * local, tokens + LANES)
    return pl.pallas_call(
        functools.partial(router_kernel, capacity, local),
        grid=(tokens // BLK,),
        in_specs=[pl.BlockSpec((BLK, d_model), lambda i: (i, FIRST)), VMEM, pl.BlockSpec((top_k, BLK), lambda i: (FIRST, i))],
        out_specs=[VMEM, pl.BlockSpec((experts, BLK), lambda i: (FIRST, i))],
        out_shape=[Shape(table, f32), Shape((experts, tokens), f32)],
        scratch_shapes=[pltpu.VMEM((experts, LANES), f32)],
        compiler_params=params(),
        cost_estimate=cost(2 * tokens * d_model * BLK, 2 * tokens * d_model),
        name="router",
    )(x_loc, w_router, ids_t)


class Blocks:
    def __init__(self, starts_ref, bmap_ref):
        self.starts, self.bmap = starts_ref, bmap_ref

    def info(self, i, e):
        at = self.bmap[2 * i + 1] + e * ALIGN
        first = self.starts[at]
        return self.bmap[2 * i], first, self.starts[at + 1] - first

    def total(self, start, count, e):
        return lax.fori_loop(start, start + count, lambda i, n: n + self.info(i, e)[LAST], i32(FIRST))


def aligned(row):
    base = (row // ALIGN) * ALIGN
    return base, row - base


def window_count(shift, count):
    return (shift + count + WIN - 1) // WIN


def padded(total):
    return (total + TILE - 1) // TILE * TILE


def row_tiles(total, body, size):
    tiles = (total + size - 1 - size // 2) // size
    loop(FIRST, tiles, lambda i: body(i * size, size))
    pl.when(padded(total) > tiles * size)(lambda: body(tiles * size, size // 2))


def start(copies):
    for cp in copies:
        cp.start()


def wait(copies):
    for cp in copies:
        cp.wait()


def taker(refs):
    refs = list(refs)

    def take(n=None):
        got = refs[:n]
        del refs[:n]
        return got

    return take


def block_count(pieces):
    return sum(count for _, _, count in pieces)


def offsets(pieces):
    counts = [count for _, _, count in pieces]
    return [(sum(counts[:k]), count) for k, count in enumerate(counts)]


def block_rows(first, count):
    return pl.ds(first * BLK, count * BLK)


def grad_kernel(g, last, local, pieces, *refs):
    take = taker(refs)
    n = len(pieces)
    starts_ref, bmap_ref, tab_ref = take(3)
    tok_refs = take(n), take(n)
    w1_ref, w3_ref, w2_ref = take(3)
    acc_in = take(2 * bool(g))
    take(3 * bool(g))
    row_outs = take(3)
    outs = take(3 if last else 2)
    xv, dv, xr, dr, acc13, acc2, stage, tok_sem, in_sem, out_sem, row_sem = take()
    accs = acc13, acc2
    e = pl.program_id(FIRST)
    slot = e % 2
    d_model = xv.shape[1]
    d_ff = w1_ref.shape[LAST]
    blocks = Blocks(starts_ref, bmap_ref)
    count = xv.shape[FIRST] // BLK

    parts = [(c, at, first + at) for c, (first, size) in enumerate(offsets(pieces)) for at in range(FIRST, size, 3)]

    def token_copies(k):
        c, at, to = parts[k]
        src_rows, dst_rows = block_rows(at, 3), block_rows(to, 3)
        return [pltpu.make_async_copy(src[c].at[src_rows], dst.at[dst_rows], tok_sem.at[w, k]) for w, (src, dst) in enumerate(zip(tok_refs, (xv, dv)))]

    def in_copies(ee, ss):
        return [pltpu.make_async_copy(src.at[ee], dst.at[ss], in_sem.at[ss, k]) for k, (src, dst) in enumerate(zip(acc_in, accs))]

    def out_copies(ee, ss):
        return [pltpu.make_async_copy(src.at[ss], dst.at[ee], out_sem.at[ss, k]) for k, (src, dst) in enumerate(zip(accs, outs))]

    @pl.when(e == FIRST)
    def _():
        for k in range(len(parts)):
            start(token_copies(k))

    if g:
        pl.when(e == FIRST)(lambda: start(in_copies(e, slot)))
    else:
        pl.when(e >= 2)(lambda: wait(out_copies(e - 2, slot)))
        for acc in accs:
            acc[slot] = jnp.zeros(acc.shape[1:], f32)

    def prefetch():
        if not last:
            pl.when(e > FIRST)(lambda: wait(out_copies(e - 1, 1 - slot)))
        start(in_copies(e + 1, 1 - slot))

    def maybe_prefetch(now):
        if g:
            pl.when(now & (e + 1 < local))(prefetch)

    row_iota = iota((WIN, BLK), FIRST).astype(f32)
    head_row = iota((ALIGN, d_model), FIRST)
    both = tuple(HALVES)

    def dispatch(i, rows_at):
        for k, (_, _, first) in enumerate(parts):
            pl.when((e == FIRST) & (i == first))(lambda: wait(token_copies(k)))
        tok = span(i * BLK, BLK)
        infos = [blocks.info(i, e + q) for q in both]
        places = [aligned(r) for r in rows_at]
        flat = infos[FIRST][FIRST]

        def picks(q, k):
            pos = tab_ref[flat, pl.ds(local + e + q, 1), :]
            gate = tab_ref[flat, pl.ds(e + q, 1), :]
            pick = (pos + (places[q][1] - infos[q][1] - k * WIN).astype(f32)) == row_iota
            return one_hot(pick), lane_sum(where0(pick, gate + jnp.zeros_like(row_iota)))

        def rows_for(one, gate_row):
            return dot(one, xv[tok, :]).astype(bf16), (dot(one, dv[tok, :]) * gate_row).astype(bf16)

        pair = [picks(q, i32(FIRST)) for q in both]
        new = rows_for(*[jnp.concatenate(v, axis=FIRST) for v in zip(*pair)])
        for q in both:
            base, shift = places[q]
            head = span(base, ALIGN)
            for value, rows in zip(new, (xr, dr)):
                value = value[q * WIN : (q + 1) * WIN]
                rows[q, head, :] = jnp.where(head_row < shift, rows[q, head, :], value[:ALIGN])
                rows[q, span(base + ALIGN, WIN - ALIGN, ALIGN), :] = value[ALIGN:]

            def more(k):
                for value, rows in zip(rows_for(*picks(q, k)), (xr, dr)):
                    rows[q, span(base + k * WIN, WIN, ALIGN), :] = value

            loop(1, window_count(shift, infos[q][LAST]), more)
        return tuple(r + info[LAST] for r, info in zip(rows_at, infos))

    @pl.when(slot == FIRST)
    def _():
        totals = lax.fori_loop(FIRST, count, dispatch, (i32(FIRST),) * len(both))
        for q in both:

            def clear(i):
                for rows in (xr, dr):
                    rows[q, span(i * ALIGN, ALIGN), :] = jnp.zeros((ALIGN, d_model), bf16)

            loop((totals[q] + ALIGN - 1) // ALIGN, padded(totals[q]) // ALIGN, clear)

    wait(in_copies(e, slot))

    def tile(at, size):
        maybe_prefetch(at == FIRST)
        rows = span(at, size)
        xt = xr[slot, rows, :]
        dt = dr[slot, rows, :]
        act_a = dot(xt, w1_ref[FIRST])
        act_b = dot(xt, w3_ref[FIRST])
        d_hidden = dot_nt(dt, w2_ref[FIRST]).astype(bf16).astype(f32)
        sig = 1.0 / (1.0 + jnp.exp(-act_a))
        silu = act_a * sig
        hidden = (silu * act_b).astype(bf16)
        d_a = (d_hidden * act_b * sig * (1.0 + act_a * (1.0 - sig))).astype(bf16)
        d_b = (d_hidden * silu).astype(bf16)
        copies = []
        for k, (value, out) in enumerate(zip((hidden, d_a, d_b), row_outs)):
            stage[k, :size] = value
            copies.append(pltpu.make_async_copy(stage.at[k, :size], out.at[g, e, rows], row_sem.at[k]))
        start(copies)
        acc13[slot, :, :d_ff] += dot_tn(xt, d_a)
        acc13[slot, :, d_ff:] += dot_tn(xt, d_b)
        acc2[slot] += dot_tn(hidden, dt)
        wait(copies)

    total = blocks.total(FIRST, count, e)
    maybe_prefetch(total == FIRST)
    row_tiles(total, tile, 2 * TILE)

    if last:
        for out, value in zip(outs, (acc13[slot, :, :d_ff], acc13[slot, :, d_ff:], acc2[slot])):
            out[FIRST] = value.astype(bf16)
    else:
        start(out_copies(e, slot))

        @pl.when(e == pl.num_programs(FIRST) - 1)
        def _():
            wait(out_copies(e - 1, 1 - slot))
            wait(out_copies(e, slot))


def per_expert(*shape):
    return pl.BlockSpec((1, *shape), lambda e: (e,) + (FIRST,) * len(shape))


def block_map(pieces, nb):
    spots = [(src, first + b) for src, first, count in pieces for b in range(count)]
    return np.asarray([v for src, b in spots for v in (src * nb + b, src * 4 * ALIGN + b)], np.int32)


def run_grad(starts, tab, g, xs, ds, weights, acc, rows, nb, row_cap):
    pieces = GROUPS[g]
    last = g == len(GROUPS) - 1
    local, d_model, d_ff = weights[FIRST].shape
    count = block_count(pieces) * BLK
    w_specs = [per_expert(*w.shape[1:]) for w in weights]
    sums = [(local, d_model, 2 * d_ff), (local, d_ff, d_model)]
    row_shape = [Shape((len(GROUPS), local, row_cap, d_ff), bf16)] * 3
    out_shape = row_shape + ([Shape(w.shape, bf16) for w in weights] if last else [Shape(s, f32) for s in sums])
    out_specs = [ANY] * 3 + (w_specs if last else [ANY] * 2)
    tokens = pltpu.VMEM((count, d_model), bf16)
    packed = pltpu.VMEM((2, row_cap + WIN, d_model), bf16)
    ins = [starts, block_map(pieces, nb), tab, *xs, *ds, *weights, *acc, *rows]
    out = pl.pallas_call(
        functools.partial(grad_kernel, g, last, local, pieces),
        grid=(local,),
        in_specs=[SMEM, SMEM, VMEM] + [ANY] * (2 * len(pieces)) + w_specs + [ANY] * (len(acc) + len(rows)),
        out_specs=out_specs,
        out_shape=out_shape,
        scratch_shapes=[tokens, tokens, packed, packed]
        + [pltpu.VMEM((2, *s[1:]), f32) for s in sums]
        + [pltpu.VMEM((3, 2 * TILE, d_ff), bf16), DMA((2, count // (3 * BLK))), DMA((2, 2)), DMA((2, 2)), DMA((3,))],
        input_output_aliases={len(ins) - len(rows) + k: k for k in range(len(rows))},
        compiler_params=params(),
        cost_estimate=cost(12 * count * d_model * d_ff, 40 << 20),
        name="expert_grad",
    )(*ins)
    return out[:3], out[3:]


def group_spans(groups):
    counts = [block_count(GROUPS[g]) for g in groups]
    return np.asarray([v for k, c in enumerate(counts) for v in (sum(counts[:k]), c)], np.int32)


def per_group(groups, *shape):
    return pl.BlockSpec((1, 1, *shape), lambda step, e: (step + groups[FIRST], e) + (FIRST,) * len(shape))


def per_local(*shape):
    return pl.BlockSpec((1, *shape), lambda g, e: (e,) + (FIRST,) * len(shape))


class Combine:
    def __init__(self, local, starts_ref, bmap_ref, spans_ref, tab_ref, rows_ref, out_ref, ring, sems):
        step = pl.program_id(FIRST)
        self.e = pl.program_id(1)
        self.blocks = Blocks(starts_ref, bmap_ref)
        self.first, self.count = spans_ref[2 * step], spans_ref[2 * step + 1]
        self.total = self.blocks.total(self.first, self.count, self.e)
        self.local, self.tab_ref, self.rows_ref = local, tab_ref, rows_ref
        self.out_ref, self.ring, self.sems = out_ref, ring, sems
        self.lane = iota((BLK, WIN), 1).astype(f32)

    def zero_tail(self):
        rows = span(padded(self.total), WIN)
        self.rows_ref[self.e, rows, :] = jnp.zeros((WIN, self.rows_ref.shape[LAST]), bf16)

    def pick(self, ee, k):
        place, info = self.places[ee], self.infos[ee]
        pos = self.tab_t[:, self.local + ee : self.local + ee + 1]
        return one_hot((pos + (place[1] - info[1] - k * WIN).astype(f32)) == self.lane)

    def held(self, ee, k, cols=slice(None)):
        return self.rows_ref[ee, span(self.places[ee][FIRST] + k * WIN, WIN, ALIGN), cols]

    def out_copy(self, i):
        slot = i % RING
        place = self.blocks.bmap[2 * i] - self.blocks.bmap[FIRST]
        return pltpu.make_async_copy(self.ring.at[slot], self.out_ref.at[place], self.sems.at[slot])

    def run(self, simple_body, full_body):
        def block(i, rows_at):
            ee = range(self.local)
            self.infos = [self.blocks.info(i, k) for k in ee]
            self.places = [aligned(r) for r in rows_at]
            self.windows = [window_count(self.places[k][1], self.infos[k][LAST]) for k in ee]
            self.flat = self.infos[FIRST][FIRST]
            self.tab_t = jnp.transpose(self.tab_ref[self.flat])
            self.tok = span((i - self.first) * BLK, BLK)
            pl.when(i - self.first >= RING)(lambda: self.out_copy(i - RING).wait())
            simple = functools.reduce(jnp.logical_and, [w <= 1 for w in self.windows])
            out = self.ring.at[i % RING]
            pl.when(simple)(lambda: simple_body(out))
            pl.when(jnp.logical_not(simple))(lambda: full_body(out))
            self.out_copy(i).start()
            return tuple(r + info[LAST] for r, info in zip(rows_at, self.infos))

        stop = self.first + self.count
        lax.fori_loop(self.first, stop, block, (i32(FIRST),) * self.local)
        loop(stop - RING, stop, lambda i: self.out_copy(i).wait())


def y_kernel(groups, local, starts_ref, bmap_ref, spans_ref, tab_ref, h_ref, w2_ref, *refs):
    take = taker(refs)
    d_refs = [take(len(GROUPS[g])) for g in groups]
    y_ref, dg_ref, o_rows, dv, ring, zacc, yacc, dgacc, tok_sem, out_sem = take()
    all_rows = Combine(local, starts_ref, bmap_ref, spans_ref, tab_ref, o_rows, y_ref, ring, out_sem)
    e = all_rows.e
    d_model = dv.shape[1]

    def token_copies(step):
        spots = offsets(GROUPS[groups[step]])
        return [pltpu.make_async_copy(src, dv.at[block_rows(*spot)], tok_sem.at[c]) for c, (src, spot) in enumerate(zip(d_refs[step], spots))]

    for step in range(len(groups)):
        pl.when((pl.program_id(FIRST) == step) & (e == FIRST))(lambda: start(token_copies(step)))

    def tile(at, size):
        rows = span(at, size)
        o_rows[e, rows, :] = dot(h_ref[FIRST, FIRST, rows, :], w2_ref[FIRST]).astype(bf16)

    row_tiles(all_rows.total, tile, 2 * TILE)
    all_rows.zero_tail()

    @pl.when(e == local - 1)
    def _():
        for step in range(len(groups)):
            pl.when(pl.program_id(FIRST) == step)(lambda: wait(token_copies(step)))
        dg_lane = iota((BLK, LANES), 1)
        width = 2 * LANES
        columns = [slice(k * width, (k + 1) * width) for k in range(d_model // width)]

        def gate(ee):
            return all_rows.tab_t[:, ee : ee + 1]

        def put_dg(sums):
            dg = sum(where0(dg_lane == ee, lane_sum(s) + jnp.zeros((BLK, LANES), f32)) for ee, s in enumerate(sums))
            dg_ref[all_rows.flat - all_rows.blocks.bmap[FIRST]] = jnp.transpose(dg)[: 2 * local, :]

        def simple(out):
            picks = [all_rows.pick(ee, i32(FIRST)) for ee in range(local)]
            sums = [None] * local
            for cols in columns:
                dy = dv[all_rows.tok, cols].astype(f32)
                y = None
                for ee in range(local):
                    z = dot(picks[ee], all_rows.held(ee, i32(FIRST), cols))
                    prod = dy * z
                    part = prod[:, :LANES] + prod[:, LANES:]
                    sums[ee] = part if sums[ee] is None else sums[ee] + part
                    y = gate(ee) * z if y is None else y + gate(ee) * z
                out[:, cols] = y.astype(bf16)
            put_dg(sums)

        def full(out):
            yacc[...] = jnp.zeros_like(yacc)
            for ee in range(local):
                zacc[...] = jnp.zeros_like(zacc)

                def more(k):
                    zacc[...] += dot(all_rows.pick(ee, k), all_rows.held(ee, k))

                loop(FIRST, all_rows.windows[ee], more)
                yacc[...] += gate(ee) * zacc[...]
                dgacc[ee] = lane_sum(dv[all_rows.tok, :].astype(f32) * zacc[...]) * jnp.where(dg_lane == FIRST, 1.0, 0.0)
            out[...] = yacc[...].astype(bf16)
            put_dg([dgacc[ee] for ee in range(local)])

        all_rows.run(simple, full)


def combine_scratch(local, row_cap, d_model):
    return [pltpu.VMEM((local, row_cap + WIN, d_model), bf16)], [pltpu.VMEM((RING, BLK, d_model), bf16), pltpu.VMEM((BLK, d_model), f32)]


def run_y(groups, starts, tab, h_rows, w2, ds, nb):
    local, d_ff, d_model = w2.shape
    row_cap = h_rows.shape[2]
    pieces = [p for g in groups for p in GROUPS[g]]
    spans = group_spans(groups)
    blocks = block_count(pieces)
    rows, work = combine_scratch(local, row_cap, d_model)
    return pl.pallas_call(
        functools.partial(y_kernel, groups, local),
        grid=(len(groups), local),
        in_specs=[SMEM, SMEM, SMEM, VMEM, per_group(groups, row_cap, d_ff), per_local(d_ff, d_model)] + [ANY] * len(pieces),
        out_specs=[ANY, VMEM],
        out_shape=[Shape((blocks, BLK, d_model), bf16), Shape((blocks, 2 * local, BLK), f32)],
        scratch_shapes=rows + [pltpu.VMEM((max(spans[1::2]) * BLK, d_model), bf16)] + work + [work[LAST], pltpu.VMEM((local, BLK, LANES), f32), DMA((4,)), DMA((RING,))],
        compiler_params=grid_params(2),
        cost_estimate=cost(4 * blocks * BLK * d_model * d_ff, 20 << 20),
        name="expert_y",
    )(starts, block_map(pieces, nb), spans, tab, h_rows, w2, *[ds[p] for p in pieces])


def dx_kernel(local, starts_ref, bmap_ref, spans_ref, tab_ref, da_ref, db_ref, w1_ref, w3_ref, dx_ref, o_rows, ring, zacc, out_sem):
    all_rows = Combine(local, starts_ref, bmap_ref, spans_ref, tab_ref, o_rows, dx_ref, ring, out_sem)
    e = all_rows.e

    def tile(at, size):
        rows = span(at, size)
        grad = dot_nt(da_ref[FIRST, FIRST, rows, :], w1_ref[FIRST]) + dot_nt(db_ref[FIRST, FIRST, rows, :], w3_ref[FIRST])
        o_rows[e, rows, :] = grad.astype(bf16)

    row_tiles(all_rows.total, tile, 2 * TILE)
    all_rows.zero_tail()

    @pl.when(e == local - 1)
    def _():
        def simple(out):
            pairs = [(ee, ee + 1) for ee in range(FIRST, local, 2)]
            zero = i32(FIRST)
            sums = [
                dot(jnp.concatenate([all_rows.pick(ee, zero) for ee in pair], axis=1), jnp.concatenate([all_rows.held(ee, zero) for ee in pair], axis=FIRST))
                for pair in pairs
            ]
            out[...] = sum(sums[1:], sums[FIRST]).astype(bf16)

        def full(out):
            zacc[...] = jnp.zeros_like(zacc)
            for ee in range(local):

                def more(k):
                    zacc[...] += dot(all_rows.pick(ee, k), all_rows.held(ee, k))

                loop(FIRST, all_rows.windows[ee], more)
            out[...] = zacc[...].astype(bf16)

        all_rows.run(simple, full)


def run_dx(groups, starts, tab, da_rows, db_rows, w1, w3, nb):
    local, d_model, d_ff = w1.shape
    row_cap = da_rows.shape[2]
    pieces = [p for g in groups for p in GROUPS[g]]
    blocks = block_count(pieces)
    rows, work = combine_scratch(local, row_cap, d_model)
    return pl.pallas_call(
        functools.partial(dx_kernel, local),
        grid=(len(groups), local),
        in_specs=[SMEM, SMEM, SMEM, VMEM] + [per_group(groups, row_cap, d_ff)] * 2 + [per_local(d_model, d_ff)] * 2,
        out_specs=ANY,
        out_shape=Shape((blocks, BLK, d_model), bf16),
        scratch_shapes=rows + work + [DMA((RING,))],
        compiler_params=grid_params(2),
        cost_estimate=cost(6 * blocks * BLK * d_model * d_ff, 20 << 20),
        name="expert_dx",
    )(starts, block_map(pieces, nb), group_spans(groups), tab, da_rows, db_rows, w1, w3)


def router_grad_kernel(scale, x_ref, prob_ref, dg_ref, ids_ref, load_ref, dlog_ref, dw_ref):
    step = pl.program_id(FIRST)
    prob = prob_ref[...]
    dg = dg_ref[...]
    chosen = chosen_mask(ids_ref[...], prob.shape[FIRST])
    gate_sum = row_sum(where0(chosen, prob))
    gate = where0(chosen, prob / gate_sum)
    d_pick = (dg - row_sum(gate * dg)) / gate_sum
    d_prob = where0(chosen, d_pick) + scale * load_ref[:, :1]
    d_logit = prob * (d_prob - row_sum(prob * d_prob))
    dlog_ref[...] = d_logit
    hi, mid, low = [dot(part, x_ref[...]) for part in split3(d_logit)]

    @pl.when(step == FIRST)
    def _():
        dw_ref[...] = jnp.zeros_like(dw_ref)

    dw_ref[...] += hi + (mid + low)


def run_router_grad(x_loc, prob_t, dg_t, ids_t, load, scale):
    tokens, d_model = x_loc.shape
    experts = prob_t.shape[FIRST]
    lanes = lambda n: pl.BlockSpec((n, BLK), lambda i: (FIRST, i))
    return pl.pallas_call(
        functools.partial(router_grad_kernel, scale),
        grid=(tokens // BLK,),
        in_specs=[pl.BlockSpec((BLK, d_model), lambda i: (i, FIRST)), lanes(experts), lanes(experts), lanes(ids_t.shape[FIRST]), VMEM],
        out_specs=[lanes(experts), VMEM],
        out_shape=[Shape((experts, tokens), f32), Shape((experts, d_model), f32)],
        compiler_params=params(),
        cost_estimate=cost(2 * tokens * d_model * BLK, 2 * tokens * d_model),
        name="router_grad",
    )(x_loc, prob_t, dg_t, ids_t, load)


def final_kernel(dlog_ref, wt_ref, *refs):
    take = taker(refs)
    y_terms, dx_terms = [[ref[...].astype(f32) for ref in take(3)] for _ in TENSORS]
    y_ref, dx_ref = take()
    lhs = split3(dlog_ref[...])
    rhs = split3(wt_ref[...])
    terms = [(i, j) for i in range(3) for j in range(3 - i)]
    left = jnp.concatenate([lhs[i] for i, _ in terms], axis=FIRST)
    right = jnp.concatenate([rhs[j] for _, j in terms], axis=FIRST)
    dx_ref[...] = (dot_tn(left, right) + sum(dx_terms[1:], dx_terms[FIRST])).astype(bf16)
    y_ref[...] = sum(y_terms[1:], y_terms[FIRST]).astype(bf16)


def run_final(dlog_t, w_t, y_terms, dx_terms):
    experts, tokens = dlog_t.shape
    d_model = w_t.shape[1]
    size = tokens // 4
    rows = pl.BlockSpec((size, d_model), lambda i: (i, FIRST))
    return pl.pallas_call(
        final_kernel,
        grid=(tokens // size,),
        in_specs=[pl.BlockSpec((experts, size), lambda i: (FIRST, i)), VMEM] + [rows] * len([*y_terms, *dx_terms]),
        out_specs=[rows] * 2,
        out_shape=[Shape((tokens, d_model), bf16)] * 2,
        compiler_params=params(),
        cost_estimate=cost(2 * tokens * d_model * BLK, 16 * tokens * d_model),
        name="final",
    )(dlog_t, w_t, *y_terms, *dx_terms)


NEAR = (X, Y)
RELAYED = {(Y, 0): 0, (X, 1): 1}
OPS = [
    (t, src, h)
    for step in ([(FAR, 0), (FAR, 1)], [(X, 0), (Y, 1)], [(X, 1), (Y, 0)], [(FIRST, 0), (FIRST, 1)])
    for t in TENSORS
    for src, h in step
]


def add_rows(dst, src):
    step = min(LANES, dst.shape[FIRST])

    def body(i):
        rows = span(i * step, step)
        dst[rows, :] = (dst[rows, :].astype(f32) + src[rows, :].astype(f32)).astype(bf16)

    loop(FIRST, dst.shape[FIRST] // step, body)


def exchange_kernel(half, mats, *refs):
    take = taker(refs)
    parts = [take(2) for _ in TENSORS]
    dws = take(mats)
    outs = [take(len(NEAR) + 1) for _ in TENSORS]
    dw_outs = take(mats)
    land, far_land, stage, z_one, z_two, z_stage = take(6)
    core_sem, stage_sem, far_sem, near_sem, own_sem, z_sem, keep_sem, load_sem, credit_one, credit_two = take()

    me = lax.axis_index("ep")
    z = lax.axis_index("dp")
    peer = {bit: me + bit - 2 * bit * ((me // bit) % 2) for bit in (CORE, X, Y)}
    z_peer = z + 1 - 2 * (z % 2)
    z_cross = 3 - z
    is_end = (z % 3) == FIRST
    is_mid = (z % 3) != FIRST

    barrier = pltpu.get_barrier_semaphore()
    ids = [{"ep": p} for p in peer.values()] + [{"dp": z_peer}, {"dp": z_cross}]
    for device in ids:
        pl.semaphore_signal(barrier, device_id=device, device_id_type=MESH)
    pl.semaphore_wait(barrier, len(ids))

    def remote(src, dst, sems, at, device):
        send, recv = sems.at[(SEND, *at)], sems.at[(RECV, *at)]
        return pltpu.make_async_remote_copy(src_ref=src, dst_ref=dst, send_sem=send, recv_sem=recv, device_id=device, device_id_type=MESH)

    def rows_at(h):
        return pl.ds(h * half, half)

    def part(t, src, h):
        own, rest = parts[t]
        return own.at[src, rows_at(h)] if src <= CORE else rest.at[src - 2, rows_at(h)]

    def core_copy(i):
        t, src, h = OPS[i]
        return remote(part(t, src | CORE, h), land.at[i], core_sem, (i,), {"ep": peer[CORE]})

    def stage_copy(i):
        t, src, h = OPS[i]
        return pltpu.make_async_copy(part(t, src, h), stage.at[i % STAGES], stage_sem.at[i % STAGES])

    def far_copy(i):
        t, _, h = OPS[i]
        return remote(land.at[i], far_land.at[t, h], far_sem, (t, h), {"ep": peer[NEAR[h]]})

    def near_copy(i):
        t, src, h = OPS[i]
        k = NEAR.index(src)
        return remote(land.at[i], outs[t][k].at[rows_at(h)], near_sem, (t, k, h), {"ep": peer[src]})

    def own_copy(i):
        t, _, h = OPS[i]
        return pltpu.make_async_copy(land.at[i], outs[t][LAST].at[rows_at(h)], own_sem.at[t, h])

    def out_copy(i):
        src = OPS[i][1]
        return (far_copy if src == FAR else near_copy if src else own_copy)(i)

    def reduce_op(i):
        t, src, h = OPS[i]
        stage_copy(i).wait()
        core_copy(i).wait_recv()
        add_rows(land.at[i], stage.at[i % STAGES])
        if i + STAGES < len(OPS):
            stage_copy(i + STAGES).start()
        if (src, h) in RELAYED:
            far_copy(OPS.index((t, FAR, RELAYED[src, h]))).wait_recv()
            add_rows(land.at[i], far_land.at[t, RELAYED[src, h]])

    rows_per = z_one.shape[1]
    chunks = [(m, e, k) for e in range(dws[FIRST].shape[FIRST]) for m in range(mats) for k in SPLIT]
    n = len(chunks)

    def piece(arrays, c):
        m, e, k = chunks[c]
        return arrays[m].at[e, pl.ds(k * rows_per, rows_per)]

    def one_copy(c):
        return remote(piece(dws, c), z_one.at[c % SLOTS], z_sem, (FIRST, c), {"dp": z_peer})

    def two_copy(c):
        return remote(z_one.at[c % SLOTS], z_two.at[c % SLOTS], z_sem, (1, c), {"dp": z_cross})

    def three_copy(c):
        return remote(z_two.at[c % SLOTS], piece(dw_outs, c), z_sem, (2, c), {"dp": z_peer})

    def keep_copy(c):
        return pltpu.make_async_copy(z_two.at[c % SLOTS], piece(dw_outs, c), keep_sem.at[c])

    def load_copy(c):
        return pltpu.make_async_copy(piece(dws, c), z_stage.at[c % STAGES], load_sem.at[c % STAGES])

    def first_add(c):
        load_copy(c).wait()
        one_copy(c).wait_recv()
        add_rows(z_one.at[c % SLOTS], z_stage.at[c % STAGES])
        if c + STAGES < n:
            load_copy(c + STAGES).start()

    def second_add(c):
        two_copy(c).wait()
        add_rows(z_two.at[c % SLOTS], z_one.at[c % SLOTS])
        if c + SLOTS < n:
            pl.semaphore_signal(credit_one, device_id={"dp": z_peer}, device_id_type=MESH)

    def retire(c):
        three_copy(c).wait_send()
        keep_copy(c).wait()
        if c + SLOTS < n:
            pl.semaphore_signal(credit_two, device_id={"dp": z_cross}, device_id_type=MESH)

    @pl.when(is_end)
    def _():
        for c in range(SLOTS):
            one_copy(c).start()

    @pl.when(is_mid)
    def _():
        for c in range(STAGES):
            load_copy(c).start()

    for i in range(len(OPS)):
        core_copy(i).start()
        if i < STAGES:
            stage_copy(i).start()

    todo = list(range(len(OPS)))
    for tick in range(n + LAG):
        mine = todo[: 2 if tick < 2 else tick % 2]
        todo = todo[len(mine) :]
        for i in mine:
            reduce_op(i)

        @pl.when(is_mid)
        def _():
            back = tick - BACK
            if tick < n:
                first_add(tick)
            if back in range(n):
                second_add(back)
            if tick < n:
                if tick >= SLOTS:
                    pl.semaphore_wait(credit_two, 1)
                two_copy(tick).start()
            if back in range(n):
                three_copy(back).start()
                keep_copy(back).start()
            if tick >= LAG:
                retire(tick - LAG)

        for i in mine:
            out_copy(i).start()

        @pl.when(is_end)
        def _():
            if tick + SLOTS < n:
                pl.semaphore_wait(credit_one, 1)
                one_copy(tick + SLOTS).start()

    for i in todo:
        reduce_op(i)
        out_copy(i).start()

    @pl.when(is_end)
    def _():
        for c in range(n):
            one_copy(c).wait_send()
            three_copy(c).wait_recv()

    for i in range(len(OPS)):
        core_copy(i).wait_send()
        (out_copy(i).wait_send if OPS[i][1] == FAR else out_copy(i).wait)()


def run_exchange(parts, dws):
    tokens, d_model = parts[FIRST][FIRST].shape[1:]
    half = tokens // 2
    local, rows, cols = dws[FIRST].shape
    chunk = (rows // len(SPLIT), cols)
    n = local * len(dws) * len(SPLIT)
    whole = Shape((tokens, d_model), bf16)
    flat = [v for tensor in parts for v in tensor] + list(dws)
    terms = len(NEAR) + 1
    out = pl.pallas_call(
        functools.partial(exchange_kernel, half, len(dws)),
        in_specs=[ANY] * len(flat),
        out_specs=[ANY] * (terms * len(TENSORS) + len(dws)),
        out_shape=[whole] * (terms * len(TENSORS)) + [Shape(v.shape, bf16) for v in dws],
        scratch_shapes=[
            pltpu.VMEM((len(OPS), half, d_model), bf16),
            pltpu.VMEM((len(TENSORS), len(HALVES), half, d_model), bf16),
            pltpu.VMEM((STAGES, half, d_model), bf16),
            pltpu.VMEM((SLOTS, *chunk), bf16),
            pltpu.VMEM((SLOTS, *chunk), bf16),
            pltpu.VMEM((STAGES, *chunk), bf16),
            DMA((2, len(OPS))),
            DMA((STAGES,)),
            DMA((2, 2, 2)),
            DMA((2, 2, 2, 2)),
            DMA((2, 2)),
            DMA((2, 3, n)),
            DMA((n,)),
            DMA((STAGES,)),
            pltpu.SemaphoreType.REGULAR,
            pltpu.SemaphoreType.REGULAR,
        ],
        compiler_params=pltpu.CompilerParams(vmem_limit_bytes=VMEM_LIMIT, collective_id=FIRST, has_side_effects=True),
        cost_estimate=cost(1 << 37, 200 << 20),
        name="exchange",
    )(*flat)
    return [out[:terms], out[terms : 2 * terms]], out[2 * terms :]


def hop(v, bit):
    return lax.ppermute(v, "ep", [(i, i ^ bit) for i in SOURCES])


def after(values, token):
    return lax.optimization_barrier((values, token))[FIRST]


def send_own(v, token):
    got = {(FIRST, *WHOLE): v, (CORE, *WHOLE): hop(v, CORE)}
    pieces = after([v[first * BLK : (first + count) * BLK] for first, count in PARTS], token)
    for part, piece in zip(PARTS, pieces):
        got.update({(bit, *part): hop(piece, bit) for bit in NEAR})
    return got


def pass_on(got, h):
    part = PARTS[h]
    got[FAR, *part] = hop(got[(Y, X)[h], *part], NEAR[h])
    for bit in NEAR:
        got[bit | CORE, *part] = hop(got[bit, *part], CORE)


def relative(v, me):
    shape = v.shape
    v = v.reshape((2, 2, 2) + shape[1:])
    for axis, bit in enumerate((Y, X, CORE)):
        v = jnp.where((me & bit) != FIRST, jnp.flip(v, axis), v)
    return v.reshape(shape)


def solution(mesh):
    dp_size = mesh.shape["dp"]
    ep_size = mesh.shape["ep"]
    row_spec = P(("dp", "ep"), None)
    expert_spec = P("ep", None, None)
    whole_spec = P(None, None)

    def per_device(x_loc, w_router, ids_loc, w1, w3, w2, dy_loc):
        tokens, d_model = x_loc.shape
        top_k = ids_loc.shape[1]
        experts = w_router.shape[1]
        local = w1.shape[FIRST]
        capacity = capacity_of(tokens, top_k, experts)
        n_total = tokens * dp_size * ep_size
        nb = tokens // BLK
        row_cap = padded(4 * capacity)
        me = lax.axis_index("ep")

        ids_t = ids_loc.T
        send_tab, prob_t = run_router(x_loc, w_router, ids_t, capacity, local, ep_size)
        tables = lax.all_to_all(send_tab, "ep", FIRST, FIRST, tiled=True)
        gathered = [send_own(v, tables) for v in (x_loc, dy_loc)]
        tab_rel = relative(tables, me)
        tab = tab_rel[:, :, :tokens].reshape(ep_size, 2 * local, nb, BLK).transpose(0, 2, 1, 3).reshape(ep_size * nb, 2 * local, BLK)
        starts = tab_rel[:, local:, tokens : tokens + ALIGN].astype(i32).reshape(LAST)

        def y_of(groups, starts):
            return run_y(groups, starts, tab, rows[FIRST], w2, gathered[1], nb)

        def dx_of(groups, starts):
            return run_dx(groups, starts, tab, rows[1], rows[2], w1, w3, nb)

        acc = rows = ()
        own, rest = (FIRST,), (1, 2, 3)
        for g, group in enumerate(GROUPS):
            if g:
                ready = [p for p in group if not p[FIRST] & CORE]
                for got in gathered:
                    got.update(after({p: got[p] for p in ready}, (acc[LAST], dg_own)))
                for got in gathered:
                    if g < len(GROUPS) - 1:
                        pass_on(got, g - 1)
                    else:
                        for src, *part in ready:
                            got[src | CORE, *part] = hop(got[src, *part], CORE)
                here = after(starts, [[got[p] for p in ready] for got in gathered])
                if g == 2:
                    dx_own = dx_of(own, here)
                    starts = after(starts, dx_own)
            rows, acc = run_grad(starts, tab, g, *[[got[p] for p in group] for got in gathered], (w1, w3, w2), acc, rows, nb, row_cap)
            if not g:
                stats = jnp.sum(after(tab_rel[:, :local, tokens:], acc[LAST]), axis=FIRST)
                for step in (1, 2):
                    stats = stats + lax.ppermute(stats, "dp", [(i, i ^ step) for i in range(dp_size)])
                y_own, dg_own = y_of(own, after(starts, stats))
                starts = after(starts, dg_own)
        dw1, dw3, dw2 = acc
        starts, dw2 = lax.optimization_barrier((starts, dw2))
        dw2_sum = lax.psum(dw2, "dp")

        y_rest, dg_rest = y_of(rest, starts)
        dg = jnp.concatenate([dg_own, dg_rest], axis=FIRST)
        dg = dg[:, :local].reshape(ep_size, nb, local, BLK).transpose(0, 2, 1, 3).reshape(ep_size, local, tokens)
        dg = jnp.concatenate([relative(dg, me), jnp.broadcast_to(stats, (ep_size, *stats.shape))], axis=2)
        starts, dg = lax.optimization_barrier((starts, dg))
        dx_rest = dx_of(rest, starts)
        dg_all = lax.all_to_all(dg, "ep", FIRST, FIRST, tiled=True).reshape(experts, tokens + LANES)
        load = dg_all[:, tokens:]
        share = AUX_COEF * experts / (n_total * top_k * n_total)
        aux_loss = share * jnp.sum(load[:, FIRST] * load[:, 1])
        dlog_t, dwr_t = run_router_grad(x_loc, prob_t, dg_all[:, :tokens], ids_t, load, share)
        dw_router = lax.psum(dwr_t, ("dp", "ep")).T

        parts = [[v.reshape(LAST, tokens, d_model) for v in pair] for pair in ((y_own, y_rest), (dx_own, dx_rest))]
        sums, grads = run_exchange(parts, [dw1, dw3])
        y_loc, dx_loc = run_final(dlog_t, w_router.T, *sums)
        return y_loc, aux_loss, dx_loc, dw_router, *grads, dw2_sum

    return jax.shard_map(
        per_device,
        mesh=mesh,
        in_specs=(row_spec, whole_spec, row_spec, expert_spec, expert_spec, expert_spec, row_spec),
        out_specs=(row_spec, P(), row_spec, whole_spec, expert_spec, expert_spec, expert_spec),
        check_vma=False,
    )
```

```python
import functools

import jax
import jax.numpy as jnp
import numpy as np
from jax import lax
from jax.experimental import pallas as pl
from jax.experimental.pallas import tpu as pltpu
from jax.sharding import PartitionSpec as P


AUX_COEF = 0.01
BLK = 256
TILE = 256
WIN = 128
LANES = 128
ALIGN = 16
NOT_KEPT = -65536.0
VMEM_LIMIT = 63 * 1024 * 1024
CORE, X, Y = 1, 2, 4
FAR = X | Y
HALVES = TENSORS = range(2)
RING = 4
SOURCES = range(8)
FIRST, LAST = 0, -1
SEND, RECV = 0, 1
STAGES = 3
SLOTS = 16
SPLIT = range(4)
BACK, LAG = 2, 4
MESH = pl.DeviceIdType.MESH

WHOLE, PARTS = (0, 6), ((0, 3), (3, 3))
GROUPS = (
    [(src, *WHOLE) for src in (FIRST, CORE)],
    [(bit | core, *PARTS[FIRST]) for bit in (X, Y) for core in (FIRST, CORE)],
    [(bit | core, *PARTS[1]) for bit in (X, Y) for core in (FIRST, CORE)],
    [(FAR | core, *part) for part in PARTS for core in (FIRST, CORE)],
)


f32 = jnp.float32
bf16 = jnp.bfloat16
i32 = jnp.int32
ANY = pl.BlockSpec(memory_space=pl.ANY)
SMEM = pl.BlockSpec(memory_space=pltpu.SMEM)
VMEM = pl.BlockSpec(memory_space=pltpu.VMEM)
DMA = pltpu.SemaphoreType.DMA
Shape = jax.ShapeDtypeStruct


def capacity_of(tokens, top_k, experts):
    return (5 * top_k * tokens + 4 * experts - 1) // (4 * experts)


def dot(a, b, ca=1, cb=0):
    return lax.dot_general(a, b, (((ca,), (cb,)), ((), ())), preferred_element_type=f32)


def dot_nt(a, b):
    return dot(a, b, 1, 1)


def dot_tn(a, b):
    return dot(a, b, 0, 0)


def grid_params(dims):
    return pltpu.CompilerParams(dimension_semantics=("arbitrary",) * dims, vmem_limit_bytes=VMEM_LIMIT)


def params():
    return grid_params(1)


def cost(flops, moved):
    return pl.CostEstimate(flops=flops, bytes_accessed=moved, transcendentals=FIRST)


def iota(shape, dim):
    return lax.broadcasted_iota(i32, shape, dim)


def span(start, size, multiple=None):
    return pl.ds(pl.multiple_of(start, multiple or size), size)


def lane_sum(v):
    return jnp.sum(v, axis=1, keepdims=True)


def row_sum(v):
    return jnp.sum(v, axis=0, keepdims=True)


def where0(mask, v):
    return jnp.where(mask, v, jnp.zeros_like(v))


def one_hot(mask):
    return jnp.where(mask, 1.0, 0.0).astype(bf16)


def split3(v):
    hi = v.astype(bf16)
    rest = v - hi.astype(f32)
    mid = rest.astype(bf16)
    return hi, mid, (rest - mid.astype(f32)).astype(bf16)


def loop(start, stop, body):
    def step(i, carry):
        body(i)
        return carry

    lax.fori_loop(start, stop, step, FIRST)


def chosen_mask(ids, experts):
    rows = iota((experts, ids.shape[1]), FIRST)
    return functools.reduce(jnp.logical_or, [rows == ids[j : j + 1, :] for j in range(ids.shape[FIRST])])


def router_kernel(capacity, local, x_ref, w_ref, ids_ref, tab_ref, prob_ref, carry):
    step = pl.program_id(FIRST)
    steps = pl.num_programs(FIRST)
    experts = w_ref.shape[1]

    @pl.when(step == FIRST)
    def _():
        carry[...] = jnp.zeros_like(carry)
        tab_ref[...] = jnp.zeros_like(tab_ref)

    x = x_ref[...]
    hi, mid, low = [dot(x, part) for part in split3(w_ref[...])]
    logits = jnp.transpose(hi + (mid + low))
    expo = jnp.exp(logits - jnp.max(logits, axis=FIRST, keepdims=True))
    prob = expo / row_sum(expo)
    chosen = chosen_mask(ids_ref[...], experts)
    hits = jnp.where(chosen, 1.0, 0.0)
    gate = where0(chosen, prob / row_sum(where0(chosen, prob)))
    earlier = one_hot(iota((BLK, BLK), FIRST) < iota((BLK, BLK), 1))
    before = carry[:, :1]
    pos = dot(hits.astype(bf16), earlier) + before
    pos = jnp.where(chosen & (pos < capacity), pos, NOT_KEPT)
    prob_ref[...] = prob
    after = before + lane_sum(hits)
    lane = iota((experts, LANES), 1)
    first = where0(lane == step, jnp.minimum(before, capacity) + jnp.zeros((experts, LANES), f32))
    first = first + where0((lane == step + 1) & (step == steps - 1), jnp.minimum(after, capacity) + jnp.zeros((experts, LANES), f32))
    stat = where0(lane == FIRST, lane_sum(hits) + jnp.zeros((experts, LANES), f32))
    stat = stat + where0(lane == 1, lane_sum(prob) + jnp.zeros((experts, LANES), f32))
    tail = slice(tab_ref.shape[LAST] - LANES, None)
    for d in range(experts // local):
        rows = slice(d * local, (d + 1) * local)
        tab_ref[d, :local, span(step * BLK, BLK)] = gate[rows]
        tab_ref[d, local:, span(step * BLK, BLK)] = pos[rows]
        tab_ref[d, :local, tail] += stat[rows]
        tab_ref[d, local:, tail] += first[rows]
    carry[:, :1] = after


def run_router(x_loc, w_router, ids_t, capacity, local, devices):
    tokens, d_model = x_loc.shape
    experts = w_router.shape[1]
    top_k = ids_t.shape[FIRST]
    table = (devices, 2 * local, tokens + LANES)
    return pl.pallas_call(
        functools.partial(router_kernel, capacity, local),
        grid=(tokens // BLK,),
        in_specs=[pl.BlockSpec((BLK, d_model), lambda i: (i, FIRST)), VMEM, pl.BlockSpec((top_k, BLK), lambda i: (FIRST, i))],
        out_specs=[VMEM, pl.BlockSpec((experts, BLK), lambda i: (FIRST, i))],
        out_shape=[Shape(table, f32), Shape((experts, tokens), f32)],
        scratch_shapes=[pltpu.VMEM((experts, LANES), f32)],
        compiler_params=params(),
        cost_estimate=cost(2 * tokens * d_model * BLK, 2 * tokens * d_model),
        name="router",
    )(x_loc, w_router, ids_t)


class Blocks:
    def __init__(self, starts_ref, bmap_ref):
        self.starts, self.bmap = starts_ref, bmap_ref

    def info(self, i, e):
        at = self.bmap[2 * i + 1] + e * ALIGN
        first = self.starts[at]
        return self.bmap[2 * i], first, self.starts[at + 1] - first

    def total(self, start, count, e):
        return lax.fori_loop(start, start + count, lambda i, n: n + self.info(i, e)[LAST], i32(FIRST))


def aligned(row):
    base = (row // ALIGN) * ALIGN
    return base, row - base


def window_count(shift, count):
    return (shift + count + WIN - 1) // WIN


def padded(total):
    return (total + TILE - 1) // TILE * TILE


def row_tiles(total, body, size):
    tiles = (total + size - 1 - size // 2) // size
    loop(FIRST, tiles, lambda i: body(i * size, size))
    pl.when(padded(total) > tiles * size)(lambda: body(tiles * size, size // 2))


def start(copies):
    for cp in copies:
        cp.start()


def wait(copies):
    for cp in copies:
        cp.wait()


def taker(refs):
    refs = list(refs)

    def take(n=None):
        got = refs[:n]
        del refs[:n]
        return got

    return take


def block_count(pieces):
    return sum(count for _, _, count in pieces)


def offsets(pieces):
    counts = [count for _, _, count in pieces]
    return [(sum(counts[:k]), count) for k, count in enumerate(counts)]


def block_rows(first, count):
    return pl.ds(first * BLK, count * BLK)


def grad_kernel(g, last, local, pieces, *refs):
    take = taker(refs)
    n = len(pieces)
    starts_ref, bmap_ref, tab_ref = take(3)
    tok_refs = take(n), take(n)
    w1_ref, w3_ref, w2_ref = take(3)
    acc_in = take(2 * bool(g))
    take(3 * bool(g))
    row_outs = take(3)
    outs = take(3 if last else 2)
    xv, dv, xr, dr, acc13, acc2, stage, tok_sem, in_sem, out_sem, row_sem = take()
    accs = acc13, acc2
    e = pl.program_id(FIRST)
    slot = e % 2
    d_model = xv.shape[1]
    d_ff = w1_ref.shape[LAST]
    blocks = Blocks(starts_ref, bmap_ref)
    count = xv.shape[FIRST] // BLK

    parts = [(c, at, first + at) for c, (first, size) in enumerate(offsets(pieces)) for at in range(FIRST, size, 3)]

    def token_copies(k):
        c, at, to = parts[k]
        src_rows, dst_rows = block_rows(at, 3), block_rows(to, 3)
        return [pltpu.make_async_copy(src[c].at[src_rows], dst.at[dst_rows], tok_sem.at[w, k]) for w, (src, dst) in enumerate(zip(tok_refs, (xv, dv)))]

    def in_copies(ee, ss):
        return [pltpu.make_async_copy(src.at[ee], dst.at[ss], in_sem.at[ss, k]) for k, (src, dst) in enumerate(zip(acc_in, accs))]

    def out_copies(ee, ss):
        return [pltpu.make_async_copy(src.at[ss], dst.at[ee], out_sem.at[ss, k]) for k, (src, dst) in enumerate(zip(accs, outs))]

    @pl.when(e == FIRST)
    def _():
        for k in range(len(parts)):
            start(token_copies(k))

    if g:
        pl.when(e == FIRST)(lambda: start(in_copies(e, slot)))
    else:
        pl.when(e >= 2)(lambda: wait(out_copies(e - 2, slot)))
        for acc in accs:
            acc[slot] = jnp.zeros(acc.shape[1:], f32)

    def prefetch():
        if not last:
            pl.when(e > FIRST)(lambda: wait(out_copies(e - 1, 1 - slot)))
        start(in_copies(e + 1, 1 - slot))

    def maybe_prefetch(now):
        if g:
            pl.when(now & (e + 1 < local))(prefetch)

    row_iota = iota((WIN, BLK), FIRST).astype(f32)
    head_row = iota((ALIGN, d_model), FIRST)
    both = tuple(HALVES)

    def dispatch(step, rows_at):
        todo = []
        for i in (2 * step, 2 * step + 1):
            for k, (_, _, first) in enumerate(parts):
                pl.when((e == FIRST) & (i == first))(lambda: wait(token_copies(k)))
            infos = [blocks.info(i, e + q) for q in both]
            todo.append((span(i * BLK, BLK), infos, [aligned(r) for r in rows_at]))
            rows_at = tuple(r + info[LAST] for r, info in zip(rows_at, infos))

        def picks(block, q, k):
            _, infos, places = block
            flat, first, _ = infos[q]
            pos = tab_ref[flat, pl.ds(local + e + q, 1), :]
            gate = tab_ref[flat, pl.ds(e + q, 1), :]
            pick = (pos + (places[q][1] - first - k * WIN).astype(f32)) == row_iota
            return one_hot(pick), lane_sum(where0(pick, gate + jnp.zeros_like(row_iota)))

        def rows_for(block, one, gate_row):
            tok = block[FIRST]
            return dot(one, xv[tok, :]).astype(bf16), (dot(one, dv[tok, :]) * gate_row).astype(bf16)

        def first_rows(block):
            pair = [picks(block, q, i32(FIRST)) for q in both]
            return rows_for(block, *[jnp.concatenate(v, axis=FIRST) for v in zip(*pair)])

        def put(block, new):
            for q in both:
                base, shift = block[LAST][q]
                head = span(base, ALIGN)
                for value, rows in zip(new, (xr, dr)):
                    value = value[q * WIN : (q + 1) * WIN]
                    rows[q, head, :] = jnp.where(head_row < shift, rows[q, head, :], value[:ALIGN])
                    rows[q, span(base + ALIGN, WIN - ALIGN, ALIGN), :] = value[ALIGN:]

        windows = [[window_count(places[q][1], infos[q][LAST]) for q in both] for _, infos, places in todo]
        simple = functools.reduce(jnp.logical_and, [w <= 1 for ws in windows for w in ws])

        @pl.when(simple)
        def _():
            for block, new in zip(todo, [first_rows(block) for block in todo]):
                put(block, new)

        @pl.when(jnp.logical_not(simple))
        def _():
            for block, ws in zip(todo, windows):
                put(block, first_rows(block))
                for q in both:

                    def more(k):
                        for value, rows in zip(rows_for(block, *picks(block, q, k)), (xr, dr)):
                            rows[q, span(block[LAST][q][FIRST] + k * WIN, WIN, ALIGN), :] = value

                    loop(1, ws[q], more)

        return rows_at

    @pl.when(slot == FIRST)
    def _():
        totals = lax.fori_loop(FIRST, count // 2, dispatch, (i32(FIRST),) * len(both))
        for q in both:

            def clear(i):
                for rows in (xr, dr):
                    rows[q, span(i * ALIGN, ALIGN), :] = jnp.zeros((ALIGN, d_model), bf16)

            loop((totals[q] + ALIGN - 1) // ALIGN, padded(totals[q]) // ALIGN, clear)

    wait(in_copies(e, slot))

    def tile(at, size):
        maybe_prefetch((at == FIRST) & (slot == FIRST))
        rows = span(at, size)
        xt = xr[slot, rows, :]
        dt = dr[slot, rows, :]
        act_a = dot(xt, w1_ref[FIRST])
        act_b = dot(xt, w3_ref[FIRST])
        d_hidden = dot_nt(dt, w2_ref[FIRST]).astype(bf16).astype(f32)
        sig = 1.0 / (1.0 + jnp.exp(-act_a))
        silu = act_a * sig
        hidden = (silu * act_b).astype(bf16)
        d_a = (d_hidden * act_b * sig * (1.0 + act_a * (1.0 - sig))).astype(bf16)
        d_b = (d_hidden * silu).astype(bf16)
        copies = []
        for k, (value, out) in enumerate(zip((hidden, d_a, d_b), row_outs)):
            stage[k, :size] = value
            copies.append(pltpu.make_async_copy(stage.at[k, :size], out.at[g, e, rows], row_sem.at[k]))
        start(copies)
        acc13[slot, :, :d_ff] += dot_tn(xt, d_a)
        acc13[slot, :, d_ff:] += dot_tn(xt, d_b)
        acc2[slot] += dot_tn(hidden, dt)
        wait(copies)

    total = blocks.total(FIRST, count, e)
    row_tiles(total, tile, 2 * TILE)
    maybe_prefetch((total == FIRST) | (slot > FIRST))

    if last:
        for out, value in zip(outs, (acc13[slot, :, :d_ff], acc13[slot, :, d_ff:], acc2[slot])):
            out[FIRST] = value.astype(bf16)
    else:
        start(out_copies(e, slot))

        @pl.when(e == pl.num_programs(FIRST) - 1)
        def _():
            wait(out_copies(e - 1, 1 - slot))
            wait(out_copies(e, slot))


def per_expert(*shape):
    return pl.BlockSpec((1, *shape), lambda e: (e,) + (FIRST,) * len(shape))


def block_map(pieces, nb):
    spots = [(src, first + b) for src, first, count in pieces for b in range(count)]
    return np.asarray([v for src, b in spots for v in (src * nb + b, src * 4 * ALIGN + b)], np.int32)


def run_grad(starts, tab, g, xs, ds, weights, acc, rows, nb, row_cap):
    pieces = GROUPS[g]
    last = g == len(GROUPS) - 1
    local, d_model, d_ff = weights[FIRST].shape
    count = block_count(pieces) * BLK
    w_specs = [per_expert(*w.shape[1:]) for w in weights]
    sums = [(local, d_model, 2 * d_ff), (local, d_ff, d_model)]
    row_shape = [Shape((len(GROUPS), local, row_cap, d_ff), bf16)] * 3
    out_shape = row_shape + ([Shape(w.shape, bf16) for w in weights] if last else [Shape(s, f32) for s in sums])
    out_specs = [ANY] * 3 + (w_specs if last else [ANY] * 2)
    tokens = pltpu.VMEM((count, d_model), bf16)
    packed = pltpu.VMEM((2, row_cap + WIN, d_model), bf16)
    ins = [starts, block_map(pieces, nb), tab, *xs, *ds, *weights, *acc, *rows]
    out = pl.pallas_call(
        functools.partial(grad_kernel, g, last, local, pieces),
        grid=(local,),
        in_specs=[SMEM, SMEM, VMEM] + [ANY] * (2 * len(pieces)) + w_specs + [ANY] * (len(acc) + len(rows)),
        out_specs=out_specs,
        out_shape=out_shape,
        scratch_shapes=[tokens, tokens, packed, packed]
        + [pltpu.VMEM((2, *s[1:]), f32) for s in sums]
        + [pltpu.VMEM((3, 2 * TILE, d_ff), bf16), DMA((2, count // (3 * BLK))), DMA((2, 2)), DMA((2, 2)), DMA((3,))],
        input_output_aliases={len(ins) - len(rows) + k: k for k in range(len(rows))},
        compiler_params=params(),
        cost_estimate=cost(12 * count * d_model * d_ff, 40 << 20),
        name="expert_grad",
    )(*ins)
    return out[:3], out[3:]


def group_spans(groups):
    counts = [block_count(GROUPS[g]) for g in groups]
    return np.asarray([v for k, c in enumerate(counts) for v in (sum(counts[:k]), c)], np.int32)


def per_group(groups, *shape):
    return pl.BlockSpec((1, 1, *shape), lambda step, e: (step + groups[FIRST], e) + (FIRST,) * len(shape))


def per_local(*shape):
    return pl.BlockSpec((1, *shape), lambda g, e: (e,) + (FIRST,) * len(shape))


class Combine:
    def __init__(self, local, starts_ref, bmap_ref, spans_ref, tab_ref, rows_ref, out_ref, ring, sems):
        step = pl.program_id(FIRST)
        self.e = pl.program_id(1)
        self.blocks = Blocks(starts_ref, bmap_ref)
        self.first, self.count = spans_ref[2 * step], spans_ref[2 * step + 1]
        self.total = self.blocks.total(self.first, self.count, self.e)
        self.local, self.tab_ref, self.rows_ref = local, tab_ref, rows_ref
        self.out_ref, self.ring, self.sems = out_ref, ring, sems
        self.lane = iota((BLK, WIN), 1).astype(f32)

    def zero_tail(self):
        rows = span(padded(self.total), WIN)
        self.rows_ref[self.e, rows, :] = jnp.zeros((WIN, self.rows_ref.shape[LAST]), bf16)

    def pick(self, ee, k):
        place, info = self.places[ee], self.infos[ee]
        pos = self.tab_t[:, self.local + ee : self.local + ee + 1]
        return one_hot((pos + (place[1] - info[1] - k * WIN).astype(f32)) == self.lane)

    def held(self, ee, k, cols=slice(None)):
        return self.rows_ref[ee, span(self.places[ee][FIRST] + k * WIN, WIN, ALIGN), cols]

    def out_copy(self, i):
        slot = i % RING
        place = self.blocks.bmap[2 * i] - self.blocks.bmap[FIRST]
        return pltpu.make_async_copy(self.ring.at[slot], self.out_ref.at[place], self.sems.at[slot])

    def run(self, simple_body, full_body):
        def block(i, rows_at):
            ee = range(self.local)
            self.infos = [self.blocks.info(i, k) for k in ee]
            self.places = [aligned(r) for r in rows_at]
            self.windows = [window_count(self.places[k][1], self.infos[k][LAST]) for k in ee]
            self.flat = self.infos[FIRST][FIRST]
            self.tab_t = jnp.transpose(self.tab_ref[self.flat])
            self.tok = span((i - self.first) * BLK, BLK)
            pl.when(i - self.first >= RING)(lambda: self.out_copy(i - RING).wait())
            simple = functools.reduce(jnp.logical_and, [w <= 1 for w in self.windows])
            out = self.ring.at[i % RING]
            pl.when(simple)(lambda: simple_body(out))
            pl.when(jnp.logical_not(simple))(lambda: full_body(out))
            self.out_copy(i).start()
            return tuple(r + info[LAST] for r, info in zip(rows_at, self.infos))

        stop = self.first + self.count
        lax.fori_loop(self.first, stop, block, (i32(FIRST),) * self.local)
        loop(stop - RING, stop, lambda i: self.out_copy(i).wait())


def y_kernel(groups, local, starts_ref, bmap_ref, spans_ref, tab_ref, h_ref, w2_ref, *refs):
    take = taker(refs)
    d_refs = [take(len(GROUPS[g])) for g in groups]
    y_ref, dg_ref, o_rows, dv, ring, zacc, yacc, dgacc, tok_sem, out_sem = take()
    all_rows = Combine(local, starts_ref, bmap_ref, spans_ref, tab_ref, o_rows, y_ref, ring, out_sem)
    e = all_rows.e
    d_model = dv.shape[1]

    def token_copies(step):
        spots = offsets(GROUPS[groups[step]])
        return [pltpu.make_async_copy(src, dv.at[block_rows(*spot)], tok_sem.at[c]) for c, (src, spot) in enumerate(zip(d_refs[step], spots))]

    for step in range(len(groups)):
        pl.when((pl.program_id(FIRST) == step) & (e == FIRST))(lambda: start(token_copies(step)))

    def tile(at, size):
        rows = span(at, size)
        o_rows[e, rows, :] = dot(h_ref[FIRST, FIRST, rows, :], w2_ref[FIRST]).astype(bf16)

    row_tiles(all_rows.total, tile, 2 * TILE)
    all_rows.zero_tail()

    @pl.when(e == local - 1)
    def _():
        for step in range(len(groups)):
            pl.when(pl.program_id(FIRST) == step)(lambda: wait(token_copies(step)))
        dg_lane = iota((BLK, LANES), 1)
        width = 2 * LANES
        columns = [slice(k * width, (k + 1) * width) for k in range(d_model // width)]

        def gate(ee):
            return all_rows.tab_t[:, ee : ee + 1]

        def put_dg(sums):
            dg = sum(where0(dg_lane == ee, lane_sum(s) + jnp.zeros((BLK, LANES), f32)) for ee, s in enumerate(sums))
            dg_ref[all_rows.flat - all_rows.blocks.bmap[FIRST]] = jnp.transpose(dg)[: 2 * local, :]

        def simple(out):
            picks = [all_rows.pick(ee, i32(FIRST)) for ee in range(local)]
            sums = [None] * local
            for cols in columns:
                dy = dv[all_rows.tok, cols].astype(f32)
                y = None
                for ee in range(local):
                    z = dot(picks[ee], all_rows.held(ee, i32(FIRST), cols))
                    prod = dy * z
                    part = prod[:, :LANES] + prod[:, LANES:]
                    sums[ee] = part if sums[ee] is None else sums[ee] + part
                    y = gate(ee) * z if y is None else y + gate(ee) * z
                out[:, cols] = y.astype(bf16)
            put_dg(sums)

        def full(out):
            yacc[...] = jnp.zeros_like(yacc)
            for ee in range(local):
                zacc[...] = jnp.zeros_like(zacc)

                def more(k):
                    zacc[...] += dot(all_rows.pick(ee, k), all_rows.held(ee, k))

                loop(FIRST, all_rows.windows[ee], more)
                yacc[...] += gate(ee) * zacc[...]
                dgacc[ee] = lane_sum(dv[all_rows.tok, :].astype(f32) * zacc[...]) * jnp.where(dg_lane == FIRST, 1.0, 0.0)
            out[...] = yacc[...].astype(bf16)
            put_dg([dgacc[ee] for ee in range(local)])

        all_rows.run(simple, full)


def combine_scratch(local, row_cap, d_model):
    return [pltpu.VMEM((local, row_cap + WIN, d_model), bf16)], [pltpu.VMEM((RING, BLK, d_model), bf16), pltpu.VMEM((BLK, d_model), f32)]


def run_y(groups, starts, tab, h_rows, w2, ds, nb):
    local, d_ff, d_model = w2.shape
    row_cap = h_rows.shape[2]
    pieces = [p for g in groups for p in GROUPS[g]]
    spans = group_spans(groups)
    blocks = block_count(pieces)
    rows, work = combine_scratch(local, row_cap, d_model)
    return pl.pallas_call(
        functools.partial(y_kernel, groups, local),
        grid=(len(groups), local),
        in_specs=[SMEM, SMEM, SMEM, VMEM, per_group(groups, row_cap, d_ff), per_local(d_ff, d_model)] + [ANY] * len(pieces),
        out_specs=[ANY, VMEM],
        out_shape=[Shape((blocks, BLK, d_model), bf16), Shape((blocks, 2 * local, BLK), f32)],
        scratch_shapes=rows + [pltpu.VMEM((max(spans[1::2]) * BLK, d_model), bf16)] + work + [work[LAST], pltpu.VMEM((local, BLK, LANES), f32), DMA((4,)), DMA((RING,))],
        compiler_params=grid_params(2),
        cost_estimate=cost(4 * blocks * BLK * d_model * d_ff, 20 << 20),
        name="expert_y",
    )(starts, block_map(pieces, nb), spans, tab, h_rows, w2, *[ds[p] for p in pieces])


def dx_kernel(local, starts_ref, bmap_ref, spans_ref, tab_ref, da_ref, db_ref, w1_ref, w3_ref, dx_ref, o_rows, ring, zacc, out_sem):
    all_rows = Combine(local, starts_ref, bmap_ref, spans_ref, tab_ref, o_rows, dx_ref, ring, out_sem)
    e = all_rows.e

    def tile(at, size):
        rows = span(at, size)
        grad = dot_nt(da_ref[FIRST, FIRST, rows, :], w1_ref[FIRST]) + dot_nt(db_ref[FIRST, FIRST, rows, :], w3_ref[FIRST])
        o_rows[e, rows, :] = grad.astype(bf16)

    row_tiles(all_rows.total, tile, 2 * TILE)
    all_rows.zero_tail()

    @pl.when(e == local - 1)
    def _():
        def simple(out):
            pairs = [(ee, ee + 1) for ee in range(FIRST, local, 2)]
            zero = i32(FIRST)
            sums = [
                dot(jnp.concatenate([all_rows.pick(ee, zero) for ee in pair], axis=1), jnp.concatenate([all_rows.held(ee, zero) for ee in pair], axis=FIRST))
                for pair in pairs
            ]
            out[...] = sum(sums[1:], sums[FIRST]).astype(bf16)

        def full(out):
            zacc[...] = jnp.zeros_like(zacc)
            for ee in range(local):

                def more(k):
                    zacc[...] += dot(all_rows.pick(ee, k), all_rows.held(ee, k))

                loop(FIRST, all_rows.windows[ee], more)
            out[...] = zacc[...].astype(bf16)

        all_rows.run(simple, full)


def run_dx(groups, starts, tab, da_rows, db_rows, w1, w3, nb):
    local, d_model, d_ff = w1.shape
    row_cap = da_rows.shape[2]
    pieces = [p for g in groups for p in GROUPS[g]]
    blocks = block_count(pieces)
    rows, work = combine_scratch(local, row_cap, d_model)
    return pl.pallas_call(
        functools.partial(dx_kernel, local),
        grid=(len(groups), local),
        in_specs=[SMEM, SMEM, SMEM, VMEM] + [per_group(groups, row_cap, d_ff)] * 2 + [per_local(d_model, d_ff)] * 2,
        out_specs=ANY,
        out_shape=Shape((blocks, BLK, d_model), bf16),
        scratch_shapes=rows + work + [DMA((RING,))],
        compiler_params=grid_params(2),
        cost_estimate=cost(6 * blocks * BLK * d_model * d_ff, 20 << 20),
        name="expert_dx",
    )(starts, block_map(pieces, nb), group_spans(groups), tab, da_rows, db_rows, w1, w3)


def router_grad_kernel(scale, x_ref, prob_ref, dg_ref, ids_ref, load_ref, dlog_ref, dw_ref):
    step = pl.program_id(FIRST)
    prob = prob_ref[...]
    dg = dg_ref[...]
    chosen = chosen_mask(ids_ref[...], prob.shape[FIRST])
    gate_sum = row_sum(where0(chosen, prob))
    gate = where0(chosen, prob / gate_sum)
    d_pick = (dg - row_sum(gate * dg)) / gate_sum
    d_prob = where0(chosen, d_pick) + scale * load_ref[:, :1]
    d_logit = prob * (d_prob - row_sum(prob * d_prob))
    dlog_ref[...] = d_logit
    hi, mid, low = [dot(part, x_ref[...]) for part in split3(d_logit)]

    @pl.when(step == FIRST)
    def _():
        dw_ref[...] = jnp.zeros_like(dw_ref)

    dw_ref[...] += hi + (mid + low)


def run_router_grad(x_loc, prob_t, dg_t, ids_t, load, scale):
    tokens, d_model = x_loc.shape
    experts = prob_t.shape[FIRST]
    lanes = lambda n: pl.BlockSpec((n, BLK), lambda i: (FIRST, i))
    return pl.pallas_call(
        functools.partial(router_grad_kernel, scale),
        grid=(tokens // BLK,),
        in_specs=[pl.BlockSpec((BLK, d_model), lambda i: (i, FIRST)), lanes(experts), lanes(experts), lanes(ids_t.shape[FIRST]), VMEM],
        out_specs=[lanes(experts), VMEM],
        out_shape=[Shape((experts, tokens), f32), Shape((experts, d_model), f32)],
        compiler_params=params(),
        cost_estimate=cost(2 * tokens * d_model * BLK, 2 * tokens * d_model),
        name="router_grad",
    )(x_loc, prob_t, dg_t, ids_t, load)


def final_kernel(dlog_ref, wt_ref, *refs):
    take = taker(refs)
    y_terms, dx_terms = [[ref[...].astype(f32) for ref in take(3)] for _ in TENSORS]
    y_ref, dx_ref = take()
    lhs = split3(dlog_ref[...])
    rhs = split3(wt_ref[...])
    terms = [(i, j) for i in range(3) for j in range(3 - i)]
    left = jnp.concatenate([lhs[i] for i, _ in terms], axis=FIRST)
    right = jnp.concatenate([rhs[j] for _, j in terms], axis=FIRST)
    dx_ref[...] = (dot_tn(left, right) + sum(dx_terms[1:], dx_terms[FIRST])).astype(bf16)
    y_ref[...] = sum(y_terms[1:], y_terms[FIRST]).astype(bf16)


def run_final(dlog_t, w_t, y_terms, dx_terms):
    experts, tokens = dlog_t.shape
    d_model = w_t.shape[1]
    size = tokens // 4
    rows = pl.BlockSpec((size, d_model), lambda i: (i, FIRST))
    return pl.pallas_call(
        final_kernel,
        grid=(tokens // size,),
        in_specs=[pl.BlockSpec((experts, size), lambda i: (FIRST, i)), VMEM] + [rows] * len([*y_terms, *dx_terms]),
        out_specs=[rows] * 2,
        out_shape=[Shape((tokens, d_model), bf16)] * 2,
        compiler_params=params(),
        cost_estimate=cost(2 * tokens * d_model * BLK, 16 * tokens * d_model),
        name="final",
    )(dlog_t, w_t, *y_terms, *dx_terms)


NEAR = (X, Y)
RELAYED = {(Y, 0): 0, (X, 1): 1}
OPS = [
    (t, src, h)
    for step in ([(FAR, 0), (FAR, 1)], [(X, 0), (Y, 1)], [(X, 1), (Y, 0)], [(FIRST, 0), (FIRST, 1)])
    for t in TENSORS
    for src, h in step
]


def add_rows(dst, src):
    step = min(LANES, dst.shape[FIRST])

    def body(i):
        rows = span(i * step, step)
        dst[rows, :] = (dst[rows, :].astype(f32) + src[rows, :].astype(f32)).astype(bf16)

    loop(FIRST, dst.shape[FIRST] // step, body)


def exchange_kernel(half, mats, *refs):
    take = taker(refs)
    parts = [take(2) for _ in TENSORS]
    dws = take(mats)
    outs = [take(len(NEAR) + 1) for _ in TENSORS]
    dw_outs = take(mats)
    land, far_land, stage, z_one, z_two, z_stage = take(6)
    core_sem, stage_sem, far_sem, near_sem, own_sem, z_sem, keep_sem, load_sem, credit_one, credit_two = take()

    me = lax.axis_index("ep")
    z = lax.axis_index("dp")
    peer = {bit: me + bit - 2 * bit * ((me // bit) % 2) for bit in (CORE, X, Y)}
    z_peer = z + 1 - 2 * (z % 2)
    z_cross = 3 - z
    is_end = (z % 3) == FIRST
    is_mid = (z % 3) != FIRST

    barrier = pltpu.get_barrier_semaphore()
    ids = [{"ep": p} for p in peer.values()] + [{"dp": z_peer}, {"dp": z_cross}]
    for device in ids:
        pl.semaphore_signal(barrier, device_id=device, device_id_type=MESH)
    pl.semaphore_wait(barrier, len(ids))

    def remote(src, dst, sems, at, device):
        send, recv = sems.at[(SEND, *at)], sems.at[(RECV, *at)]
        return pltpu.make_async_remote_copy(src_ref=src, dst_ref=dst, send_sem=send, recv_sem=recv, device_id=device, device_id_type=MESH)

    def rows_at(h):
        return pl.ds(h * half, half)

    def part(t, src, h):
        own, rest = parts[t]
        return own.at[src, rows_at(h)] if src <= CORE else rest.at[src - 2, rows_at(h)]

    def core_copy(i):
        t, src, h = OPS[i]
        return remote(part(t, src | CORE, h), land.at[i], core_sem, (i,), {"ep": peer[CORE]})

    def stage_copy(i):
        t, src, h = OPS[i]
        return pltpu.make_async_copy(part(t, src, h), stage.at[i % STAGES], stage_sem.at[i % STAGES])

    def far_copy(i):
        t, _, h = OPS[i]
        return remote(land.at[i], far_land.at[t, h], far_sem, (t, h), {"ep": peer[NEAR[h]]})

    def near_copy(i):
        t, src, h = OPS[i]
        k = NEAR.index(src)
        return remote(land.at[i], outs[t][k].at[rows_at(h)], near_sem, (t, k, h), {"ep": peer[src]})

    def own_copy(i):
        t, _, h = OPS[i]
        return pltpu.make_async_copy(land.at[i], outs[t][LAST].at[rows_at(h)], own_sem.at[t, h])

    def out_copy(i):
        src = OPS[i][1]
        return (far_copy if src == FAR else near_copy if src else own_copy)(i)

    def reduce_op(i):
        t, src, h = OPS[i]
        stage_copy(i).wait()
        core_copy(i).wait_recv()
        add_rows(land.at[i], stage.at[i % STAGES])
        if i + STAGES < len(OPS):
            stage_copy(i + STAGES).start()
        if (src, h) in RELAYED:
            far_copy(OPS.index((t, FAR, RELAYED[src, h]))).wait_recv()
            add_rows(land.at[i], far_land.at[t, RELAYED[src, h]])

    rows_per = z_one.shape[1]
    chunks = [(m, e, k) for e in range(dws[FIRST].shape[FIRST]) for m in range(mats) for k in SPLIT]
    n = len(chunks)

    def piece(arrays, c):
        m, e, k = chunks[c]
        return arrays[m].at[e, pl.ds(k * rows_per, rows_per)]

    def one_copy(c):
        return remote(piece(dws, c), z_one.at[c % SLOTS], z_sem, (FIRST, c), {"dp": z_peer})

    def two_copy(c):
        return remote(z_one.at[c % SLOTS], z_two.at[c % SLOTS], z_sem, (1, c), {"dp": z_cross})

    def three_copy(c):
        return remote(z_two.at[c % SLOTS], piece(dw_outs, c), z_sem, (2, c), {"dp": z_peer})

    def keep_copy(c):
        return pltpu.make_async_copy(z_two.at[c % SLOTS], piece(dw_outs, c), keep_sem.at[c])

    def load_copy(c):
        return pltpu.make_async_copy(piece(dws, c), z_stage.at[c % STAGES], load_sem.at[c % STAGES])

    def first_add(c):
        load_copy(c).wait()
        one_copy(c).wait_recv()
        add_rows(z_one.at[c % SLOTS], z_stage.at[c % STAGES])
        if c + STAGES < n:
            load_copy(c + STAGES).start()

    def second_add(c):
        two_copy(c).wait()
        add_rows(z_two.at[c % SLOTS], z_one.at[c % SLOTS])
        if c + SLOTS < n:
            pl.semaphore_signal(credit_one, device_id={"dp": z_peer}, device_id_type=MESH)

    def retire(c):
        three_copy(c).wait_send()
        keep_copy(c).wait()
        if c + SLOTS < n:
            pl.semaphore_signal(credit_two, device_id={"dp": z_cross}, device_id_type=MESH)

    @pl.when(is_end)
    def _():
        for c in range(SLOTS):
            one_copy(c).start()

    @pl.when(is_mid)
    def _():
        for c in range(STAGES):
            load_copy(c).start()

    for i in range(len(OPS)):
        core_copy(i).start()
        if i < STAGES:
            stage_copy(i).start()

    todo = list(range(len(OPS)))
    for tick in range(n + LAG):
        mine = todo[: 2 if tick < 2 else tick % 2]
        todo = todo[len(mine) :]
        for i in mine:
            reduce_op(i)

        @pl.when(is_mid)
        def _():
            back = tick - BACK
            if tick < n:
                first_add(tick)
            if back in range(n):
                second_add(back)
            if tick < n:
                if tick >= SLOTS:
                    pl.semaphore_wait(credit_two, 1)
                two_copy(tick).start()
            if back in range(n):
                three_copy(back).start()
                keep_copy(back).start()
            if tick >= LAG:
                retire(tick - LAG)

        for i in mine:
            out_copy(i).start()

        @pl.when(is_end)
        def _():
            if tick + SLOTS < n:
                pl.semaphore_wait(credit_one, 1)
                one_copy(tick + SLOTS).start()

    for i in todo:
        reduce_op(i)
        out_copy(i).start()

    @pl.when(is_end)
    def _():
        for c in range(n):
            one_copy(c).wait_send()
            three_copy(c).wait_recv()

    for i in range(len(OPS)):
        core_copy(i).wait_send()
        (out_copy(i).wait_send if OPS[i][1] == FAR else out_copy(i).wait)()


def run_exchange(parts, dws):
    tokens, d_model = parts[FIRST][FIRST].shape[1:]
    half = tokens // 2
    local, rows, cols = dws[FIRST].shape
    chunk = (rows // len(SPLIT), cols)
    n = local * len(dws) * len(SPLIT)
    whole = Shape((tokens, d_model), bf16)
    flat = [v for tensor in parts for v in tensor] + list(dws)
    terms = len(NEAR) + 1
    out = pl.pallas_call(
        functools.partial(exchange_kernel, half, len(dws)),
        in_specs=[ANY] * len(flat),
        out_specs=[ANY] * (terms * len(TENSORS) + len(dws)),
        out_shape=[whole] * (terms * len(TENSORS)) + [Shape(v.shape, bf16) for v in dws],
        scratch_shapes=[
            pltpu.VMEM((len(OPS), half, d_model), bf16),
            pltpu.VMEM((len(TENSORS), len(HALVES), half, d_model), bf16),
            pltpu.VMEM((STAGES, half, d_model), bf16),
            pltpu.VMEM((SLOTS, *chunk), bf16),
            pltpu.VMEM((SLOTS, *chunk), bf16),
            pltpu.VMEM((STAGES, *chunk), bf16),
            DMA((2, len(OPS))),
            DMA((STAGES,)),
            DMA((2, 2, 2)),
            DMA((2, 2, 2, 2)),
            DMA((2, 2)),
            DMA((2, 3, n)),
            DMA((n,)),
            DMA((STAGES,)),
            pltpu.SemaphoreType.REGULAR,
            pltpu.SemaphoreType.REGULAR,
        ],
        compiler_params=pltpu.CompilerParams(vmem_limit_bytes=VMEM_LIMIT, collective_id=FIRST, has_side_effects=True),
        cost_estimate=cost(1 << 37, 200 << 20),
        name="exchange",
    )(*flat)
    return [out[:terms], out[terms : 2 * terms]], out[2 * terms :]


def hop(v, bit):
    return lax.ppermute(v, "ep", [(i, i ^ bit) for i in SOURCES])


def after(values, token):
    return lax.optimization_barrier((values, token))[FIRST]


def send_own(v, token):
    got = {(FIRST, *WHOLE): v, (CORE, *WHOLE): hop(v, CORE)}
    pieces = after([v[first * BLK : (first + count) * BLK] for first, count in PARTS], token)
    for part, piece in zip(PARTS, pieces):
        got.update({(bit, *part): hop(piece, bit) for bit in NEAR})
    return got


def pass_on(got, h):
    part = PARTS[h]
    got[FAR, *part] = hop(got[(Y, X)[h], *part], NEAR[h])
    for bit in NEAR:
        got[bit | CORE, *part] = hop(got[bit, *part], CORE)


def relative(v, me):
    shape = v.shape
    v = v.reshape((2, 2, 2) + shape[1:])
    for axis, bit in enumerate((Y, X, CORE)):
        v = jnp.where((me & bit) != FIRST, jnp.flip(v, axis), v)
    return v.reshape(shape)


def solution(mesh):
    dp_size = mesh.shape["dp"]
    ep_size = mesh.shape["ep"]
    row_spec = P(("dp", "ep"), None)
    expert_spec = P("ep", None, None)
    whole_spec = P(None, None)

    def per_device(x_loc, w_router, ids_loc, w1, w3, w2, dy_loc):
        tokens, d_model = x_loc.shape
        top_k = ids_loc.shape[1]
        experts = w_router.shape[1]
        local = w1.shape[FIRST]
        capacity = capacity_of(tokens, top_k, experts)
        n_total = tokens * dp_size * ep_size
        nb = tokens // BLK
        row_cap = padded(4 * capacity)
        me = lax.axis_index("ep")

        ids_t = ids_loc.T
        send_tab, prob_t = run_router(x_loc, w_router, ids_t, capacity, local, ep_size)
        tables = lax.all_to_all(send_tab, "ep", FIRST, FIRST, tiled=True)
        gathered = [send_own(v, tables) for v in (x_loc, dy_loc)]
        tab_rel = relative(tables, me)
        tab = tab_rel[:, :, :tokens].reshape(ep_size, 2 * local, nb, BLK).transpose(0, 2, 1, 3).reshape(ep_size * nb, 2 * local, BLK)
        starts = tab_rel[:, local:, tokens : tokens + ALIGN].astype(i32).reshape(LAST)

        def y_of(groups, starts):
            return run_y(groups, starts, tab, rows[FIRST], w2, gathered[1], nb)

        def dx_of(groups, starts):
            return run_dx(groups, starts, tab, rows[1], rows[2], w1, w3, nb)

        acc = rows = ()
        own, rest = (FIRST,), (1, 2, 3)
        for g, group in enumerate(GROUPS):
            if g:
                ready = [p for p in group if not p[FIRST] & CORE]
                for got in gathered:
                    got.update(after({p: got[p] for p in ready}, acc[LAST]))
                for got in gathered:
                    if g < len(GROUPS) - 1:
                        pass_on(got, g - 1)
                    else:
                        for src, *part in ready:
                            got[src | CORE, *part] = hop(got[src, *part], CORE)
                here = after(starts, [[got[p] for p in ready] for got in gathered])
                if g == 2:
                    y_own, dg_own = y_of(own, here)
                    starts = after(starts, dg_own)
                if g > 2:
                    dx_own = dx_of(own, here)
                    starts = after(starts, dx_own)
            rows, acc = run_grad(starts, tab, g, *[[got[p] for p in group] for got in gathered], (w1, w3, w2), acc, rows, nb, row_cap)
            if not g:
                stats = jnp.sum(after(tab_rel[:, :local, tokens:], acc[LAST]), axis=FIRST)
                for step in (1, 2):
                    stats = stats + lax.ppermute(stats, "dp", [(i, i ^ step) for i in range(dp_size)])
                starts = after(starts, stats)
        dw1, dw3, dw2 = acc
        starts, dw2 = lax.optimization_barrier((starts, dw2))
        dw2_sum = lax.psum(dw2, "dp")

        y_rest, dg_rest = y_of(rest, starts)
        dg = jnp.concatenate([dg_own, dg_rest], axis=FIRST)
        dg = dg[:, :local].reshape(ep_size, nb, local, BLK).transpose(0, 2, 1, 3).reshape(ep_size, local, tokens)
        dg = jnp.concatenate([relative(dg, me), jnp.broadcast_to(stats, (ep_size, *stats.shape))], axis=2)
        starts, dg = lax.optimization_barrier((starts, dg))
        dx_rest = dx_of(rest, starts)
        dg_all = lax.all_to_all(dg, "ep", FIRST, FIRST, tiled=True).reshape(experts, tokens + LANES)
        load = dg_all[:, tokens:]
        share = AUX_COEF * experts / (n_total * top_k * n_total)
        aux_loss = share * jnp.sum(load[:, FIRST] * load[:, 1])
        dlog_t, dwr_t = run_router_grad(x_loc, prob_t, dg_all[:, :tokens], ids_t, load, share)
        dw_router = lax.psum(dwr_t, ("dp", "ep")).T

        parts = [[v.reshape(LAST, tokens, d_model) for v in pair] for pair in ((y_own, y_rest), (dx_own, dx_rest))]
        sums, grads = run_exchange(parts, [dw1, dw3])
        y_loc, dx_loc = run_final(dlog_t, w_router.T, *sums)
        return y_loc, aux_loss, dx_loc, dw_router, *grads, dw2_sum

    return jax.shard_map(
        per_device,
        mesh=mesh,
        in_specs=(row_spec, whole_spec, row_spec, expert_spec, expert_spec, expert_spec, row_spec),
        out_specs=(row_spec, P(), row_spec, whole_spec, expert_spec, expert_spec, expert_spec),
        check_vma=False,
    )
```

```python
import functools

import jax
import jax.numpy as jnp
import numpy as np
from jax import lax
from jax.experimental import pallas as pl
from jax.experimental.pallas import tpu as pltpu
from jax.sharding import PartitionSpec as P


AUX_COEF = 0.01
BLK = 256
TILE = 256
WIN = 128
LANES = 128
ALIGN = 16
NOT_KEPT = -65536.0
VMEM_LIMIT = 63 * 1024 * 1024
CORE, X, Y = 1, 2, 4
FAR = X | Y
HALVES = TENSORS = range(2)
RING = 4
SOURCES = range(8)
FIRST, LAST = 0, -1
SEND, RECV = 0, 1
STAGES = 3
SLOTS = 16
SPLIT = range(4)
BACK, LAG = 2, 4
MESH = pl.DeviceIdType.MESH

WHOLE, PARTS = (0, 6), ((0, 3), (3, 3))
GROUPS = (
    [(src, *WHOLE) for src in (FIRST, CORE)],
    [(bit | core, *PARTS[FIRST]) for bit in (X, Y) for core in (FIRST, CORE)],
    [(bit | core, *PARTS[1]) for bit in (X, Y) for core in (FIRST, CORE)],
    [(FAR | core, *part) for part in PARTS for core in (FIRST, CORE)],
)


f32 = jnp.float32
bf16 = jnp.bfloat16
i32 = jnp.int32
ANY = pl.BlockSpec(memory_space=pl.ANY)
SMEM = pl.BlockSpec(memory_space=pltpu.SMEM)
VMEM = pl.BlockSpec(memory_space=pltpu.VMEM)
DMA = pltpu.SemaphoreType.DMA
Shape = jax.ShapeDtypeStruct


def capacity_of(tokens, top_k, experts):
    return (5 * top_k * tokens + 4 * experts - 1) // (4 * experts)


def dot(a, b, ca=1, cb=0):
    return lax.dot_general(a, b, (((ca,), (cb,)), ((), ())), preferred_element_type=f32)


def dot_nt(a, b):
    return dot(a, b, 1, 1)


def dot_tn(a, b):
    return dot(a, b, 0, 0)


def grid_params(dims):
    return pltpu.CompilerParams(dimension_semantics=("arbitrary",) * dims, vmem_limit_bytes=VMEM_LIMIT)


def params():
    return grid_params(1)


def cost(flops, moved):
    return pl.CostEstimate(flops=flops, bytes_accessed=moved, transcendentals=FIRST)


def iota(shape, dim):
    return lax.broadcasted_iota(i32, shape, dim)


def span(start, size, multiple=None):
    return pl.ds(pl.multiple_of(start, multiple or size), size)


def lane_sum(v):
    return jnp.sum(v, axis=1, keepdims=True)


def row_sum(v):
    return jnp.sum(v, axis=0, keepdims=True)


def where0(mask, v):
    return jnp.where(mask, v, jnp.zeros_like(v))


def one_hot(mask):
    return jnp.where(mask, 1.0, 0.0).astype(bf16)


def split3(v):
    hi = v.astype(bf16)
    rest = v - hi.astype(f32)
    mid = rest.astype(bf16)
    return hi, mid, (rest - mid.astype(f32)).astype(bf16)


def loop(start, stop, body):
    def step(i, carry):
        body(i)
        return carry

    lax.fori_loop(start, stop, step, FIRST)


def chosen_mask(ids, experts):
    rows = iota((experts, ids.shape[1]), FIRST)
    return functools.reduce(jnp.logical_or, [rows == ids[j : j + 1, :] for j in range(ids.shape[FIRST])])


def router_kernel(capacity, local, x_ref, w_ref, ids_ref, tab_ref, prob_ref, carry):
    step = pl.program_id(FIRST)
    steps = pl.num_programs(FIRST)
    experts = w_ref.shape[1]

    @pl.when(step == FIRST)
    def _():
        carry[...] = jnp.zeros_like(carry)
        tab_ref[...] = jnp.zeros_like(tab_ref)

    x = x_ref[...]
    hi, mid, low = [dot(x, part) for part in split3(w_ref[...])]
    logits = jnp.transpose(hi + (mid + low))
    expo = jnp.exp(logits - jnp.max(logits, axis=FIRST, keepdims=True))
    prob = expo / row_sum(expo)
    chosen = chosen_mask(ids_ref[...], experts)
    hits = jnp.where(chosen, 1.0, 0.0)
    gate = where0(chosen, prob / row_sum(where0(chosen, prob)))
    earlier = one_hot(iota((BLK, BLK), FIRST) < iota((BLK, BLK), 1))
    before = carry[:, :1]
    pos = dot(hits.astype(bf16), earlier) + before
    pos = jnp.where(chosen & (pos < capacity), pos, NOT_KEPT)
    prob_ref[...] = prob
    after = before + lane_sum(hits)
    lane = iota((experts, LANES), 1)
    first = where0(lane == step, jnp.minimum(before, capacity) + jnp.zeros((experts, LANES), f32))
    first = first + where0((lane == step + 1) & (step == steps - 1), jnp.minimum(after, capacity) + jnp.zeros((experts, LANES), f32))
    stat = where0(lane == FIRST, lane_sum(hits) + jnp.zeros((experts, LANES), f32))
    stat = stat + where0(lane == 1, lane_sum(prob) + jnp.zeros((experts, LANES), f32))
    tail = slice(tab_ref.shape[LAST] - LANES, None)
    for d in range(experts // local):
        rows = slice(d * local, (d + 1) * local)
        tab_ref[d, :local, span(step * BLK, BLK)] = gate[rows]
        tab_ref[d, local:, span(step * BLK, BLK)] = pos[rows]
        tab_ref[d, :local, tail] += stat[rows]
        tab_ref[d, local:, tail] += first[rows]
    carry[:, :1] = after


def run_router(x_loc, w_router, ids_t, capacity, local, devices):
    tokens, d_model = x_loc.shape
    experts = w_router.shape[1]
    top_k = ids_t.shape[FIRST]
    table = (devices, 2 * local, tokens + LANES)
    return pl.pallas_call(
        functools.partial(router_kernel, capacity, local),
        grid=(tokens // BLK,),
        in_specs=[pl.BlockSpec((BLK, d_model), lambda i: (i, FIRST)), VMEM, pl.BlockSpec((top_k, BLK), lambda i: (FIRST, i))],
        out_specs=[VMEM, pl.BlockSpec((experts, BLK), lambda i: (FIRST, i))],
        out_shape=[Shape(table, f32), Shape((experts, tokens), f32)],
        scratch_shapes=[pltpu.VMEM((experts, LANES), f32)],
        compiler_params=params(),
        cost_estimate=cost(2 * tokens * d_model * BLK, 2 * tokens * d_model),
        name="router",
    )(x_loc, w_router, ids_t)


class Blocks:
    def __init__(self, starts_ref, bmap_ref):
        self.starts, self.bmap = starts_ref, bmap_ref

    def info(self, i, e):
        at = self.bmap[2 * i + 1] + e * ALIGN
        first = self.starts[at]
        return self.bmap[2 * i], first, self.starts[at + 1] - first

    def total(self, start, count, e):
        return lax.fori_loop(start, start + count, lambda i, n: n + self.info(i, e)[LAST], i32(FIRST))


def aligned(row):
    base = (row // ALIGN) * ALIGN
    return base, row - base


def window_count(shift, count):
    return (shift + count + WIN - 1) // WIN


def padded(total):
    return (total + TILE - 1) // TILE * TILE


def row_tiles(total, body, size):
    tiles = (total + size - 1 - size // 2) // size
    loop(FIRST, tiles, lambda i: body(i * size, size))
    pl.when(padded(total) > tiles * size)(lambda: body(tiles * size, size // 2))


def start(copies):
    for cp in copies:
        cp.start()


def wait(copies):
    for cp in copies:
        cp.wait()


def taker(refs):
    refs = list(refs)

    def take(n=None):
        got = refs[:n]
        del refs[:n]
        return got

    return take


def block_count(pieces):
    return sum(count for _, _, count in pieces)


def offsets(pieces):
    counts = [count for _, _, count in pieces]
    return [(sum(counts[:k]), count) for k, count in enumerate(counts)]


def block_rows(first, count):
    return pl.ds(first * BLK, count * BLK)


def grad_kernel(g, last, local, pieces, *refs):
    take = taker(refs)
    n = len(pieces)
    starts_ref, bmap_ref, tab_ref = take(3)
    tok_refs = take(n), take(n)
    w1_ref, w3_ref, w2_ref = take(3)
    acc_in = take(2 * bool(g))
    take(3 * bool(g))
    row_outs = take(3)
    outs = take(3 if last else 2)
    xv, dv, xr, dr, acc13, acc2, stage, tok_sem, in_sem, out_sem, row_sem = take()
    accs = acc13, acc2
    e = pl.program_id(FIRST)
    slot = e % 2
    d_model = xv.shape[1]
    d_ff = w1_ref.shape[LAST]
    blocks = Blocks(starts_ref, bmap_ref)
    count = xv.shape[FIRST] // BLK

    parts = [(c, at, first + at) for c, (first, size) in enumerate(offsets(pieces)) for at in range(FIRST, size, 3)]

    def token_copies(k):
        c, at, to = parts[k]
        src_rows, dst_rows = block_rows(at, 3), block_rows(to, 3)
        return [pltpu.make_async_copy(src[c].at[src_rows], dst.at[dst_rows], tok_sem.at[w, k]) for w, (src, dst) in enumerate(zip(tok_refs, (xv, dv)))]

    def in_copies(ee, ss):
        return [pltpu.make_async_copy(src.at[ee], dst.at[ss], in_sem.at[ss, k]) for k, (src, dst) in enumerate(zip(acc_in, accs))]

    def out_copies(ee, ss):
        return [pltpu.make_async_copy(src.at[ss], dst.at[ee], out_sem.at[ss, k]) for k, (src, dst) in enumerate(zip(accs, outs))]

    @pl.when(e == FIRST)
    def _():
        for k in range(len(parts)):
            start(token_copies(k))

    if g:
        pl.when(e == FIRST)(lambda: start(in_copies(e, slot)))
    else:
        pl.when(e >= 2)(lambda: wait(out_copies(e - 2, slot)))
        for acc in accs:
            acc[slot] = jnp.zeros(acc.shape[1:], f32)

    def prefetch():
        if not last:
            pl.when(e > FIRST)(lambda: wait(out_copies(e - 1, 1 - slot)))
        start(in_copies(e + 1, 1 - slot))

    def maybe_prefetch(now):
        if g:
            pl.when(now & (e + 1 < local))(prefetch)

    row_iota = iota((WIN, BLK), FIRST).astype(f32)
    head_row = iota((ALIGN, d_model), FIRST)
    both = tuple(HALVES)

    def dispatch(step, rows_at):
        todo = []
        for i in (2 * step, 2 * step + 1):
            for k, (_, _, first) in enumerate(parts):
                pl.when((e == FIRST) & (i == first))(lambda: wait(token_copies(k)))
            infos = [blocks.info(i, e + q) for q in both]
            todo.append((span(i * BLK, BLK), infos, [aligned(r) for r in rows_at]))
            rows_at = tuple(r + info[LAST] for r, info in zip(rows_at, infos))

        def picks(block, q, k):
            _, infos, places = block
            flat, first, _ = infos[q]
            pos = tab_ref[flat, pl.ds(local + e + q, 1), :]
            gate = tab_ref[flat, pl.ds(e + q, 1), :]
            pick = (pos + (places[q][1] - first - k * WIN).astype(f32)) == row_iota
            return one_hot(pick), lane_sum(where0(pick, gate + jnp.zeros_like(row_iota)))

        def rows_for(block, one, gate_row):
            tok = block[FIRST]
            return dot(one, xv[tok, :]).astype(bf16), (dot(one, dv[tok, :]) * gate_row).astype(bf16)

        def first_rows(block):
            pair = [picks(block, q, i32(FIRST)) for q in both]
            return rows_for(block, *[jnp.concatenate(v, axis=FIRST) for v in zip(*pair)])

        def put(block, new):
            for q in both:
                base, shift = block[LAST][q]
                head = span(base, ALIGN)
                for value, rows in zip(new, (xr, dr)):
                    value = value[q * WIN : (q + 1) * WIN]
                    rows[q, head, :] = jnp.where(head_row < shift, rows[q, head, :], value[:ALIGN])
                    rows[q, span(base + ALIGN, WIN - ALIGN, ALIGN), :] = value[ALIGN:]

        windows = [[window_count(places[q][1], infos[q][LAST]) for q in both] for _, infos, places in todo]
        simple = functools.reduce(jnp.logical_and, [w <= 1 for ws in windows for w in ws])

        @pl.when(simple)
        def _():
            for block, new in zip(todo, [first_rows(block) for block in todo]):
                put(block, new)

        @pl.when(jnp.logical_not(simple))
        def _():
            for block, ws in zip(todo, windows):
                put(block, first_rows(block))
                for q in both:

                    def more(k):
                        for value, rows in zip(rows_for(block, *picks(block, q, k)), (xr, dr)):
                            rows[q, span(block[LAST][q][FIRST] + k * WIN, WIN, ALIGN), :] = value

                    loop(1, ws[q], more)

        return rows_at

    @pl.when(slot == FIRST)
    def _():
        totals = lax.fori_loop(FIRST, count // 2, dispatch, (i32(FIRST),) * len(both))
        for q in both:

            def clear(i):
                for rows in (xr, dr):
                    rows[q, span(i * ALIGN, ALIGN), :] = jnp.zeros((ALIGN, d_model), bf16)

            loop((totals[q] + ALIGN - 1) // ALIGN, padded(totals[q]) // ALIGN, clear)

    wait(in_copies(e, slot))

    def tile(at, size):
        maybe_prefetch((at == FIRST) & (slot == FIRST))
        rows = span(at, size)
        xt = xr[slot, rows, :]
        dt = dr[slot, rows, :]
        act_a = dot(xt, w1_ref[FIRST])
        act_b = dot(xt, w3_ref[FIRST])
        d_hidden = dot_nt(dt, w2_ref[FIRST]).astype(bf16).astype(f32)
        sig = 1.0 / (1.0 + jnp.exp(-act_a))
        silu = act_a * sig
        hidden = (silu * act_b).astype(bf16)
        d_a = (d_hidden * act_b * sig * (1.0 + act_a * (1.0 - sig))).astype(bf16)
        d_b = (d_hidden * silu).astype(bf16)
        copies = []
        for k, (value, out) in enumerate(zip((hidden, d_a, d_b), row_outs)):
            stage[k, :size] = value
            copies.append(pltpu.make_async_copy(stage.at[k, :size], out.at[g, e, rows], row_sem.at[k]))
        start(copies)
        acc13[slot, :, :d_ff] += dot_tn(xt, d_a)
        acc13[slot, :, d_ff:] += dot_tn(xt, d_b)
        acc2[slot] += dot_tn(hidden, dt)
        wait(copies)

    total = blocks.total(FIRST, count, e)
    row_tiles(total, tile, 2 * TILE)
    maybe_prefetch((total == FIRST) | (slot > FIRST))

    if last:
        for out, value in zip(outs, (acc13[slot, :, :d_ff], acc13[slot, :, d_ff:], acc2[slot])):
            out[FIRST] = value.astype(bf16)
    else:
        start(out_copies(e, slot))

        @pl.when(e == pl.num_programs(FIRST) - 1)
        def _():
            wait(out_copies(e - 1, 1 - slot))
            wait(out_copies(e, slot))


def per_expert(*shape):
    return pl.BlockSpec((1, *shape), lambda e: (e,) + (FIRST,) * len(shape))


def block_map(pieces, nb):
    spots = [(src, first + b) for src, first, count in pieces for b in range(count)]
    return np.asarray([v for src, b in spots for v in (src * nb + b, src * 4 * ALIGN + b)], np.int32)


def run_grad(starts, tab, g, xs, ds, weights, acc, rows, nb, row_cap):
    pieces = GROUPS[g]
    last = g == len(GROUPS) - 1
    local, d_model, d_ff = weights[FIRST].shape
    count = block_count(pieces) * BLK
    w_specs = [per_expert(*w.shape[1:]) for w in weights]
    sums = [(local, d_model, 2 * d_ff), (local, d_ff, d_model)]
    row_shape = [Shape((len(GROUPS), local, row_cap, d_ff), bf16)] * 3
    out_shape = row_shape + ([Shape(w.shape, bf16) for w in weights] if last else [Shape(s, f32) for s in sums])
    out_specs = [ANY] * 3 + (w_specs if last else [ANY] * 2)
    tokens = pltpu.VMEM((count, d_model), bf16)
    packed = pltpu.VMEM((2, row_cap + WIN, d_model), bf16)
    ins = [starts, block_map(pieces, nb), tab, *xs, *ds, *weights, *acc, *rows]
    out = pl.pallas_call(
        functools.partial(grad_kernel, g, last, local, pieces),
        grid=(local,),
        in_specs=[SMEM, SMEM, VMEM] + [ANY] * (2 * len(pieces)) + w_specs + [ANY] * (len(acc) + len(rows)),
        out_specs=out_specs,
        out_shape=out_shape,
        scratch_shapes=[tokens, tokens, packed, packed]
        + [pltpu.VMEM((2, *s[1:]), f32) for s in sums]
        + [pltpu.VMEM((3, 2 * TILE, d_ff), bf16), DMA((2, count // (3 * BLK))), DMA((2, 2)), DMA((2, 2)), DMA((3,))],
        input_output_aliases={len(ins) - len(rows) + k: k for k in range(len(rows))},
        compiler_params=params(),
        cost_estimate=cost(12 * count * d_model * d_ff, 40 << 20),
        name="expert_grad",
    )(*ins)
    return out[:3], out[3:]


def group_spans(groups):
    counts = [block_count(GROUPS[g]) for g in groups]
    return np.asarray([v for k, c in enumerate(counts) for v in (sum(counts[:k]), c)], np.int32)


def per_group(groups, *shape):
    return pl.BlockSpec((1, 1, *shape), lambda step, e: (step + groups[FIRST], e) + (FIRST,) * len(shape))


def per_local(*shape):
    return pl.BlockSpec((1, *shape), lambda g, e: (e,) + (FIRST,) * len(shape))


class BlockRows:
    def __init__(self, owner, i, rows_at):
        ee = range(owner.local)
        self.owner, self.i = owner, i
        self.infos = [owner.blocks.info(i, k) for k in ee]
        self.places = [aligned(r) for r in rows_at]
        self.windows = [window_count(self.places[k][1], self.infos[k][LAST]) for k in ee]
        self.simple = functools.reduce(jnp.logical_and, [w <= 1 for w in self.windows])
        self.flat = self.infos[FIRST][FIRST]
        self.tok = span((i - owner.first) * BLK, BLK)
        self.out = owner.ring.at[i % RING]
        self.after = tuple(r + info[LAST] for r, info in zip(rows_at, self.infos))

    def load(self):
        self.tab_t = jnp.transpose(self.owner.tab_ref[self.flat])

    def gate(self, ee):
        return self.tab_t[:, ee : ee + 1]

    def pick(self, ee, k=FIRST):
        at = self.owner.local + ee
        shift = self.places[ee][1] - self.infos[ee][1] - k * WIN
        return one_hot((self.tab_t[:, at : at + 1] + shift.astype(f32)) == self.owner.lane)

    def held(self, ee, k=FIRST, cols=slice(None)):
        return self.owner.rows_ref[ee, span(self.places[ee][FIRST] + k * WIN, WIN, ALIGN), cols]


class Combine:
    def __init__(self, local, starts_ref, bmap_ref, spans_ref, tab_ref, rows_ref, out_ref, ring, sems):
        step = pl.program_id(FIRST)
        self.e = pl.program_id(1)
        self.blocks = Blocks(starts_ref, bmap_ref)
        self.first, self.count = spans_ref[2 * step], spans_ref[2 * step + 1]
        self.total = self.blocks.total(self.first, self.count, self.e)
        self.local, self.tab_ref, self.rows_ref = local, tab_ref, rows_ref
        self.out_ref, self.ring, self.sems = out_ref, ring, sems
        self.lane = iota((BLK, WIN), 1).astype(f32)

    def zero_tail(self):
        rows = span(padded(self.total), WIN)
        self.rows_ref[self.e, rows, :] = jnp.zeros((WIN, self.rows_ref.shape[LAST]), bf16)

    def out_copy(self, i):
        slot = i % RING
        place = self.blocks.bmap[2 * i] - self.blocks.bmap[FIRST]
        return pltpu.make_async_copy(self.ring.at[slot], self.out_ref.at[place], self.sems.at[slot])

    def run(self, simple_body, full_body):
        def pair(step, rows_at):
            i = self.first + 2 * step
            one = BlockRows(self, i, rows_at)
            two = BlockRows(self, i + 1, one.after)
            for block in (one, two):
                pl.when(block.i - self.first >= RING)(lambda: self.out_copy(block.i - RING).wait())
            simple = one.simple & two.simple

            @pl.when(simple)
            def _():
                for block in (one, two):
                    block.load()
                for block in (one, two):
                    simple_body(block)

            @pl.when(jnp.logical_not(simple))
            def _():
                def full(k, rows_at):
                    block = BlockRows(self, i + k, rows_at)
                    block.load()
                    full_body(block)
                    return block.after

                lax.fori_loop(FIRST, 2, full, rows_at)

            for block in (one, two):
                self.out_copy(block.i).start()
            return two.after

        stop = self.first + self.count
        lax.fori_loop(FIRST, self.count // 2, pair, (i32(FIRST),) * self.local)
        loop(stop - RING, stop, lambda i: self.out_copy(i).wait())


def y_kernel(groups, local, starts_ref, bmap_ref, spans_ref, tab_ref, h_ref, w2_ref, *refs):
    take = taker(refs)
    d_refs = [take(len(GROUPS[g])) for g in groups]
    y_ref, dg_ref, o_rows, dv, ring, zacc, yacc, dgacc, tok_sem, out_sem = take()
    all_rows = Combine(local, starts_ref, bmap_ref, spans_ref, tab_ref, o_rows, y_ref, ring, out_sem)
    e = all_rows.e
    d_model = dv.shape[1]

    def token_copies(step):
        spots = offsets(GROUPS[groups[step]])
        return [pltpu.make_async_copy(src, dv.at[block_rows(*spot)], tok_sem.at[c]) for c, (src, spot) in enumerate(zip(d_refs[step], spots))]

    for step in range(len(groups)):
        pl.when((pl.program_id(FIRST) == step) & (e == FIRST))(lambda: start(token_copies(step)))

    def tile(at, size):
        rows = span(at, size)
        o_rows[e, rows, :] = dot(h_ref[FIRST, FIRST, rows, :], w2_ref[FIRST]).astype(bf16)

    row_tiles(all_rows.total, tile, 2 * TILE)
    all_rows.zero_tail()

    @pl.when(e == local - 1)
    def _():
        for step in range(len(groups)):
            pl.when(pl.program_id(FIRST) == step)(lambda: wait(token_copies(step)))
        dg_lane = iota((BLK, LANES), 1)
        width = 2 * LANES
        columns = [slice(k * width, (k + 1) * width) for k in range(d_model // width)]

        def put_dg(block, sums):
            dg = sum(where0(dg_lane == ee, lane_sum(s) + jnp.zeros((BLK, LANES), f32)) for ee, s in enumerate(sums))
            dg_ref[block.flat - all_rows.blocks.bmap[FIRST]] = jnp.transpose(dg)[: 2 * local, :]

        def simple(block):
            picks = [block.pick(ee) for ee in range(local)]
            sums = [None] * local
            for cols in columns:
                dy = dv[block.tok, cols].astype(f32)
                y = None
                for ee in range(local):
                    z = dot(picks[ee], block.held(ee, cols=cols))
                    prod = dy * z
                    part = prod[:, :LANES] + prod[:, LANES:]
                    sums[ee] = part if sums[ee] is None else sums[ee] + part
                    y = block.gate(ee) * z if y is None else y + block.gate(ee) * z
                block.out[:, cols] = y.astype(bf16)
            put_dg(block, sums)

        def full(block):
            yacc[...] = jnp.zeros_like(yacc)
            for ee in range(local):
                zacc[...] = jnp.zeros_like(zacc)

                def more(k):
                    zacc[...] += dot(block.pick(ee, k), block.held(ee, k))

                loop(FIRST, block.windows[ee], more)
                yacc[...] += block.gate(ee) * zacc[...]
                dgacc[ee] = lane_sum(dv[block.tok, :].astype(f32) * zacc[...]) * jnp.where(dg_lane == FIRST, 1.0, 0.0)
            block.out[...] = yacc[...].astype(bf16)
            put_dg(block, [dgacc[ee] for ee in range(local)])

        all_rows.run(simple, full)


def combine_scratch(local, row_cap, d_model):
    return [pltpu.VMEM((local, row_cap + WIN, d_model), bf16)], [pltpu.VMEM((RING, BLK, d_model), bf16), pltpu.VMEM((BLK, d_model), f32)]


def run_y(groups, starts, tab, h_rows, w2, ds, nb):
    local, d_ff, d_model = w2.shape
    row_cap = h_rows.shape[2]
    pieces = [p for g in groups for p in GROUPS[g]]
    spans = group_spans(groups)
    blocks = block_count(pieces)
    rows, work = combine_scratch(local, row_cap, d_model)
    return pl.pallas_call(
        functools.partial(y_kernel, groups, local),
        grid=(len(groups), local),
        in_specs=[SMEM, SMEM, SMEM, VMEM, per_group(groups, row_cap, d_ff), per_local(d_ff, d_model)] + [ANY] * len(pieces),
        out_specs=[ANY, VMEM],
        out_shape=[Shape((blocks, BLK, d_model), bf16), Shape((blocks, 2 * local, BLK), f32)],
        scratch_shapes=rows + [pltpu.VMEM((max(spans[1::2]) * BLK, d_model), bf16)] + work + [work[LAST], pltpu.VMEM((local, BLK, LANES), f32), DMA((4,)), DMA((RING,))],
        compiler_params=grid_params(2),
        cost_estimate=cost(4 * blocks * BLK * d_model * d_ff, 20 << 20),
        name="expert_y",
    )(starts, block_map(pieces, nb), spans, tab, h_rows, w2, *[ds[p] for p in pieces])


def dx_kernel(local, starts_ref, bmap_ref, spans_ref, tab_ref, da_ref, db_ref, w1_ref, w3_ref, dx_ref, o_rows, ring, zacc, out_sem):
    all_rows = Combine(local, starts_ref, bmap_ref, spans_ref, tab_ref, o_rows, dx_ref, ring, out_sem)
    e = all_rows.e

    def tile(at, size):
        rows = span(at, size)
        grad = dot_nt(da_ref[FIRST, FIRST, rows, :], w1_ref[FIRST]) + dot_nt(db_ref[FIRST, FIRST, rows, :], w3_ref[FIRST])
        o_rows[e, rows, :] = grad.astype(bf16)

    row_tiles(all_rows.total, tile, 2 * TILE)
    all_rows.zero_tail()

    @pl.when(e == local - 1)
    def _():
        def simple(block):
            pairs = [(ee, ee + 1) for ee in range(FIRST, local, 2)]
            sums = [
                dot(jnp.concatenate([block.pick(ee) for ee in pair], axis=1), jnp.concatenate([block.held(ee) for ee in pair], axis=FIRST))
                for pair in pairs
            ]
            block.out[...] = sum(sums[1:], sums[FIRST]).astype(bf16)

        def full(block):
            zacc[...] = jnp.zeros_like(zacc)
            for ee in range(local):

                def more(k):
                    zacc[...] += dot(block.pick(ee, k), block.held(ee, k))

                loop(FIRST, block.windows[ee], more)
            block.out[...] = zacc[...].astype(bf16)

        all_rows.run(simple, full)


def run_dx(groups, starts, tab, da_rows, db_rows, w1, w3, nb):
    local, d_model, d_ff = w1.shape
    row_cap = da_rows.shape[2]
    pieces = [p for g in groups for p in GROUPS[g]]
    blocks = block_count(pieces)
    rows, work = combine_scratch(local, row_cap, d_model)
    return pl.pallas_call(
        functools.partial(dx_kernel, local),
        grid=(len(groups), local),
        in_specs=[SMEM, SMEM, SMEM, VMEM] + [per_group(groups, row_cap, d_ff)] * 2 + [per_local(d_model, d_ff)] * 2,
        out_specs=ANY,
        out_shape=Shape((blocks, BLK, d_model), bf16),
        scratch_shapes=rows + work + [DMA((RING,))],
        compiler_params=grid_params(2),
        cost_estimate=cost(6 * blocks * BLK * d_model * d_ff, 20 << 20),
        name="expert_dx",
    )(starts, block_map(pieces, nb), group_spans(groups), tab, da_rows, db_rows, w1, w3)


def router_grad_kernel(scale, x_ref, prob_ref, dg_ref, ids_ref, load_ref, dlog_ref, dw_ref):
    step = pl.program_id(FIRST)
    prob = prob_ref[...]
    dg = dg_ref[...]
    chosen = chosen_mask(ids_ref[...], prob.shape[FIRST])
    gate_sum = row_sum(where0(chosen, prob))
    gate = where0(chosen, prob / gate_sum)
    d_pick = (dg - row_sum(gate * dg)) / gate_sum
    d_prob = where0(chosen, d_pick) + scale * load_ref[:, :1]
    d_logit = prob * (d_prob - row_sum(prob * d_prob))
    dlog_ref[...] = d_logit
    hi, mid, low = [dot(part, x_ref[...]) for part in split3(d_logit)]

    @pl.when(step == FIRST)
    def _():
        dw_ref[...] = jnp.zeros_like(dw_ref)

    dw_ref[...] += hi + (mid + low)


def run_router_grad(x_loc, prob_t, dg_t, ids_t, load, scale):
    tokens, d_model = x_loc.shape
    experts = prob_t.shape[FIRST]
    lanes = lambda n: pl.BlockSpec((n, BLK), lambda i: (FIRST, i))
    return pl.pallas_call(
        functools.partial(router_grad_kernel, scale),
        grid=(tokens // BLK,),
        in_specs=[pl.BlockSpec((BLK, d_model), lambda i: (i, FIRST)), lanes(experts), lanes(experts), lanes(ids_t.shape[FIRST]), VMEM],
        out_specs=[lanes(experts), VMEM],
        out_shape=[Shape((experts, tokens), f32), Shape((experts, d_model), f32)],
        compiler_params=params(),
        cost_estimate=cost(2 * tokens * d_model * BLK, 2 * tokens * d_model),
        name="router_grad",
    )(x_loc, prob_t, dg_t, ids_t, load)


def final_kernel(dlog_ref, wt_ref, *refs):
    take = taker(refs)
    y_terms, dx_terms = [[ref[...].astype(f32) for ref in take(3)] for _ in TENSORS]
    y_ref, dx_ref = take()
    lhs = split3(dlog_ref[...])
    rhs = split3(wt_ref[...])
    terms = [(i, j) for i in range(3) for j in range(3 - i)]
    left = jnp.concatenate([lhs[i] for i, _ in terms], axis=FIRST)
    right = jnp.concatenate([rhs[j] for _, j in terms], axis=FIRST)
    dx_ref[...] = (dot_tn(left, right) + sum(dx_terms[1:], dx_terms[FIRST])).astype(bf16)
    y_ref[...] = sum(y_terms[1:], y_terms[FIRST]).astype(bf16)


def run_final(dlog_t, w_t, y_terms, dx_terms):
    experts, tokens = dlog_t.shape
    d_model = w_t.shape[1]
    size = tokens // 4
    rows = pl.BlockSpec((size, d_model), lambda i: (i, FIRST))
    return pl.pallas_call(
        final_kernel,
        grid=(tokens // size,),
        in_specs=[pl.BlockSpec((experts, size), lambda i: (FIRST, i)), VMEM] + [rows] * len([*y_terms, *dx_terms]),
        out_specs=[rows] * 2,
        out_shape=[Shape((tokens, d_model), bf16)] * 2,
        compiler_params=params(),
        cost_estimate=cost(2 * tokens * d_model * BLK, 16 * tokens * d_model),
        name="final",
    )(dlog_t, w_t, *y_terms, *dx_terms)


NEAR = (X, Y)
RELAYED = {(Y, 0): 0, (X, 1): 1}
OPS = [
    (t, src, h)
    for step in ([(FAR, 0), (FAR, 1)], [(X, 0), (Y, 1)], [(X, 1), (Y, 0)], [(FIRST, 0), (FIRST, 1)])
    for t in TENSORS
    for src, h in step
]


def add_rows(dst, src):
    step = min(LANES, dst.shape[FIRST])

    def body(i):
        rows = span(i * step, step)
        dst[rows, :] = (dst[rows, :].astype(f32) + src[rows, :].astype(f32)).astype(bf16)

    loop(FIRST, dst.shape[FIRST] // step, body)


def exchange_kernel(half, mats, *refs):
    take = taker(refs)
    parts = [take(2) for _ in TENSORS]
    dws = take(mats)
    outs = [take(len(NEAR) + 1) for _ in TENSORS]
    dw_outs = take(mats)
    land, far_land, stage, z_one, z_two, z_stage = take(6)
    core_sem, stage_sem, far_sem, near_sem, own_sem, z_sem, keep_sem, load_sem, credit_one, credit_two = take()

    me = lax.axis_index("ep")
    z = lax.axis_index("dp")
    peer = {bit: me + bit - 2 * bit * ((me // bit) % 2) for bit in (CORE, X, Y)}
    z_peer = z + 1 - 2 * (z % 2)
    z_cross = 3 - z
    is_end = (z % 3) == FIRST
    is_mid = (z % 3) != FIRST

    barrier = pltpu.get_barrier_semaphore()
    ids = [{"ep": p} for p in peer.values()] + [{"dp": z_peer}, {"dp": z_cross}]
    for device in ids:
        pl.semaphore_signal(barrier, device_id=device, device_id_type=MESH)
    pl.semaphore_wait(barrier, len(ids))

    def remote(src, dst, sems, at, device):
        send, recv = sems.at[(SEND, *at)], sems.at[(RECV, *at)]
        return pltpu.make_async_remote_copy(src_ref=src, dst_ref=dst, send_sem=send, recv_sem=recv, device_id=device, device_id_type=MESH)

    def rows_at(h):
        return pl.ds(h * half, half)

    def part(t, src, h):
        own, rest = parts[t]
        return own.at[src, rows_at(h)] if src <= CORE else rest.at[src - 2, rows_at(h)]

    def core_copy(i):
        t, src, h = OPS[i]
        return remote(part(t, src | CORE, h), land.at[i], core_sem, (i,), {"ep": peer[CORE]})

    def stage_copy(i):
        t, src, h = OPS[i]
        return pltpu.make_async_copy(part(t, src, h), stage.at[i % STAGES], stage_sem.at[i % STAGES])

    def far_copy(i):
        t, _, h = OPS[i]
        return remote(land.at[i], far_land.at[t, h], far_sem, (t, h), {"ep": peer[NEAR[h]]})

    def near_copy(i):
        t, src, h = OPS[i]
        k = NEAR.index(src)
        return remote(land.at[i], outs[t][k].at[rows_at(h)], near_sem, (t, k, h), {"ep": peer[src]})

    def own_copy(i):
        t, _, h = OPS[i]
        return pltpu.make_async_copy(land.at[i], outs[t][LAST].at[rows_at(h)], own_sem.at[t, h])

    def out_copy(i):
        src = OPS[i][1]
        return (far_copy if src == FAR else near_copy if src else own_copy)(i)

    def reduce_op(i):
        t, src, h = OPS[i]
        stage_copy(i).wait()
        core_copy(i).wait_recv()
        add_rows(land.at[i], stage.at[i % STAGES])
        if i + STAGES < len(OPS):
            stage_copy(i + STAGES).start()
        if (src, h) in RELAYED:
            far_copy(OPS.index((t, FAR, RELAYED[src, h]))).wait_recv()
            add_rows(land.at[i], far_land.at[t, RELAYED[src, h]])

    rows_per = z_one.shape[1]
    chunks = [(m, e, k) for e in range(dws[FIRST].shape[FIRST]) for m in range(mats) for k in SPLIT]
    n = len(chunks)

    def piece(arrays, c):
        m, e, k = chunks[c]
        return arrays[m].at[e, pl.ds(k * rows_per, rows_per)]

    def one_copy(c):
        return remote(piece(dws, c), z_one.at[c % SLOTS], z_sem, (FIRST, c), {"dp": z_peer})

    def two_copy(c):
        return remote(z_one.at[c % SLOTS], z_two.at[c % SLOTS], z_sem, (1, c), {"dp": z_cross})

    def three_copy(c):
        return remote(z_two.at[c % SLOTS], piece(dw_outs, c), z_sem, (2, c), {"dp": z_peer})

    def keep_copy(c):
        return pltpu.make_async_copy(z_two.at[c % SLOTS], piece(dw_outs, c), keep_sem.at[c])

    def load_copy(c):
        return pltpu.make_async_copy(piece(dws, c), z_stage.at[c % STAGES], load_sem.at[c % STAGES])

    def first_add(c):
        load_copy(c).wait()
        one_copy(c).wait_recv()
        add_rows(z_one.at[c % SLOTS], z_stage.at[c % STAGES])
        if c + STAGES < n:
            load_copy(c + STAGES).start()

    def second_add(c):
        two_copy(c).wait()
        add_rows(z_two.at[c % SLOTS], z_one.at[c % SLOTS])
        if c + SLOTS < n:
            pl.semaphore_signal(credit_one, device_id={"dp": z_peer}, device_id_type=MESH)

    def retire(c):
        three_copy(c).wait_send()
        keep_copy(c).wait()
        if c + SLOTS < n:
            pl.semaphore_signal(credit_two, device_id={"dp": z_cross}, device_id_type=MESH)

    @pl.when(is_end)
    def _():
        for c in range(SLOTS):
            one_copy(c).start()

    @pl.when(is_mid)
    def _():
        for c in range(STAGES):
            load_copy(c).start()

    for i in range(len(OPS)):
        core_copy(i).start()
        if i < STAGES:
            stage_copy(i).start()

    todo = list(range(len(OPS)))
    for tick in range(n + LAG):
        mine = todo[: 2 if tick < 2 else tick % 2]
        todo = todo[len(mine) :]
        for i in mine:
            reduce_op(i)

        @pl.when(is_mid)
        def _():
            back = tick - BACK
            if tick < n:
                first_add(tick)
            if back in range(n):
                second_add(back)
            if tick < n:
                if tick >= SLOTS:
                    pl.semaphore_wait(credit_two, 1)
                two_copy(tick).start()
            if back in range(n):
                three_copy(back).start()
                keep_copy(back).start()
            if tick >= LAG:
                retire(tick - LAG)

        for i in mine:
            out_copy(i).start()

        @pl.when(is_end)
        def _():
            if tick + SLOTS < n:
                pl.semaphore_wait(credit_one, 1)
                one_copy(tick + SLOTS).start()

    for i in todo:
        reduce_op(i)
        out_copy(i).start()

    @pl.when(is_end)
    def _():
        for c in range(n):
            one_copy(c).wait_send()
            three_copy(c).wait_recv()

    for i in range(len(OPS)):
        core_copy(i).wait_send()
        (out_copy(i).wait_send if OPS[i][1] == FAR else out_copy(i).wait)()


def run_exchange(parts, dws):
    tokens, d_model = parts[FIRST][FIRST].shape[1:]
    half = tokens // 2
    local, rows, cols = dws[FIRST].shape
    chunk = (rows // len(SPLIT), cols)
    n = local * len(dws) * len(SPLIT)
    whole = Shape((tokens, d_model), bf16)
    flat = [v for tensor in parts for v in tensor] + list(dws)
    terms = len(NEAR) + 1
    out = pl.pallas_call(
        functools.partial(exchange_kernel, half, len(dws)),
        in_specs=[ANY] * len(flat),
        out_specs=[ANY] * (terms * len(TENSORS) + len(dws)),
        out_shape=[whole] * (terms * len(TENSORS)) + [Shape(v.shape, bf16) for v in dws],
        scratch_shapes=[
            pltpu.VMEM((len(OPS), half, d_model), bf16),
            pltpu.VMEM((len(TENSORS), len(HALVES), half, d_model), bf16),
            pltpu.VMEM((STAGES, half, d_model), bf16),
            pltpu.VMEM((SLOTS, *chunk), bf16),
            pltpu.VMEM((SLOTS, *chunk), bf16),
            pltpu.VMEM((STAGES, *chunk), bf16),
            DMA((2, len(OPS))),
            DMA((STAGES,)),
            DMA((2, 2, 2)),
            DMA((2, 2, 2, 2)),
            DMA((2, 2)),
            DMA((2, 3, n)),
            DMA((n,)),
            DMA((STAGES,)),
            pltpu.SemaphoreType.REGULAR,
            pltpu.SemaphoreType.REGULAR,
        ],
        compiler_params=pltpu.CompilerParams(vmem_limit_bytes=VMEM_LIMIT, collective_id=FIRST, has_side_effects=True),
        cost_estimate=cost(1 << 37, 200 << 20),
        name="exchange",
    )(*flat)
    return [out[:terms], out[terms : 2 * terms]], out[2 * terms :]


def hop(v, bit):
    return lax.ppermute(v, "ep", [(i, i ^ bit) for i in SOURCES])


def after(values, token):
    return lax.optimization_barrier((values, token))[FIRST]


def send_own(v, token):
    got = {(FIRST, *WHOLE): v, (CORE, *WHOLE): hop(v, CORE)}
    pieces = after([v[first * BLK : (first + count) * BLK] for first, count in PARTS], token)
    for part, piece in zip(PARTS, pieces):
        got.update({(bit, *part): hop(piece, bit) for bit in NEAR})
    return got


def pass_on(got, h):
    part = PARTS[h]
    got[FAR, *part] = hop(got[(Y, X)[h], *part], NEAR[h])
    for bit in NEAR:
        got[bit | CORE, *part] = hop(got[bit, *part], CORE)


def relative(v, me):
    shape = v.shape
    v = v.reshape((2, 2, 2) + shape[1:])
    for axis, bit in enumerate((Y, X, CORE)):
        v = jnp.where((me & bit) != FIRST, jnp.flip(v, axis), v)
    return v.reshape(shape)


def solution(mesh):
    dp_size = mesh.shape["dp"]
    ep_size = mesh.shape["ep"]
    row_spec = P(("dp", "ep"), None)
    expert_spec = P("ep", None, None)
    whole_spec = P(None, None)

    def per_device(x_loc, w_router, ids_loc, w1, w3, w2, dy_loc):
        tokens, d_model = x_loc.shape
        top_k = ids_loc.shape[1]
        experts = w_router.shape[1]
        local = w1.shape[FIRST]
        capacity = capacity_of(tokens, top_k, experts)
        n_total = tokens * dp_size * ep_size
        nb = tokens // BLK
        row_cap = padded(4 * capacity)
        me = lax.axis_index("ep")

        ids_t = ids_loc.T
        send_tab, prob_t = run_router(x_loc, w_router, ids_t, capacity, local, ep_size)
        tables = lax.all_to_all(send_tab, "ep", FIRST, FIRST, tiled=True)
        gathered = [send_own(v, tables) for v in (x_loc, dy_loc)]
        tab_rel = relative(tables, me)
        tab = tab_rel[:, :, :tokens].reshape(ep_size, 2 * local, nb, BLK).transpose(0, 2, 1, 3).reshape(ep_size * nb, 2 * local, BLK)
        starts = tab_rel[:, local:, tokens : tokens + ALIGN].astype(i32).reshape(LAST)

        def y_of(groups, starts):
            return run_y(groups, starts, tab, rows[FIRST], w2, gathered[1], nb)

        def dx_of(groups, starts):
            return run_dx(groups, starts, tab, rows[1], rows[2], w1, w3, nb)

        acc = rows = ()
        own, rest = (FIRST,), (1, 2, 3)
        for g, group in enumerate(GROUPS):
            if g:
                ready = [p for p in group if not p[FIRST] & CORE]
                for got in gathered:
                    got.update(after({p: got[p] for p in ready}, (acc[LAST], dg_own)))
                for got in gathered:
                    if g < len(GROUPS) - 1:
                        pass_on(got, g - 1)
                    else:
                        for src, *part in ready:
                            got[src | CORE, *part] = hop(got[src, *part], CORE)
                here = after(starts, [[got[p] for p in ready] for got in gathered])
                if g == 2:
                    dx_own = dx_of(own, here)
                    starts = after(starts, dx_own)
            rows, acc = run_grad(starts, tab, g, *[[got[p] for p in group] for got in gathered], (w1, w3, w2), acc, rows, nb, row_cap)
            if not g:
                stats = jnp.sum(after(tab_rel[:, :local, tokens:], acc[LAST]), axis=FIRST)
                for step in (1, 2):
                    stats = stats + lax.ppermute(stats, "dp", [(i, i ^ step) for i in range(dp_size)])
                y_own, dg_own = y_of(own, after(starts, stats))
                starts = after(starts, dg_own)
        dw1, dw3, dw2 = acc
        starts, dw2 = lax.optimization_barrier((starts, dw2))
        dw2_sum = lax.psum(dw2, "dp")

        y_rest, dg_rest = y_of(rest, starts)
        dg = jnp.concatenate([dg_own, dg_rest], axis=FIRST)
        dg = dg[:, :local].reshape(ep_size, nb, local, BLK).transpose(0, 2, 1, 3).reshape(ep_size, local, tokens)
        dg = jnp.concatenate([relative(dg, me), jnp.broadcast_to(stats, (ep_size, *stats.shape))], axis=2)
        starts, dg = lax.optimization_barrier((starts, dg))
        dx_rest = dx_of(rest, starts)
        dg_all = lax.all_to_all(dg, "ep", FIRST, FIRST, tiled=True).reshape(experts, tokens + LANES)
        load = dg_all[:, tokens:]
        share = AUX_COEF * experts / (n_total * top_k * n_total)
        aux_loss = share * jnp.sum(load[:, FIRST] * load[:, 1])
        dlog_t, dwr_t = run_router_grad(x_loc, prob_t, dg_all[:, :tokens], ids_t, load, share)
        dw_router = lax.psum(dwr_t, ("dp", "ep")).T

        parts = [[v.reshape(LAST, tokens, d_model) for v in pair] for pair in ((y_own, y_rest), (dx_own, dx_rest))]
        sums, grads = run_exchange(parts, [dw1, dw3])
        y_loc, dx_loc = run_final(dlog_t, w_router.T, *sums)
        return y_loc, aux_loss, dx_loc, dw_router, *grads, dw2_sum

    return jax.shard_map(
        per_device,
        mesh=mesh,
        in_specs=(row_spec, whole_spec, row_spec, expert_spec, expert_spec, expert_spec, row_spec),
        out_specs=(row_spec, P(), row_spec, whole_spec, expert_spec, expert_spec, expert_spec),
        check_vma=False,
    )
```

```python
import functools

import jax
import jax.numpy as jnp
import numpy as np
from jax import lax
from jax.experimental import pallas as pl
from jax.experimental.pallas import tpu as pltpu
from jax.sharding import PartitionSpec as P


AUX_COEF = 0.01
BLK = 256
TILE = 256
WIN = 128
LANES = 128
ALIGN = 16
NOT_KEPT = -65536.0
VMEM_LIMIT = 63 * 1024 * 1024
CORE, X, Y = 1, 2, 4
FAR = X | Y
HALVES = TENSORS = range(2)
RING = 4
SOURCES = range(8)
FIRST, LAST = 0, -1
SEND, RECV = 0, 1
STAGES = 3
SLOTS = 16
SPLIT = range(4)
BACK, LAG = 2, 4
MESH = pl.DeviceIdType.MESH

WHOLE, PARTS = (0, 6), ((0, 3), (3, 3))
GROUPS = (
    [(src, *WHOLE) for src in (FIRST, CORE)],
    [(bit | core, *PARTS[FIRST]) for bit in (X, Y) for core in (FIRST, CORE)],
    [(bit | core, *PARTS[1]) for bit in (X, Y) for core in (FIRST, CORE)],
    [(FAR | core, *part) for part in PARTS for core in (FIRST, CORE)],
)


f32 = jnp.float32
bf16 = jnp.bfloat16
i32 = jnp.int32
ANY = pl.BlockSpec(memory_space=pl.ANY)
SMEM = pl.BlockSpec(memory_space=pltpu.SMEM)
VMEM = pl.BlockSpec(memory_space=pltpu.VMEM)
DMA = pltpu.SemaphoreType.DMA
Shape = jax.ShapeDtypeStruct


def capacity_of(tokens, top_k, experts):
    return (5 * top_k * tokens + 4 * experts - 1) // (4 * experts)


def dot(a, b, ca=1, cb=0):
    return lax.dot_general(a, b, (((ca,), (cb,)), ((), ())), preferred_element_type=f32)


def dot_nt(a, b):
    return dot(a, b, 1, 1)


def dot_tn(a, b):
    return dot(a, b, 0, 0)


def grid_params(dims):
    return pltpu.CompilerParams(dimension_semantics=("arbitrary",) * dims, vmem_limit_bytes=VMEM_LIMIT)


def params():
    return grid_params(1)


def cost(flops, moved):
    return pl.CostEstimate(flops=flops, bytes_accessed=moved, transcendentals=FIRST)


def iota(shape, dim):
    return lax.broadcasted_iota(i32, shape, dim)


def span(start, size, multiple=None):
    return pl.ds(pl.multiple_of(start, multiple or size), size)


def lane_sum(v):
    return jnp.sum(v, axis=1, keepdims=True)


def row_sum(v):
    return jnp.sum(v, axis=0, keepdims=True)


def where0(mask, v):
    return jnp.where(mask, v, jnp.zeros_like(v))


def one_hot(mask):
    return jnp.where(mask, 1.0, 0.0).astype(bf16)


def split3(v):
    hi = v.astype(bf16)
    rest = v - hi.astype(f32)
    mid = rest.astype(bf16)
    return hi, mid, (rest - mid.astype(f32)).astype(bf16)


def loop(start, stop, body):
    def step(i, carry):
        body(i)
        return carry

    lax.fori_loop(start, stop, step, FIRST)


def chosen_mask(ids, experts):
    rows = iota((experts, ids.shape[1]), FIRST)
    return functools.reduce(jnp.logical_or, [rows == ids[j : j + 1, :] for j in range(ids.shape[FIRST])])


def router_kernel(capacity, local, x_ref, wt_ref, ids_ref, tab_ref, prob_ref, stat_ref, carry):
    step = pl.program_id(FIRST)
    steps = pl.num_programs(FIRST)
    experts = wt_ref.shape[FIRST]

    @pl.when(step == FIRST)
    def _():
        carry[...] = jnp.zeros_like(carry)
        stat_ref[...] = jnp.zeros_like(stat_ref)
        tab_ref[...] = jnp.zeros_like(tab_ref)

    x = x_ref[...]
    hi, mid, low = [dot_nt(part, x) for part in split3(wt_ref[...])]
    logits = hi + (mid + low)
    expo = jnp.exp(logits - jnp.max(logits, axis=FIRST, keepdims=True))
    prob = expo / row_sum(expo)
    chosen = chosen_mask(ids_ref[...], experts)
    hits = jnp.where(chosen, 1.0, 0.0)
    gate = where0(chosen, prob / row_sum(where0(chosen, prob)))
    earlier = one_hot(iota((BLK, BLK), FIRST) < iota((BLK, BLK), 1))
    before = carry[:, :1]
    pos = dot(hits.astype(bf16), earlier) + before
    pos = jnp.where(chosen & (pos < capacity), pos, NOT_KEPT)
    prob_ref[...] = prob
    after = before + lane_sum(hits)
    lane = iota((experts, LANES), 1)
    first = where0(lane == step, jnp.minimum(before, capacity) + jnp.zeros((experts, LANES), f32))
    first = first + where0((lane == step + 1) & (step == steps - 1), jnp.minimum(after, capacity) + jnp.zeros((experts, LANES), f32))
    stat_ref[...] += where0(lane == FIRST, lane_sum(hits) + jnp.zeros((experts, LANES), f32))
    stat_ref[...] += where0(lane == 1, lane_sum(prob) + jnp.zeros((experts, LANES), f32))
    tail = slice(tab_ref.shape[LAST] - LANES, None)
    for d in range(experts // local):
        rows = slice(d * local, (d + 1) * local)
        tab_ref[d, :local, span(step * BLK, BLK)] = gate[rows]
        tab_ref[d, local:, span(step * BLK, BLK)] = pos[rows]
        tab_ref[d, local:, tail] += first[rows]
    carry[:, :1] = after


def run_router(x_loc, w_t, ids_t, capacity, local, devices):
    tokens, d_model = x_loc.shape
    experts = w_t.shape[FIRST]
    top_k = ids_t.shape[FIRST]
    table = (devices, 2 * local, tokens + LANES)
    return pl.pallas_call(
        functools.partial(router_kernel, capacity, local),
        grid=(tokens // BLK,),
        in_specs=[pl.BlockSpec((BLK, d_model), lambda i: (i, FIRST)), VMEM, pl.BlockSpec((top_k, BLK), lambda i: (FIRST, i))],
        out_specs=[VMEM, pl.BlockSpec((experts, BLK), lambda i: (FIRST, i)), VMEM],
        out_shape=[Shape(table, f32), Shape((experts, tokens), f32), Shape((experts, LANES), f32)],
        scratch_shapes=[pltpu.VMEM((experts, LANES), f32)],
        compiler_params=params(),
        cost_estimate=cost(2 * tokens * d_model * BLK, 2 * tokens * d_model),
        name="router",
    )(x_loc, w_t, ids_t)


class Blocks:
    def __init__(self, starts_ref, bmap_ref):
        self.starts, self.bmap = starts_ref, bmap_ref

    def info(self, i, e):
        at = self.bmap[2 * i + 1] + e * ALIGN
        first = self.starts[at]
        return self.bmap[2 * i], first, self.starts[at + 1] - first

    def total(self, start, count, e):
        return lax.fori_loop(start, start + count, lambda i, n: n + self.info(i, e)[LAST], i32(FIRST))


def aligned(row):
    base = (row // ALIGN) * ALIGN
    return base, row - base


def window_count(shift, count):
    return (shift + count + WIN - 1) // WIN


def padded(total):
    return (total + TILE - 1) // TILE * TILE


def row_tiles(total, body, size):
    tiles = (total + size - 1 - size // 2) // size
    loop(FIRST, tiles, lambda i: body(i * size, size))
    pl.when(padded(total) > tiles * size)(lambda: body(tiles * size, size // 2))


def start(copies):
    for cp in copies:
        cp.start()


def wait(copies):
    for cp in copies:
        cp.wait()


def taker(refs):
    refs = list(refs)

    def take(n=None):
        got = refs[:n]
        del refs[:n]
        return got

    return take


def block_count(pieces):
    return sum(count for _, _, count in pieces)


def offsets(pieces):
    counts = [count for _, _, count in pieces]
    return [(sum(counts[:k]), count) for k, count in enumerate(counts)]


def block_rows(first, count):
    return pl.ds(first * BLK, count * BLK)


def tokens_in(ref, which):
    return ref.at[which] if len(ref.shape) == 3 else ref


def grad_kernel(g, last, local, pieces, *refs):
    take = taker(refs)
    n = len(pieces)
    starts_ref, bmap_ref, tab_ref = take(3)
    tok_refs = take(n), take(n)
    w1_ref, w3_ref, w2_ref = take(3)
    acc_in = take(2 * bool(g))
    take(3 * bool(g))
    row_outs = take(3)
    outs = take(3 if last else 2)
    xv, dv, xr, dr, acc13, acc2, stage, tok_sem, in_sem, out_sem, row_sem = take()
    accs = acc13, acc2
    e = pl.program_id(FIRST)
    slot = e % 2
    d_model = xv.shape[1]
    d_ff = w1_ref.shape[LAST]
    blocks = Blocks(starts_ref, bmap_ref)
    count = xv.shape[FIRST] // BLK

    parts = [(c, at, first + at) for c, (first, size) in enumerate(offsets(pieces)) for at in range(FIRST, size, 3)]

    def token_copies(k):
        c, at, to = parts[k]
        src_rows, dst_rows = block_rows(at, 3), block_rows(to, 3)
        return [pltpu.make_async_copy(tokens_in(src[c], w).at[src_rows], dst.at[dst_rows], tok_sem.at[w, k]) for w, (src, dst) in enumerate(zip(tok_refs, (xv, dv)))]

    def in_copies(ee, ss):
        return [pltpu.make_async_copy(src.at[ee], dst.at[ss], in_sem.at[ss, k]) for k, (src, dst) in enumerate(zip(acc_in, accs))]

    def out_copies(ee, ss):
        return [pltpu.make_async_copy(src.at[ss], dst.at[ee], out_sem.at[ss, k]) for k, (src, dst) in enumerate(zip(accs, outs))]

    @pl.when(e == FIRST)
    def _():
        for k in range(len(parts)):
            start(token_copies(k))

    if g:
        pl.when(e == FIRST)(lambda: start(in_copies(e, slot)))
    else:
        pl.when(e >= 2)(lambda: wait(out_copies(e - 2, slot)))
        for acc in accs:
            acc[slot] = jnp.zeros(acc.shape[1:], f32)

    def prefetch():
        if not last:
            pl.when(e > FIRST)(lambda: wait(out_copies(e - 1, 1 - slot)))
        start(in_copies(e + 1, 1 - slot))

    def maybe_prefetch(now):
        if g:
            pl.when(now & (e + 1 < local))(prefetch)

    row_iota = iota((WIN, BLK), FIRST).astype(f32)
    head_row = iota((ALIGN, d_model), FIRST)
    both = tuple(HALVES)

    def dispatch(step, rows_at):
        todo = []
        for i in (2 * step, 2 * step + 1):
            for k, (_, _, first) in enumerate(parts):
                pl.when((e == FIRST) & (i == first))(lambda: wait(token_copies(k)))
            infos = [blocks.info(i, e + q) for q in both]
            todo.append((span(i * BLK, BLK), infos, [aligned(r) for r in rows_at]))
            rows_at = tuple(r + info[LAST] for r, info in zip(rows_at, infos))

        def picks(block, q, k):
            _, infos, places = block
            flat, first, _ = infos[q]
            pos = tab_ref[flat, pl.ds(local + e + q, 1), :]
            gate = tab_ref[flat, pl.ds(e + q, 1), :]
            pick = (pos + (places[q][1] - first - k * WIN).astype(f32)) == row_iota
            return one_hot(pick), lane_sum(where0(pick, gate + jnp.zeros_like(row_iota)))

        def rows_for(block, one, gate_row):
            tok = block[FIRST]
            return dot(one, xv[tok, :]).astype(bf16), (dot(one, dv[tok, :]) * gate_row).astype(bf16)

        def first_rows(block):
            pair = [picks(block, q, i32(FIRST)) for q in both]
            return rows_for(block, *[jnp.concatenate(v, axis=FIRST) for v in zip(*pair)])

        def put(block, new):
            for q in both:
                base, shift = block[LAST][q]
                head = span(base, ALIGN)
                for value, rows in zip(new, (xr, dr)):
                    value = value[q * WIN : (q + 1) * WIN]
                    rows[q, head, :] = jnp.where(head_row < shift, rows[q, head, :], value[:ALIGN])
                    rows[q, span(base + ALIGN, WIN - ALIGN, ALIGN), :] = value[ALIGN:]

        windows = [[window_count(places[q][1], infos[q][LAST]) for q in both] for _, infos, places in todo]
        simple = functools.reduce(jnp.logical_and, [w <= 1 for ws in windows for w in ws])

        @pl.when(simple)
        def _():
            for block, new in zip(todo, [first_rows(block) for block in todo]):
                put(block, new)

        @pl.when(jnp.logical_not(simple))
        def _():
            for block, ws in zip(todo, windows):
                put(block, first_rows(block))
                for q in both:

                    def more(k):
                        for value, rows in zip(rows_for(block, *picks(block, q, k)), (xr, dr)):
                            rows[q, span(block[LAST][q][FIRST] + k * WIN, WIN, ALIGN), :] = value

                    loop(1, ws[q], more)

        return rows_at

    @pl.when(slot == FIRST)
    def _():
        totals = lax.fori_loop(FIRST, count // 2, dispatch, (i32(FIRST),) * len(both))
        for q in both:

            def clear(i):
                for rows in (xr, dr):
                    rows[q, span(i * ALIGN, ALIGN), :] = jnp.zeros((ALIGN, d_model), bf16)

            loop((totals[q] + ALIGN - 1) // ALIGN, padded(totals[q]) // ALIGN, clear)

    wait(in_copies(e, slot))

    def tile(at, size):
        maybe_prefetch((at == FIRST) & (slot == FIRST))
        rows = span(at, size)
        xt = xr[slot, rows, :]
        dt = dr[slot, rows, :]
        act_a = dot(xt, w1_ref[FIRST])
        act_b = dot(xt, w3_ref[FIRST])
        d_hidden = dot_nt(dt, w2_ref[FIRST]).astype(bf16).astype(f32)
        sig = 1.0 / (1.0 + jnp.exp(-act_a))
        silu = act_a * sig
        hidden = (silu * act_b).astype(bf16)
        d_a = (d_hidden * act_b * sig * (1.0 + act_a * (1.0 - sig))).astype(bf16)
        d_b = (d_hidden * silu).astype(bf16)
        copies = []
        for k, (value, out) in enumerate(zip((hidden, d_a, d_b), row_outs)):
            stage[k, :size] = value
            copies.append(pltpu.make_async_copy(stage.at[k, :size], out.at[g, e, rows], row_sem.at[k]))
        start(copies)
        acc13[slot, :, :d_ff] += dot_tn(xt, d_a)
        acc13[slot, :, d_ff:] += dot_tn(xt, d_b)
        acc2[slot] += dot_tn(hidden, dt)
        wait(copies)

    total = blocks.total(FIRST, count, e)
    row_tiles(total, tile, 2 * TILE)
    maybe_prefetch((total == FIRST) | (slot > FIRST))

    if last:
        for out, value in zip(outs, (acc13[slot, :, :d_ff], acc13[slot, :, d_ff:], acc2[slot])):
            out[FIRST] = value.astype(bf16)
    else:
        start(out_copies(e, slot))

        @pl.when(e == pl.num_programs(FIRST) - 1)
        def _():
            wait(out_copies(e - 1, 1 - slot))
            wait(out_copies(e, slot))


def per_expert(*shape):
    return pl.BlockSpec((1, *shape), lambda e: (e,) + (FIRST,) * len(shape))


def block_map(pieces, nb):
    spots = [(src, first + b) for src, first, count in pieces for b in range(count)]
    return np.asarray([v for src, b in spots for v in (src * nb + b, src * 4 * ALIGN + b)], np.int32)


def run_grad(starts, tab, g, xs, ds, weights, acc, rows, nb, row_cap):
    pieces = GROUPS[g]
    last = g == len(GROUPS) - 1
    local, d_model, d_ff = weights[FIRST].shape
    count = block_count(pieces) * BLK
    w_specs = [per_expert(*w.shape[1:]) for w in weights]
    sums = [(local, d_model, 2 * d_ff), (local, d_ff, d_model)]
    row_shape = [Shape((len(GROUPS), local, row_cap, d_ff), bf16)] * 3
    out_shape = row_shape + ([Shape(w.shape, bf16) for w in weights] if last else [Shape(s, f32) for s in sums])
    out_specs = [ANY] * 3 + (w_specs if last else [ANY] * 2)
    tokens = pltpu.VMEM((count, d_model), bf16)
    packed = pltpu.VMEM((2, row_cap + WIN, d_model), bf16)
    ins = [starts, block_map(pieces, nb), tab, *xs, *ds, *weights, *acc, *rows]
    out = pl.pallas_call(
        functools.partial(grad_kernel, g, last, local, pieces),
        grid=(local,),
        in_specs=[SMEM, SMEM, VMEM] + [ANY] * (2 * len(pieces)) + w_specs + [ANY] * (len(acc) + len(rows)),
        out_specs=out_specs,
        out_shape=out_shape,
        scratch_shapes=[tokens, tokens, packed, packed]
        + [pltpu.VMEM((2, *s[1:]), f32) for s in sums]
        + [pltpu.VMEM((3, 2 * TILE, d_ff), bf16), DMA((2, count // (3 * BLK))), DMA((2, 2)), DMA((2, 2)), DMA((3,))],
        input_output_aliases={len(ins) - len(rows) + k: k for k in range(len(rows))},
        compiler_params=params(),
        cost_estimate=cost(12 * count * d_model * d_ff, 40 << 20),
        name="expert_grad",
    )(*ins)
    return out[:3], out[3:]


def group_spans(groups):
    counts = [block_count(GROUPS[g]) for g in groups]
    return np.asarray([v for k, c in enumerate(counts) for v in (sum(counts[:k]), c)], np.int32)


def per_local(*shape):
    return pl.BlockSpec((1, *shape), lambda g, e: (e,) + (FIRST,) * len(shape))


class BlockRows:
    def __init__(self, owner, i, rows_at):
        ee = range(owner.local)
        self.owner, self.i = owner, i
        self.infos = [owner.blocks.info(i, k) for k in ee]
        self.places = [aligned(r) for r in rows_at]
        self.windows = [window_count(self.places[k][1], self.infos[k][LAST]) for k in ee]
        self.simple = functools.reduce(jnp.logical_and, [w <= 1 for w in self.windows])
        self.flat = self.infos[FIRST][FIRST]
        self.tok = span((i - owner.first) * BLK, BLK)
        self.out = owner.ring.at[i % RING]
        self.after = tuple(r + info[LAST] for r, info in zip(rows_at, self.infos))

    def load(self):
        self.tab_t = jnp.transpose(self.owner.tab_ref[self.flat])

    def gate(self, ee):
        return self.tab_t[:, ee : ee + 1]

    def pick(self, ee, k=FIRST):
        at = self.owner.local + ee
        shift = self.places[ee][1] - self.infos[ee][1] - k * WIN
        return one_hot((self.tab_t[:, at : at + 1] + shift.astype(f32)) == self.owner.lane)

    def held(self, ee, k=FIRST, cols=slice(None)):
        return self.owner.rows_ref[ee, span(self.places[ee][FIRST] + k * WIN, WIN, ALIGN), cols]


class Combine:
    def __init__(self, local, starts_ref, bmap_ref, spans_ref, tab_ref, rows_ref, out_ref, ring, sems):
        step = pl.program_id(FIRST)
        self.e = pl.program_id(1)
        self.blocks = Blocks(starts_ref, bmap_ref)
        self.spans = spans_ref
        self.first, self.count = spans_ref[2 * step], spans_ref[2 * step + 1]
        self.total = self.blocks.total(self.first, self.count, self.e)
        self.local, self.tab_ref, self.rows_ref = local, tab_ref, rows_ref
        self.out_ref, self.ring, self.sems = out_ref, ring, sems
        self.lane = iota((BLK, WIN), 1).astype(f32)

    def zero_tail(self):
        rows = span(padded(self.total), WIN)
        self.rows_ref[self.e, rows, :] = jnp.zeros((WIN, self.rows_ref.shape[LAST]), bf16)

    def fetch(self, groups, arrays, held, sems):
        now = pl.program_id(FIRST) * self.local + self.e

        def each(step, act):
            k, e = step // self.local, step % self.local
            total = self.blocks.total(self.spans[2 * k], self.spans[2 * k + 1], e)

            def one(i):
                rows = span(i * TILE, TILE)
                for w, array in enumerate(arrays):
                    act(pltpu.make_async_copy(array.at[k + groups[FIRST], e, rows], held.at[step % 2, w, rows], sems.at[step % 2, w]))

            loop(FIRST, padded(total) // TILE, one)

        pl.when(now == FIRST)(lambda: each(now, lambda cp: cp.start()))
        pl.when(now + 1 < self.local * len(groups))(lambda: each(now + 1, lambda cp: cp.start()))
        each(now, lambda cp: cp.wait())
        return now % 2

    def out_copy(self, i):
        slot = i % RING
        place = self.blocks.bmap[2 * i] - self.blocks.bmap[FIRST]
        return pltpu.make_async_copy(self.ring.at[slot], self.out_ref.at[place], self.sems.at[slot])

    def run(self, simple_body, full_body):
        def pair(step, rows_at):
            i = self.first + 2 * step
            one = BlockRows(self, i, rows_at)
            two = BlockRows(self, i + 1, one.after)
            for block in (one, two):
                pl.when(block.i - self.first >= RING)(lambda: self.out_copy(block.i - RING).wait())
            simple = one.simple & two.simple

            @pl.when(simple)
            def _():
                for block in (one, two):
                    block.load()
                for block in (one, two):
                    simple_body(block)

            @pl.when(jnp.logical_not(simple))
            def _():
                def full(k, rows_at):
                    block = BlockRows(self, i + k, rows_at)
                    block.load()
                    full_body(block)
                    return block.after

                lax.fori_loop(FIRST, 2, full, rows_at)

            for block in (one, two):
                self.out_copy(block.i).start()
            return two.after

        stop = self.first + self.count
        lax.fori_loop(FIRST, self.count // 2, pair, (i32(FIRST),) * self.local)
        loop(stop - RING, stop, lambda i: self.out_copy(i).wait())


def y_kernel(groups, local, starts_ref, bmap_ref, spans_ref, tab_ref, h_rows, w2_ref, *refs):
    take = taker(refs)
    d_refs = [take(len(GROUPS[g])) for g in groups]
    y_ref, dg_ref, o_rows, dv, ring, zacc, yacc, dgacc, tok_sem, out_sem, held, row_sem = take()
    all_rows = Combine(local, starts_ref, bmap_ref, spans_ref, tab_ref, o_rows, y_ref, ring, out_sem)
    e = all_rows.e
    d_model = dv.shape[1]

    def token_copies(step):
        spots = offsets(GROUPS[groups[step]])
        return [pltpu.make_async_copy(tokens_in(src, 1), dv.at[block_rows(*spot)], tok_sem.at[c]) for c, (src, spot) in enumerate(zip(d_refs[step], spots))]

    for step in range(len(groups)):
        pl.when((pl.program_id(FIRST) == step) & (e == FIRST))(lambda: start(token_copies(step)))

    slot = all_rows.fetch(groups, [h_rows], held, row_sem)

    def tile(at, size):
        rows = span(at, size)
        o_rows[e, rows, :] = dot(held[slot, FIRST, rows, :], w2_ref[FIRST]).astype(bf16)

    row_tiles(all_rows.total, tile, 2 * TILE)
    all_rows.zero_tail()

    @pl.when(e == local - 1)
    def _():
        for step in range(len(groups)):
            pl.when(pl.program_id(FIRST) == step)(lambda: wait(token_copies(step)))
        dg_lane = iota((BLK, LANES), 1)
        width = 2 * LANES
        columns = [slice(k * width, (k + 1) * width) for k in range(d_model // width)]

        def put_dg(block, sums):
            dg = sum(where0(dg_lane == ee, lane_sum(s) + jnp.zeros((BLK, LANES), f32)) for ee, s in enumerate(sums))
            dg_ref[block.flat - all_rows.blocks.bmap[FIRST]] = jnp.transpose(dg)[: 2 * local, :]

        def simple(block):
            picks = [block.pick(ee) for ee in range(local)]
            sums = [None] * local
            for cols in columns:
                dy = dv[block.tok, cols].astype(f32)
                y = None
                for ee in range(local):
                    z = dot(picks[ee], block.held(ee, cols=cols))
                    prod = dy * z
                    part = prod[:, :LANES] + prod[:, LANES:]
                    sums[ee] = part if sums[ee] is None else sums[ee] + part
                    y = block.gate(ee) * z if y is None else y + block.gate(ee) * z
                block.out[:, cols] = y.astype(bf16)
            put_dg(block, sums)

        def full(block):
            yacc[...] = jnp.zeros_like(yacc)
            for ee in range(local):
                zacc[...] = jnp.zeros_like(zacc)

                def more(k):
                    zacc[...] += dot(block.pick(ee, k), block.held(ee, k))

                loop(FIRST, block.windows[ee], more)
                yacc[...] += block.gate(ee) * zacc[...]
                dgacc[ee] = lane_sum(dv[block.tok, :].astype(f32) * zacc[...]) * jnp.where(dg_lane == FIRST, 1.0, 0.0)
            block.out[...] = yacc[...].astype(bf16)
            put_dg(block, [dgacc[ee] for ee in range(local)])

        all_rows.run(simple, full)


def combine_scratch(local, row_cap, d_model):
    return [pltpu.VMEM((local, row_cap + WIN, d_model), bf16)], [pltpu.VMEM((RING, BLK, d_model), bf16), pltpu.VMEM((BLK, d_model), f32)]


def run_y(groups, starts, tab, h_rows, w2, ds, nb):
    local, d_ff, d_model = w2.shape
    row_cap = h_rows.shape[2]
    pieces = [p for g in groups for p in GROUPS[g]]
    spans = group_spans(groups)
    blocks = block_count(pieces)
    rows, work = combine_scratch(local, row_cap, d_model)
    return pl.pallas_call(
        functools.partial(y_kernel, groups, local),
        grid=(len(groups), local),
        in_specs=[SMEM, SMEM, SMEM, VMEM, ANY, per_local(d_ff, d_model)] + [ANY] * len(pieces),
        out_specs=[ANY, VMEM],
        out_shape=[Shape((blocks, BLK, d_model), bf16), Shape((blocks, 2 * local, BLK), f32)],
        scratch_shapes=rows + [pltpu.VMEM((max(spans[1::2]) * BLK, d_model), bf16)] + work + [work[LAST], pltpu.VMEM((local, BLK, LANES), f32), DMA((4,)), DMA((RING,)), pltpu.VMEM((2, 1, row_cap, d_ff), bf16), DMA((2, 1))],
        compiler_params=grid_params(2),
        cost_estimate=cost(4 * blocks * BLK * d_model * d_ff, 20 << 20),
        name="expert_y",
    )(starts, block_map(pieces, nb), spans, tab, h_rows, w2, *[ds[p] for p in pieces])


def dx_kernel(groups, local, starts_ref, bmap_ref, spans_ref, tab_ref, da_rows, db_rows, w1_ref, w3_ref, dx_ref, o_rows, ring, zacc, out_sem, held, row_sem):
    all_rows = Combine(local, starts_ref, bmap_ref, spans_ref, tab_ref, o_rows, dx_ref, ring, out_sem)
    e = all_rows.e

    slot = all_rows.fetch(groups, [da_rows, db_rows], held, row_sem)

    def tile(at, size):
        rows = span(at, size)
        grad = dot_nt(held[slot, FIRST, rows, :], w1_ref[FIRST]) + dot_nt(held[slot, 1, rows, :], w3_ref[FIRST])
        o_rows[e, rows, :] = grad.astype(bf16)

    row_tiles(all_rows.total, tile, 2 * TILE)
    all_rows.zero_tail()

    @pl.when(e == local - 1)
    def _():
        def simple(block):
            pairs = [(ee, ee + 1) for ee in range(FIRST, local, 2)]
            sums = [
                dot(jnp.concatenate([block.pick(ee) for ee in pair], axis=1), jnp.concatenate([block.held(ee) for ee in pair], axis=FIRST))
                for pair in pairs
            ]
            block.out[...] = sum(sums[1:], sums[FIRST]).astype(bf16)

        def full(block):
            zacc[...] = jnp.zeros_like(zacc)
            for ee in range(local):

                def more(k):
                    zacc[...] += dot(block.pick(ee, k), block.held(ee, k))

                loop(FIRST, block.windows[ee], more)
            block.out[...] = zacc[...].astype(bf16)

        all_rows.run(simple, full)


def run_dx(groups, starts, tab, da_rows, db_rows, w1, w3, nb):
    local, d_model, d_ff = w1.shape
    row_cap = da_rows.shape[2]
    pieces = [p for g in groups for p in GROUPS[g]]
    blocks = block_count(pieces)
    rows, work = combine_scratch(local, row_cap, d_model)
    return pl.pallas_call(
        functools.partial(dx_kernel, groups, local),
        grid=(len(groups), local),
        in_specs=[SMEM, SMEM, SMEM, VMEM] + [ANY] * 2 + [per_local(d_model, d_ff)] * 2,
        out_specs=ANY,
        out_shape=Shape((blocks, BLK, d_model), bf16),
        scratch_shapes=rows + work + [DMA((RING,)), pltpu.VMEM((2, 2, row_cap, d_ff), bf16), DMA((2, 2))],
        compiler_params=grid_params(2),
        cost_estimate=cost(6 * blocks * BLK * d_model * d_ff, 20 << 20),
        name="expert_dx",
    )(starts, block_map(pieces, nb), group_spans(groups), tab, da_rows, db_rows, w1, w3)


def router_grad_kernel(scale, x_ref, prob_ref, dg_ref, ids_ref, load_ref, dlog_ref, dw_ref):
    step = pl.program_id(FIRST)
    prob = prob_ref[...]
    dg = dg_ref[...]
    chosen = chosen_mask(ids_ref[...], prob.shape[FIRST])
    gate_sum = row_sum(where0(chosen, prob))
    gate = where0(chosen, prob / gate_sum)
    d_pick = (dg - row_sum(gate * dg)) / gate_sum
    d_prob = where0(chosen, d_pick) + scale * load_ref[:, :1]
    d_logit = prob * (d_prob - row_sum(prob * d_prob))
    dlog_ref[...] = d_logit
    hi, mid, low = [dot(part, x_ref[...]) for part in split3(d_logit)]

    @pl.when(step == FIRST)
    def _():
        dw_ref[...] = jnp.zeros_like(dw_ref)

    dw_ref[...] += hi + (mid + low)


def run_router_grad(x_loc, prob_t, dg_t, ids_t, load, scale):
    tokens, d_model = x_loc.shape
    experts = prob_t.shape[FIRST]
    lanes = lambda n: pl.BlockSpec((n, BLK), lambda i: (FIRST, i))
    return pl.pallas_call(
        functools.partial(router_grad_kernel, scale),
        grid=(tokens // BLK,),
        in_specs=[pl.BlockSpec((BLK, d_model), lambda i: (i, FIRST)), lanes(experts), lanes(experts), lanes(ids_t.shape[FIRST]), VMEM],
        out_specs=[lanes(experts), VMEM],
        out_shape=[Shape((experts, tokens), f32), Shape((experts, d_model), f32)],
        compiler_params=params(),
        cost_estimate=cost(2 * tokens * d_model * BLK, 2 * tokens * d_model),
        name="router_grad",
    )(x_loc, prob_t, dg_t, ids_t, load)


def final_kernel(dlog_ref, wt_ref, *refs):
    take = taker(refs)
    y_terms, dx_terms = [[ref[...].astype(f32) for ref in take(3)] for _ in TENSORS]
    y_ref, dx_ref = take()
    lhs = split3(dlog_ref[...])
    rhs = split3(wt_ref[...])
    terms = [(i, j) for i in range(3) for j in range(3 - i)]
    left = jnp.concatenate([lhs[i] for i, _ in terms], axis=FIRST)
    right = jnp.concatenate([rhs[j] for _, j in terms], axis=FIRST)
    dx_ref[...] = (dot_tn(left, right) + sum(dx_terms[1:], dx_terms[FIRST])).astype(bf16)
    y_ref[...] = sum(y_terms[1:], y_terms[FIRST]).astype(bf16)


def run_final(dlog_t, w_t, y_terms, dx_terms):
    experts, tokens = dlog_t.shape
    d_model = w_t.shape[1]
    size = tokens // 4
    rows = pl.BlockSpec((size, d_model), lambda i: (i, FIRST))
    return pl.pallas_call(
        final_kernel,
        grid=(tokens // size,),
        in_specs=[pl.BlockSpec((experts, size), lambda i: (FIRST, i)), VMEM] + [rows] * len([*y_terms, *dx_terms]),
        out_specs=[rows] * 2,
        out_shape=[Shape((tokens, d_model), bf16)] * 2,
        compiler_params=params(),
        cost_estimate=cost(2 * tokens * d_model * BLK, 16 * tokens * d_model),
        name="final",
    )(dlog_t, w_t, *y_terms, *dx_terms)


NEAR = (X, Y)
RELAYED = {(Y, 0): 0, (X, 1): 1}
OPS = [
    (t, src, h)
    for step in ([(FAR, 0), (FAR, 1)], [(X, 0), (Y, 1)], [(X, 1), (Y, 0)], [(FIRST, 0), (FIRST, 1)])
    for t in TENSORS
    for src, h in step
]


def add_rows(dst, src):
    step = min(LANES, dst.shape[FIRST])

    def body(i):
        rows = span(i * step, step)
        dst[rows, :] = (dst[rows, :].astype(f32) + src[rows, :].astype(f32)).astype(bf16)

    loop(FIRST, dst.shape[FIRST] // step, body)


def exchange_kernel(half, mats, *refs):
    take = taker(refs)
    parts = [take(2) for _ in TENSORS]
    dws = take(mats)
    outs = [take(len(NEAR) + 1) for _ in TENSORS]
    dw_outs = take(mats)
    land, far_land, stage, z_one, z_two, z_stage = take(6)
    core_sem, stage_sem, far_sem, near_sem, own_sem, z_sem, keep_sem, load_sem, credit_one, credit_two = take()

    me = lax.axis_index("ep")
    z = lax.axis_index("dp")
    peer = {bit: me + bit - 2 * bit * ((me // bit) % 2) for bit in (CORE, X, Y)}
    z_peer = z + 1 - 2 * (z % 2)
    z_cross = 3 - z
    is_end = (z % 3) == FIRST
    is_mid = (z % 3) != FIRST

    barrier = pltpu.get_barrier_semaphore()
    ids = [{"ep": p} for p in peer.values()] + [{"dp": z_peer}, {"dp": z_cross}]
    for device in ids:
        pl.semaphore_signal(barrier, device_id=device, device_id_type=MESH)
    pl.semaphore_wait(barrier, len(ids))

    def remote(src, dst, sems, at, device):
        send, recv = sems.at[(SEND, *at)], sems.at[(RECV, *at)]
        return pltpu.make_async_remote_copy(src_ref=src, dst_ref=dst, send_sem=send, recv_sem=recv, device_id=device, device_id_type=MESH)

    def rows_at(h):
        return pl.ds(h * half, half)

    def part(t, src, h):
        own, rest = parts[t]
        return own.at[src, rows_at(h)] if src <= CORE else rest.at[src - 2, rows_at(h)]

    def core_copy(i):
        t, src, h = OPS[i]
        return remote(part(t, src | CORE, h), land.at[i], core_sem, (i,), {"ep": peer[CORE]})

    def stage_copy(i):
        t, src, h = OPS[i]
        return pltpu.make_async_copy(part(t, src, h), stage.at[i % STAGES], stage_sem.at[i % STAGES])

    def far_copy(i):
        t, _, h = OPS[i]
        return remote(land.at[i], far_land.at[t, h], far_sem, (t, h), {"ep": peer[NEAR[h]]})

    def near_copy(i):
        t, src, h = OPS[i]
        k = NEAR.index(src)
        return remote(land.at[i], outs[t][k].at[rows_at(h)], near_sem, (t, k, h), {"ep": peer[src]})

    def own_copy(i):
        t, _, h = OPS[i]
        return pltpu.make_async_copy(land.at[i], outs[t][LAST].at[rows_at(h)], own_sem.at[t, h])

    def out_copy(i):
        src = OPS[i][1]
        return (far_copy if src == FAR else near_copy if src else own_copy)(i)

    def reduce_op(i):
        t, src, h = OPS[i]
        stage_copy(i).wait()
        core_copy(i).wait_recv()
        add_rows(land.at[i], stage.at[i % STAGES])
        if i + STAGES < len(OPS):
            stage_copy(i + STAGES).start()
        if (src, h) in RELAYED:
            far_copy(OPS.index((t, FAR, RELAYED[src, h]))).wait_recv()
            add_rows(land.at[i], far_land.at[t, RELAYED[src, h]])

    rows_per = z_one.shape[1]
    chunks = [(m, e, k) for e in range(dws[FIRST].shape[FIRST]) for m in range(mats) for k in SPLIT]
    n = len(chunks)

    def piece(arrays, c):
        m, e, k = chunks[c]
        return arrays[m].at[e, pl.ds(k * rows_per, rows_per)]

    def one_copy(c):
        return remote(piece(dws, c), z_one.at[c % SLOTS], z_sem, (FIRST, c), {"dp": z_peer})

    def two_copy(c):
        return remote(z_one.at[c % SLOTS], z_two.at[c % SLOTS], z_sem, (1, c), {"dp": z_cross})

    def three_copy(c):
        return remote(z_two.at[c % SLOTS], piece(dw_outs, c), z_sem, (2, c), {"dp": z_peer})

    def keep_copy(c):
        return pltpu.make_async_copy(z_two.at[c % SLOTS], piece(dw_outs, c), keep_sem.at[c])

    def load_copy(c):
        return pltpu.make_async_copy(piece(dws, c), z_stage.at[c % STAGES], load_sem.at[c % STAGES])

    def first_add(c):
        load_copy(c).wait()
        one_copy(c).wait_recv()
        add_rows(z_one.at[c % SLOTS], z_stage.at[c % STAGES])
        if c + STAGES < n:
            load_copy(c + STAGES).start()

    def second_add(c):
        two_copy(c).wait()
        add_rows(z_two.at[c % SLOTS], z_one.at[c % SLOTS])
        if c + SLOTS < n:
            pl.semaphore_signal(credit_one, device_id={"dp": z_peer}, device_id_type=MESH)

    def retire(c):
        three_copy(c).wait_send()
        keep_copy(c).wait()
        if c + SLOTS < n:
            pl.semaphore_signal(credit_two, device_id={"dp": z_cross}, device_id_type=MESH)

    @pl.when(is_end)
    def _():
        for c in range(SLOTS):
            one_copy(c).start()

    @pl.when(is_mid)
    def _():
        for c in range(STAGES):
            load_copy(c).start()

    for i in range(len(OPS)):
        core_copy(i).start()
        if i < STAGES:
            stage_copy(i).start()

    todo = list(range(len(OPS)))
    for tick in range(n + LAG):
        mine = todo[: 2 if tick < 2 else tick % 2]
        todo = todo[len(mine) :]
        for i in mine:
            reduce_op(i)

        @pl.when(is_mid)
        def _():
            back = tick - BACK
            if tick < n:
                first_add(tick)
            if back in range(n):
                second_add(back)
            if tick < n:
                if tick >= SLOTS:
                    pl.semaphore_wait(credit_two, 1)
                two_copy(tick).start()
            if back in range(n):
                three_copy(back).start()
                keep_copy(back).start()
            if tick >= LAG:
                retire(tick - LAG)

        for i in mine:
            out_copy(i).start()

        @pl.when(is_end)
        def _():
            if tick + SLOTS < n:
                pl.semaphore_wait(credit_one, 1)
                one_copy(tick + SLOTS).start()

    for i in todo:
        reduce_op(i)
        out_copy(i).start()

    @pl.when(is_end)
    def _():
        for c in range(n):
            one_copy(c).wait_send()
            three_copy(c).wait_recv()

    for i in range(len(OPS)):
        core_copy(i).wait_send()
        (out_copy(i).wait_send if OPS[i][1] == FAR else out_copy(i).wait)()


def run_exchange(parts, dws):
    tokens, d_model = parts[FIRST][FIRST].shape[1:]
    half = tokens // 2
    local, rows, cols = dws[FIRST].shape
    chunk = (rows // len(SPLIT), cols)
    n = local * len(dws) * len(SPLIT)
    whole = Shape((tokens, d_model), bf16)
    flat = [v for tensor in parts for v in tensor] + list(dws)
    terms = len(NEAR) + 1
    out = pl.pallas_call(
        functools.partial(exchange_kernel, half, len(dws)),
        in_specs=[ANY] * len(flat),
        out_specs=[ANY] * (terms * len(TENSORS) + len(dws)),
        out_shape=[whole] * (terms * len(TENSORS)) + [Shape(v.shape, bf16) for v in dws],
        scratch_shapes=[
            pltpu.VMEM((len(OPS), half, d_model), bf16),
            pltpu.VMEM((len(TENSORS), len(HALVES), half, d_model), bf16),
            pltpu.VMEM((STAGES, half, d_model), bf16),
            pltpu.VMEM((SLOTS, *chunk), bf16),
            pltpu.VMEM((SLOTS, *chunk), bf16),
            pltpu.VMEM((STAGES, *chunk), bf16),
            DMA((2, len(OPS))),
            DMA((STAGES,)),
            DMA((2, 2, 2)),
            DMA((2, 2, 2, 2)),
            DMA((2, 2)),
            DMA((2, 3, n)),
            DMA((n,)),
            DMA((STAGES,)),
            pltpu.SemaphoreType.REGULAR,
            pltpu.SemaphoreType.REGULAR,
        ],
        compiler_params=pltpu.CompilerParams(vmem_limit_bytes=VMEM_LIMIT, collective_id=FIRST, has_side_effects=True),
        cost_estimate=cost(1 << 37, 200 << 20),
        name="exchange",
    )(*flat)
    return [out[:terms], out[terms : 2 * terms]], out[2 * terms :]


def hop(v, bit):
    return lax.ppermute(v, "ep", [(i, i ^ bit) for i in SOURCES])


def after(values, token):
    return lax.optimization_barrier((values, token))[FIRST]


def send_own(x_loc, dy_loc, token):
    got = {(FIRST, *WHOLE): (x_loc, dy_loc), (CORE, *WHOLE): (hop(x_loc, CORE), hop(dy_loc, CORE))}
    both = [jnp.stack([v[first * BLK : (first + count) * BLK] for v in (x_loc, dy_loc)]) for first, count in PARTS]
    for part, piece in zip(PARTS, after(both, token)):
        got.update({(bit, *part): (hop(piece, bit),) * 2 for bit in NEAR})
    return got


def pass_on(got, h):
    part = PARTS[h]
    got[FAR, *part] = (hop(got[(Y, X)[h], *part][FIRST], NEAR[h]),) * 2
    for bit in NEAR:
        pass_core(got, bit, part)


def pass_core(got, bits, part):
    got[bits | CORE, *part] = (hop(got[bits, *part][FIRST], CORE),) * 2


def relative(v, me):
    shape = v.shape
    v = v.reshape((2, 2, 2) + shape[1:])
    for axis, bit in enumerate((Y, X, CORE)):
        v = jnp.where((me & bit) != FIRST, jnp.flip(v, axis), v)
    return v.reshape(shape)


def solution(mesh):
    dp_size = mesh.shape["dp"]
    ep_size = mesh.shape["ep"]
    row_spec = P(("dp", "ep"), None)
    expert_spec = P("ep", None, None)
    whole_spec = P(None, None)

    def per_device(x_loc, w_router, ids_loc, w1, w3, w2, dy_loc):
        tokens, d_model = x_loc.shape
        top_k = ids_loc.shape[1]
        experts = w_router.shape[1]
        local = w1.shape[FIRST]
        capacity = capacity_of(tokens, top_k, experts)
        n_total = tokens * dp_size * ep_size
        nb = tokens // BLK
        row_cap = padded(4 * capacity)
        me = lax.axis_index("ep")

        ids_t = ids_loc.T
        w_t = w_router.T
        send_tab, prob_t, stats = run_router(x_loc, w_t, ids_t, capacity, local, ep_size)
        tables = lax.all_to_all(send_tab, "ep", FIRST, FIRST, tiled=True)
        stats = jnp.pad(stats[:, :2].T, ((0, local - 2), (0, LANES - experts)))
        for step in (1, 2):
            stats = stats + lax.ppermute(stats, "dp", [(i, i ^ step) for i in range(dp_size)])
        gathered = send_own(x_loc, dy_loc, (tables, stats))
        tab_rel = relative(tables, me)
        tab = tab_rel[:, :, :tokens].reshape(ep_size, 2 * local, nb, BLK).transpose(0, 2, 1, 3).reshape(ep_size * nb, 2 * local, BLK)
        starts = tab_rel[:, local:, tokens : tokens + ALIGN].astype(i32).reshape(LAST)

        def y_of(groups, starts):
            return run_y(groups, starts, tab, rows[FIRST], w2, {p: v[1] for p, v in gathered.items()}, nb)

        def dx_of(groups, starts):
            return run_dx(groups, starts, tab, rows[1], rows[2], w1, w3, nb)

        acc = rows = ()
        own, rest = (FIRST,), (1, 2, 3)
        for g, group in enumerate(GROUPS):
            if g:
                ready = [p for p in group if not p[FIRST] & CORE]
                arrived = after([gathered[p][FIRST] for p in ready], (acc[LAST], dg_own))
                gathered.update({p: (v, v) for p, v in zip(ready, arrived)})
                if g < len(GROUPS) - 1:
                    pass_on(gathered, g - 1)
                else:
                    for src, *part in ready:
                        pass_core(gathered, src, part)
                here = after(starts, arrived)
                if g == 2:
                    dx_own = dx_of(own, here)
                    starts = after(starts, dx_own)
            rows, acc = run_grad(starts, tab, g, *zip(*[gathered[p] for p in group]), (w1, w3, w2), acc, rows, nb, row_cap)
            if not g:
                y_own, dg_own = y_of(own, after(starts, acc[LAST]))
                starts = after(starts, dg_own)
        dw1, dw3, dw2 = acc
        starts, dw2 = lax.optimization_barrier((starts, dw2))
        dw2_sum = lax.psum(dw2, "dp")

        y_rest, dg_rest = y_of(rest, starts)
        dg = jnp.concatenate([dg_own, dg_rest], axis=FIRST)
        dg = dg[:, :local].reshape(ep_size, nb, local, BLK).transpose(0, 2, 1, 3).reshape(ep_size, local, tokens)
        dg = jnp.concatenate([relative(dg, me), jnp.broadcast_to(stats, (ep_size, *stats.shape))], axis=2)
        starts, dg = lax.optimization_barrier((starts, dg))
        dx_rest = dx_of(rest, starts)
        dg_all = lax.all_to_all(dg, "ep", FIRST, FIRST, tiled=True)
        load, prob_sum = jnp.sum(dg_all[:, :2, tokens : tokens + experts], axis=FIRST)
        share = AUX_COEF * experts / (n_total * top_k * n_total)
        aux_loss = share * jnp.sum(load * prob_sum)
        load = jnp.broadcast_to(load[:, None], (experts, LANES))
        dlog_t, dwr_t = run_router_grad(x_loc, prob_t, dg_all[:, :, :tokens].reshape(experts, tokens), ids_t, load, share)
        dw_router = lax.psum(dwr_t, ("dp", "ep")).T

        parts = [[v.reshape(LAST, tokens, d_model) for v in pair] for pair in ((y_own, y_rest), (dx_own, dx_rest))]
        sums, grads = run_exchange(parts, [dw1, dw3])
        y_loc, dx_loc = run_final(dlog_t, w_t, *sums)
        return y_loc, aux_loss, dx_loc, dw_router, *grads, dw2_sum

    return jax.shard_map(
        per_device,
        mesh=mesh,
        in_specs=(row_spec, whole_spec, row_spec, expert_spec, expert_spec, expert_spec, row_spec),
        out_specs=(row_spec, P(), row_spec, whole_spec, expert_spec, expert_spec, expert_spec),
        check_vma=False,
    )
```

```python
import functools

import jax
import jax.numpy as jnp
import numpy as np
from jax import lax
from jax.experimental import pallas as pl
from jax.experimental.pallas import tpu as pltpu
from jax.sharding import PartitionSpec as P


AUX_COEF = 0.01
BLK = 256
TILE = 256
WIN = 128
LANES = 128
ALIGN = 16
NOT_KEPT = -65536.0
VMEM_LIMIT = 63 * 1024 * 1024
CORE, X, Y = 1, 2, 4
FAR = X | Y
HALVES = TENSORS = range(2)
RING = 4
SOURCES = range(8)
FIRST, LAST = 0, -1
SEND, RECV = 0, 1
STAGES = 3
SLOTS = 16
SPLIT = range(4)
BACK, LAG = 2, 4
MESH = pl.DeviceIdType.MESH

WHOLE, PARTS = (0, 6), ((0, 3), (3, 3))
GROUPS = (
    [(src, *WHOLE) for src in (FIRST, CORE)],
    [(bit | core, *PARTS[FIRST]) for bit in (X, Y) for core in (FIRST, CORE)],
    [(bit | core, *PARTS[1]) for bit in (X, Y) for core in (FIRST, CORE)],
    [(FAR | core, *part) for part in PARTS for core in (FIRST, CORE)],
)


f32 = jnp.float32
bf16 = jnp.bfloat16
i32 = jnp.int32
ANY = pl.BlockSpec(memory_space=pl.ANY)
SMEM = pl.BlockSpec(memory_space=pltpu.SMEM)
VMEM = pl.BlockSpec(memory_space=pltpu.VMEM)
DMA = pltpu.SemaphoreType.DMA
Shape = jax.ShapeDtypeStruct


def capacity_of(tokens, top_k, experts):
    return (5 * top_k * tokens + 4 * experts - 1) // (4 * experts)


def dot(a, b, ca=1, cb=0):
    return lax.dot_general(a, b, (((ca,), (cb,)), ((), ())), preferred_element_type=f32)


def dot_nt(a, b):
    return dot(a, b, 1, 1)


def dot_tn(a, b):
    return dot(a, b, 0, 0)


def grid_params(dims):
    return pltpu.CompilerParams(dimension_semantics=("arbitrary",) * dims, vmem_limit_bytes=VMEM_LIMIT)


def params():
    return grid_params(1)


def cost(flops, moved):
    return pl.CostEstimate(flops=flops, bytes_accessed=moved, transcendentals=FIRST)


def iota(shape, dim):
    return lax.broadcasted_iota(i32, shape, dim)


def span(start, size, multiple=None):
    return pl.ds(pl.multiple_of(start, multiple or size), size)


def lane_sum(v):
    return jnp.sum(v, axis=1, keepdims=True)


def row_sum(v):
    return jnp.sum(v, axis=0, keepdims=True)


def where0(mask, v):
    return jnp.where(mask, v, jnp.zeros_like(v))


def one_hot(mask):
    return jnp.where(mask, 1.0, 0.0).astype(bf16)


def split3(v):
    hi = v.astype(bf16)
    rest = v - hi.astype(f32)
    mid = rest.astype(bf16)
    return hi, mid, (rest - mid.astype(f32)).astype(bf16)


def loop(start, stop, body):
    def step(i, carry):
        body(i)
        return carry

    lax.fori_loop(start, stop, step, FIRST)


def chosen_mask(ids, experts):
    rows = iota((experts, ids.shape[1]), FIRST)
    return functools.reduce(jnp.logical_or, [rows == ids[j : j + 1, :] for j in range(ids.shape[FIRST])])


def router_kernel(capacity, local, x_ref, wt_ref, ids_ref, tab_ref, prob_ref, stat_ref, carry):
    step = pl.program_id(FIRST)
    steps = pl.num_programs(FIRST)
    experts = wt_ref.shape[FIRST]

    @pl.when(step == FIRST)
    def _():
        carry[...] = jnp.zeros_like(carry)
        stat_ref[...] = jnp.zeros_like(stat_ref)
        tab_ref[...] = jnp.zeros_like(tab_ref)

    x = x_ref[...]
    hi, mid, low = [dot_nt(part, x) for part in split3(wt_ref[...])]
    logits = hi + (mid + low)
    expo = jnp.exp(logits - jnp.max(logits, axis=FIRST, keepdims=True))
    prob = expo / row_sum(expo)
    chosen = chosen_mask(ids_ref[...], experts)
    hits = jnp.where(chosen, 1.0, 0.0)
    gate = where0(chosen, prob / row_sum(where0(chosen, prob)))
    earlier = one_hot(iota((BLK, BLK), FIRST) < iota((BLK, BLK), 1))
    before = carry[:, :1]
    pos = dot(hits.astype(bf16), earlier) + before
    pos = jnp.where(chosen & (pos < capacity), pos, NOT_KEPT)
    prob_ref[...] = prob
    after = before + lane_sum(hits)
    lane = iota((experts, LANES), 1)
    first = where0(lane == step, jnp.minimum(before, capacity) + jnp.zeros((experts, LANES), f32))
    first = first + where0((lane == step + 1) & (step == steps - 1), jnp.minimum(after, capacity) + jnp.zeros((experts, LANES), f32))
    stat_ref[...] += where0(lane == FIRST, lane_sum(hits) + jnp.zeros((experts, LANES), f32))
    stat_ref[...] += where0(lane == 1, lane_sum(prob) + jnp.zeros((experts, LANES), f32))
    tail = slice(tab_ref.shape[LAST] - LANES, None)
    for d in range(experts // local):
        rows = slice(d * local, (d + 1) * local)
        tab_ref[d, :local, span(step * BLK, BLK)] = gate[rows]
        tab_ref[d, local:, span(step * BLK, BLK)] = pos[rows]
        tab_ref[d, local:, tail] += first[rows]
    carry[:, :1] = after


def run_router(x_loc, w_t, ids_t, capacity, local, devices):
    tokens, d_model = x_loc.shape
    experts = w_t.shape[FIRST]
    top_k = ids_t.shape[FIRST]
    table = (devices, 2 * local, tokens + LANES)
    return pl.pallas_call(
        functools.partial(router_kernel, capacity, local),
        grid=(tokens // BLK,),
        in_specs=[pl.BlockSpec((BLK, d_model), lambda i: (i, FIRST)), VMEM, pl.BlockSpec((top_k, BLK), lambda i: (FIRST, i))],
        out_specs=[VMEM, pl.BlockSpec((experts, BLK), lambda i: (FIRST, i)), VMEM],
        out_shape=[Shape(table, f32), Shape((experts, tokens), f32), Shape((experts, LANES), f32)],
        scratch_shapes=[pltpu.VMEM((experts, LANES), f32)],
        compiler_params=params(),
        cost_estimate=cost(2 * tokens * d_model * BLK, 2 * tokens * d_model),
        name="router",
    )(x_loc, w_t, ids_t)


class Blocks:
    def __init__(self, starts_ref, bmap_ref):
        self.starts, self.bmap = starts_ref, bmap_ref

    def info(self, i, e):
        at = self.bmap[2 * i + 1] + e * ALIGN
        first = self.starts[at]
        return self.bmap[2 * i], first, self.starts[at + 1] - first

    def total(self, start, count, e):
        return lax.fori_loop(start, start + count, lambda i, n: n + self.info(i, e)[LAST], i32(FIRST))


def aligned(row):
    base = (row // ALIGN) * ALIGN
    return base, row - base


def window_count(shift, count):
    return (shift + count + WIN - 1) // WIN


def padded(total):
    return (total + TILE - 1) // TILE * TILE


def row_tiles(total, body, size):
    tiles = (total + size - 1 - size // 2) // size
    loop(FIRST, tiles, lambda i: body(i * size, size))
    pl.when(padded(total) > tiles * size)(lambda: body(tiles * size, size // 2))


def start(copies):
    for cp in copies:
        cp.start()


def wait(copies):
    for cp in copies:
        cp.wait()


def taker(refs):
    refs = list(refs)

    def take(n=None):
        got = refs[:n]
        del refs[:n]
        return got

    return take


def block_count(pieces):
    return sum(count for _, _, count in pieces)


def offsets(pieces):
    counts = [count for _, _, count in pieces]
    return [(sum(counts[:k]), count) for k, count in enumerate(counts)]


def block_rows(first, count):
    return pl.ds(first * BLK, count * BLK)


def tokens_in(ref, which):
    return ref.at[which] if len(ref.shape) == 3 else ref


def grad_kernel(g, last, local, pieces, *refs):
    take = taker(refs)
    n = len(pieces)
    starts_ref, bmap_ref, tab_ref = take(3)
    tok_refs = take(n), take(n)
    w1_ref, w3_ref, w2_ref = take(3)
    acc_in = take(2 * bool(g))
    take(3 * bool(g))
    row_outs = take(3)
    outs = take(3 if last else 2)
    xv, dv, xr, dr, acc13, acc2, stage, tok_sem, in_sem, out_sem, row_sem = take()
    accs = acc13, acc2
    e = pl.program_id(FIRST)
    slot = e % 2
    d_model = xv.shape[1]
    d_ff = w1_ref.shape[LAST]
    blocks = Blocks(starts_ref, bmap_ref)
    count = xv.shape[FIRST] // BLK

    parts = [(c, at, first + at) for c, (first, size) in enumerate(offsets(pieces)) for at in range(FIRST, size, 3)]

    def token_copies(k):
        c, at, to = parts[k]
        src_rows, dst_rows = block_rows(at, 3), block_rows(to, 3)
        return [pltpu.make_async_copy(tokens_in(src[c], w).at[src_rows], dst.at[dst_rows], tok_sem.at[w, k]) for w, (src, dst) in enumerate(zip(tok_refs, (xv, dv)))]

    def in_copies(ee, ss):
        return [pltpu.make_async_copy(src.at[ee], dst.at[ss], in_sem.at[ss, k]) for k, (src, dst) in enumerate(zip(acc_in, accs))]

    def out_copies(ee, ss):
        return [pltpu.make_async_copy(src.at[ss], dst.at[ee], out_sem.at[ss, k]) for k, (src, dst) in enumerate(zip(accs, outs))]

    @pl.when(e == FIRST)
    def _():
        for k in range(len(parts)):
            start(token_copies(k))

    if g:
        pl.when(e == FIRST)(lambda: start(in_copies(e, slot)))
    else:
        pl.when(e >= 2)(lambda: wait(out_copies(e - 2, slot)))
        for acc in accs:
            acc[slot] = jnp.zeros(acc.shape[1:], f32)

    def prefetch():
        if not last:
            pl.when(e > FIRST)(lambda: wait(out_copies(e - 1, 1 - slot)))
        start(in_copies(e + 1, 1 - slot))

    def maybe_prefetch(now):
        if g:
            pl.when(now & (e + 1 < local))(prefetch)

    row_iota = iota((WIN, BLK), FIRST).astype(f32)
    head_row = iota((ALIGN, d_model), FIRST)
    both = tuple(HALVES)

    def dispatch(step, rows_at):
        todo = []
        for i in (2 * step, 2 * step + 1):
            for k, (_, _, first) in enumerate(parts):
                pl.when((e == FIRST) & (i == first))(lambda: wait(token_copies(k)))
            infos = [blocks.info(i, e + q) for q in both]
            todo.append((span(i * BLK, BLK), infos, [aligned(r) for r in rows_at]))
            rows_at = tuple(r + info[LAST] for r, info in zip(rows_at, infos))

        def picks(block, q, k):
            _, infos, places = block
            flat, first, _ = infos[q]
            pos = tab_ref[flat, pl.ds(local + e + q, 1), :]
            gate = tab_ref[flat, pl.ds(e + q, 1), :]
            pick = (pos + (places[q][1] - first - k * WIN).astype(f32)) == row_iota
            return one_hot(pick), lane_sum(where0(pick, gate + jnp.zeros_like(row_iota)))

        def rows_for(block, one, gate_row):
            tok = block[FIRST]
            return dot(one, xv[tok, :]).astype(bf16), (dot(one, dv[tok, :]) * gate_row).astype(bf16)

        def first_rows(block):
            pair = [picks(block, q, i32(FIRST)) for q in both]
            return rows_for(block, *[jnp.concatenate(v, axis=FIRST) for v in zip(*pair)])

        def put(block, new):
            for q in both:
                base, shift = block[LAST][q]
                head = span(base, ALIGN)
                for value, rows in zip(new, (xr, dr)):
                    value = value[q * WIN : (q + 1) * WIN]
                    rows[q, head, :] = jnp.where(head_row < shift, rows[q, head, :], value[:ALIGN])
                    rows[q, span(base + ALIGN, WIN - ALIGN, ALIGN), :] = value[ALIGN:]

        windows = [[window_count(places[q][1], infos[q][LAST]) for q in both] for _, infos, places in todo]
        simple = functools.reduce(jnp.logical_and, [w <= 1 for ws in windows for w in ws])

        @pl.when(simple)
        def _():
            for block, new in zip(todo, [first_rows(block) for block in todo]):
                put(block, new)

        @pl.when(jnp.logical_not(simple))
        def _():
            for block, ws in zip(todo, windows):
                put(block, first_rows(block))
                for q in both:

                    def more(k):
                        for value, rows in zip(rows_for(block, *picks(block, q, k)), (xr, dr)):
                            rows[q, span(block[LAST][q][FIRST] + k * WIN, WIN, ALIGN), :] = value

                    loop(1, ws[q], more)

        return rows_at

    @pl.when(slot == FIRST)
    def _():
        totals = lax.fori_loop(FIRST, count // 2, dispatch, (i32(FIRST),) * len(both))
        for q in both:

            def clear(i):
                for rows in (xr, dr):
                    rows[q, span(i * ALIGN, ALIGN), :] = jnp.zeros((ALIGN, d_model), bf16)

            loop((totals[q] + ALIGN - 1) // ALIGN, padded(totals[q]) // ALIGN, clear)

    wait(in_copies(e, slot))

    def tile(at, size):
        maybe_prefetch((at == FIRST) & (slot == FIRST))
        rows = span(at, size)
        xt = xr[slot, rows, :]
        dt = dr[slot, rows, :]
        act_a = dot(xt, w1_ref[FIRST])
        act_b = dot(xt, w3_ref[FIRST])
        d_hidden = dot_nt(dt, w2_ref[FIRST]).astype(bf16).astype(f32)
        sig = 1.0 / (1.0 + jnp.exp(-act_a))
        silu = act_a * sig
        hidden = (silu * act_b).astype(bf16)
        d_a = (d_hidden * act_b * sig * (1.0 + act_a * (1.0 - sig))).astype(bf16)
        d_b = (d_hidden * silu).astype(bf16)
        copies = []
        for k, (value, out) in enumerate(zip((hidden, d_a, d_b), row_outs)):
            stage[k, :size] = value
            copies.append(pltpu.make_async_copy(stage.at[k, :size], out.at[g, e, rows], row_sem.at[k]))
        start(copies)
        acc13[slot, :, :d_ff] += dot_tn(xt, d_a)
        acc13[slot, :, d_ff:] += dot_tn(xt, d_b)
        acc2[slot] += dot_tn(hidden, dt)
        wait(copies)

    total = blocks.total(FIRST, count, e)
    row_tiles(total, tile, 2 * TILE)
    maybe_prefetch((total == FIRST) | (slot > FIRST))

    if last:
        for out, value in zip(outs, (acc13[slot, :, :d_ff], acc13[slot, :, d_ff:], acc2[slot])):
            out[FIRST] = value.astype(bf16)
    else:
        start(out_copies(e, slot))

        @pl.when(e == pl.num_programs(FIRST) - 1)
        def _():
            wait(out_copies(e - 1, 1 - slot))
            wait(out_copies(e, slot))


def per_expert(*shape):
    return pl.BlockSpec((1, *shape), lambda e: (e,) + (FIRST,) * len(shape))


def block_map(pieces, nb):
    spots = [(src, first + b) for src, first, count in pieces for b in range(count)]
    return np.asarray([v for src, b in spots for v in (src * nb + b, src * 4 * ALIGN + b)], np.int32)


def run_grad(starts, tab, g, xs, ds, weights, acc, rows, nb, row_cap):
    pieces = GROUPS[g]
    last = g == len(GROUPS) - 1
    local, d_model, d_ff = weights[FIRST].shape
    count = block_count(pieces) * BLK
    w_specs = [per_expert(*w.shape[1:]) for w in weights]
    sums = [(local, d_model, 2 * d_ff), (local, d_ff, d_model)]
    row_shape = [Shape((len(GROUPS), local, row_cap, d_ff), bf16)] * 3
    out_shape = row_shape + ([Shape(w.shape, bf16) for w in weights] if last else [Shape(s, f32) for s in sums])
    out_specs = [ANY] * 3 + (w_specs if last else [ANY] * 2)
    tokens = pltpu.VMEM((count, d_model), bf16)
    packed = pltpu.VMEM((2, row_cap + WIN, d_model), bf16)
    ins = [starts, block_map(pieces, nb), tab, *xs, *ds, *weights, *acc, *rows]
    out = pl.pallas_call(
        functools.partial(grad_kernel, g, last, local, pieces),
        grid=(local,),
        in_specs=[SMEM, SMEM, VMEM] + [ANY] * (2 * len(pieces)) + w_specs + [ANY] * (len(acc) + len(rows)),
        out_specs=out_specs,
        out_shape=out_shape,
        scratch_shapes=[tokens, tokens, packed, packed]
        + [pltpu.VMEM((2, *s[1:]), f32) for s in sums]
        + [pltpu.VMEM((3, 2 * TILE, d_ff), bf16), DMA((2, count // (3 * BLK))), DMA((2, 2)), DMA((2, 2)), DMA((3,))],
        input_output_aliases={len(ins) - len(rows) + k: k for k in range(len(rows))},
        compiler_params=params(),
        cost_estimate=cost(12 * count * d_model * d_ff, 40 << 20),
        name="expert_grad",
    )(*ins)
    return out[:3], out[3:]


def group_spans(groups):
    counts = [block_count(GROUPS[g]) for g in groups]
    return np.asarray([v for k, c in enumerate(counts) for v in (sum(counts[:k]), c)], np.int32)


def row_totals(groups, starts):
    firsts = starts.reshape(len(SOURCES), LAST, ALIGN)
    use = np.zeros((len(groups), len(SOURCES), 1, ALIGN), np.int32)
    for k, g in enumerate(groups):
        for src, first, count in GROUPS[g]:
            use[k, src, FIRST, first + count] += 1
            use[k, src, FIRST, first] -= 1
    return jnp.sum(use * firsts, axis=(1, 3)).reshape(LAST)


def per_local(*shape):
    return pl.BlockSpec((1, *shape), lambda g, e: (e,) + (FIRST,) * len(shape))


class BlockRows:
    def __init__(self, owner, i, rows_at):
        ee = range(owner.local)
        self.owner, self.i = owner, i
        self.infos = [owner.blocks.info(i, k) for k in ee]
        self.places = [aligned(r) for r in rows_at]
        self.windows = [window_count(self.places[k][1], self.infos[k][LAST]) for k in ee]
        self.simple = functools.reduce(jnp.logical_and, [w <= 1 for w in self.windows])
        self.flat = self.infos[FIRST][FIRST]
        self.tok = span((i - owner.first) * BLK, BLK)
        self.out = owner.ring.at[i % RING]
        self.after = tuple(r + info[LAST] for r, info in zip(rows_at, self.infos))

    def load(self):
        self.tab_t = jnp.transpose(self.owner.tab_ref[self.flat])

    def gate(self, ee):
        return self.tab_t[:, ee : ee + 1]

    def pick(self, ee, k=FIRST):
        at = self.owner.local + ee
        shift = self.places[ee][1] - self.infos[ee][1] - k * WIN
        return one_hot((self.tab_t[:, at : at + 1] + shift.astype(f32)) == self.owner.lane)

    def held(self, ee, k=FIRST, cols=slice(None)):
        return self.owner.rows_ref[ee, span(self.places[ee][FIRST] + k * WIN, WIN, ALIGN), cols]


class Combine:
    def __init__(self, local, starts_ref, bmap_ref, spans_ref, totals_ref, tab_ref, rows_ref, out_ref, ring, sems):
        step = pl.program_id(FIRST)
        self.totals = totals_ref
        self.e = pl.program_id(1)
        self.blocks = Blocks(starts_ref, bmap_ref)
        self.first, self.count = spans_ref[2 * step], spans_ref[2 * step + 1]
        self.total = totals_ref[step * local + self.e]
        self.local, self.tab_ref, self.rows_ref = local, tab_ref, rows_ref
        self.out_ref, self.ring, self.sems = out_ref, ring, sems
        self.lane = iota((BLK, WIN), 1).astype(f32)

    def zero_tail(self):
        rows = span(padded(self.total), WIN)
        self.rows_ref[self.e, rows, :] = jnp.zeros((WIN, self.rows_ref.shape[LAST]), bf16)

    def fetch(self, groups, arrays, held, sems):
        now = pl.program_id(FIRST) * self.local + self.e

        def each(step, act):
            k, e = step // self.local, step % self.local

            def one(i):
                rows = span(i * TILE, TILE)
                for w, array in enumerate(arrays):
                    act(pltpu.make_async_copy(array.at[k + groups[FIRST], e, rows], held.at[step % 2, w, rows], sems.at[step % 2, w]))

            loop(FIRST, padded(self.totals[step]) // TILE, one)

        pl.when(now == FIRST)(lambda: each(now, lambda cp: cp.start()))
        pl.when(now + 1 < self.local * len(groups))(lambda: each(now + 1, lambda cp: cp.start()))
        each(now, lambda cp: cp.wait())
        return now % 2

    def out_copy(self, i):
        slot = i % RING
        place = self.blocks.bmap[2 * i] - self.blocks.bmap[FIRST]
        return pltpu.make_async_copy(self.ring.at[slot], self.out_ref.at[place], self.sems.at[slot])

    def run(self, simple_body, full_body):
        def pair(step, rows_at):
            i = self.first + 2 * step
            one = BlockRows(self, i, rows_at)
            two = BlockRows(self, i + 1, one.after)
            for block in (one, two):
                pl.when(block.i - self.first >= RING)(lambda: self.out_copy(block.i - RING).wait())
            simple = one.simple & two.simple

            @pl.when(simple)
            def _():
                for block in (one, two):
                    block.load()
                for block in (one, two):
                    simple_body(block)

            @pl.when(jnp.logical_not(simple))
            def _():
                def full(k, rows_at):
                    block = BlockRows(self, i + k, rows_at)
                    block.load()
                    full_body(block)
                    return block.after

                lax.fori_loop(FIRST, 2, full, rows_at)

            for block in (one, two):
                self.out_copy(block.i).start()
            return two.after

        stop = self.first + self.count
        lax.fori_loop(FIRST, self.count // 2, pair, (i32(FIRST),) * self.local)
        loop(stop - RING, stop, lambda i: self.out_copy(i).wait())


def y_kernel(groups, local, starts_ref, bmap_ref, spans_ref, totals_ref, tab_ref, h_rows, w2_ref, *refs):
    take = taker(refs)
    d_refs = [take(len(GROUPS[g])) for g in groups]
    y_ref, dg_ref, o_rows, dv, ring, zacc, yacc, dgacc, tok_sem, out_sem, held, row_sem = take()
    all_rows = Combine(local, starts_ref, bmap_ref, spans_ref, totals_ref, tab_ref, o_rows, y_ref, ring, out_sem)
    e = all_rows.e
    d_model = dv.shape[1]

    def token_copies(step):
        spots = offsets(GROUPS[groups[step]])
        return [pltpu.make_async_copy(tokens_in(src, 1), dv.at[block_rows(*spot)], tok_sem.at[c]) for c, (src, spot) in enumerate(zip(d_refs[step], spots))]

    for step in range(len(groups)):
        pl.when((pl.program_id(FIRST) == step) & (e == FIRST))(lambda: start(token_copies(step)))

    slot = all_rows.fetch(groups, [h_rows], held, row_sem)

    def tile(at, size):
        rows = span(at, size)
        o_rows[e, rows, :] = dot(held[slot, FIRST, rows, :], w2_ref[FIRST]).astype(bf16)

    row_tiles(all_rows.total, tile, 2 * TILE)
    all_rows.zero_tail()

    @pl.when(e == local - 1)
    def _():
        for step in range(len(groups)):
            pl.when(pl.program_id(FIRST) == step)(lambda: wait(token_copies(step)))
        dg_lane = iota((BLK, LANES), 1)
        width = 2 * LANES
        columns = [slice(k * width, (k + 1) * width) for k in range(d_model // width)]

        def put_dg(block, sums):
            dg = sum(where0(dg_lane == ee, lane_sum(s) + jnp.zeros((BLK, LANES), f32)) for ee, s in enumerate(sums))
            dg_ref[block.flat - all_rows.blocks.bmap[FIRST]] = jnp.transpose(dg)[: 2 * local, :]

        def simple(block):
            picks = [block.pick(ee) for ee in range(local)]
            sums = [None] * local
            for cols in columns:
                dy = dv[block.tok, cols].astype(f32)
                y = None
                for ee in range(local):
                    z = dot(picks[ee], block.held(ee, cols=cols))
                    prod = dy * z
                    part = prod[:, :LANES] + prod[:, LANES:]
                    sums[ee] = part if sums[ee] is None else sums[ee] + part
                    y = block.gate(ee) * z if y is None else y + block.gate(ee) * z
                block.out[:, cols] = y.astype(bf16)
            put_dg(block, sums)

        def full(block):
            yacc[...] = jnp.zeros_like(yacc)
            for ee in range(local):
                zacc[...] = jnp.zeros_like(zacc)

                def more(k):
                    zacc[...] += dot(block.pick(ee, k), block.held(ee, k))

                loop(FIRST, block.windows[ee], more)
                yacc[...] += block.gate(ee) * zacc[...]
                dgacc[ee] = lane_sum(dv[block.tok, :].astype(f32) * zacc[...]) * jnp.where(dg_lane == FIRST, 1.0, 0.0)
            block.out[...] = yacc[...].astype(bf16)
            put_dg(block, [dgacc[ee] for ee in range(local)])

        all_rows.run(simple, full)


def combine_scratch(local, row_cap, d_model):
    return [pltpu.VMEM((local, row_cap + WIN, d_model), bf16)], [pltpu.VMEM((RING, BLK, d_model), bf16), pltpu.VMEM((BLK, d_model), f32)]


def run_y(groups, starts, tab, h_rows, w2, ds, nb):
    local, d_ff, d_model = w2.shape
    row_cap = h_rows.shape[2]
    pieces = [p for g in groups for p in GROUPS[g]]
    spans = group_spans(groups)
    blocks = block_count(pieces)
    rows, work = combine_scratch(local, row_cap, d_model)
    return pl.pallas_call(
        functools.partial(y_kernel, groups, local),
        grid=(len(groups), local),
        in_specs=[SMEM, SMEM, SMEM, SMEM, VMEM, ANY, per_local(d_ff, d_model)] + [ANY] * len(pieces),
        out_specs=[ANY, VMEM],
        out_shape=[Shape((blocks, BLK, d_model), bf16), Shape((blocks, 2 * local, BLK), f32)],
        scratch_shapes=rows + [pltpu.VMEM((max(spans[1::2]) * BLK, d_model), bf16)] + work + [work[LAST], pltpu.VMEM((local, BLK, LANES), f32), DMA((4,)), DMA((RING,)), pltpu.VMEM((2, 1, row_cap, d_ff), bf16), DMA((2, 1))],
        compiler_params=grid_params(2),
        cost_estimate=cost(4 * blocks * BLK * d_model * d_ff, 20 << 20),
        name="expert_y",
    )(starts, block_map(pieces, nb), spans, row_totals(groups, starts), tab, h_rows, w2, *[ds[p] for p in pieces])


def dx_kernel(groups, local, starts_ref, bmap_ref, spans_ref, totals_ref, tab_ref, da_rows, db_rows, w1_ref, w3_ref, dx_ref, o_rows, ring, zacc, out_sem, held, row_sem):
    all_rows = Combine(local, starts_ref, bmap_ref, spans_ref, totals_ref, tab_ref, o_rows, dx_ref, ring, out_sem)
    e = all_rows.e

    slot = all_rows.fetch(groups, [da_rows, db_rows], held, row_sem)

    def tile(at, size):
        rows = span(at, size)
        grad = dot_nt(held[slot, FIRST, rows, :], w1_ref[FIRST]) + dot_nt(held[slot, 1, rows, :], w3_ref[FIRST])
        o_rows[e, rows, :] = grad.astype(bf16)

    row_tiles(all_rows.total, tile, 2 * TILE)
    all_rows.zero_tail()

    @pl.when(e == local - 1)
    def _():
        def simple(block):
            pairs = [(ee, ee + 1) for ee in range(FIRST, local, 2)]
            sums = [
                dot(jnp.concatenate([block.pick(ee) for ee in pair], axis=1), jnp.concatenate([block.held(ee) for ee in pair], axis=FIRST))
                for pair in pairs
            ]
            block.out[...] = sum(sums[1:], sums[FIRST]).astype(bf16)

        def full(block):
            zacc[...] = jnp.zeros_like(zacc)
            for ee in range(local):

                def more(k):
                    zacc[...] += dot(block.pick(ee, k), block.held(ee, k))

                loop(FIRST, block.windows[ee], more)
            block.out[...] = zacc[...].astype(bf16)

        all_rows.run(simple, full)


def run_dx(groups, starts, tab, da_rows, db_rows, w1, w3, nb):
    local, d_model, d_ff = w1.shape
    row_cap = da_rows.shape[2]
    pieces = [p for g in groups for p in GROUPS[g]]
    blocks = block_count(pieces)
    rows, work = combine_scratch(local, row_cap, d_model)
    return pl.pallas_call(
        functools.partial(dx_kernel, groups, local),
        grid=(len(groups), local),
        in_specs=[SMEM, SMEM, SMEM, SMEM, VMEM] + [ANY] * 2 + [per_local(d_model, d_ff)] * 2,
        out_specs=ANY,
        out_shape=Shape((blocks, BLK, d_model), bf16),
        scratch_shapes=rows + work + [DMA((RING,)), pltpu.VMEM((2, 2, row_cap, d_ff), bf16), DMA((2, 2))],
        compiler_params=grid_params(2),
        cost_estimate=cost(6 * blocks * BLK * d_model * d_ff, 20 << 20),
        name="expert_dx",
    )(starts, block_map(pieces, nb), group_spans(groups), row_totals(groups, starts), tab, da_rows, db_rows, w1, w3)


def router_grad_kernel(scale, x_ref, prob_ref, dg_ref, ids_ref, load_ref, dlog_ref, dw_ref):
    step = pl.program_id(FIRST)
    prob = prob_ref[...]
    dg = dg_ref[...]
    chosen = chosen_mask(ids_ref[...], prob.shape[FIRST])
    gate_sum = row_sum(where0(chosen, prob))
    gate = where0(chosen, prob / gate_sum)
    d_pick = (dg - row_sum(gate * dg)) / gate_sum
    d_prob = where0(chosen, d_pick) + scale * load_ref[:, :1]
    d_logit = prob * (d_prob - row_sum(prob * d_prob))
    dlog_ref[...] = d_logit
    hi, mid, low = [dot(part, x_ref[...]) for part in split3(d_logit)]

    @pl.when(step == FIRST)
    def _():
        dw_ref[...] = jnp.zeros_like(dw_ref)

    dw_ref[...] += hi + (mid + low)


def run_router_grad(x_loc, prob_t, dg_t, ids_t, load, scale):
    tokens, d_model = x_loc.shape
    experts = prob_t.shape[FIRST]
    lanes = lambda n: pl.BlockSpec((n, BLK), lambda i: (FIRST, i))
    return pl.pallas_call(
        functools.partial(router_grad_kernel, scale),
        grid=(tokens // BLK,),
        in_specs=[pl.BlockSpec((BLK, d_model), lambda i: (i, FIRST)), lanes(experts), lanes(experts), lanes(ids_t.shape[FIRST]), VMEM],
        out_specs=[lanes(experts), VMEM],
        out_shape=[Shape((experts, tokens), f32), Shape((experts, d_model), f32)],
        compiler_params=params(),
        cost_estimate=cost(2 * tokens * d_model * BLK, 2 * tokens * d_model),
        name="router_grad",
    )(x_loc, prob_t, dg_t, ids_t, load)


def final_kernel(dlog_ref, wt_ref, *refs):
    take = taker(refs)
    y_terms, dx_terms = [[ref[...].astype(f32) for ref in take(3)] for _ in TENSORS]
    y_ref, dx_ref = take()
    lhs = split3(dlog_ref[...])
    rhs = split3(wt_ref[...])
    terms = [(i, j) for i in range(3) for j in range(3 - i)]
    left = jnp.concatenate([lhs[i] for i, _ in terms], axis=FIRST)
    right = jnp.concatenate([rhs[j] for _, j in terms], axis=FIRST)
    dx_ref[...] = (dot_tn(left, right) + sum(dx_terms[1:], dx_terms[FIRST])).astype(bf16)
    y_ref[...] = sum(y_terms[1:], y_terms[FIRST]).astype(bf16)


def run_final(dlog_t, w_t, y_terms, dx_terms):
    experts, tokens = dlog_t.shape
    d_model = w_t.shape[1]
    size = tokens // 4
    rows = pl.BlockSpec((size, d_model), lambda i: (i, FIRST))
    return pl.pallas_call(
        final_kernel,
        grid=(tokens // size,),
        in_specs=[pl.BlockSpec((experts, size), lambda i: (FIRST, i)), VMEM] + [rows] * len([*y_terms, *dx_terms]),
        out_specs=[rows] * 2,
        out_shape=[Shape((tokens, d_model), bf16)] * 2,
        compiler_params=params(),
        cost_estimate=cost(2 * tokens * d_model * BLK, 16 * tokens * d_model),
        name="final",
    )(dlog_t, w_t, *y_terms, *dx_terms)


NEAR = (X, Y)
RELAYED = {(Y, 0): 0, (X, 1): 1}
OPS = [
    (t, src, h)
    for step in ([(FAR, 0), (FAR, 1)], [(X, 0), (Y, 1)], [(X, 1), (Y, 0)], [(FIRST, 0), (FIRST, 1)])
    for t in TENSORS
    for src, h in step
]


def add_rows(dst, src):
    step = min(LANES, dst.shape[FIRST])

    def body(i):
        rows = span(i * step, step)
        dst[rows, :] = (dst[rows, :].astype(f32) + src[rows, :].astype(f32)).astype(bf16)

    loop(FIRST, dst.shape[FIRST] // step, body)


def exchange_kernel(half, mats, *refs):
    take = taker(refs)
    parts = [take(2) for _ in TENSORS]
    dws = take(mats)
    outs = [take(len(NEAR) + 1) for _ in TENSORS]
    dw_outs = take(mats)
    land, far_land, stage, z_one, z_two, z_stage = take(6)
    core_sem, stage_sem, far_sem, near_sem, own_sem, z_sem, keep_sem, load_sem, credit_one, credit_two = take()

    me = lax.axis_index("ep")
    z = lax.axis_index("dp")
    peer = {bit: me + bit - 2 * bit * ((me // bit) % 2) for bit in (CORE, X, Y)}
    z_peer = z + 1 - 2 * (z % 2)
    z_cross = 3 - z
    is_end = (z % 3) == FIRST
    is_mid = (z % 3) != FIRST

    barrier = pltpu.get_barrier_semaphore()
    ids = [{"ep": p} for p in peer.values()] + [{"dp": z_peer}, {"dp": z_cross}]
    for device in ids:
        pl.semaphore_signal(barrier, device_id=device, device_id_type=MESH)
    pl.semaphore_wait(barrier, len(ids))

    def remote(src, dst, sems, at, device):
        send, recv = sems.at[(SEND, *at)], sems.at[(RECV, *at)]
        return pltpu.make_async_remote_copy(src_ref=src, dst_ref=dst, send_sem=send, recv_sem=recv, device_id=device, device_id_type=MESH)

    def rows_at(h):
        return pl.ds(h * half, half)

    def part(t, src, h):
        own, rest = parts[t]
        return own.at[src, rows_at(h)] if src <= CORE else rest.at[src - 2, rows_at(h)]

    def core_copy(i):
        t, src, h = OPS[i]
        return remote(part(t, src | CORE, h), land.at[i], core_sem, (i,), {"ep": peer[CORE]})

    def stage_copy(i):
        t, src, h = OPS[i]
        return pltpu.make_async_copy(part(t, src, h), stage.at[i % STAGES], stage_sem.at[i % STAGES])

    def far_copy(i):
        t, _, h = OPS[i]
        return remote(land.at[i], far_land.at[t, h], far_sem, (t, h), {"ep": peer[NEAR[h]]})

    def near_copy(i):
        t, src, h = OPS[i]
        k = NEAR.index(src)
        return remote(land.at[i], outs[t][k].at[rows_at(h)], near_sem, (t, k, h), {"ep": peer[src]})

    def own_copy(i):
        t, _, h = OPS[i]
        return pltpu.make_async_copy(land.at[i], outs[t][LAST].at[rows_at(h)], own_sem.at[t, h])

    def out_copy(i):
        src = OPS[i][1]
        return (far_copy if src == FAR else near_copy if src else own_copy)(i)

    def reduce_op(i):
        t, src, h = OPS[i]
        stage_copy(i).wait()
        core_copy(i).wait_recv()
        add_rows(land.at[i], stage.at[i % STAGES])
        if i + STAGES < len(OPS):
            stage_copy(i + STAGES).start()
        if (src, h) in RELAYED:
            far_copy(OPS.index((t, FAR, RELAYED[src, h]))).wait_recv()
            add_rows(land.at[i], far_land.at[t, RELAYED[src, h]])

    rows_per = z_one.shape[1]
    chunks = [(m, e, k) for e in range(dws[FIRST].shape[FIRST]) for m in range(mats) for k in SPLIT]
    n = len(chunks)

    def piece(arrays, c):
        m, e, k = chunks[c]
        return arrays[m].at[e, pl.ds(k * rows_per, rows_per)]

    def one_copy(c):
        return remote(piece(dws, c), z_one.at[c % SLOTS], z_sem, (FIRST, c), {"dp": z_peer})

    def two_copy(c):
        return remote(z_one.at[c % SLOTS], z_two.at[c % SLOTS], z_sem, (1, c), {"dp": z_cross})

    def three_copy(c):
        return remote(z_two.at[c % SLOTS], piece(dw_outs, c), z_sem, (2, c), {"dp": z_peer})

    def keep_copy(c):
        return pltpu.make_async_copy(z_two.at[c % SLOTS], piece(dw_outs, c), keep_sem.at[c])

    def load_copy(c):
        return pltpu.make_async_copy(piece(dws, c), z_stage.at[c % STAGES], load_sem.at[c % STAGES])

    def first_add(c):
        load_copy(c).wait()
        one_copy(c).wait_recv()
        add_rows(z_one.at[c % SLOTS], z_stage.at[c % STAGES])
        if c + STAGES < n:
            load_copy(c + STAGES).start()

    def second_add(c):
        two_copy(c).wait()
        add_rows(z_two.at[c % SLOTS], z_one.at[c % SLOTS])
        if c + SLOTS < n:
            pl.semaphore_signal(credit_one, device_id={"dp": z_peer}, device_id_type=MESH)

    def retire(c):
        three_copy(c).wait_send()
        keep_copy(c).wait()
        if c + SLOTS < n:
            pl.semaphore_signal(credit_two, device_id={"dp": z_cross}, device_id_type=MESH)

    @pl.when(is_end)
    def _():
        for c in range(SLOTS):
            one_copy(c).start()

    @pl.when(is_mid)
    def _():
        for c in range(STAGES):
            load_copy(c).start()

    for i in range(len(OPS)):
        core_copy(i).start()
        if i < STAGES:
            stage_copy(i).start()

    todo = list(range(len(OPS)))
    for tick in range(n + LAG):
        mine = todo[: 2 if tick < 2 else tick % 2]
        todo = todo[len(mine) :]
        for i in mine:
            reduce_op(i)

        @pl.when(is_mid)
        def _():
            back = tick - BACK
            if tick < n:
                first_add(tick)
            if back in range(n):
                second_add(back)
            if tick < n:
                if tick >= SLOTS:
                    pl.semaphore_wait(credit_two, 1)
                two_copy(tick).start()
            if back in range(n):
                three_copy(back).start()
                keep_copy(back).start()
            if tick >= LAG:
                retire(tick - LAG)

        for i in mine:
            out_copy(i).start()

        @pl.when(is_end)
        def _():
            if tick + SLOTS < n:
                pl.semaphore_wait(credit_one, 1)
                one_copy(tick + SLOTS).start()

    for i in todo:
        reduce_op(i)
        out_copy(i).start()

    @pl.when(is_end)
    def _():
        for c in range(n):
            one_copy(c).wait_send()
            three_copy(c).wait_recv()

    for i in range(len(OPS)):
        core_copy(i).wait_send()
        (out_copy(i).wait_send if OPS[i][1] == FAR else out_copy(i).wait)()


def run_exchange(parts, dws):
    tokens, d_model = parts[FIRST][FIRST].shape[1:]
    half = tokens // 2
    local, rows, cols = dws[FIRST].shape
    chunk = (rows // len(SPLIT), cols)
    n = local * len(dws) * len(SPLIT)
    whole = Shape((tokens, d_model), bf16)
    flat = [v for tensor in parts for v in tensor] + list(dws)
    terms = len(NEAR) + 1
    out = pl.pallas_call(
        functools.partial(exchange_kernel, half, len(dws)),
        in_specs=[ANY] * len(flat),
        out_specs=[ANY] * (terms * len(TENSORS) + len(dws)),
        out_shape=[whole] * (terms * len(TENSORS)) + [Shape(v.shape, bf16) for v in dws],
        scratch_shapes=[
            pltpu.VMEM((len(OPS), half, d_model), bf16),
            pltpu.VMEM((len(TENSORS), len(HALVES), half, d_model), bf16),
            pltpu.VMEM((STAGES, half, d_model), bf16),
            pltpu.VMEM((SLOTS, *chunk), bf16),
            pltpu.VMEM((SLOTS, *chunk), bf16),
            pltpu.VMEM((STAGES, *chunk), bf16),
            DMA((2, len(OPS))),
            DMA((STAGES,)),
            DMA((2, 2, 2)),
            DMA((2, 2, 2, 2)),
            DMA((2, 2)),
            DMA((2, 3, n)),
            DMA((n,)),
            DMA((STAGES,)),
            pltpu.SemaphoreType.REGULAR,
            pltpu.SemaphoreType.REGULAR,
        ],
        compiler_params=pltpu.CompilerParams(vmem_limit_bytes=VMEM_LIMIT, collective_id=FIRST, has_side_effects=True),
        cost_estimate=cost(1 << 37, 200 << 20),
        name="exchange",
    )(*flat)
    return [out[:terms], out[terms : 2 * terms]], out[2 * terms :]


def hop(v, bit):
    return lax.ppermute(v, "ep", [(i, i ^ bit) for i in SOURCES])


def after(values, token):
    return lax.optimization_barrier((values, token))[FIRST]


def send_own(x_loc, dy_loc, token):
    got = {(FIRST, *WHOLE): (x_loc, dy_loc), (CORE, *WHOLE): (hop(x_loc, CORE), hop(dy_loc, CORE))}
    both = [jnp.stack([v[first * BLK : (first + count) * BLK] for v in (x_loc, dy_loc)]) for first, count in PARTS]
    for part, piece in zip(PARTS, after(both, token)):
        got.update({(bit, *part): (hop(piece, bit),) * 2 for bit in NEAR})
    return got


def pass_on(got, h):
    part = PARTS[h]
    got[FAR, *part] = (hop(got[(Y, X)[h], *part][FIRST], NEAR[h]),) * 2
    for bit in NEAR:
        pass_core(got, bit, part)


def pass_core(got, bits, part):
    got[bits | CORE, *part] = (hop(got[bits, *part][FIRST], CORE),) * 2


def relative(v, me):
    shape = v.shape
    v = v.reshape((2, 2, 2) + shape[1:])
    for axis, bit in enumerate((Y, X, CORE)):
        v = jnp.where((me & bit) != FIRST, jnp.flip(v, axis), v)
    return v.reshape(shape)


def solution(mesh):
    dp_size = mesh.shape["dp"]
    ep_size = mesh.shape["ep"]
    row_spec = P(("dp", "ep"), None)
    expert_spec = P("ep", None, None)
    whole_spec = P(None, None)

    def per_device(x_loc, w_router, ids_loc, w1, w3, w2, dy_loc):
        tokens, d_model = x_loc.shape
        top_k = ids_loc.shape[1]
        experts = w_router.shape[1]
        local = w1.shape[FIRST]
        capacity = capacity_of(tokens, top_k, experts)
        n_total = tokens * dp_size * ep_size
        nb = tokens // BLK
        row_cap = padded(4 * capacity)
        me = lax.axis_index("ep")

        ids_t = ids_loc.T
        w_t = w_router.T
        send_tab, prob_t, stats = run_router(x_loc, w_t, ids_t, capacity, local, ep_size)
        tables = lax.all_to_all(send_tab, "ep", FIRST, FIRST, tiled=True)
        stats = jnp.pad(stats[:, :2].T, ((0, local - 2), (0, LANES - experts)))
        for step in (1, 2):
            stats = stats + lax.ppermute(stats, "dp", [(i, i ^ step) for i in range(dp_size)])
        gathered = send_own(x_loc, dy_loc, (tables, stats))
        tab_rel = relative(tables, me)
        tab = tab_rel[:, :, :tokens].reshape(ep_size, 2 * local, nb, BLK).transpose(0, 2, 1, 3).reshape(ep_size * nb, 2 * local, BLK)
        starts = tab_rel[:, local:, tokens : tokens + ALIGN].astype(i32).reshape(LAST)

        def y_of(groups, starts):
            return run_y(groups, starts, tab, rows[FIRST], w2, {p: v[1] for p, v in gathered.items()}, nb)

        def dx_of(groups, starts):
            return run_dx(groups, starts, tab, rows[1], rows[2], w1, w3, nb)

        acc = rows = ()
        own, rest = (FIRST,), (1, 2, 3)
        for g, group in enumerate(GROUPS):
            if g:
                ready = [p for p in group if not p[FIRST] & CORE]
                arrived = after([gathered[p][FIRST] for p in ready], (acc[LAST], dg_own))
                gathered.update({p: (v, v) for p, v in zip(ready, arrived)})
                if g < len(GROUPS) - 1:
                    pass_on(gathered, g - 1)
                else:
                    for src, *part in ready:
                        pass_core(gathered, src, part)
                here = after(starts, arrived)
                if g == 2:
                    dx_own = dx_of(own, here)
                    starts = after(starts, dx_own)
            rows, acc = run_grad(starts, tab, g, *zip(*[gathered[p] for p in group]), (w1, w3, w2), acc, rows, nb, row_cap)
            if not g:
                y_own, dg_own = y_of(own, after(starts, acc[LAST]))
                starts = after(starts, dg_own)
        dw1, dw3, dw2 = acc
        starts, dw2 = lax.optimization_barrier((starts, dw2))
        dw2_sum = lax.psum(dw2, "dp")

        y_rest, dg_rest = y_of(rest, starts)
        dg = jnp.concatenate([dg_own, dg_rest], axis=FIRST)
        dg = dg[:, :local].reshape(ep_size, nb, local, BLK).transpose(0, 2, 1, 3).reshape(ep_size, local, tokens)
        dg = jnp.concatenate([relative(dg, me), jnp.broadcast_to(stats, (ep_size, *stats.shape))], axis=2)
        starts, dg = lax.optimization_barrier((starts, dg))
        dx_rest = dx_of(rest, starts)
        dg_all = lax.all_to_all(dg, "ep", FIRST, FIRST, tiled=True)
        load, prob_sum = jnp.sum(dg_all[:, :2, tokens : tokens + experts], axis=FIRST)
        share = AUX_COEF * experts / (n_total * top_k * n_total)
        aux_loss = share * jnp.sum(load * prob_sum)
        load = jnp.broadcast_to(load[:, None], (experts, LANES))
        dlog_t, dwr_t = run_router_grad(x_loc, prob_t, dg_all[:, :, :tokens].reshape(experts, tokens), ids_t, load, share)
        dw_router = lax.psum(dwr_t, ("dp", "ep")).T

        parts = [[v.reshape(LAST, tokens, d_model) for v in pair] for pair in ((y_own, y_rest), (dx_own, dx_rest))]
        sums, grads = run_exchange(parts, [dw1, dw3])
        y_loc, dx_loc = run_final(dlog_t, w_t, *sums)
        return y_loc, aux_loss, dx_loc, dw_router, *grads, dw2_sum

    return jax.shard_map(
        per_device,
        mesh=mesh,
        in_specs=(row_spec, whole_spec, row_spec, expert_spec, expert_spec, expert_spec, row_spec),
        out_specs=(row_spec, P(), row_spec, whole_spec, expert_spec, expert_spec, expert_spec),
        check_vma=False,
    )
```
